16 devices in a mesh: model: 2 (over z), data: 2 (over y), stage: 4 (over x, core).
Axes of the slice: x: 2, y: 2, z: 2, core: 2. Of those that a mesh axis runs over, the one named last changes fastest.
Arguments:
- w_up: float32 [4, 1024, 4096], P('stage', None, 'model')
- w_down: float32 [4, 4096, 1024], P('stage', 'model')
- m_up: float32 [4, 1024, 4096], P('stage', None, 'model')
- m_down: float32 [4, 4096, 1024], P('stage', 'model')
- v_up: float32 [4, 1024, 4096], P('stage', None, 'model')
- v_down: float32 [4, 4096, 1024], P('stage', 'model')
- g_up: float32 [2, 4, 1024, 4096], P('data', 'stage', None, 'model')
- g_down: float32 [2, 4, 4096, 1024], P('data', 'stage', 'model')
- acts_last: bfloat16 [4, 128, 1024], P('stage', 'data')
- grad_out: bfloat16 [128, 1024], P('data')
- x_next: bfloat16 [4, 128, 1024], P(None, 'data')
- learn_rate: float32 [1], replicated
- max_norm: float32 [1], replicated
Outputs:
- output 1: float32 [4, 1024, 4096], P('stage', None, 'model')
- output 2: float32 [4, 4096, 1024], P('stage', 'model')
- output 3: float32 [4, 1024, 4096], P('stage', None, 'model')
- output 4: float32 [4, 4096, 1024], P('stage', 'model')
- output 5: float32 [4, 1024, 4096], P('stage', None, 'model')
- output 6: float32 [4, 4096, 1024], P('stage', 'model')
- output 7: bfloat16 [4, 128, 1024], P(None, 'data')
All inputs are finite; a program needn't handle non-finite values.
Results may differ from the reference program's by a relative error of at most 0.00798702.
Values are sent between devices in bfloat16 or wider.
A program may use at most 1 GiB of HBM per device.

```python
import jax
import jax.numpy as jnp
from jax import lax

STAGES = 4
REPLICAS = 2
D_MODEL = 1024
FF_WIDTH = 4096
MICRO_ROWS = 64
NEXT_MICRO = 4
ADAM_STEP = 10
BETA_ONE = 0.9
BETA_TWO = 0.95
ADAM_EPS = 1e-8
WEIGHT_DECAY = 0.1
NORM_EPS = 1e-6
ALL_ROWS = REPLICAS * MICRO_ROWS


def gelu_vjp(pre_act, upstream):
    pull_back = jax.vjp(jax.nn.gelu, pre_act)[1]
    return pull_back(upstream)[0]


def stage_apply(acts_in, up_bf, down_bf):
    pre_act = jnp.dot(acts_in, up_bf, preferred_element_type=jnp.float32)
    hidden = jax.nn.gelu(pre_act).astype(jnp.bfloat16)
    branch = jnp.dot(hidden, down_bf, preferred_element_type=jnp.float32)
    return (acts_in.astype(jnp.float32) + branch).astype(jnp.bfloat16)


def averaged_grads(w_up, w_down, g_up, g_down, acts_last, grad_out):
    def back_step(upstream, layer_in):
        up_bf, down_bf, acts_in = layer_in
        pre_act = jnp.dot(acts_in, up_bf, preferred_element_type=jnp.float32)
        hidden = jax.nn.gelu(pre_act).astype(jnp.bfloat16)
        grad_down = jnp.dot(hidden.T, upstream, preferred_element_type=jnp.float32)
        grad_hid = jnp.dot(upstream, down_bf.T, preferred_element_type=jnp.float32)
        grad_pre = gelu_vjp(pre_act, grad_hid).astype(jnp.bfloat16)
        grad_up = jnp.dot(acts_in.T, grad_pre, preferred_element_type=jnp.float32)
        back_in = jnp.dot(grad_pre, up_bf.T, preferred_element_type=jnp.float32)
        grad_in = (upstream.astype(jnp.float32) + back_in).astype(jnp.bfloat16)
        return grad_in, (grad_up, grad_down)
    layer_all = (w_up.astype(jnp.bfloat16), w_down.astype(jnp.bfloat16), acts_last)
    grad_pair = lax.scan(back_step, grad_out, layer_all, reverse=True)[1]
    mean_up = (jnp.sum(g_up, axis=0) + grad_pair[0]) / REPLICAS
    mean_down = (jnp.sum(g_down, axis=0) + grad_pair[1]) / REPLICAS
    return mean_up, mean_down


def adamw_update(weight, moment_one, moment_two, grad_step, step_rate):
    mom_new = BETA_ONE * moment_one + (1.0 - BETA_ONE) * grad_step
    sec_new = BETA_TWO * moment_two + (1.0 - BETA_TWO) * grad_step * grad_step
    one_corr = 1.0 - BETA_ONE ** ADAM_STEP
    two_corr = 1.0 - BETA_TWO ** ADAM_STEP
    direction = (mom_new / one_corr) / (jnp.sqrt(sec_new / two_corr) + ADAM_EPS)
    weight_new = weight - step_rate * (direction + WEIGHT_DECAY * weight)
    return weight_new, mom_new, sec_new


def forward_all(up_bf, down_bf, x_next):
    def one_micro(acts_in):
        def fwd_step(acts_carry, layer_in):
            return stage_apply(acts_carry, layer_in[0], layer_in[1]), None
        return lax.scan(fwd_step, acts_in, (up_bf, down_bf))[0]
    return lax.map(one_micro, x_next)


def setup_inputs(seed: int = 0) -> dict:
    key_list = jax.random.split(jax.random.key(seed), 13)
    up_scale = D_MODEL ** -0.5
    down_scale = FF_WIDTH ** -0.5
    grad_scale = MICRO_ROWS ** 0.5
    w_up = jax.random.normal(key_list[0], (STAGES, D_MODEL, FF_WIDTH), jnp.float32) * up_scale
    w_down = jax.random.normal(key_list[1], (STAGES, FF_WIDTH, D_MODEL), jnp.float32) * down_scale
    g_up = jax.random.normal(key_list[2], (REPLICAS, STAGES, D_MODEL, FF_WIDTH), jnp.float32) * (0.3 * grad_scale)
    g_down = jax.random.normal(key_list[3], (REPLICAS, STAGES, FF_WIDTH, D_MODEL), jnp.float32) * (0.5 * grad_scale)
    acts_last = jax.random.normal(key_list[4], (STAGES, ALL_ROWS, D_MODEL), jnp.float32).astype(jnp.bfloat16)
    grad_out = jax.random.normal(key_list[5], (ALL_ROWS, D_MODEL), jnp.float32).astype(jnp.bfloat16)
    x_next = jax.random.normal(key_list[6], (NEXT_MICRO, ALL_ROWS, D_MODEL), jnp.float32).astype(jnp.bfloat16)
    learn_rate = jax.random.uniform(key_list[7], (1,), jnp.float32, 0.1, 0.25) * up_scale
    mean_up, mean_down = averaged_grads(w_up, w_down, g_up, g_down, acts_last, grad_out)
    grad_norm = jnp.sqrt(jnp.sum(mean_up * mean_up) + jnp.sum(mean_down * mean_down))
    clip_frac = jax.random.uniform(key_list[8], (1,), jnp.float32, 0.35, 0.65)
    max_norm = clip_frac * grad_norm
    up_rms = clip_frac[0] * jnp.sqrt(jnp.mean(mean_up * mean_up))
    down_rms = clip_frac[0] * jnp.sqrt(jnp.mean(mean_down * mean_down))
    m_up = jax.random.normal(key_list[9], w_up.shape, jnp.float32) * (0.1 * up_rms)
    m_down = jax.random.normal(key_list[10], w_down.shape, jnp.float32) * (0.1 * down_rms)
    v_up = (0.5 + jax.random.uniform(key_list[11], w_up.shape, jnp.float32)) * (0.02 * up_rms * up_rms)
    v_down = (0.5 + jax.random.uniform(key_list[12], w_down.shape, jnp.float32)) * (0.02 * down_rms * down_rms)
    return {'w_up': w_up, 'w_down': w_down, 'm_up': m_up, 'm_down': m_down, 'v_up': v_up, 'v_down': v_down, 'g_up': g_up, 'g_down': g_down, 'acts_last': acts_last, 'grad_out': grad_out, 'x_next': x_next, 'learn_rate': learn_rate, 'max_norm': max_norm}


def reference(w_up, w_down, m_up, m_down, v_up, v_down, g_up, g_down, acts_last, grad_out, x_next, learn_rate, max_norm):
    mean_up, mean_down = averaged_grads(w_up, w_down, g_up, g_down, acts_last, grad_out)
    norm_sq = jnp.sum(mean_up * mean_up) + jnp.sum(mean_down * mean_down)
    clip_scale = jnp.minimum(1.0, max_norm[0] / (jnp.sqrt(norm_sq) + NORM_EPS))
    up_new, up_mom, up_sec = adamw_update(w_up, m_up, v_up, clip_scale * mean_up, learn_rate[0])
    down_new, down_mom, down_sec = adamw_update(w_down, m_down, v_down, clip_scale * mean_down, learn_rate[0])
    y_next = forward_all(up_new.astype(jnp.bfloat16), down_new.astype(jnp.bfloat16), x_next)
    return (up_new, down_new, up_mom, down_mom, up_sec, down_sec, y_next)
```

```python
import functools

import jax
import jax.numpy as jnp
from jax import lax
from jax.experimental import pallas as pl
from jax.experimental.pallas import tpu as pltpu
from jax.sharding import PartitionSpec as P

ADAM_STEP = 10
BETA_ONE = 0.9
BETA_TWO = 0.95
ADAM_EPS = 1e-8
WEIGHT_DECAY = 0.1
NORM_EPS = 1e-6
CONTRACT_LAST = (((1,), (1,)), ((), ()))
BLOCK = 256


def gelu_vjp(pre_act, upstream):
    pull_back = jax.vjp(jax.nn.gelu, pre_act)[1]
    return pull_back(upstream)[0]


def sum_body(half_ref, own_ref, recv_ref, left_ref, right_ref, out_ref, sq_ref):
    prod = jnp.dot(left_ref[...], right_ref[...], preferred_element_type=jnp.float32)
    mean = (own_ref[...] + recv_ref[...] + prod) * 0.5
    out_ref[...] = mean

    @pl.when(pl.program_id(0) == 0)
    def _():
        sq_ref[...] = jnp.zeros_like(sq_ref)

    sq_ref[...] += jnp.sum((mean * mean).reshape(-1, 8, mean.shape[1]), axis=0)


def sum_call(half, own, recv, left, right, own_map):
    rows, cols = recv.shape
    block = min(BLOCK, rows)
    return pl.pallas_call(
        sum_body,
        grid_spec=pltpu.PrefetchScalarGridSpec(
            num_scalar_prefetch=1,
            grid=(rows // block,),
            in_specs=[
                pl.BlockSpec((block, cols), own_map),
                pl.BlockSpec((block, cols), lambda i, h: (i, 0)),
                pl.BlockSpec((block, left.shape[1]), lambda i, h: (i, 0)),
                pl.BlockSpec(right.shape, lambda i, h: (0, 0)),
            ],
            out_specs=[
                pl.BlockSpec((block, cols), lambda i, h: (i, 0)),
                pl.BlockSpec((8, cols), lambda i, h: (0, 0)),
            ],
        ),
        out_shape=[
            jax.ShapeDtypeStruct((rows, cols), jnp.float32),
            jax.ShapeDtypeStruct((8, cols), jnp.float32),
        ],
        cost_estimate=pl.CostEstimate(flops=20 * rows * cols, bytes_accessed=12 * rows * cols, transcendentals=0),
        name="sum_half",
    )(half, own, recv, left, right)


def update_body(half_ref, rate_ref, w_ref, m_ref, v_ref, g_ref, *refs):
    ow_ref, om_ref, ov_ref, ob_ref = refs[-4:]
    clip, rate = rate_ref[0], rate_ref[1]
    grad = clip * g_ref[...]
    weight = w_ref[...]
    mom = BETA_ONE * m_ref[...] + (1.0 - BETA_ONE) * grad
    sec = BETA_TWO * v_ref[...] + (1.0 - BETA_TWO) * grad * grad
    one_corr = 1.0 - BETA_ONE**ADAM_STEP
    two_corr = 1.0 - BETA_TWO**ADAM_STEP
    direction = (mom * (1.0 / one_corr)) / (jnp.sqrt(sec * (1.0 / two_corr)) + ADAM_EPS)
    new = weight - rate * (direction + WEIGHT_DECAY * weight)
    ow_ref[...] = new
    om_ref[...] = mom
    ov_ref[...] = sec
    ob_ref[...] = new.astype(jnp.bfloat16)


def update_call(half, rates, weights, grad, full_map, previous):
    rows, cols = grad.shape
    block = min(BLOCK, rows)
    shape = weights[0].shape
    spec = pl.BlockSpec((block, cols), full_map)
    anywhere = pl.BlockSpec(memory_space=pl.ANY)
    extra = list(previous or ())
    return pl.pallas_call(
        update_body,
        grid_spec=pltpu.PrefetchScalarGridSpec(
            num_scalar_prefetch=2,
            grid=(rows // block,),
            in_specs=[spec, spec, spec, pl.BlockSpec((block, cols), lambda i, h, r: (i, 0))] + [anywhere] * len(extra),
            out_specs=[spec] * 4,
        ),
        out_shape=[jax.ShapeDtypeStruct(shape, jnp.float32)] * 3 + [jax.ShapeDtypeStruct(shape, jnp.bfloat16)],
        input_output_aliases={6 + i: i for i in range(len(extra))},
        cost_estimate=pl.CostEstimate(flops=60 * rows * cols, bytes_accessed=30 * rows * cols, transcendentals=0),
        name="adamw_half",
    )(half, rates, *weights, grad, *extra)


def solution(mesh):
    n_stage = mesh.shape['stage']
    down_perm = [(sender, sender - 1) for sender in range(1, n_stage)]
    up_perm = [(sender, sender + 1) for sender in range(n_stage - 1)]
    swap = [(0, 1), (1, 0)]
    up_spec = P('stage', None, 'model')
    down_spec = P('stage', 'model', None)
    row_spec = P(None, 'data', None)
    in_specs = (up_spec, down_spec, up_spec, down_spec, up_spec, down_spec, P('data', 'stage', None, 'model'), P('data', 'stage', 'model', None), P('stage', 'data', None), P('data', None), row_spec, P(None), P(None))
    out_specs = (up_spec, down_spec, up_spec, down_spec, up_spec, down_spec, row_spec)

    def device_step(w_up, w_down, m_up, m_down, v_up, v_down, g_up, g_down, acts_last, grad_out, x_next, learn_rate, max_norm):
        stage_id = lax.axis_index('stage')
        data_id = lax.axis_index('data')
        half = data_id.astype(jnp.int32).reshape(1)
        other = (1 - half).astype(jnp.int32)
        acts_in = acts_last[0]
        g_up, g_down = g_up[0, 0], g_down[0, 0]
        d_model, ff_local = g_up.shape
        ff_half = ff_local // 2
        n_chunk = 2
        rows_up = d_model // n_chunk
        rows_down = ff_half // n_chunk

        def trade(value):
            return lax.ppermute(value, 'data', swap)

        def both(own, got):
            low = jnp.where(data_id == 0, own, got)
            high = jnp.where(data_id == 0, got, own)
            return jnp.concatenate([low, high], axis=0)

        def up_piece(which, k):
            return lax.dynamic_slice(g_up, (k * rows_up, which * ff_half), (rows_up, ff_half))

        def down_piece(which, k):
            return lax.dynamic_slice(g_down, (which * ff_half + k * rows_down, 0), (rows_down, d_model))

        got_up = [trade(up_piece(1 - data_id, k)) for k in range(n_chunk)]
        got_down = [trade(down_piece(1 - data_id, k)) for k in range(n_chunk - 1)]

        up_bf = w_up[0].astype(jnp.bfloat16)
        down_bf = w_down[0].astype(jnp.bfloat16)
        pre_act = jnp.dot(acts_in, up_bf, preferred_element_type=jnp.float32)
        hidden = jax.nn.gelu(pre_act).astype(jnp.bfloat16)
        upstream = grad_out
        for step_idx in range(n_stage):
            grad_hid = lax.dot_general(upstream, down_bf, CONTRACT_LAST, preferred_element_type=jnp.float32)
            grad_pre = gelu_vjp(pre_act, grad_hid).astype(jnp.bfloat16)
            if step_idx == n_stage - 1:
                break
            part = lax.dot_general(grad_pre, up_bf, CONTRACT_LAST, preferred_element_type=jnp.float32)
            summed = part + lax.ppermute(part, 'model', swap)
            grad_in = (upstream.astype(jnp.float32) + summed).astype(jnp.bfloat16)
            passed = lax.ppermute(grad_in, 'stage', down_perm)
            upstream = jnp.where(stage_id == n_stage - 2 - step_idx, passed, upstream)

        def half_of(value, which):
            return lax.dynamic_slice(value, (0, which * ff_half), (value.shape[0], ff_half))

        rows_out = (acts_in, upstream, half_of(grad_pre, 1 - data_id), half_of(hidden, 1 - data_id))
        rows_own = (acts_in, upstream, half_of(grad_pre, data_id), half_of(hidden, data_id))
        rows_got = [trade(value) for value in rows_out]
        last_piece, rows_got = lax.optimization_barrier((down_piece(1 - data_id, n_chunk - 1), rows_got))
        got_down.append(trade(last_piece))
        all_acts, all_up, all_pre, all_hid = [both(own, got) for own, got in zip(rows_own, rows_got)]
        acts_t = all_acts.T
        hid_t = all_hid.T

        mean_up, mean_down, squares = [], [], []
        per_up, per_down = rows_up // min(BLOCK, rows_up), rows_down // min(BLOCK, rows_down)
        for k in range(n_chunk):
            own_map = lambda i, h, k=k: (k * per_up + i, h[0])
            mean, square = sum_call(half, g_up, got_up[k], acts_t[k * rows_up:(k + 1) * rows_up], all_pre, own_map)
            mean_up.append(mean)
            squares.append(square)
        for k in range(n_chunk):
            own_map = lambda i, h, k=k: (h[0] * n_chunk * per_down + k * per_down + i, 0)
            mean, square = sum_call(half, g_down, got_down[k], hid_t[k * rows_down:(k + 1) * rows_down], all_up, own_map)
            mean_down.append(mean)
            squares.append(square)

        far_up = [trade(mean_up[0])]
        norm_sq = sum(jnp.sum(square) for square in squares)
        norm_sq = norm_sq + trade(norm_sq)
        norm_sq, rest = lax.optimization_barrier((norm_sq, (mean_up[1:], mean_down)))
        far_up += [trade(value) for value in rest[0]]
        far_down = [trade(value) for value in rest[1]]
        norm_sq = norm_sq + lax.ppermute(norm_sq, 'model', swap)
        for bit in (1, 2):
            norm_sq = norm_sq + lax.ppermute(norm_sq, 'stage', [(i, i ^ bit) for i in range(n_stage)])
        clip = jnp.minimum(1.0, max_norm[0] / (jnp.sqrt(norm_sq) + NORM_EPS))
        rates = jnp.stack([clip, learn_rate[0]])

        ups = (w_up[0], m_up[0], v_up[0])
        downs = (w_down[0], m_down[0], v_down[0])
        new_up = new_down = None
        for which, parts_up, parts_down in ((half, mean_up, mean_down), (other, far_up, far_down)):
            for k in range(n_chunk):
                full_map = lambda i, h, r, k=k: (k * per_up + i, h[0])
                new_up = update_call(which, rates, ups, parts_up[k], full_map, new_up)
            for k in range(n_chunk):
                full_map = lambda i, h, r, k=k: (h[0] * n_chunk * per_down + k * per_down + i, 0)
                new_down = update_call(which, rates, downs, parts_down[k], full_map, new_down)

        up_new_bf, down_new_bf = new_up[3], new_down[3]
        n_micro, row_count = x_next.shape[:2]
        acts = x_next.reshape(n_micro * row_count, d_model)
        for step_idx in range(n_stage):
            pre = jnp.dot(acts, up_new_bf, preferred_element_type=jnp.float32)
            hid = jax.nn.gelu(pre).astype(jnp.bfloat16)
            part = jnp.dot(hid, down_new_bf, preferred_element_type=jnp.float32)
            summed = part + lax.ppermute(part, 'model', swap)
            result = (acts.astype(jnp.float32) + summed).astype(jnp.bfloat16)
            if step_idx < n_stage - 1:
                acts = lax.ppermute(result, 'stage', up_perm)
        last = n_stage - 1
        y_next = result
        for target in range(last):
            got = lax.ppermute(result, 'stage', [(last, target)])
            y_next = jnp.where(stage_id == target, got, y_next)
        y_next = y_next.reshape(n_micro, row_count, d_model)
        return (new_up[0][None], new_down[0][None], new_up[1][None], new_down[1][None], new_up[2][None], new_down[2][None], y_next)

    return jax.shard_map(device_step, mesh=mesh, in_specs=in_specs, out_specs=out_specs, check_vma=False)
```

```python
import functools

import jax
import jax.numpy as jnp
from jax import lax
from jax.experimental import pallas as pl
from jax.experimental.pallas import tpu as pltpu
from jax.sharding import PartitionSpec as P

ADAM_STEP = 10
BETA_ONE = 0.9
BETA_TWO = 0.95
ADAM_EPS = 1e-8
WEIGHT_DECAY = 0.1
NORM_EPS = 1e-6
CONTRACT_LAST = (((1,), (1,)), ((), ()))
BLOCK = 256


def gelu_vjp(pre_act, upstream):
    pull_back = jax.vjp(jax.nn.gelu, pre_act)[1]
    return pull_back(upstream)[0]


def sum_body(half_ref, own_ref, recv_ref, left_ref, right_ref, out_ref, sq_ref):
    prod = jnp.dot(left_ref[...], right_ref[...], preferred_element_type=jnp.float32)
    mean = (own_ref[...] + recv_ref[...] + prod) * 0.5
    out_ref[...] = mean

    @pl.when(pl.program_id(0) == 0)
    def _():
        sq_ref[...] = jnp.zeros_like(sq_ref)

    sq_ref[...] += jnp.sum((mean * mean).reshape(-1, 8, mean.shape[1]), axis=0)


def sum_call(half, own, recv, left, right, own_map):
    rows, cols = recv.shape
    block = min(BLOCK, rows)
    return pl.pallas_call(
        sum_body,
        grid_spec=pltpu.PrefetchScalarGridSpec(
            num_scalar_prefetch=1,
            grid=(rows // block,),
            in_specs=[
                pl.BlockSpec((block, cols), own_map),
                pl.BlockSpec((block, cols), lambda i, h: (i, 0)),
                pl.BlockSpec((block, left.shape[1]), lambda i, h: (i, 0)),
                pl.BlockSpec(right.shape, lambda i, h: (0, 0)),
            ],
            out_specs=[
                pl.BlockSpec((block, cols), lambda i, h: (i, 0)),
                pl.BlockSpec((8, cols), lambda i, h: (0, 0)),
            ],
        ),
        out_shape=[
            jax.ShapeDtypeStruct((rows, cols), jnp.float32),
            jax.ShapeDtypeStruct((8, cols), jnp.float32),
        ],
        cost_estimate=pl.CostEstimate(flops=20 * rows * cols, bytes_accessed=12 * rows * cols, transcendentals=0),
        name="sum_half",
    )(half, own, recv, left, right)


def update_body(half_ref, rate_ref, w_ref, m_ref, v_ref, g_ref, *refs):
    ow_ref, om_ref, ov_ref, ob_ref = refs[-4:]
    clip, rate = rate_ref[0], rate_ref[1]
    grad = clip * g_ref[...]
    weight = w_ref[...]
    mom = BETA_ONE * m_ref[...] + (1.0 - BETA_ONE) * grad
    sec = BETA_TWO * v_ref[...] + (1.0 - BETA_TWO) * grad * grad
    one_corr = 1.0 - BETA_ONE**ADAM_STEP
    two_corr = 1.0 - BETA_TWO**ADAM_STEP
    direction = (mom * (1.0 / one_corr)) / (jnp.sqrt(sec * (1.0 / two_corr)) + ADAM_EPS)
    new = weight - rate * (direction + WEIGHT_DECAY * weight)
    ow_ref[...] = new
    om_ref[...] = mom
    ov_ref[...] = sec
    ob_ref[...] = new.astype(jnp.bfloat16)


def update_call(half, rates, weights, grad, full_map, previous):
    rows, cols = grad.shape
    block = min(BLOCK, rows)
    shape = weights[0].shape
    spec = pl.BlockSpec((block, cols), full_map)
    anywhere = pl.BlockSpec(memory_space=pl.ANY)
    extra = list(previous or ())
    return pl.pallas_call(
        update_body,
        grid_spec=pltpu.PrefetchScalarGridSpec(
            num_scalar_prefetch=2,
            grid=(rows // block,),
            in_specs=[spec, spec, spec, pl.BlockSpec((block, cols), lambda i, h, r: (i, 0))] + [anywhere] * len(extra),
            out_specs=[spec] * 4,
        ),
        out_shape=[jax.ShapeDtypeStruct(shape, jnp.float32)] * 3 + [jax.ShapeDtypeStruct(shape, jnp.bfloat16)],
        input_output_aliases={6 + i: i for i in range(len(extra))},
        cost_estimate=pl.CostEstimate(flops=60 * rows * cols, bytes_accessed=30 * rows * cols, transcendentals=0),
        name="adamw_half",
    )(half, rates, *weights, grad, *extra)


def forward_body(n_stage, n_micro, x_ref, up_ref, down_ref, y_ref, inbox, hid, mine, outbox, landed, ready, local_sem, in_sem, part_ssem, part_rsem, pass_ssem, y_ssem, y_rsem):
    model = lax.axis_index('model')
    stage = lax.axis_index('stage')
    mesh_id = pl.DeviceIdType.MESH
    last = n_stage - 1
    half = mine.shape[2]
    barrier = pltpu.get_barrier_semaphore()
    peers = [(dm, ds) for dm in range(2) for ds in range(n_stage) if dm or ds]
    for dm, ds in peers:
        pl.semaphore_signal(barrier, inc=1, device_id={'model': lax.rem(model + dm, 2), 'stage': lax.rem(stage + ds, n_stage)}, device_id_type=mesh_id)

    def load(b, c):
        return pltpu.make_async_copy(x_ref.at[b, :, pl.ds(c * half, half)], inbox.at[b, c], local_sem.at[b, c])

    @pl.when(stage == 0)
    def _():
        for b in range(n_micro):
            for c in range(2):
                load(b, c).start()

    pl.semaphore_wait(barrier, len(peers))

    def arrival(b, c):
        return pltpu.make_async_remote_copy(src_ref=ready.at[b], dst_ref=inbox.at[b, c], send_sem=pass_ssem.at[b, 0], recv_sem=in_sem.at[b, c], device_id={'model': model}, device_id_type=mesh_id)

    def trade(b):
        return pltpu.make_async_remote_copy(src_ref=outbox.at[b], dst_ref=landed.at[b], send_sem=part_ssem.at[b], recv_sem=part_rsem.at[b], device_id={'model': 1 - model}, device_id_type=mesh_id)

    def hand_on(b, to):
        return pltpu.make_async_remote_copy(src_ref=ready.at[b], dst_ref=inbox.at[b, model], send_sem=pass_ssem.at[b, to], recv_sem=in_sem.at[b, model], device_id={'model': to, 'stage': stage + 1}, device_id_type=mesh_id)

    def publish(b, k):
        dm, ds = peers[k]
        return pltpu.make_async_remote_copy(src_ref=ready.at[b], dst_ref=landing(b, model), send_sem=y_ssem.at[b, k], recv_sem=y_rsem.at[b, model], device_id={'model': lax.rem(model + dm, 2), 'stage': lax.rem(stage + ds, n_stage)}, device_id_type=mesh_id)

    def landing(b, c):
        return y_ref.at[b, :, pl.ds(pl.multiple_of(c * half, half), half)]

    def y_arrival(b, c):
        return pltpu.make_async_remote_copy(src_ref=ready.at[b], dst_ref=landing(b, c), send_sem=y_ssem.at[b, 0], recv_sem=y_rsem.at[b, c], device_id={'model': model}, device_id_type=mesh_id)

    def step(b, carry):
        @pl.when(b < n_micro)
        def _():
            @pl.when(stage == 0)
            def _():
                for c in range(2):
                    load(b, c).wait()

            @pl.when(stage > 0)
            def _():
                for c in range(2):
                    arrival(b, c).wait_recv()

            pre = jnp.dot(inbox[b, 0], up_ref[:half], preferred_element_type=jnp.float32)
            pre = pre + jnp.dot(inbox[b, 1], up_ref[half:], preferred_element_type=jnp.float32)
            hid[...] = jax.nn.gelu(pre).astype(jnp.bfloat16)

        @pl.when(b > 0)
        def _():
            p = b - 1
            trade(p).wait_recv()
            total = inbox[p, model].astype(jnp.float32) + (mine[p] + landed[p])
            done = total.astype(jnp.bfloat16)
            ready[p] = done

            @pl.when(stage < last)
            def _():
                for to in range(2):
                    hand_on(p, to).start()

            @pl.when(stage == last)
            def _():
                y_ref[p, :, pl.ds(pl.multiple_of(model * half, half), half)] = done
                for k in range(len(peers)):
                    publish(p, k).start()

        @pl.when(b < n_micro)
        def _():
            far = pl.multiple_of((1 - model) * half, half)
            near = pl.multiple_of(model * half, half)
            outbox[b] = jnp.dot(hid[...], down_ref[:, pl.ds(far, half)], preferred_element_type=jnp.float32)
            trade(b).start()
            mine[b] = jnp.dot(hid[...], down_ref[:, pl.ds(near, half)], preferred_element_type=jnp.float32)

        return carry

    lax.fori_loop(0, n_micro + 1, step, 0)

    for b in range(n_micro):
        trade(b).wait_send()

    @pl.when(stage < last)
    def _():
        for b in range(n_micro):
            for to in range(2):
                hand_on(b, to).wait_send()
            for c in range(2):
                y_arrival(b, c).wait_recv()

    @pl.when(stage == last)
    def _():
        for b in range(n_micro):
            for k in range(len(peers)):
                publish(b, k).wait_send()
            y_arrival(b, 1 - model).wait_recv()


def forward_call(n_stage, x_next, up_bf, down_bf):
    n_micro, rows, d_model = x_next.shape
    ff_local = up_bf.shape[1]
    half = d_model // 2
    dma = pltpu.SemaphoreType.DMA
    in_vmem = pl.BlockSpec(memory_space=pltpu.VMEM)
    return pl.pallas_call(
        functools.partial(forward_body, n_stage, n_micro),
        out_shape=jax.ShapeDtypeStruct(x_next.shape, jnp.bfloat16),
        in_specs=[pl.BlockSpec(memory_space=pl.ANY), in_vmem, in_vmem],
        out_specs=in_vmem,
        scratch_shapes=[
            pltpu.VMEM((n_micro, 2, rows, half), jnp.bfloat16),
            pltpu.VMEM((rows, ff_local), jnp.bfloat16),
            pltpu.VMEM((n_micro, rows, half), jnp.float32),
            pltpu.VMEM((n_micro, rows, half), jnp.float32),
            pltpu.VMEM((n_micro, rows, half), jnp.float32),
            pltpu.VMEM((n_micro, rows, half), jnp.bfloat16),
            dma((n_micro, 2)),
            dma((n_micro, 2)),
            dma((n_micro,)),
            dma((n_micro,)),
            dma((n_micro, 2)),
            dma((n_micro, 2 * n_stage - 1)),
            dma((n_micro, 2)),
        ],
        compiler_params=pltpu.CompilerParams(collective_id=1, has_side_effects=True, vmem_limit_bytes=48 << 20),
        name="forward_pipe",
    )(x_next, up_bf, down_bf)


def solution(mesh):
    n_stage = mesh.shape['stage']
    down_perm = [(sender, sender - 1) for sender in range(1, n_stage)]
    swap = [(0, 1), (1, 0)]
    up_spec = P('stage', None, 'model')
    down_spec = P('stage', 'model', None)
    row_spec = P(None, 'data', None)
    in_specs = (up_spec, down_spec, up_spec, down_spec, up_spec, down_spec, P('data', 'stage', None, 'model'), P('data', 'stage', 'model', None), P('stage', 'data', None), P('data', None), row_spec, P(None), P(None))
    out_specs = (up_spec, down_spec, up_spec, down_spec, up_spec, down_spec, row_spec)

    def device_step(w_up, w_down, m_up, m_down, v_up, v_down, g_up, g_down, acts_last, grad_out, x_next, learn_rate, max_norm):
        stage_id = lax.axis_index('stage')
        data_id = lax.axis_index('data')
        half = data_id.astype(jnp.int32).reshape(1)
        other = (1 - half).astype(jnp.int32)
        acts_in = acts_last[0]
        g_up, g_down = g_up[0, 0], g_down[0, 0]
        d_model, ff_local = g_up.shape
        ff_half = ff_local // 2
        n_chunk = 2
        rows_up = d_model // n_chunk
        rows_down = ff_half // n_chunk

        def trade(value):
            return lax.ppermute(value, 'data', swap)

        def both(own, got):
            low = jnp.where(data_id == 0, own, got)
            high = jnp.where(data_id == 0, got, own)
            return jnp.concatenate([low, high], axis=0)

        def up_piece(which, k):
            return lax.dynamic_slice(g_up, (k * rows_up, which * ff_half), (rows_up, ff_half))

        def down_piece(which, k):
            return lax.dynamic_slice(g_down, (which * ff_half + k * rows_down, 0), (rows_down, d_model))

        got_up = [trade(up_piece(1 - data_id, k)) for k in range(n_chunk)]
        got_down = [trade(down_piece(1 - data_id, k)) for k in range(n_chunk - 1)]

        up_bf = w_up[0].astype(jnp.bfloat16)
        down_bf = w_down[0].astype(jnp.bfloat16)
        pre_act = jnp.dot(acts_in, up_bf, preferred_element_type=jnp.float32)
        hidden = jax.nn.gelu(pre_act).astype(jnp.bfloat16)
        upstream = grad_out
        for step_idx in range(n_stage):
            grad_hid = lax.dot_general(upstream, down_bf, CONTRACT_LAST, preferred_element_type=jnp.float32)
            grad_pre = gelu_vjp(pre_act, grad_hid).astype(jnp.bfloat16)
            if step_idx == n_stage - 1:
                break
            part = lax.dot_general(grad_pre, up_bf, CONTRACT_LAST, preferred_element_type=jnp.float32)
            summed = part + lax.ppermute(part, 'model', swap)
            grad_in = (upstream.astype(jnp.float32) + summed).astype(jnp.bfloat16)
            passed = lax.ppermute(grad_in, 'stage', down_perm)
            upstream = jnp.where(stage_id == n_stage - 2 - step_idx, passed, upstream)

        def half_of(value, which):
            return lax.dynamic_slice(value, (0, which * ff_half), (value.shape[0], ff_half))

        rows_out = (acts_in, upstream, half_of(grad_pre, 1 - data_id), half_of(hidden, 1 - data_id))
        rows_own = (acts_in, upstream, half_of(grad_pre, data_id), half_of(hidden, data_id))
        rows_got = [trade(value) for value in rows_out]
        last_piece, rows_got = lax.optimization_barrier((down_piece(1 - data_id, n_chunk - 1), rows_got))
        got_down.append(trade(last_piece))
        all_acts, all_up, all_pre, all_hid = [both(own, got) for own, got in zip(rows_own, rows_got)]
        acts_t = all_acts.T
        hid_t = all_hid.T

        mean_up, mean_down, squares = [], [], []
        per_up, per_down = rows_up // min(BLOCK, rows_up), rows_down // min(BLOCK, rows_down)
        for k in range(n_chunk):
            own_map = lambda i, h, k=k: (k * per_up + i, h[0])
            mean, square = sum_call(half, g_up, got_up[k], acts_t[k * rows_up:(k + 1) * rows_up], all_pre, own_map)
            mean_up.append(mean)
            squares.append(square)
        for k in range(n_chunk):
            own_map = lambda i, h, k=k: (h[0] * n_chunk * per_down + k * per_down + i, 0)
            mean, square = sum_call(half, g_down, got_down[k], hid_t[k * rows_down:(k + 1) * rows_down], all_up, own_map)
            mean_down.append(mean)
            squares.append(square)

        far_up = [trade(mean_up[0])]
        norm_sq = sum(jnp.sum(square) for square in squares)
        norm_sq = norm_sq + trade(norm_sq)
        norm_sq, rest = lax.optimization_barrier((norm_sq, (mean_up[1:], mean_down)))
        far_up += [trade(value) for value in rest[0]]
        far_down = [trade(value) for value in rest[1]]
        norm_sq = norm_sq + lax.ppermute(norm_sq, 'model', swap)
        for bit in (1, 2):
            norm_sq = norm_sq + lax.ppermute(norm_sq, 'stage', [(i, i ^ bit) for i in range(n_stage)])
        clip = jnp.minimum(1.0, max_norm[0] / (jnp.sqrt(norm_sq) + NORM_EPS))
        rates = jnp.stack([clip, learn_rate[0]])

        ups = (w_up[0], m_up[0], v_up[0])
        downs = (w_down[0], m_down[0], v_down[0])
        new_up = new_down = None
        for which, parts_up, parts_down in ((half, mean_up, mean_down), (other, far_up, far_down)):
            for k in range(n_chunk):
                full_map = lambda i, h, r, k=k: (k * per_up + i, h[0])
                new_up = update_call(which, rates, ups, parts_up[k], full_map, new_up)
            for k in range(n_chunk):
                full_map = lambda i, h, r, k=k: (h[0] * n_chunk * per_down + k * per_down + i, 0)
                new_down = update_call(which, rates, downs, parts_down[k], full_map, new_down)

        y_next = forward_call(n_stage, x_next, new_up[3], new_down[3])
        return (new_up[0][None], new_down[0][None], new_up[1][None], new_down[1][None], new_up[2][None], new_down[2][None], y_next)

    return jax.shard_map(device_step, mesh=mesh, in_specs=in_specs, out_specs=out_specs, check_vma=False)
```

```python
import functools

import jax
import jax.numpy as jnp
from jax import lax
from jax.experimental import pallas as pl
from jax.experimental.pallas import tpu as pltpu
from jax.sharding import PartitionSpec as P

ADAM_STEP = 10
BETA_ONE = 0.9
BETA_TWO = 0.95
ADAM_EPS = 1e-8
WEIGHT_DECAY = 0.1
NORM_EPS = 1e-6
CONTRACT_LAST = (((1,), (1,)), ((), ()))
BLOCK = 256


def update_body(half_ref, rate_ref, clip_ref, w_ref, m_ref, v_ref, g_ref, *refs):
    ow_ref, om_ref, ov_ref, ob_ref = refs[-4:]
    rate = rate_ref[0]
    grad = clip_ref[0:1] * g_ref[...]
    weight = w_ref[...]
    mom = BETA_ONE * m_ref[...] + (1.0 - BETA_ONE) * grad
    sec = BETA_TWO * v_ref[...] + (1.0 - BETA_TWO) * grad * grad
    one_corr = 1.0 - BETA_ONE**ADAM_STEP
    two_corr = 1.0 - BETA_TWO**ADAM_STEP
    direction = (mom * (1.0 / one_corr)) / (jnp.sqrt(sec * (1.0 / two_corr)) + ADAM_EPS)
    new = weight - rate * (direction + WEIGHT_DECAY * weight)
    ow_ref[...] = new
    om_ref[...] = mom
    ov_ref[...] = sec
    ob_ref[...] = new.astype(jnp.bfloat16)


def update_call(half, rate, clip, weights, grad, full_map, previous):
    rows, cols = grad.shape
    block = min(BLOCK, rows)
    shape = weights[0].shape
    spec = pl.BlockSpec((block, cols), full_map)
    anywhere = pl.BlockSpec(memory_space=pl.ANY)
    extra = list(previous or ())
    return pl.pallas_call(
        update_body,
        grid_spec=pltpu.PrefetchScalarGridSpec(
            num_scalar_prefetch=2,
            grid=(rows // block,),
            in_specs=[pl.BlockSpec(clip.shape, lambda i, h, r: (0, 0)), spec, spec, spec, pl.BlockSpec((block, cols), lambda i, h, r: (i, 0))] + [anywhere] * len(extra),
            out_specs=[spec] * 4,
        ),
        out_shape=[jax.ShapeDtypeStruct(shape, jnp.float32)] * 3 + [jax.ShapeDtypeStruct(shape, jnp.bfloat16)],
        input_output_aliases={7 + i: i for i in range(len(extra))},
        cost_estimate=pl.CostEstimate(flops=60 * rows * cols, bytes_accessed=30 * rows * cols, transcendentals=0),
        name="adamw_half",
    )(half, rate, clip, *weights, grad, *extra)


def backward_body(n_stage, n_raw, bounds_up, bounds_down, gu_ref, gd_ref, wu_ref, wd_ref, acts_ref, gout_ref, max_ref, *refs):
    n_up, n_down = len(bounds_up), len(bounds_down)
    outs_up, outs_down = refs[:n_up], refs[n_up:n_up + n_down]
    far_ref, clip_ref = refs[n_up + n_down:n_up + n_down + 2]
    (up_bf, down_bf, st_up, st_down, acc_up, acc_down, got_up, got_down, fold, hid, slope, grad_pre, gbuf, outbox, landed, ready, rows_a, rows_z, norm_box, norm_pair,
     st_sem, loc_sem, fold_sem, own_sem, out_sem, g_rsem, trade_sem, pass_ssem, rs_ssem, rs_rsem, row_ssem, row_rsem, far_sem, norm_ssem, norm_rsem) = refs[n_up + n_down + 2:]
    model, data, stage = lax.axis_index('model'), lax.axis_index('data'), lax.axis_index('stage')
    mesh_id = pl.DeviceIdType.MESH
    last = n_stage - 1
    d_model, ff_half = acc_up.shape
    half = d_model // 2
    n_row = acts_ref.shape[0]
    n_up_chunk, n_down_chunk = d_model // BLOCK, ff_half // BLOCK
    peer = {'data': 1 - data}
    near = pl.ds(pl.multiple_of(model * half, half), half)
    far = pl.ds(pl.multiple_of((1 - model) * half, half), half)
    own_cols = pl.ds(pl.multiple_of(data * ff_half, ff_half), ff_half)
    peer_cols = pl.ds(pl.multiple_of((1 - data) * ff_half, ff_half), ff_half)
    own_rows = pl.ds(pl.multiple_of(data * n_row, n_row), n_row)
    first_dims = (((0,), (0,)), ((), ()))

    def remote(src, dst, ssem, rsem, where):
        return pltpu.make_async_remote_copy(src_ref=src, dst_ref=dst, send_sem=ssem, recv_sem=rsem, device_id=where, device_id_type=mesh_id)

    barrier = pltpu.get_barrier_semaphore()
    group = [(dm, ds) for dm in range(2) for ds in range(n_stage) if dm or ds]
    where = [{'model': lax.rem(model + dm, 2), 'stage': lax.rem(stage + ds, n_stage)} for dm, ds in group]
    for target in where + [peer]:
        pl.semaphore_signal(barrier, inc=1, device_id=target, device_id_type=mesh_id)

    n_st_up, n_st_down = d_model // st_up.shape[1], 2 * ff_half // st_down.shape[1]

    def load_up(r):
        return pltpu.make_async_copy(wu_ref.at[pl.ds(r * st_up.shape[1], st_up.shape[1])], st_up.at[r % 2], st_sem.at[0, r % 2])

    def load_down(r):
        return pltpu.make_async_copy(wd_ref.at[pl.ds(r * st_down.shape[1], st_down.shape[1])], st_down.at[r % 2], st_sem.at[1, r % 2])

    load_acts = pltpu.make_async_copy(acts_ref, rows_a.at[own_rows], loc_sem.at[0])
    load_acts.start()
    load_up(0).start()
    load_up(1).start()
    load_down(0).start()
    load_down(1).start()

    def load_g(c):
        return pltpu.make_async_copy(gout_ref.at[:, pl.ds(c * half, half)], gbuf.at[c], loc_sem.at[1 + c])

    @pl.when(stage == last)
    def _():
        for c in range(2):
            load_g(c).start()

    pl.semaphore_wait(barrier, len(where) + 1)

    def chunk(k):
        return pl.ds(k * BLOCK, BLOCK)

    raw = [remote(gu_ref.at[chunk(k), peer_cols], got_up.at[chunk(k)], rs_ssem.at[0, k], rs_rsem.at[0, k], peer) for k in range(n_up_chunk)]
    for copy in raw:
        copy.start()
    send_a = remote(acts_ref, rows_a.at[own_rows], row_ssem.at[0], row_rsem.at[0], peer)
    send_a.start()

    for r in range(n_st_up):
        load_up(r).wait()
        up_bf[pl.ds(r * st_up.shape[1], st_up.shape[1])] = st_up[r % 2].astype(jnp.bfloat16)
        if r + 2 < n_st_up:
            load_up(r + 2).start()
    load_acts.wait()

    tile = 256
    n_tile = hid.shape[1] // tile
    scale = 0.7978845608028654
    cubic = 0.044715

    def pre_tile(j, carry):
        cols = pl.ds(pl.multiple_of(j * tile, tile), tile)
        pre = jnp.dot(rows_a[own_rows], up_bf[:, cols], preferred_element_type=jnp.float32)
        square = pre * pre
        bend = jnp.tanh(scale * (pre + cubic * square * pre))
        hid[:, cols] = (pre * (0.5 * (1.0 + bend))).astype(jnp.bfloat16)
        slope[:, cols] = 0.5 * (1.0 + bend) + 0.5 * pre * (1.0 - bend * bend) * (scale * (1.0 + 3.0 * cubic * square))
        return carry

    lax.fori_loop(0, n_tile, pre_tile, 0)

    for r in range(n_st_down):
        load_down(r).wait()
        down_bf[pl.ds(r * st_down.shape[1], st_down.shape[1])] = st_down[r % 2].astype(jnp.bfloat16)
        if r + 2 < n_st_down:
            load_down(r + 2).start()

    own_up = pltpu.make_async_copy(gu_ref.at[:, own_cols], acc_up, own_sem.at[0])
    own_down = pltpu.make_async_copy(gd_ref.at[own_cols], acc_down, own_sem.at[1])
    load_fold = pltpu.make_async_copy(gd_ref.at[peer_cols], fold, fold_sem)
    load_fold.start()
    own_up.start()
    own_down.start()

    @pl.when(stage == last)
    def _():
        for c in range(2):
            load_g(c).wait()

    @pl.when(stage < last)
    def _():
        for c in range(2):
            remote(ready, gbuf.at[c], pass_ssem.at[0], g_rsem.at[c], {'model': model}).wait_recv()

    def slope_tile(j, carry):
        cols = pl.ds(pl.multiple_of(j * tile, tile), tile)
        grad = lax.dot_general(gbuf[0], down_bf[cols, :half], CONTRACT_LAST, preferred_element_type=jnp.float32)
        grad = grad + lax.dot_general(gbuf[1], down_bf[cols, half:], CONTRACT_LAST, preferred_element_type=jnp.float32)
        grad_pre[:, cols] = (slope[:, cols] * grad).astype(jnp.bfloat16)
        return carry

    lax.fori_loop(0, n_tile, slope_tile, 0)

    trade = remote(outbox, landed, trade_sem.at[0], trade_sem.at[1], {'model': 1 - model})

    def hand_on(to):
        return remote(ready, gbuf.at[model], pass_ssem.at[to], g_rsem.at[model], {'model': to, 'stage': stage - 1})

    @pl.when(stage > 0)
    def _():
        outbox[...] = lax.dot_general(grad_pre[...], up_bf[far], CONTRACT_LAST, preferred_element_type=jnp.float32)
        trade.start()
        mine = lax.dot_general(grad_pre[...], up_bf[near], CONTRACT_LAST, preferred_element_type=jnp.float32)
        trade.wait_recv()
        ready[...] = (gbuf[model].astype(jnp.float32) + (mine + landed[...])).astype(jnp.bfloat16)
        for to in range(2):
            hand_on(to).start()

    rows_z[own_rows] = grad_pre[:, own_cols]
    send_z = remote(grad_pre.at[:, peer_cols], rows_z.at[own_rows], row_ssem.at[1], row_rsem.at[1], peer)
    send_z.start()

    def down_product(k, side):
        cols = pl.ds(pl.multiple_of(side * ff_half + k * BLOCK, BLOCK), BLOCK)
        left = hid[:, cols]
        return [lax.dot_general(left, gbuf[c], first_dims, preferred_element_type=jnp.float32) for c in range(2)]

    load_fold.wait()

    def send_fold(k):
        rows = pl.ds(pl.multiple_of(k * BLOCK, BLOCK), BLOCK)
        return remote(fold.at[rows], got_down.at[rows], rs_ssem.at[1, k], rs_rsem.at[1, k], peer)

    def fold_step(k, carry):
        rows = pl.ds(pl.multiple_of(k * BLOCK, BLOCK), BLOCK)
        low, high = down_product(k, 1 - data)
        fold[rows, :half] += low
        fold[rows, half:] += high
        send_fold(k).start()
        return carry

    lax.fori_loop(0, n_down_chunk, fold_step, 0)
    own_down.wait()

    def own_step(k, carry):
        rows = pl.ds(pl.multiple_of(k * BLOCK, BLOCK), BLOCK)
        low, high = down_product(k, data)
        acc_down[rows, :half] += low
        acc_down[rows, half:] += high
        return carry

    lax.fori_loop(0, n_down_chunk, own_step, 0)

    @pl.when(stage > 0)
    def _():
        trade.wait_send()
        for to in range(2):
            hand_on(to).wait_send()

    own_up.wait()
    send_a.wait_recv()
    squares = jnp.zeros((8, ff_half), jnp.float32)

    def fold_squares(mean):
        return jnp.sum((mean * mean).reshape(-1, 8, mean.shape[1]), axis=0)

    def put(acc, bounds, outs, sem_row):
        copies = []
        for i, (lo, hi) in enumerate(bounds):
            copies.append(pltpu.make_async_copy(acc.at[pl.ds(lo, hi - lo)], outs[i], out_sem.at[sem_row, i]))
        return copies

    put_up = put(acc_up, bounds_up, outs_up, 0)
    put_down = put(acc_down, bounds_down, outs_down, 1)
    for k in range(n_up_chunk):
        raw[k].wait_recv()
        if k == 0:
            send_z.wait_recv()
        product = lax.dot_general(rows_a[:, k * BLOCK:(k + 1) * BLOCK], rows_z[...], first_dims, preferred_element_type=jnp.float32)
        mean = (acc_up[chunk(k)] + got_up[chunk(k)] + product) * 0.5
        acc_up[chunk(k)] = mean
        squares = squares + fold_squares(mean)
        for i, (lo, hi) in enumerate(bounds_up):
            if hi == (k + 1) * BLOCK:
                put_up[i].start()
    first = bounds_up[0][1]
    send_far = remote(acc_up.at[pl.ds(0, first)], far_ref, far_sem.at[0], far_sem.at[1], peer)
    send_far.start()
    for k in range(n_down_chunk):
        send_fold(k).wait_recv()
        mean = (acc_down[chunk(k)] + got_down[chunk(k)]) * 0.5
        acc_down[chunk(k)] = mean
        squares = squares + fold_squares(mean)
        for i, (lo, hi) in enumerate(bounds_down):
            if hi == (k + 1) * BLOCK:
                put_down[i].start()

    lanes = norm_box.shape[2]
    part = squares[:, :lanes]
    for j in range(1, ff_half // lanes):
        part = part + squares[:, j * lanes:(j + 1) * lanes]
    me = model * n_stage + stage
    norm_box[me] = part

    def spread(i):
        return remote(norm_box.at[me], norm_box.at[me], norm_ssem.at[i], norm_rsem.at[me], where[i])

    for i in range(len(group)):
        spread(i).start()
    for i, (dm, ds) in enumerate(group):
        them = lax.rem(model + dm, 2) * n_stage + lax.rem(stage + ds, n_stage)
        remote(norm_box.at[me], norm_box.at[them], norm_ssem.at[i], norm_rsem.at[them], where[i]).wait_recv()
    total = norm_box[0]
    for i in range(1, 2 * n_stage):
        total = total + norm_box[i]
    norm_pair[0] = total
    swap = remote(norm_pair.at[0], norm_pair.at[1], norm_ssem.at[len(group)], norm_rsem.at[2 * n_stage], peer)
    swap.start()
    swap.wait_recv()
    norm_sq = jnp.sum(norm_pair[0] + norm_pair[1], axis=(0, 1), keepdims=True)
    norm = jnp.sqrt(jnp.broadcast_to(norm_sq, clip_ref.shape)) + NORM_EPS
    clip_ref[...] = jnp.minimum(1.0, max_ref[0] / norm)

    swap.wait_send()
    for i in range(len(group)):
        spread(i).wait_send()
    for copy in raw + [send_a, send_z]:
        copy.wait_send()
    for k in range(n_down_chunk):
        send_fold(k).wait_send()
    for copy in put_up + put_down:
        copy.wait()
    send_far.wait()


def backward_call(n_stage, bounds_up, bounds_down, g_up, g_down, w_up, w_down, acts, grad_out, max_norm):
    d_model, ff_local = g_up.shape
    ff_half, half, n_row = ff_local // 2, d_model // 2, acts.shape[0]
    dma = pltpu.SemaphoreType.DMA
    anywhere = pl.BlockSpec(memory_space=pl.ANY)
    f32, bf16 = jnp.float32, jnp.bfloat16
    shapes = [jax.ShapeDtypeStruct((hi - lo, ff_half), f32) for lo, hi in bounds_up]
    shapes += [jax.ShapeDtypeStruct((hi - lo, d_model), f32) for lo, hi in bounds_down]
    shapes += [jax.ShapeDtypeStruct((bounds_up[0][1], ff_half), f32), jax.ShapeDtypeStruct((8, ff_half), f32)]
    n_chunk = max(d_model, ff_half) // BLOCK
    return pl.pallas_call(
        functools.partial(backward_body, n_stage, n_chunk, bounds_up, bounds_down),
        out_shape=shapes,
        in_specs=[anywhere] * 6 + [pl.BlockSpec(memory_space=pltpu.SMEM)],
        out_specs=[anywhere] * (len(shapes) - 1) + [pl.BlockSpec(memory_space=pltpu.VMEM)],
        scratch_shapes=[
            pltpu.VMEM((d_model, ff_local), bf16),
            pltpu.VMEM((ff_local, d_model), bf16),
            pltpu.VMEM((2, 256, ff_local), f32),
            pltpu.VMEM((2, 512, d_model), f32),
            pltpu.VMEM((d_model, ff_half), f32),
            pltpu.VMEM((ff_half, d_model), f32),
            pltpu.VMEM((d_model, ff_half), f32),
            pltpu.VMEM((ff_half, d_model), f32),
            pltpu.VMEM((ff_half, d_model), f32),
            pltpu.VMEM((n_row, ff_local), bf16),
            pltpu.VMEM((n_row, ff_local), f32),
            pltpu.VMEM((n_row, ff_local), bf16),
            pltpu.VMEM((2, n_row, half), bf16),
            pltpu.VMEM((n_row, half), f32),
            pltpu.VMEM((n_row, half), f32),
            pltpu.VMEM((n_row, half), bf16),
            pltpu.VMEM((2 * n_row, d_model), bf16),
            pltpu.VMEM((2 * n_row, ff_half), bf16),
            pltpu.VMEM((2 * n_stage, 8, 128), f32),
            pltpu.VMEM((2, 8, 128), f32),
            dma((2, 2)),
            dma((3,)),
            dma(()),
            dma((2,)),
            dma((2, max(len(bounds_up), len(bounds_down)))),
            dma((2,)),
            dma((2,)),
            dma((2,)),
            dma((2, n_chunk)),
            dma((2, n_chunk)),
            dma((2,)),
            dma((2,)),
            dma((2,)),
            dma((2 * n_stage,)),
            dma((2 * n_stage + 1,)),
        ],
        compiler_params=pltpu.CompilerParams(collective_id=0, has_side_effects=True, vmem_limit_bytes=60 << 20),
        name="reduce_and_norm",
    )(g_up, g_down, w_up, w_down, acts, grad_out, max_norm)


def forward_body(n_stage, n_micro, x_ref, up_ref, down_ref, y_ref, inbox, hid, mine, outbox, landed, ready, local_sem, in_sem, part_ssem, part_rsem, pass_ssem, y_ssem, y_rsem):
    model = lax.axis_index('model')
    stage = lax.axis_index('stage')
    mesh_id = pl.DeviceIdType.MESH
    last = n_stage - 1
    half = mine.shape[2]
    barrier = pltpu.get_barrier_semaphore()
    peers = [(dm, ds) for dm in range(2) for ds in range(n_stage) if dm or ds]
    for dm, ds in peers:
        pl.semaphore_signal(barrier, inc=1, device_id={'model': lax.rem(model + dm, 2), 'stage': lax.rem(stage + ds, n_stage)}, device_id_type=mesh_id)

    def load(b, c):
        return pltpu.make_async_copy(x_ref.at[b, :, pl.ds(c * half, half)], inbox.at[b, c], local_sem.at[b, c])

    @pl.when(stage == 0)
    def _():
        for b in range(n_micro):
            for c in range(2):
                load(b, c).start()

    pl.semaphore_wait(barrier, len(peers))

    def arrival(b, c):
        return pltpu.make_async_remote_copy(src_ref=ready.at[b], dst_ref=inbox.at[b, c], send_sem=pass_ssem.at[b, 0], recv_sem=in_sem.at[b, c], device_id={'model': model}, device_id_type=mesh_id)

    def trade(b):
        return pltpu.make_async_remote_copy(src_ref=outbox.at[b], dst_ref=landed.at[b], send_sem=part_ssem.at[b], recv_sem=part_rsem.at[b], device_id={'model': 1 - model}, device_id_type=mesh_id)

    def hand_on(b, to):
        return pltpu.make_async_remote_copy(src_ref=ready.at[b], dst_ref=inbox.at[b, model], send_sem=pass_ssem.at[b, to], recv_sem=in_sem.at[b, model], device_id={'model': to, 'stage': stage + 1}, device_id_type=mesh_id)

    def publish(b, k):
        dm, ds = peers[k]
        return pltpu.make_async_remote_copy(src_ref=ready.at[b], dst_ref=landing(b, model), send_sem=y_ssem.at[b, k], recv_sem=y_rsem.at[b, model], device_id={'model': lax.rem(model + dm, 2), 'stage': lax.rem(stage + ds, n_stage)}, device_id_type=mesh_id)

    def landing(b, c):
        return y_ref.at[b, :, pl.ds(pl.multiple_of(c * half, half), half)]

    def y_arrival(b, c):
        return pltpu.make_async_remote_copy(src_ref=ready.at[b], dst_ref=landing(b, c), send_sem=y_ssem.at[b, 0], recv_sem=y_rsem.at[b, c], device_id={'model': model}, device_id_type=mesh_id)

    def step(b, carry):
        @pl.when(b < n_micro)
        def _():
            @pl.when(stage == 0)
            def _():
                for c in range(2):
                    load(b, c).wait()

            @pl.when(stage > 0)
            def _():
                for c in range(2):
                    arrival(b, c).wait_recv()

            pre = jnp.dot(inbox[b, 0], up_ref[:half], preferred_element_type=jnp.float32)
            pre = pre + jnp.dot(inbox[b, 1], up_ref[half:], preferred_element_type=jnp.float32)
            hid[...] = jax.nn.gelu(pre).astype(jnp.bfloat16)

        @pl.when(b > 0)
        def _():
            p = b - 1
            trade(p).wait_recv()
            total = inbox[p, model].astype(jnp.float32) + (mine[p] + landed[p])
            done = total.astype(jnp.bfloat16)
            ready[p] = done

            @pl.when(stage < last)
            def _():
                for to in range(2):
                    hand_on(p, to).start()

            @pl.when(stage == last)
            def _():
                y_ref[p, :, pl.ds(pl.multiple_of(model * half, half), half)] = done
                for k in range(len(peers)):
                    publish(p, k).start()

        @pl.when(b < n_micro)
        def _():
            far = pl.multiple_of((1 - model) * half, half)
            near = pl.multiple_of(model * half, half)
            outbox[b] = jnp.dot(hid[...], down_ref[:, pl.ds(far, half)], preferred_element_type=jnp.float32)
            trade(b).start()
            mine[b] = jnp.dot(hid[...], down_ref[:, pl.ds(near, half)], preferred_element_type=jnp.float32)

        return carry

    lax.fori_loop(0, n_micro + 1, step, 0)

    for b in range(n_micro):
        trade(b).wait_send()

    @pl.when(stage < last)
    def _():
        for b in range(n_micro):
            for to in range(2):
                hand_on(b, to).wait_send()
            for c in range(2):
                y_arrival(b, c).wait_recv()

    @pl.when(stage == last)
    def _():
        for b in range(n_micro):
            for k in range(len(peers)):
                publish(b, k).wait_send()
            y_arrival(b, 1 - model).wait_recv()


def forward_call(n_stage, x_next, up_bf, down_bf):
    n_micro, rows, d_model = x_next.shape
    ff_local = up_bf.shape[1]
    half = d_model // 2
    dma = pltpu.SemaphoreType.DMA
    in_vmem = pl.BlockSpec(memory_space=pltpu.VMEM)
    return pl.pallas_call(
        functools.partial(forward_body, n_stage, n_micro),
        out_shape=jax.ShapeDtypeStruct(x_next.shape, jnp.bfloat16),
        in_specs=[pl.BlockSpec(memory_space=pl.ANY), in_vmem, in_vmem],
        out_specs=in_vmem,
        scratch_shapes=[
            pltpu.VMEM((n_micro, 2, rows, half), jnp.bfloat16),
            pltpu.VMEM((rows, ff_local), jnp.bfloat16),
            pltpu.VMEM((n_micro, rows, half), jnp.float32),
            pltpu.VMEM((n_micro, rows, half), jnp.float32),
            pltpu.VMEM((n_micro, rows, half), jnp.float32),
            pltpu.VMEM((n_micro, rows, half), jnp.bfloat16),
            dma((n_micro, 2)),
            dma((n_micro, 2)),
            dma((n_micro,)),
            dma((n_micro,)),
            dma((n_micro, 2)),
            dma((n_micro, 2 * n_stage - 1)),
            dma((n_micro, 2)),
        ],
        compiler_params=pltpu.CompilerParams(collective_id=1, has_side_effects=True, vmem_limit_bytes=48 << 20),
        name="forward_pipe",
    )(x_next, up_bf, down_bf)


def solution(mesh):
    n_stage = mesh.shape['stage']
    swap = [(0, 1), (1, 0)]
    up_spec = P('stage', None, 'model')
    down_spec = P('stage', 'model', None)
    row_spec = P(None, 'data', None)
    in_specs = (up_spec, down_spec, up_spec, down_spec, up_spec, down_spec, P('data', 'stage', None, 'model'), P('data', 'stage', 'model', None), P('stage', 'data', None), P('data', None), row_spec, P(None), P(None))
    out_specs = (up_spec, down_spec, up_spec, down_spec, up_spec, down_spec, row_spec)

    def device_step(w_up, w_down, m_up, m_down, v_up, v_down, g_up, g_down, acts_last, grad_out, x_next, learn_rate, max_norm):
        data_id = lax.axis_index('data')
        half = data_id.astype(jnp.int32).reshape(1)
        other = (1 - half).astype(jnp.int32)
        d_model, ff_local = w_up.shape[1:]
        ff_half = ff_local // 2
        bounds_up = ((0, BLOCK), (BLOCK, d_model))
        bounds_down = ((0, ff_half // 2), (ff_half // 2, 3 * ff_half // 4), (3 * ff_half // 4, ff_half))
        n_up = len(bounds_up)

        def trade(value):
            return lax.ppermute(value, 'data', swap)

        *means, far_first, clip = backward_call(n_stage, bounds_up, bounds_down, g_up[0, 0], g_down[0, 0], w_up[0], w_down[0], acts_last[0], grad_out, max_norm)
        fars = [far_first] + [trade(value) for value in means[1:]]
        ups = (w_up[0], m_up[0], v_up[0])
        downs = (w_down[0], m_down[0], v_down[0])
        new_up = new_down = None
        for which, parts in ((half, means), (other, fars)):
            for (low, _), part in zip(bounds_up, parts[:n_up]):
                full_map = lambda i, h, r, base=low // BLOCK: (base + i, h[0])
                new_up = update_call(which, learn_rate, clip, ups, part, full_map, new_up)
            for (low, _), part in zip(bounds_down, parts[n_up:]):
                full_map = lambda i, h, r, base=low // BLOCK, step=ff_half // BLOCK: (h[0] * step + base + i, 0)
                new_down = update_call(which, learn_rate, clip, downs, part, full_map, new_down)

        y_next = forward_call(n_stage, x_next, new_up[3], new_down[3])
        return (new_up[0][None], new_down[0][None], new_up[1][None], new_down[1][None], new_up[2][None], new_down[2][None], y_next)

    return jax.shard_map(device_step, mesh=mesh, in_specs=in_specs, out_specs=out_specs, check_vma=False)
```

```python
import functools

import jax
import jax.numpy as jnp
from jax import lax
from jax.experimental import pallas as pl
from jax.experimental.pallas import tpu as pltpu
from jax.sharding import PartitionSpec as P

ADAM_STEP = 10
BETA_ONE = 0.9
BETA_TWO = 0.95
ADAM_EPS = 1e-8
WEIGHT_DECAY = 0.1
NORM_EPS = 1e-6
CONTRACT_LAST = (((1,), (1,)), ((), ()))
BLOCK = 256
STEP = 128


def update_body(half_ref, rate_ref, clip_ref, w_ref, m_ref, v_ref, g_ref, *refs):
    ow_ref, om_ref, ov_ref, ob_ref = refs[-4:]
    rate = rate_ref[0]
    grad = clip_ref[0:1] * g_ref[...]
    weight = w_ref[...]
    mom = BETA_ONE * m_ref[...] + (1.0 - BETA_ONE) * grad
    sec = BETA_TWO * v_ref[...] + (1.0 - BETA_TWO) * grad * grad
    one_corr = 1.0 - BETA_ONE**ADAM_STEP
    two_corr = 1.0 - BETA_TWO**ADAM_STEP
    direction = (mom * (1.0 / one_corr)) / (jnp.sqrt(sec * (1.0 / two_corr)) + ADAM_EPS)
    new = weight - rate * (direction + WEIGHT_DECAY * weight)
    ow_ref[...] = new
    om_ref[...] = mom
    ov_ref[...] = sec
    ob_ref[...] = new.astype(jnp.bfloat16)


def update_call(half, rate, clip, weights, grad, full_map, previous, after=()):
    rows, cols = grad.shape
    block = min(STEP, rows)
    shape = weights[0].shape
    spec = pl.BlockSpec((block, cols), full_map)
    anywhere = pl.BlockSpec(memory_space=pl.ANY)
    extra = list(previous or ()) + list(after)
    return pl.pallas_call(
        update_body,
        grid_spec=pltpu.PrefetchScalarGridSpec(
            num_scalar_prefetch=2,
            grid=(rows // block,),
            in_specs=[pl.BlockSpec(clip.shape, lambda i, h, r: (0, 0)), spec, spec, spec, pl.BlockSpec((block, cols), lambda i, h, r: (i, 0))] + [anywhere] * len(extra),
            out_specs=[spec] * 4,
        ),
        out_shape=[jax.ShapeDtypeStruct(shape, jnp.float32)] * 3 + [jax.ShapeDtypeStruct(shape, jnp.bfloat16)],
        input_output_aliases={7 + i: i for i in range(len(previous or ()))},
        cost_estimate=pl.CostEstimate(flops=60 * rows * cols, bytes_accessed=30 * rows * cols, transcendentals=0),
        name="adamw_half",
    )(half, rate, clip, *weights, grad, *extra)


def backward_body(n_stage, n_raw, bounds_up, bounds_down, gu_ref, gd_ref, wu_ref, wd_ref, acts_ref, gout_ref, max_ref, *refs):
    n_up, n_down = len(bounds_up) - 1, len(bounds_down)
    outs_up, outs_down = refs[:n_up], refs[n_up:n_up + n_down]
    whole_up, whole_down, far_ref, clip_ref = refs[n_up + n_down:n_up + n_down + 4]
    (up_bf, down_bf, st_up, st_down, acc_up, acc_down, got_up, got_down, fold, hid, slope, grad_pre, gbuf, outbox, landed, ready, rows_a, rows_z, norm_box, norm_pair,
     st_sem, loc_sem, fold_sem, own_sem, out_sem, g_rsem, trade_sem, pass_ssem, rs_ssem, rs_rsem, row_ssem, row_rsem, far_sem, norm_ssem, norm_rsem) = refs[n_up + n_down + 4:]
    model, data, stage = lax.axis_index('model'), lax.axis_index('data'), lax.axis_index('stage')
    mesh_id = pl.DeviceIdType.MESH
    last = n_stage - 1
    d_model, ff_half = acc_up.shape
    half = d_model // 2
    n_row = acts_ref.shape[0]
    n_up_chunk, n_down_chunk = d_model // BLOCK, ff_half // BLOCK
    peer = {'data': 1 - data}
    near = pl.ds(pl.multiple_of(model * half, half), half)
    far = pl.ds(pl.multiple_of((1 - model) * half, half), half)
    own_cols = pl.ds(pl.multiple_of(data * ff_half, ff_half), ff_half)
    peer_cols = pl.ds(pl.multiple_of((1 - data) * ff_half, ff_half), ff_half)
    own_rows = pl.ds(pl.multiple_of(data * n_row, n_row), n_row)
    first_dims = (((0,), (0,)), ((), ()))

    def remote(src, dst, ssem, rsem, where):
        return pltpu.make_async_remote_copy(src_ref=src, dst_ref=dst, send_sem=ssem, recv_sem=rsem, device_id=where, device_id_type=mesh_id)

    barrier = pltpu.get_barrier_semaphore()
    group = [(dm, ds) for dm in range(2) for ds in range(n_stage) if dm or ds]
    where = [{'model': lax.rem(model + dm, 2), 'stage': lax.rem(stage + ds, n_stage)} for dm, ds in group]
    for target in where + [peer]:
        pl.semaphore_signal(barrier, inc=1, device_id=target, device_id_type=mesh_id)

    n_st_up, n_st_down = d_model // st_up.shape[1], 2 * ff_half // st_down.shape[1]

    def load_up(r):
        return pltpu.make_async_copy(wu_ref.at[pl.ds(r * st_up.shape[1], st_up.shape[1])], st_up.at[r % 2], st_sem.at[0, r % 2])

    def load_down(r):
        return pltpu.make_async_copy(wd_ref.at[pl.ds(r * st_down.shape[1], st_down.shape[1])], st_down.at[r % 2], st_sem.at[1, r % 2])

    load_acts = pltpu.make_async_copy(acts_ref, rows_a.at[own_rows], loc_sem.at[0])
    load_acts.start()
    load_up(0).start()
    load_up(1).start()
    load_down(0).start()
    load_down(1).start()

    def load_g(c):
        return pltpu.make_async_copy(gout_ref.at[:, pl.ds(c * half, half)], gbuf.at[c], loc_sem.at[1 + c])

    @pl.when(stage == last)
    def _():
        for c in range(2):
            load_g(c).start()

    pl.semaphore_wait(barrier, len(where) + 1)

    def chunk(k):
        return pl.ds(k * BLOCK, BLOCK)

    raw = [remote(gu_ref.at[chunk(k), peer_cols], got_up.at[chunk(k)], rs_ssem.at[0, k], rs_rsem.at[0, k], peer) for k in range(n_up_chunk)]
    for copy in raw:
        copy.start()
    send_a = remote(acts_ref, rows_a.at[own_rows], row_ssem.at[0], row_rsem.at[0], peer)
    send_a.start()

    for r in range(n_st_up):
        load_up(r).wait()
        up_bf[pl.ds(r * st_up.shape[1], st_up.shape[1])] = st_up[r % 2].astype(jnp.bfloat16)
        if r + 2 < n_st_up:
            load_up(r + 2).start()
    load_acts.wait()

    tile = 256
    n_tile = hid.shape[1] // tile
    scale = 0.7978845608028654
    cubic = 0.044715

    def pre_tile(j, carry):
        cols = pl.ds(pl.multiple_of(j * tile, tile), tile)
        pre = jnp.dot(rows_a[own_rows], up_bf[:, cols], preferred_element_type=jnp.float32)
        square = pre * pre
        bend = jnp.tanh(scale * (pre + cubic * square * pre))
        hid[:, cols] = (pre * (0.5 * (1.0 + bend))).astype(jnp.bfloat16)
        slope[:, cols] = 0.5 * (1.0 + bend) + 0.5 * pre * (1.0 - bend * bend) * (scale * (1.0 + 3.0 * cubic * square))
        return carry

    lax.fori_loop(0, n_tile, pre_tile, 0)

    for r in range(n_st_down):
        load_down(r).wait()
        down_bf[pl.ds(r * st_down.shape[1], st_down.shape[1])] = st_down[r % 2].astype(jnp.bfloat16)
        if r + 2 < n_st_down:
            load_down(r + 2).start()

    own_up = pltpu.make_async_copy(gu_ref.at[:, own_cols], acc_up, own_sem.at[0])
    own_down = pltpu.make_async_copy(gd_ref.at[own_cols], acc_down, own_sem.at[1])
    load_fold = pltpu.make_async_copy(gd_ref.at[peer_cols], fold, fold_sem)
    load_fold.start()
    own_up.start()
    own_down.start()

    @pl.when(stage == last)
    def _():
        for c in range(2):
            load_g(c).wait()

    @pl.when(stage < last)
    def _():
        for c in range(2):
            remote(ready, gbuf.at[c], pass_ssem.at[0], g_rsem.at[c], {'model': model}).wait_recv()

    def slope_tile(j, carry):
        cols = pl.ds(pl.multiple_of(j * tile, tile), tile)
        grad = lax.dot_general(gbuf[0], down_bf[cols, :half], CONTRACT_LAST, preferred_element_type=jnp.float32)
        grad = grad + lax.dot_general(gbuf[1], down_bf[cols, half:], CONTRACT_LAST, preferred_element_type=jnp.float32)
        grad_pre[:, cols] = (slope[:, cols] * grad).astype(jnp.bfloat16)
        return carry

    lax.fori_loop(0, n_tile, slope_tile, 0)

    trade = remote(outbox, landed, trade_sem.at[0], trade_sem.at[1], {'model': 1 - model})

    def hand_on(to):
        return remote(ready, gbuf.at[model], pass_ssem.at[to], g_rsem.at[model], {'model': to, 'stage': stage - 1})

    @pl.when(stage > 0)
    def _():
        outbox[...] = lax.dot_general(grad_pre[...], up_bf[far], CONTRACT_LAST, preferred_element_type=jnp.float32)
        trade.start()
        mine = lax.dot_general(grad_pre[...], up_bf[near], CONTRACT_LAST, preferred_element_type=jnp.float32)
        trade.wait_recv()
        ready[...] = (gbuf[model].astype(jnp.float32) + (mine + landed[...])).astype(jnp.bfloat16)
        for to in range(2):
            hand_on(to).start()

    rows_z[own_rows] = grad_pre[:, own_cols]
    send_z = remote(grad_pre.at[:, peer_cols], rows_z.at[own_rows], row_ssem.at[1], row_rsem.at[1], peer)
    send_z.start()

    def down_product(k, side):
        cols = pl.ds(pl.multiple_of(side * ff_half + k * BLOCK, BLOCK), BLOCK)
        left = hid[:, cols]
        return [lax.dot_general(left, gbuf[c], first_dims, preferred_element_type=jnp.float32) for c in range(2)]

    load_fold.wait()

    def send_fold(k):
        rows = pl.ds(pl.multiple_of(k * BLOCK, BLOCK), BLOCK)
        return remote(fold.at[rows], got_down.at[rows], rs_ssem.at[1, k], rs_rsem.at[1, k], peer)

    def fold_step(k, carry):
        rows = pl.ds(pl.multiple_of(k * BLOCK, BLOCK), BLOCK)
        low, high = down_product(k, 1 - data)
        fold[rows, :half] += low
        fold[rows, half:] += high
        send_fold(k).start()
        return carry

    lax.fori_loop(0, n_down_chunk, fold_step, 0)
    own_down.wait()

    def own_step(k, carry):
        rows = pl.ds(pl.multiple_of(k * BLOCK, BLOCK), BLOCK)
        low, high = down_product(k, data)
        acc_down[rows, :half] += low
        acc_down[rows, half:] += high
        return carry

    lax.fori_loop(0, n_down_chunk, own_step, 0)

    @pl.when(stage > 0)
    def _():
        trade.wait_send()
        for to in range(2):
            hand_on(to).wait_send()

    own_up.wait()
    send_a.wait_recv()
    squares = jnp.zeros((8, ff_half), jnp.float32)

    def fold_squares(mean):
        return jnp.sum((mean * mean).reshape(-1, 8, mean.shape[1]), axis=0)

    def put(acc, bounds, outs, whole, sem_row):
        copies = []
        for i, (lo, hi) in enumerate(bounds):
            rows = pl.ds(lo, hi - lo)
            copies.append(pltpu.make_async_copy(acc.at[rows], whole.at[rows], out_sem.at[sem_row, 2 * i]))
            if outs[i] is not None:
                copies.append(pltpu.make_async_copy(acc.at[rows], outs[i], out_sem.at[sem_row, 2 * i + 1]))
        return copies

    def put_start(k, bounds, copies, outs):
        at = 0
        for i, (lo, hi) in enumerate(bounds):
            count = 1 if outs[i] is None else 2
            if hi == (k + 1) * BLOCK:
                for copy in copies[at:at + count]:
                    copy.start()
            at += count

    outs_up = (None,) + tuple(outs_up)
    put_up = put(acc_up, bounds_up, outs_up, whole_up, 0)
    put_down = put(acc_down, bounds_down, outs_down, whole_down, 1)
    for k in range(n_up_chunk):
        raw[k].wait_recv()
        if k == 0:
            send_z.wait_recv()
        product = lax.dot_general(rows_a[:, k * BLOCK:(k + 1) * BLOCK], rows_z[...], first_dims, preferred_element_type=jnp.float32)
        mean = (acc_up[chunk(k)] + got_up[chunk(k)] + product) * 0.5
        acc_up[chunk(k)] = mean
        squares = squares + fold_squares(mean)
        put_start(k, bounds_up, put_up, outs_up)
    first = bounds_up[0][1]
    send_far = remote(acc_up.at[pl.ds(0, first)], far_ref, far_sem.at[0], far_sem.at[1], peer)
    send_far.start()
    for k in range(n_down_chunk):
        send_fold(k).wait_recv()
        mean = (acc_down[chunk(k)] + got_down[chunk(k)]) * 0.5
        acc_down[chunk(k)] = mean
        squares = squares + fold_squares(mean)
        put_start(k, bounds_down, put_down, outs_down)

    lanes = norm_box.shape[2]
    part = squares[:, :lanes]
    for j in range(1, ff_half // lanes):
        part = part + squares[:, j * lanes:(j + 1) * lanes]
    me = model * n_stage + stage
    norm_box[me] = part

    def spread(i):
        return remote(norm_box.at[me], norm_box.at[me], norm_ssem.at[i], norm_rsem.at[me], where[i])

    for i in range(len(group)):
        spread(i).start()
    for i, (dm, ds) in enumerate(group):
        them = lax.rem(model + dm, 2) * n_stage + lax.rem(stage + ds, n_stage)
        remote(norm_box.at[me], norm_box.at[them], norm_ssem.at[i], norm_rsem.at[them], where[i]).wait_recv()
    total = norm_box[0]
    for i in range(1, 2 * n_stage):
        total = total + norm_box[i]
    norm_pair[0] = total
    swap = remote(norm_pair.at[0], norm_pair.at[1], norm_ssem.at[len(group)], norm_rsem.at[2 * n_stage], peer)
    swap.start()
    swap.wait_recv()
    norm_sq = jnp.sum(norm_pair[0] + norm_pair[1], axis=(0, 1), keepdims=True)
    norm = jnp.sqrt(jnp.broadcast_to(norm_sq, clip_ref.shape)) + NORM_EPS
    clip_ref[...] = jnp.minimum(1.0, max_ref[0] / norm)

    swap.wait_send()
    for i in range(len(group)):
        spread(i).wait_send()
    for copy in raw + [send_a, send_z]:
        copy.wait_send()
    for k in range(n_down_chunk):
        send_fold(k).wait_send()
    for copy in put_up + put_down:
        copy.wait()
    send_far.wait()


def backward_call(n_stage, bounds_up, bounds_down, g_up, g_down, w_up, w_down, acts, grad_out, max_norm):
    d_model, ff_local = g_up.shape
    ff_half, half, n_row = ff_local // 2, d_model // 2, acts.shape[0]
    dma = pltpu.SemaphoreType.DMA
    anywhere = pl.BlockSpec(memory_space=pl.ANY)
    f32, bf16 = jnp.float32, jnp.bfloat16
    shapes = [jax.ShapeDtypeStruct((hi - lo, ff_half), f32) for lo, hi in bounds_up[1:]]
    shapes += [jax.ShapeDtypeStruct((hi - lo, d_model), f32) for lo, hi in bounds_down]
    shapes += [jax.ShapeDtypeStruct((d_model, ff_half), f32), jax.ShapeDtypeStruct((ff_half, d_model), f32)]
    shapes += [jax.ShapeDtypeStruct((bounds_up[0][1], ff_half), f32), jax.ShapeDtypeStruct((8, ff_half), f32)]
    n_chunk = max(d_model, ff_half) // BLOCK
    return pl.pallas_call(
        functools.partial(backward_body, n_stage, n_chunk, bounds_up, bounds_down),
        out_shape=shapes,
        in_specs=[anywhere] * 6 + [pl.BlockSpec(memory_space=pltpu.SMEM)],
        out_specs=[anywhere] * (len(shapes) - 1) + [pl.BlockSpec(memory_space=pltpu.VMEM)],
        scratch_shapes=[
            pltpu.VMEM((d_model, ff_local), bf16),
            pltpu.VMEM((ff_local, d_model), bf16),
            pltpu.VMEM((2, 256, ff_local), f32),
            pltpu.VMEM((2, 512, d_model), f32),
            pltpu.VMEM((d_model, ff_half), f32),
            pltpu.VMEM((ff_half, d_model), f32),
            pltpu.VMEM((d_model, ff_half), f32),
            pltpu.VMEM((ff_half, d_model), f32),
            pltpu.VMEM((ff_half, d_model), f32),
            pltpu.VMEM((n_row, ff_local), bf16),
            pltpu.VMEM((n_row, ff_local), f32),
            pltpu.VMEM((n_row, ff_local), bf16),
            pltpu.VMEM((2, n_row, half), bf16),
            pltpu.VMEM((n_row, half), f32),
            pltpu.VMEM((n_row, half), f32),
            pltpu.VMEM((n_row, half), bf16),
            pltpu.VMEM((2 * n_row, d_model), bf16),
            pltpu.VMEM((2 * n_row, ff_half), bf16),
            pltpu.VMEM((2 * n_stage, 8, 128), f32),
            pltpu.VMEM((2, 8, 128), f32),
            dma((2, 2)),
            dma((3,)),
            dma(()),
            dma((2,)),
            dma((2, 2 * max(len(bounds_up), len(bounds_down)))),
            dma((2,)),
            dma((2,)),
            dma((2,)),
            dma((2, n_chunk)),
            dma((2, n_chunk)),
            dma((2,)),
            dma((2,)),
            dma((2,)),
            dma((2 * n_stage,)),
            dma((2 * n_stage + 1,)),
        ],
        compiler_params=pltpu.CompilerParams(collective_id=0, has_side_effects=True, vmem_limit_bytes=60 << 20),
        name="reduce_and_norm",
    )(g_up, g_down, w_up, w_down, acts, grad_out, max_norm)


def forward_body(n_stage, n_micro, x_ref, up_ref, down_ref, y_ref, inbox, hid, mine, outbox, landed, ready, local_sem, in_sem, part_ssem, part_rsem, pass_ssem, y_ssem, y_rsem):
    model = lax.axis_index('model')
    stage = lax.axis_index('stage')
    mesh_id = pl.DeviceIdType.MESH
    last = n_stage - 1
    half = mine.shape[2]
    barrier = pltpu.get_barrier_semaphore()
    peers = [(dm, ds) for dm in range(2) for ds in range(n_stage) if dm or ds]
    for dm, ds in peers:
        pl.semaphore_signal(barrier, inc=1, device_id={'model': lax.rem(model + dm, 2), 'stage': lax.rem(stage + ds, n_stage)}, device_id_type=mesh_id)

    def load(b, c):
        return pltpu.make_async_copy(x_ref.at[b, :, pl.ds(c * half, half)], inbox.at[b, c], local_sem.at[b, c])

    @pl.when(stage == 0)
    def _():
        for b in range(n_micro):
            for c in range(2):
                load(b, c).start()

    pl.semaphore_wait(barrier, len(peers))

    def arrival(b, c):
        return pltpu.make_async_remote_copy(src_ref=ready.at[b], dst_ref=inbox.at[b, c], send_sem=pass_ssem.at[b, 0], recv_sem=in_sem.at[b, c], device_id={'model': model}, device_id_type=mesh_id)

    def trade(b):
        return pltpu.make_async_remote_copy(src_ref=outbox.at[b], dst_ref=landed.at[b], send_sem=part_ssem.at[b], recv_sem=part_rsem.at[b], device_id={'model': 1 - model}, device_id_type=mesh_id)

    def hand_on(b, to):
        return pltpu.make_async_remote_copy(src_ref=ready.at[b], dst_ref=inbox.at[b, model], send_sem=pass_ssem.at[b, to], recv_sem=in_sem.at[b, model], device_id={'model': to, 'stage': stage + 1}, device_id_type=mesh_id)

    def publish(b, k):
        dm, ds = peers[k]
        return pltpu.make_async_remote_copy(src_ref=ready.at[b], dst_ref=landing(b, model), send_sem=y_ssem.at[b, k], recv_sem=y_rsem.at[b, model], device_id={'model': lax.rem(model + dm, 2), 'stage': lax.rem(stage + ds, n_stage)}, device_id_type=mesh_id)

    def landing(b, c):
        return y_ref.at[b, :, pl.ds(pl.multiple_of(c * half, half), half)]

    def y_arrival(b, c):
        return pltpu.make_async_remote_copy(src_ref=ready.at[b], dst_ref=landing(b, c), send_sem=y_ssem.at[b, 0], recv_sem=y_rsem.at[b, c], device_id={'model': model}, device_id_type=mesh_id)

    def step(b, carry):
        @pl.when(b < n_micro)
        def _():
            @pl.when(stage == 0)
            def _():
                for c in range(2):
                    load(b, c).wait()

            @pl.when(stage > 0)
            def _():
                for c in range(2):
                    arrival(b, c).wait_recv()

            pre = jnp.dot(inbox[b, 0], up_ref[:half], preferred_element_type=jnp.float32)
            pre = pre + jnp.dot(inbox[b, 1], up_ref[half:], preferred_element_type=jnp.float32)
            hid[...] = jax.nn.gelu(pre).astype(jnp.bfloat16)

        @pl.when(b > 0)
        def _():
            p = b - 1
            trade(p).wait_recv()
            total = inbox[p, model].astype(jnp.float32) + (mine[p] + landed[p])
            done = total.astype(jnp.bfloat16)
            ready[p] = done

            @pl.when(stage < last)
            def _():
                for to in range(2):
                    hand_on(p, to).start()

            @pl.when(stage == last)
            def _():
                y_ref[p, :, pl.ds(pl.multiple_of(model * half, half), half)] = done
                for k in range(len(peers)):
                    publish(p, k).start()

        @pl.when(b < n_micro)
        def _():
            far = pl.multiple_of((1 - model) * half, half)
            near = pl.multiple_of(model * half, half)
            outbox[b] = jnp.dot(hid[...], down_ref[:, pl.ds(far, half)], preferred_element_type=jnp.float32)
            trade(b).start()
            mine[b] = jnp.dot(hid[...], down_ref[:, pl.ds(near, half)], preferred_element_type=jnp.float32)

        return carry

    lax.fori_loop(0, n_micro + 1, step, 0)

    for b in range(n_micro):
        trade(b).wait_send()

    @pl.when(stage < last)
    def _():
        for b in range(n_micro):
            for to in range(2):
                hand_on(b, to).wait_send()
            for c in range(2):
                y_arrival(b, c).wait_recv()

    @pl.when(stage == last)
    def _():
        for b in range(n_micro):
            for k in range(len(peers)):
                publish(b, k).wait_send()
            y_arrival(b, 1 - model).wait_recv()


def forward_call(n_stage, x_next, up_bf, down_bf):
    n_micro, rows, d_model = x_next.shape
    ff_local = up_bf.shape[1]
    half = d_model // 2
    dma = pltpu.SemaphoreType.DMA
    in_vmem = pl.BlockSpec(memory_space=pltpu.VMEM)
    return pl.pallas_call(
        functools.partial(forward_body, n_stage, n_micro),
        out_shape=jax.ShapeDtypeStruct(x_next.shape, jnp.bfloat16),
        in_specs=[pl.BlockSpec(memory_space=pl.ANY), in_vmem, in_vmem],
        out_specs=in_vmem,
        scratch_shapes=[
            pltpu.VMEM((n_micro, 2, rows, half), jnp.bfloat16),
            pltpu.VMEM((rows, ff_local), jnp.bfloat16),
            pltpu.VMEM((n_micro, rows, half), jnp.float32),
            pltpu.VMEM((n_micro, rows, half), jnp.float32),
            pltpu.VMEM((n_micro, rows, half), jnp.float32),
            pltpu.VMEM((n_micro, rows, half), jnp.bfloat16),
            dma((n_micro, 2)),
            dma((n_micro, 2)),
            dma((n_micro,)),
            dma((n_micro,)),
            dma((n_micro, 2)),
            dma((n_micro, 2 * n_stage - 1)),
            dma((n_micro, 2)),
        ],
        compiler_params=pltpu.CompilerParams(collective_id=1, has_side_effects=True, vmem_limit_bytes=48 << 20),
        name="forward_pipe",
    )(x_next, up_bf, down_bf)


def solution(mesh):
    n_stage = mesh.shape['stage']
    swap = [(0, 1), (1, 0)]
    up_spec = P('stage', None, 'model')
    down_spec = P('stage', 'model', None)
    row_spec = P(None, 'data', None)
    in_specs = (up_spec, down_spec, up_spec, down_spec, up_spec, down_spec, P('data', 'stage', None, 'model'), P('data', 'stage', 'model', None), P('stage', 'data', None), P('data', None), row_spec, P(None), P(None))
    out_specs = (up_spec, down_spec, up_spec, down_spec, up_spec, down_spec, row_spec)

    def device_step(w_up, w_down, m_up, m_down, v_up, v_down, g_up, g_down, acts_last, grad_out, x_next, learn_rate, max_norm):
        data_id = lax.axis_index('data')
        half = data_id.astype(jnp.int32).reshape(1)
        other = (1 - half).astype(jnp.int32)
        d_model, ff_local = w_up.shape[1:]
        ff_half = ff_local // 2
        bounds_up = ((0, BLOCK), (BLOCK, d_model))
        bounds_down = ((0, ff_half // 2), (ff_half // 2, 3 * ff_half // 4), (3 * ff_half // 4, ff_half))
        n_up = len(bounds_up)

        def trade(value):
            return lax.ppermute(value, 'data', swap)

        *parts, whole_up, whole_down, far_first, clip = backward_call(n_stage, bounds_up, bounds_down, g_up[0, 0], g_down[0, 0], w_up[0], w_down[0], acts_last[0], grad_out, max_norm)
        fars = [far_first] + [trade(value) for value in parts]
        ups = (w_up[0], m_up[0], v_up[0])
        downs = (w_down[0], m_down[0], v_down[0])

        def map_up(low):
            return lambda i, h, r: (low // STEP + i, h[0])

        def map_down(low):
            return lambda i, h, r: ((h[0] * ff_half + low) // STEP + i, 0)

        new_up = update_call(half, learn_rate, clip, ups, whole_up, map_up(0), None)
        new_down = update_call(half, learn_rate, clip, downs, whole_down, map_down(0), None, (new_up[3],))
        after = (new_down[3],)
        for (low, _), part in zip(bounds_up, fars[:n_up]):
            new_up = update_call(other, learn_rate, clip, ups, part, map_up(low), new_up, after)
            after = ()
        after = (new_up[3],)
        for (low, _), part in zip(bounds_down, fars[n_up:]):
            new_down = update_call(other, learn_rate, clip, downs, part, map_down(low), new_down, after)
            after = ()
        y_next = forward_call(n_stage, x_next, new_up[3], new_down[3])
        return (new_up[0][None], new_down[0][None], new_up[1][None], new_down[1][None], new_up[2][None], new_down[2][None], y_next)

    return jax.shard_map(device_step, mesh=mesh, in_specs=in_specs, out_specs=out_specs, check_vma=False)
```

```python
import functools

import jax
import jax.numpy as jnp
from jax import lax
from jax.experimental import pallas as pl
from jax.experimental.pallas import tpu as pltpu
from jax.sharding import PartitionSpec as P

ADAM_STEP = 10
BETA_ONE = 0.9
BETA_TWO = 0.95
ADAM_EPS = 1e-8
WEIGHT_DECAY = 0.1
NORM_EPS = 1e-6
CONTRACT_LAST = (((1,), (1,)), ((), ()))
BLOCK = 128
STEP = 128
N_GROUP = 8
N_PIECE = 32
LEAD = (2, 7)


def update_body(skip, half_ref, rate_ref, clip_ref, w_ref, m_ref, v_ref, g_ref, *refs):
    outs = refs[skip:]
    ow_ref, om_ref, ov_ref = outs[:3]
    rate = rate_ref[0]
    grad = clip_ref[0:1] * g_ref[...]
    weight = w_ref[...]
    mom = BETA_ONE * m_ref[...] + (1.0 - BETA_ONE) * grad
    sec = BETA_TWO * v_ref[...] + (1.0 - BETA_TWO) * grad * grad
    one_corr = 1.0 - BETA_ONE**ADAM_STEP
    two_corr = 1.0 - BETA_TWO**ADAM_STEP
    direction = (mom * (1.0 / one_corr)) / (jnp.sqrt(sec * (1.0 / two_corr)) + ADAM_EPS)
    new = weight - rate * (direction + WEIGHT_DECAY * weight)
    ow_ref[...] = new
    om_ref[...] = mom
    ov_ref[...] = sec
    if len(outs) == 4:
        outs[3][...] = new.astype(jnp.bfloat16)


def update_call(half, rate, clip, weights, grad, full_map, previous, after=()):
    rows, cols = grad.shape
    block = min(STEP, rows)
    shape = weights[0].shape
    spec = pl.BlockSpec((block, cols), full_map)
    flat = pl.BlockSpec((block, cols), lambda i, h, r: (i, 0))
    anywhere = pl.BlockSpec(memory_space=pl.ANY)
    first = previous is None
    extra = list(previous or ()) + list(after)
    return pl.pallas_call(
        functools.partial(update_body, len(extra)),
        grid_spec=pltpu.PrefetchScalarGridSpec(
            num_scalar_prefetch=2,
            grid=(rows // block,),
            in_specs=[pl.BlockSpec(clip.shape, lambda i, h, r: (0, 0)), spec, spec, spec, flat] + [anywhere] * len(extra),
            out_specs=[spec] * 3 + [flat] * first,
        ),
        out_shape=[jax.ShapeDtypeStruct(shape, jnp.float32)] * 3 + [jax.ShapeDtypeStruct(grad.shape, jnp.bfloat16)] * first,
        input_output_aliases={7 + i: i for i in range(len(previous or ()))},
        cost_estimate=pl.CostEstimate(flops=60 * rows * cols, bytes_accessed=30 * rows * cols, transcendentals=0),
        name="adamw_half",
    )(half, rate, clip, *weights, grad, *extra)


def backward_body(n_stage, n_raw, bounds_up, bounds_down, gu_ref, gd_ref, wu_ref, wd_ref, acts_ref, gout_ref, max_ref, *refs):
    n_up = len(bounds_up) - 1
    outs_up = refs[:n_up]
    whole_up, whole_down, far_ref, clip_ref = refs[n_up:n_up + 4]
    (up_bf, down_bf, st_up, st_down, acc_up, acc_down, got_up, got_down, fold, hid, slope, grad_pre, gbuf, outbox, landed, ready, rows_a, rows_z, norm_box, norm_pair,
     st_sem, loc_sem, fold_sem, own_sem, out_sem, g_rsem, trade_sem, pass_ssem, rs_ssem, rs_rsem, row_ssem, row_rsem, far_sem, norm_ssem, norm_rsem) = refs[n_up + 4:]
    model, data, stage = lax.axis_index('model'), lax.axis_index('data'), lax.axis_index('stage')
    mesh_id = pl.DeviceIdType.MESH
    last = n_stage - 1
    d_model, ff_half = acc_up.shape
    half = d_model // 2
    n_row = acts_ref.shape[0]
    n_up_chunk, n_down_chunk = d_model // BLOCK, ff_half // BLOCK
    peer = {'data': 1 - data}
    near = pl.ds(pl.multiple_of(model * half, half), half)
    far = pl.ds(pl.multiple_of((1 - model) * half, half), half)
    own_cols = pl.ds(pl.multiple_of(data * ff_half, ff_half), ff_half)
    peer_cols = pl.ds(pl.multiple_of((1 - data) * ff_half, ff_half), ff_half)
    own_rows = pl.ds(pl.multiple_of(data * n_row, n_row), n_row)
    first_dims = (((0,), (0,)), ((), ()))

    def remote(src, dst, ssem, rsem, where):
        return pltpu.make_async_remote_copy(src_ref=src, dst_ref=dst, send_sem=ssem, recv_sem=rsem, device_id=where, device_id_type=mesh_id)

    barrier = pltpu.get_barrier_semaphore()
    group = [(dm, ds) for dm in range(2) for ds in range(n_stage) if dm or ds]
    where = [{'model': lax.rem(model + dm, 2), 'stage': lax.rem(stage + ds, n_stage)} for dm, ds in group]
    for target in where + [peer]:
        pl.semaphore_signal(barrier, inc=1, device_id=target, device_id_type=mesh_id)

    n_st_up, n_st_down = d_model // st_up.shape[1], 2 * ff_half // st_down.shape[1]

    def load_up(r):
        return pltpu.make_async_copy(wu_ref.at[pl.ds(r * st_up.shape[1], st_up.shape[1])], st_up.at[r % 2], st_sem.at[0, r % 2])

    def load_down(r):
        return pltpu.make_async_copy(wd_ref.at[pl.ds(r * st_down.shape[1], st_down.shape[1])], st_down.at[r % 2], st_sem.at[1, r % 2])

    load_acts = pltpu.make_async_copy(acts_ref, rows_a.at[own_rows], loc_sem.at[0])
    load_acts.start()
    load_up(0).start()
    load_up(1).start()
    load_down(0).start()
    load_down(1).start()

    def load_g(c):
        return pltpu.make_async_copy(gout_ref.at[:, pl.ds(c * half, half)], gbuf.at[c], loc_sem.at[1 + c])

    @pl.when(stage == last)
    def _():
        for c in range(2):
            load_g(c).start()

    pl.semaphore_wait(barrier, len(where) + 1)

    def chunk(k):
        return pl.ds(k * BLOCK, BLOCK)

    raw = [remote(gu_ref.at[chunk(k), peer_cols], got_up.at[chunk(k)], rs_ssem.at[0, k], rs_rsem.at[0, k], peer) for k in range(n_up_chunk)]
    for copy in raw:
        copy.start()
    send_a = remote(acts_ref, rows_a.at[own_rows], row_ssem.at[0], row_rsem.at[0], peer)
    send_a.start()

    for r in range(n_st_up):
        load_up(r).wait()
        up_bf[pl.ds(r * st_up.shape[1], st_up.shape[1])] = st_up[r % 2].astype(jnp.bfloat16)
        if r + 2 < n_st_up:
            load_up(r + 2).start()
    load_acts.wait()

    tile = 256
    n_tile = hid.shape[1] // tile
    scale = 0.7978845608028654
    cubic = 0.044715

    def pre_tile(j, carry):
        cols = pl.ds(pl.multiple_of(j * tile, tile), tile)
        pre = jnp.dot(rows_a[own_rows], up_bf[:, cols], preferred_element_type=jnp.float32)
        square = pre * pre
        bend = jnp.tanh(scale * (pre + cubic * square * pre))
        hid[:, cols] = (pre * (0.5 * (1.0 + bend))).astype(jnp.bfloat16)
        slope[:, cols] = 0.5 * (1.0 + bend) + 0.5 * pre * (1.0 - bend * bend) * (scale * (1.0 + 3.0 * cubic * square))
        return carry

    lax.fori_loop(0, n_tile, pre_tile, 0)

    for r in range(n_st_down):
        load_down(r).wait()
        down_bf[pl.ds(r * st_down.shape[1], st_down.shape[1])] = st_down[r % 2].astype(jnp.bfloat16)
        if r + 2 < n_st_down:
            load_down(r + 2).start()

    own_up = pltpu.make_async_copy(gu_ref.at[:, own_cols], acc_up, own_sem.at[0])
    own_down = pltpu.make_async_copy(gd_ref.at[own_cols], acc_down, own_sem.at[1])
    load_fold = pltpu.make_async_copy(gd_ref.at[peer_cols], fold, fold_sem)
    load_fold.start()
    own_up.start()
    own_down.start()

    @pl.when(stage == last)
    def _():
        for c in range(2):
            load_g(c).wait()

    @pl.when(stage < last)
    def _():
        for c in range(2):
            remote(ready, gbuf.at[c], pass_ssem.at[0], g_rsem.at[c], {'model': model}).wait_recv()

    def slope_tile(j, carry):
        cols = pl.ds(pl.multiple_of(j * tile, tile), tile)
        grad = lax.dot_general(gbuf[0], down_bf[cols, :half], CONTRACT_LAST, preferred_element_type=jnp.float32)
        grad = grad + lax.dot_general(gbuf[1], down_bf[cols, half:], CONTRACT_LAST, preferred_element_type=jnp.float32)
        grad_pre[:, cols] = (slope[:, cols] * grad).astype(jnp.bfloat16)
        return carry

    lax.fori_loop(0, n_tile, slope_tile, 0)

    trade = remote(outbox, landed, trade_sem.at[0], trade_sem.at[1], {'model': 1 - model})

    def hand_on(to):
        return remote(ready, gbuf.at[model], pass_ssem.at[to], g_rsem.at[model], {'model': to, 'stage': stage - 1})

    @pl.when(stage > 0)
    def _():
        outbox[...] = lax.dot_general(grad_pre[...], up_bf[far], CONTRACT_LAST, preferred_element_type=jnp.float32)
        trade.start()
        mine = lax.dot_general(grad_pre[...], up_bf[near], CONTRACT_LAST, preferred_element_type=jnp.float32)
        trade.wait_recv()
        ready[...] = (gbuf[model].astype(jnp.float32) + (mine + landed[...])).astype(jnp.bfloat16)
        for to in range(2):
            hand_on(to).start()

    rows_z[own_rows] = grad_pre[:, own_cols]
    send_z = remote(grad_pre.at[:, peer_cols], rows_z.at[own_rows], row_ssem.at[1], row_rsem.at[1], peer)
    send_z.start()

    def down_product(k, side):
        cols = pl.ds(pl.multiple_of(side * ff_half + k * BLOCK, BLOCK), BLOCK)
        left = hid[:, cols]
        return [lax.dot_general(left, gbuf[c], first_dims, preferred_element_type=jnp.float32) for c in range(2)]

    load_fold.wait()

    def send_fold(k):
        rows = pl.ds(pl.multiple_of(k * BLOCK, BLOCK), BLOCK)
        return remote(fold.at[rows], got_down.at[rows], rs_ssem.at[1, k], rs_rsem.at[1, k], peer)

    def fold_step(k, carry):
        rows = pl.ds(pl.multiple_of(k * BLOCK, BLOCK), BLOCK)
        low, high = down_product(k, 1 - data)
        fold[rows, :half] += low
        fold[rows, half:] += high
        send_fold(k).start()
        return carry

    lax.fori_loop(0, n_down_chunk, fold_step, 0)
    own_down.wait()

    def own_step(k, carry):
        rows = pl.ds(pl.multiple_of(k * BLOCK, BLOCK), BLOCK)
        low, high = down_product(k, data)
        acc_down[rows, :half] += low
        acc_down[rows, half:] += high
        return carry

    lax.fori_loop(0, n_down_chunk, own_step, 0)

    @pl.when(stage > 0)
    def _():
        trade.wait_send()
        for to in range(2):
            hand_on(to).wait_send()

    own_up.wait()
    send_a.wait_recv()
    squares = jnp.zeros((8, ff_half), jnp.float32)

    def fold_squares(mean):
        return jnp.sum((mean * mean).reshape(-1, 8, mean.shape[1]), axis=0)

    def put(acc, bounds, outs, whole, sem_row):
        copies = []
        for i, (lo, hi) in enumerate(bounds):
            rows = pl.ds(lo, hi - lo)
            copies.append(pltpu.make_async_copy(acc.at[rows], whole.at[rows], out_sem.at[sem_row, i]))
            if outs[i] is not None:
                copies.append(pltpu.make_async_copy(acc.at[rows], outs[i], out_sem.at[sem_row, len(bounds) + i]))
        return copies

    def put_start(k, bounds, copies, outs):
        at = 0
        for i, (lo, hi) in enumerate(bounds):
            count = 1 if outs[i] is None else 2
            if hi == (k + 1) * BLOCK:
                for copy in copies[at:at + count]:
                    copy.start()
            at += count

    outs_up = (None,) + tuple(outs_up)
    outs_down = (None,) * len(bounds_down)
    put_up = put(acc_up, bounds_up, outs_up, whole_up, 0)
    put_down = put(acc_down, bounds_down, outs_down, whole_down, 1)
    for k in range(n_up_chunk):
        raw[k].wait_recv()
        if k == 0:
            send_z.wait_recv()
        product = lax.dot_general(rows_a[:, k * BLOCK:(k + 1) * BLOCK], rows_z[...], first_dims, preferred_element_type=jnp.float32)
        mean = (acc_up[chunk(k)] + got_up[chunk(k)] + product) * 0.5
        acc_up[chunk(k)] = mean
        squares = squares + fold_squares(mean)
        put_start(k, bounds_up, put_up, outs_up)
    first = bounds_up[0][1]
    send_far = remote(acc_up.at[pl.ds(0, first)], far_ref, far_sem.at[0], far_sem.at[1], peer)
    send_far.start()
    for k in range(n_down_chunk):
        send_fold(k).wait_recv()
        mean = (acc_down[chunk(k)] + got_down[chunk(k)]) * 0.5
        acc_down[chunk(k)] = mean
        squares = squares + fold_squares(mean)
        put_start(k, bounds_down, put_down, outs_down)

    lanes = norm_box.shape[2]
    part = squares[:, :lanes]
    for j in range(1, ff_half // lanes):
        part = part + squares[:, j * lanes:(j + 1) * lanes]
    me = model * n_stage + stage
    norm_box[me] = part

    def spread(i):
        return remote(norm_box.at[me], norm_box.at[me], norm_ssem.at[i], norm_rsem.at[me], where[i])

    for i in range(len(group)):
        spread(i).start()
    for i, (dm, ds) in enumerate(group):
        them = lax.rem(model + dm, 2) * n_stage + lax.rem(stage + ds, n_stage)
        remote(norm_box.at[me], norm_box.at[them], norm_ssem.at[i], norm_rsem.at[them], where[i]).wait_recv()
    total = norm_box[0]
    for i in range(1, 2 * n_stage):
        total = total + norm_box[i]
    norm_pair[0] = total
    swap = remote(norm_pair.at[0], norm_pair.at[1], norm_ssem.at[len(group)], norm_rsem.at[2 * n_stage], peer)
    swap.start()
    swap.wait_recv()
    norm_sq = jnp.sum(norm_pair[0] + norm_pair[1], axis=(0, 1), keepdims=True)
    norm = jnp.sqrt(jnp.broadcast_to(norm_sq, clip_ref.shape)) + NORM_EPS
    clip_ref[...] = jnp.minimum(1.0, max_ref[0] / norm)

    swap.wait_send()
    for i in range(len(group)):
        spread(i).wait_send()
    for copy in raw + [send_a, send_z]:
        copy.wait_send()
    for k in range(n_down_chunk):
        send_fold(k).wait_send()
    for copy in put_up + put_down:
        copy.wait()
    send_far.wait()


def backward_call(n_stage, bounds_up, bounds_down, g_up, g_down, w_up, w_down, acts, grad_out, max_norm):
    d_model, ff_local = g_up.shape
    ff_half, half, n_row = ff_local // 2, d_model // 2, acts.shape[0]
    dma = pltpu.SemaphoreType.DMA
    anywhere = pl.BlockSpec(memory_space=pl.ANY)
    f32, bf16 = jnp.float32, jnp.bfloat16
    shapes = [jax.ShapeDtypeStruct((hi - lo, ff_half), f32) for lo, hi in bounds_up[1:]]
    shapes += [jax.ShapeDtypeStruct((d_model, ff_half), f32), jax.ShapeDtypeStruct((ff_half, d_model), f32)]
    shapes += [jax.ShapeDtypeStruct((bounds_up[0][1], ff_half), f32), jax.ShapeDtypeStruct((8, ff_half), f32)]
    n_chunk = max(d_model, ff_half) // BLOCK
    return pl.pallas_call(
        functools.partial(backward_body, n_stage, n_chunk, bounds_up, bounds_down),
        out_shape=shapes,
        in_specs=[anywhere] * 6 + [pl.BlockSpec(memory_space=pltpu.SMEM)],
        out_specs=[anywhere] * (len(shapes) - 1) + [pl.BlockSpec(memory_space=pltpu.VMEM)],
        scratch_shapes=[
            pltpu.VMEM((d_model, ff_local), bf16),
            pltpu.VMEM((ff_local, d_model), bf16),
            pltpu.VMEM((2, 256, ff_local), f32),
            pltpu.VMEM((2, 512, d_model), f32),
            pltpu.VMEM((d_model, ff_half), f32),
            pltpu.VMEM((ff_half, d_model), f32),
            pltpu.VMEM((d_model, ff_half), f32),
            pltpu.VMEM((ff_half, d_model), f32),
            pltpu.VMEM((ff_half, d_model), f32),
            pltpu.VMEM((n_row, ff_local), bf16),
            pltpu.VMEM((n_row, ff_local), f32),
            pltpu.VMEM((n_row, ff_local), bf16),
            pltpu.VMEM((2, n_row, half), bf16),
            pltpu.VMEM((n_row, half), f32),
            pltpu.VMEM((n_row, half), f32),
            pltpu.VMEM((n_row, half), bf16),
            pltpu.VMEM((2 * n_row, d_model), bf16),
            pltpu.VMEM((2 * n_row, ff_half), bf16),
            pltpu.VMEM((2 * n_stage, 8, 128), f32),
            pltpu.VMEM((2, 8, 128), f32),
            dma((2, 2)),
            dma((3,)),
            dma(()),
            dma((2,)),
            dma((2, max(2 * len(bounds_up), len(bounds_down)))),
            dma((2,)),
            dma((2,)),
            dma((2,)),
            dma((2, n_chunk)),
            dma((2, n_chunk)),
            dma((2,)),
            dma((2,)),
            dma((2,)),
            dma((2 * n_stage,)),
            dma((2 * n_stage + 1,)),
        ],
        compiler_params=pltpu.CompilerParams(collective_id=0, has_side_effects=True, vmem_limit_bytes=60 << 20),
        name="reduce_and_norm",
    )(g_up, g_down, w_up, w_down, acts, grad_out, max_norm)


def forward_body(n_stage, lead, x_ref, up_ref, down_ref, mean_ref, y_ref, far_ref, inbox, hid, mine, zout, zin, keep, yout, yin, done, x_sem, x_ssem, x_rsem, in_sem, z_ssem, z_rsem, s_ssem, s_rsem, r_ssem, r_rsem, pass_ssem, y_ssem, y_rsem, piece_ssem, piece_rsem):
    model, data, stage = lax.axis_index('model'), lax.axis_index('data'), lax.axis_index('stage')
    mesh_id = pl.DeviceIdType.MESH
    last = n_stage - 1
    n_group, _, rows2, half = inbox.shape
    rows = rows2 // 2
    n_piece = piece_ssem.shape[0]
    piece = mean_ref.shape[0] // n_piece
    peer = {'data': 1 - data}
    near = pl.ds(pl.multiple_of(model * half, half), half)
    far = pl.ds(pl.multiple_of((1 - model) * half, half), half)
    own_rows = pl.ds(pl.multiple_of(data * rows, rows), rows)
    peer_rows = pl.ds(pl.multiple_of((1 - data) * rows, rows), rows)

    def remote(src, dst, ssem, rsem, where):
        return pltpu.make_async_remote_copy(src_ref=src, dst_ref=dst, send_sem=ssem, recv_sem=rsem, device_id=where, device_id_type=mesh_id)

    barrier = pltpu.get_barrier_semaphore()
    group = [(dm, ds) for dm in range(2) for ds in range(n_stage) if dm or ds]
    where = [{'model': lax.rem(model + dm, 2), 'stage': lax.rem(stage + ds, n_stage)} for dm, ds in group]
    for target in where + [peer]:
        pl.semaphore_signal(barrier, inc=1, device_id=target, device_id_type=mesh_id)

    def load_x(b, c):
        return pltpu.make_async_copy(x_ref.at[b, :, pl.ds(c * half, half)], inbox.at[b, c, own_rows], x_sem.at[b, c])

    def swap_x(b, c):
        return remote(x_ref.at[b, :, pl.ds(c * half, half)], inbox.at[b, c, own_rows], x_ssem.at[b, c], x_rsem.at[b, c], peer)

    @pl.when(stage == 0)
    def _():
        for b in range(n_group):
            for c in range(2):
                load_x(b, c).start()

    pl.semaphore_wait(barrier, len(where) + 1)

    @pl.when(stage == 0)
    def _():
        for b in range(n_group):
            for c in range(2):
                swap_x(b, c).start()

    def send_piece(p):
        span = pl.ds(pl.multiple_of(p * piece, piece), piece)
        return remote(mean_ref.at[span], far_ref.at[span], piece_ssem.at[p], piece_rsem.at[p], peer)

    def start_pieces(low, high):
        def one(p, carry):
            send_piece(p).start()
            return carry

        lax.fori_loop(low, high, one, 0)

    n_turn = n_group + 3
    base, slope = lead
    begin = base + slope * stage
    start_pieces(0, begin)

    def arrival(b, c):
        return remote(done.at[b], inbox.at[b, c], pass_ssem.at[b, 0], in_sem.at[b, c], {'model': model})

    def trade_z(b):
        return remote(zout.at[b], zin.at[b], z_ssem.at[b], z_rsem.at[b], {'model': 1 - model})

    def trade_s(b):
        return remote(yout.at[b], yin.at[b], s_ssem.at[b], s_rsem.at[b], peer)

    def trade_r(b):
        return remote(done.at[b, own_rows], done.at[b, own_rows], r_ssem.at[b], r_rsem.at[b], peer)

    def hand_on(b, to):
        return remote(done.at[b], inbox.at[b, model], pass_ssem.at[b, to], in_sem.at[b, model], {'model': to, 'stage': stage + 1})

    def landing(b, c):
        return y_ref.at[b, :, pl.ds(pl.multiple_of(c * half, half), half)]

    def publish(b, k):
        return remote(done.at[b, own_rows], landing(b, model), y_ssem.at[b, k], y_rsem.at[b, model], where[k])

    def y_arrival(b, c):
        return remote(done.at[b, own_rows], landing(b, c), y_ssem.at[b, 0], y_rsem.at[b, c], {'model': model})

    def turn(t, carry):
        @pl.when(t < n_group)
        def _():
            @pl.when(stage == 0)
            def _():
                for c in range(2):
                    load_x(t, c).wait()
                    swap_x(t, c).wait_recv()

            @pl.when(stage > 0)
            def _():
                for c in range(2):
                    arrival(t, c).wait_recv()

            pre = jnp.dot(inbox[t, 0], up_ref[:half], preferred_element_type=jnp.float32)
            pre = pre + jnp.dot(inbox[t, 1], up_ref[half:], preferred_element_type=jnp.float32)
            hid[...] = jax.nn.gelu(pre).astype(jnp.bfloat16)
            zout[t] = jnp.dot(hid[...], down_ref[:, far], preferred_element_type=jnp.float32)
            trade_z(t).start()
            mine[t] = jnp.dot(hid[...], down_ref[:, near], preferred_element_type=jnp.float32)

        @pl.when((t >= 1) & (t < n_group + 1))
        def _():
            b = t - 1
            trade_z(b).wait_recv()
            yout[b] = mine[b, peer_rows] + zin[b, peer_rows]
            trade_s(b).start()
            keep[b] = mine[b, own_rows] + zin[b, own_rows]

        @pl.when((t >= 2) & (t < n_group + 2))
        def _():
            b = t - 2
            trade_s(b).wait_recv()
            total = inbox[b, model, own_rows].astype(jnp.float32) + (keep[b] + yin[b])
            result = total.astype(jnp.bfloat16)
            done[b, own_rows] = result

            @pl.when(stage < last)
            def _():
                trade_r(b).start()

            @pl.when(stage == last)
            def _():
                y_ref[b, :, near] = result
                for k in range(len(group)):
                    publish(b, k).start()

        @pl.when((t >= 3) & (stage < last))
        def _():
            b = t - 3
            remote(done.at[b, own_rows], done.at[b, peer_rows], r_ssem.at[b], r_rsem.at[b], peer).wait_recv()
            for to in range(2):
                hand_on(b, to).start()

        @pl.when(begin + t < n_piece)
        def _():
            send_piece(begin + t).start()

        return carry

    lax.fori_loop(0, n_turn, turn, 0)
    start_pieces(jnp.minimum(begin + n_turn, n_piece), n_piece)

    @pl.when(stage == 0)
    def _():
        for b in range(n_group):
            for c in range(2):
                swap_x(b, c).wait_send()

    for b in range(n_group):
        trade_z(b).wait_send()
        trade_s(b).wait_send()

    @pl.when(stage < last)
    def _():
        for b in range(n_group):
            trade_r(b).wait_send()
            for to in range(2):
                hand_on(b, to).wait_send()
            for c in range(2):
                y_arrival(b, c).wait_recv()

    @pl.when(stage == last)
    def _():
        for b in range(n_group):
            for k in range(len(group)):
                publish(b, k).wait_send()
            y_arrival(b, 1 - model).wait_recv()

    def finish(p, carry):
        send_piece(p).wait()
        return carry

    lax.fori_loop(0, n_piece, finish, 0)


def forward_call(n_stage, n_group, n_piece, lead, x_next, up_bf, down_bf, mean):
    d_model = x_next.shape[2]
    x_next = x_next.reshape(n_group, -1, d_model)
    rows, half, ff_half = x_next.shape[1], d_model // 2, up_bf.shape[1]
    dma = pltpu.SemaphoreType.DMA
    f32, bf16 = jnp.float32, jnp.bfloat16
    in_vmem = pl.BlockSpec(memory_space=pltpu.VMEM)
    anywhere = pl.BlockSpec(memory_space=pl.ANY)
    return pl.pallas_call(
        functools.partial(forward_body, n_stage, lead),
        out_shape=[jax.ShapeDtypeStruct(x_next.shape, bf16), jax.ShapeDtypeStruct(mean.shape, f32)],
        in_specs=[anywhere, in_vmem, in_vmem, anywhere],
        out_specs=[in_vmem, anywhere],
        scratch_shapes=[
            pltpu.VMEM((n_group, 2, 2 * rows, half), bf16),
            pltpu.VMEM((2 * rows, ff_half), bf16),
            pltpu.VMEM((n_group, 2 * rows, half), f32),
            pltpu.VMEM((n_group, 2 * rows, half), f32),
            pltpu.VMEM((n_group, 2 * rows, half), f32),
            pltpu.VMEM((n_group, rows, half), f32),
            pltpu.VMEM((n_group, rows, half), f32),
            pltpu.VMEM((n_group, rows, half), f32),
            pltpu.VMEM((n_group, 2 * rows, half), bf16),
            dma((n_group, 2)),
            dma((n_group, 2)),
            dma((n_group, 2)),
            dma((n_group, 2)),
            dma((n_group,)),
            dma((n_group,)),
            dma((n_group,)),
            dma((n_group,)),
            dma((n_group,)),
            dma((n_group,)),
            dma((n_group, 2)),
            dma((n_group, 2 * n_stage - 1)),
            dma((n_group, 2)),
            dma((n_piece,)),
            dma((n_piece,)),
        ],
        compiler_params=pltpu.CompilerParams(collective_id=1, has_side_effects=True, vmem_limit_bytes=48 << 20),
        name="forward_pipe",
    )(x_next, up_bf, down_bf, mean)


def solution(mesh):
    n_stage = mesh.shape['stage']
    swap = [(0, 1), (1, 0)]
    up_spec = P('stage', None, 'model')
    down_spec = P('stage', 'model', None)
    row_spec = P(None, 'data', None)
    in_specs = (up_spec, down_spec, up_spec, down_spec, up_spec, down_spec, P('data', 'stage', None, 'model'), P('data', 'stage', 'model', None), P('stage', 'data', None), P('data', None), row_spec, P(None), P(None))
    out_specs = (up_spec, down_spec, up_spec, down_spec, up_spec, down_spec, row_spec)

    def device_step(w_up, w_down, m_up, m_down, v_up, v_down, g_up, g_down, acts_last, grad_out, x_next, learn_rate, max_norm):
        data_id = lax.axis_index('data')
        half = data_id.astype(jnp.int32).reshape(1)
        other = (1 - half).astype(jnp.int32)
        d_model, ff_local = w_up.shape[1:]
        ff_half = ff_local // 2
        bounds_up = ((0, 256), (256, 640), (640, 896), (896, d_model))
        bounds_down = ((0, ff_half // 2), (ff_half // 2, ff_half))

        def trade(value):
            return lax.ppermute(value, 'data', swap)

        early, *late, whole_up, whole_down, far_first, clip = backward_call(n_stage, bounds_up, bounds_down, g_up[0, 0], g_down[0, 0], w_up[0], w_down[0], acts_last[0], grad_out, max_norm)
        ups = (w_up[0], m_up[0], v_up[0])
        downs = (w_down[0], m_down[0], v_down[0])

        def map_up(low):
            return lambda i, h, r: (low // STEP + i, h[0])

        def map_down(low):
            return lambda i, h, r: ((h[0] * ff_half + low) // STEP + i, 0)

        far_early = trade(early)
        *new_up, up_bf = update_call(half, learn_rate, clip, ups, whole_up, map_up(0), None)
        *new_down, down_bf = update_call(half, learn_rate, clip, downs, whole_down, map_down(0), None, (up_bf,))
        y_next, far_down = forward_call(n_stage, N_GROUP, N_PIECE, LEAD, x_next, up_bf, down_bf, whole_down)
        y_next = y_next.reshape(x_next.shape)
        late, far_down = lax.optimization_barrier((late, far_down))
        fars = [far_first, far_early] + [trade(value) for value in late]
        new_down = update_call(other, learn_rate, clip, downs, far_down, map_down(0), new_down)
        for (low, _), part in zip(bounds_up, fars):
            new_up = update_call(other, learn_rate, clip, ups, part, map_up(low), new_up)
        return (new_up[0][None], new_down[0][None], new_up[1][None], new_down[1][None], new_up[2][None], new_down[2][None], y_next)

    return jax.shard_map(device_step, mesh=mesh, in_specs=in_specs, out_specs=out_specs, check_vma=False)
```

```python
import functools

import jax
import jax.numpy as jnp
from jax import lax
from jax.experimental import pallas as pl
from jax.experimental.pallas import tpu as pltpu
from jax.sharding import PartitionSpec as P

ADAM_STEP = 10
BETA_ONE = 0.9
BETA_TWO = 0.95
ADAM_EPS = 1e-8
WEIGHT_DECAY = 0.1
NORM_EPS = 1e-6
CONTRACT_LAST = (((1,), (1,)), ((), ()))
BLOCK = 128
STEP = 128
N_GROUP = 8
N_PIECE = 32
LEAD = (2, 7)


def update_body(skip, carry, half_ref, rate_ref, clip_ref, w_ref, m_ref, v_ref, g_ref, *refs):
    outs = refs[skip:]
    if carry:
        outs[-1][...] = refs[skip - 1][...]
        outs = outs[:-1]
    ow_ref, om_ref, ov_ref = outs[:3]
    rate = rate_ref[0]
    grad = clip_ref[0:1] * g_ref[...]
    weight = w_ref[...]
    mom = BETA_ONE * m_ref[...] + (1.0 - BETA_ONE) * grad
    sec = BETA_TWO * v_ref[...] + (1.0 - BETA_TWO) * grad * grad
    one_corr = 1.0 - BETA_ONE**ADAM_STEP
    two_corr = 1.0 - BETA_TWO**ADAM_STEP
    direction = (mom * (1.0 / one_corr)) / (jnp.sqrt(sec * (1.0 / two_corr)) + ADAM_EPS)
    new = weight - rate * (direction + WEIGHT_DECAY * weight)
    ow_ref[...] = new
    om_ref[...] = mom
    ov_ref[...] = sec
    if len(outs) == 4:
        outs[3][...] = new.astype(jnp.bfloat16)


def update_call(half, rate, clip, weights, grad, full_map, previous, after=(), carry=()):
    rows, cols = grad.shape
    block = min(STEP, rows)
    shape = weights[0].shape
    spec = pl.BlockSpec((block, cols), full_map)
    flat = pl.BlockSpec((block, cols), lambda i, h, r: (i, 0))
    anywhere = pl.BlockSpec(memory_space=pl.ANY)
    first = previous is None
    extra = list(previous or ()) + list(after)
    passed = [pl.BlockSpec((1,) + value.shape[1:], lambda i, h, r: (i, 0, 0)) for value in carry]
    return pl.pallas_call(
        functools.partial(update_body, len(extra) + len(carry), len(carry)),
        grid_spec=pltpu.PrefetchScalarGridSpec(
            num_scalar_prefetch=2,
            grid=(rows // block,),
            in_specs=[pl.BlockSpec(clip.shape, lambda i, h, r: (0, 0)), spec, spec, spec, flat] + [anywhere] * len(extra) + passed,
            out_specs=[spec] * 3 + [flat] * first + passed,
        ),
        out_shape=[jax.ShapeDtypeStruct(shape, jnp.float32)] * 3 + [jax.ShapeDtypeStruct(grad.shape, jnp.bfloat16)] * first + [jax.ShapeDtypeStruct(value.shape, value.dtype) for value in carry],
        input_output_aliases={7 + i: i for i in range(len(previous or ()))},
        cost_estimate=pl.CostEstimate(flops=60 * rows * cols, bytes_accessed=30 * rows * cols, transcendentals=0),
        compiler_params=pltpu.CompilerParams(vmem_limit_bytes=67043328),
        name="adamw_half",
    )(half, rate, clip, *weights, grad, *extra, *carry)


def backward_body(n_stage, n_raw, bounds_up, bounds_down, gu_ref, gd_ref, wu_ref, wd_ref, acts_ref, gout_ref, x_ref, max_ref, *refs):
    n_up = len(bounds_up) - 1
    outs_up = refs[:n_up]
    whole_up, whole_down, far_ref, x_far, clip_ref = refs[n_up:n_up + 5]
    (up_bf, down_bf, st_up, st_down, acc_up, acc_down, got_up, got_down, fold, hid, slope, grad_pre, gbuf, outbox, landed, ready, rows_a, rows_z, norm_box, norm_pair,
     st_sem, loc_sem, fold_sem, own_sem, out_sem, g_rsem, trade_sem, pass_ssem, rs_ssem, rs_rsem, row_ssem, row_rsem, far_sem, norm_ssem, norm_rsem, x_land, x_sem, xf_ssem, xf_rsem) = refs[n_up + 5:]
    model, data, stage = lax.axis_index('model'), lax.axis_index('data'), lax.axis_index('stage')
    mesh_id = pl.DeviceIdType.MESH
    last = n_stage - 1
    d_model, ff_half = acc_up.shape
    half = d_model // 2
    n_row = acts_ref.shape[0]
    n_up_chunk, n_down_chunk = d_model // BLOCK, ff_half // BLOCK
    peer = {'data': 1 - data}
    near = pl.ds(pl.multiple_of(model * half, half), half)
    far = pl.ds(pl.multiple_of((1 - model) * half, half), half)
    own_cols = pl.ds(pl.multiple_of(data * ff_half, ff_half), ff_half)
    peer_cols = pl.ds(pl.multiple_of((1 - data) * ff_half, ff_half), ff_half)
    own_rows = pl.ds(pl.multiple_of(data * n_row, n_row), n_row)
    first_dims = (((0,), (0,)), ((), ()))

    def remote(src, dst, ssem, rsem, where):
        return pltpu.make_async_remote_copy(src_ref=src, dst_ref=dst, send_sem=ssem, recv_sem=rsem, device_id=where, device_id_type=mesh_id)

    barrier = pltpu.get_barrier_semaphore()
    group = [(dm, ds) for dm in range(2) for ds in range(n_stage) if dm or ds]
    where = [{'model': lax.rem(model + dm, 2), 'stage': lax.rem(stage + ds, n_stage)} for dm, ds in group]
    for target in where + [peer]:
        pl.semaphore_signal(barrier, inc=1, device_id=target, device_id_type=mesh_id)

    n_st_up, n_st_down = d_model // st_up.shape[1], 2 * ff_half // st_down.shape[1]

    def load_up(r):
        return pltpu.make_async_copy(wu_ref.at[pl.ds(r * st_up.shape[1], st_up.shape[1])], st_up.at[r % 2], st_sem.at[0, r % 2])

    def load_down(r):
        return pltpu.make_async_copy(wd_ref.at[pl.ds(r * st_down.shape[1], st_down.shape[1])], st_down.at[r % 2], st_sem.at[1, r % 2])

    load_acts = pltpu.make_async_copy(acts_ref, rows_a.at[own_rows], loc_sem.at[0])
    load_acts.start()
    load_up(0).start()
    load_up(1).start()
    load_down(0).start()
    load_down(1).start()

    def load_g(c):
        return pltpu.make_async_copy(gout_ref.at[:, pl.ds(c * half, half)], gbuf.at[c], loc_sem.at[1 + c])

    @pl.when(stage == last)
    def _():
        for c in range(2):
            load_g(c).start()

    pl.semaphore_wait(barrier, len(where) + 1)

    def chunk(k):
        return pl.ds(k * BLOCK, BLOCK)

    raw = [remote(gu_ref.at[chunk(k), peer_cols], got_up.at[chunk(k)], rs_ssem.at[0, k], rs_rsem.at[0, k], peer) for k in range(n_up_chunk)]
    send_x = remote(x_ref.at[stage, :, near], x_land, x_sem.at[0], x_sem.at[1], peer)
    send_x.start()
    for copy in raw:
        copy.start()
    send_a = remote(acts_ref, rows_a.at[own_rows], row_ssem.at[0], row_rsem.at[0], peer)
    send_a.start()

    for r in range(n_st_up):
        load_up(r).wait()
        up_bf[pl.ds(r * st_up.shape[1], st_up.shape[1])] = st_up[r % 2].astype(jnp.bfloat16)
        if r + 2 < n_st_up:
            load_up(r + 2).start()
    load_acts.wait()

    tile = 256
    n_tile = hid.shape[1] // tile
    scale = 0.7978845608028654
    cubic = 0.044715

    def pre_tile(j, carry):
        cols = pl.ds(pl.multiple_of(j * tile, tile), tile)
        pre = jnp.dot(rows_a[own_rows], up_bf[:, cols], preferred_element_type=jnp.float32)
        square = pre * pre
        bend = jnp.tanh(scale * (pre + cubic * square * pre))
        hid[:, cols] = (pre * (0.5 * (1.0 + bend))).astype(jnp.bfloat16)
        slope[:, cols] = 0.5 * (1.0 + bend) + 0.5 * pre * (1.0 - bend * bend) * (scale * (1.0 + 3.0 * cubic * square))
        return carry

    lax.fori_loop(0, n_tile, pre_tile, 0)

    for r in range(n_st_down):
        load_down(r).wait()
        down_bf[pl.ds(r * st_down.shape[1], st_down.shape[1])] = st_down[r % 2].astype(jnp.bfloat16)
        if r + 2 < n_st_down:
            load_down(r + 2).start()

    own_up = pltpu.make_async_copy(gu_ref.at[:, own_cols], acc_up, own_sem.at[0])
    own_down = pltpu.make_async_copy(gd_ref.at[own_cols], acc_down, own_sem.at[1])
    load_fold = pltpu.make_async_copy(gd_ref.at[peer_cols], fold, fold_sem)
    load_fold.start()
    own_up.start()
    own_down.start()

    @pl.when(stage == last)
    def _():
        for c in range(2):
            load_g(c).wait()

    @pl.when(stage < last)
    def _():
        for c in range(2):
            remote(ready, gbuf.at[c], pass_ssem.at[0], g_rsem.at[c], {'model': model}).wait_recv()

    def slope_tile(j, carry):
        cols = pl.ds(pl.multiple_of(j * tile, tile), tile)
        grad = lax.dot_general(gbuf[0], down_bf[cols, :half], CONTRACT_LAST, preferred_element_type=jnp.float32)
        grad = grad + lax.dot_general(gbuf[1], down_bf[cols, half:], CONTRACT_LAST, preferred_element_type=jnp.float32)
        grad_pre[:, cols] = (slope[:, cols] * grad).astype(jnp.bfloat16)
        return carry

    lax.fori_loop(0, n_tile, slope_tile, 0)

    trade = remote(outbox, landed, trade_sem.at[0], trade_sem.at[1], {'model': 1 - model})

    def hand_on(to):
        return remote(ready, gbuf.at[model], pass_ssem.at[to], g_rsem.at[model], {'model': to, 'stage': stage - 1})

    @pl.when(stage > 0)
    def _():
        outbox[...] = lax.dot_general(grad_pre[...], up_bf[far], CONTRACT_LAST, preferred_element_type=jnp.float32)
        trade.start()
        mine = lax.dot_general(grad_pre[...], up_bf[near], CONTRACT_LAST, preferred_element_type=jnp.float32)
        trade.wait_recv()
        ready[...] = (gbuf[model].astype(jnp.float32) + (mine + landed[...])).astype(jnp.bfloat16)
        for to in range(2):
            hand_on(to).start()

    rows_z[own_rows] = grad_pre[:, own_cols]
    send_z = remote(grad_pre.at[:, peer_cols], rows_z.at[own_rows], row_ssem.at[1], row_rsem.at[1], peer)
    send_z.start()

    home = x_far.at[stage, :, near]
    keep_x = pltpu.make_async_copy(x_land, home, x_sem.at[2])

    def forward_x(to):
        return remote(x_land, home, xf_ssem.at[to], xf_rsem.at[stage, model], {'model': to, 'stage': 0})

    def each_x(do_local, do_remote):
        for to in range(2):
            at_home = (stage == 0) & (model == to)

            @pl.when(at_home)
            def _():
                do_local()

            @pl.when(jnp.logical_not(at_home))
            def _():
                do_remote(to)

    send_x.wait_recv()
    each_x(lambda: keep_x.start(), lambda to: forward_x(to).start())

    def down_product(k, side):
        cols = pl.ds(pl.multiple_of(side * ff_half + k * BLOCK, BLOCK), BLOCK)
        left = hid[:, cols]
        return [lax.dot_general(left, gbuf[c], first_dims, preferred_element_type=jnp.float32) for c in range(2)]

    load_fold.wait()

    def send_fold(k):
        rows = pl.ds(pl.multiple_of(k * BLOCK, BLOCK), BLOCK)
        return remote(fold.at[rows], got_down.at[rows], rs_ssem.at[1, k], rs_rsem.at[1, k], peer)

    def fold_step(k, carry):
        rows = pl.ds(pl.multiple_of(k * BLOCK, BLOCK), BLOCK)
        low, high = down_product(k, 1 - data)
        fold[rows, :half] += low
        fold[rows, half:] += high
        send_fold(k).start()
        return carry

    lax.fori_loop(0, n_down_chunk, fold_step, 0)
    own_down.wait()

    def own_step(k, carry):
        rows = pl.ds(pl.multiple_of(k * BLOCK, BLOCK), BLOCK)
        low, high = down_product(k, data)
        acc_down[rows, :half] += low
        acc_down[rows, half:] += high
        return carry

    lax.fori_loop(0, n_down_chunk, own_step, 0)

    @pl.when(stage > 0)
    def _():
        trade.wait_send()
        for to in range(2):
            hand_on(to).wait_send()

    own_up.wait()
    send_a.wait_recv()
    squares = jnp.zeros((8, ff_half), jnp.float32)

    def fold_squares(mean):
        return jnp.sum((mean * mean).reshape(-1, 8, mean.shape[1]), axis=0)

    def put(acc, bounds, outs, whole, sem_row):
        copies = []
        for i, (lo, hi) in enumerate(bounds):
            rows = pl.ds(lo, hi - lo)
            copies.append(pltpu.make_async_copy(acc.at[rows], whole.at[rows], out_sem.at[sem_row, i]))
            if outs[i] is not None:
                copies.append(pltpu.make_async_copy(acc.at[rows], outs[i], out_sem.at[sem_row, len(bounds) + i]))
        return copies

    def put_start(k, bounds, copies, outs):
        at = 0
        for i, (lo, hi) in enumerate(bounds):
            count = 1 if outs[i] is None else 2
            if hi == (k + 1) * BLOCK:
                for copy in copies[at:at + count]:
                    copy.start()
            at += count

    outs_up = (None,) + tuple(outs_up)
    outs_down = (None,) * len(bounds_down)
    put_up = put(acc_up, bounds_up, outs_up, whole_up, 0)
    put_down = put(acc_down, bounds_down, outs_down, whole_down, 1)
    for k in range(n_up_chunk):
        raw[k].wait_recv()
        if k == 0:
            send_z.wait_recv()
        product = lax.dot_general(rows_a[:, k * BLOCK:(k + 1) * BLOCK], rows_z[...], first_dims, preferred_element_type=jnp.float32)
        mean = (acc_up[chunk(k)] + got_up[chunk(k)] + product) * 0.5
        acc_up[chunk(k)] = mean
        squares = squares + fold_squares(mean)
        put_start(k, bounds_up, put_up, outs_up)
    first = bounds_up[0][1]
    send_far = remote(acc_up.at[pl.ds(0, first)], far_ref, far_sem.at[0], far_sem.at[1], peer)
    send_far.start()
    for k in range(n_down_chunk):
        send_fold(k).wait_recv()
        mean = (acc_down[chunk(k)] + got_down[chunk(k)]) * 0.5
        acc_down[chunk(k)] = mean
        squares = squares + fold_squares(mean)
        put_start(k, bounds_down, put_down, outs_down)

    lanes = norm_box.shape[2]
    part = squares[:, :lanes]
    for j in range(1, ff_half // lanes):
        part = part + squares[:, j * lanes:(j + 1) * lanes]
    me = model * n_stage + stage
    norm_box[me] = part

    def spread(i):
        return remote(norm_box.at[me], norm_box.at[me], norm_ssem.at[i], norm_rsem.at[me], where[i])

    for i in range(len(group)):
        spread(i).start()
    for i, (dm, ds) in enumerate(group):
        them = lax.rem(model + dm, 2) * n_stage + lax.rem(stage + ds, n_stage)
        remote(norm_box.at[me], norm_box.at[them], norm_ssem.at[i], norm_rsem.at[them], where[i]).wait_recv()
    total = norm_box[0]
    for i in range(1, 2 * n_stage):
        total = total + norm_box[i]
    norm_pair[0] = total
    swap = remote(norm_pair.at[0], norm_pair.at[1], norm_ssem.at[len(group)], norm_rsem.at[2 * n_stage], peer)
    swap.start()
    swap.wait_recv()
    norm_sq = jnp.sum(norm_pair[0] + norm_pair[1], axis=(0, 1), keepdims=True)
    norm = jnp.sqrt(jnp.broadcast_to(norm_sq, clip_ref.shape)) + NORM_EPS
    clip_ref[...] = jnp.minimum(1.0, max_ref[0] / norm)

    each_x(lambda: keep_x.wait(), lambda to: forward_x(to).wait_send())

    @pl.when(stage == 0)
    def _():
        for s in range(n_stage):
            for m in range(2):
                arrive = remote(x_land, x_far.at[s, :, pl.ds(m * half, half)], xf_ssem.at[m], xf_rsem.at[s, m], {'model': model})
                if s:
                    arrive.wait_recv()
                else:
                    pl.when(model != m)(arrive.wait_recv)

    send_x.wait_send()
    swap.wait_send()
    for i in range(len(group)):
        spread(i).wait_send()
    for copy in raw + [send_a, send_z]:
        copy.wait_send()
    for k in range(n_down_chunk):
        send_fold(k).wait_send()
    for copy in put_up + put_down:
        copy.wait()
    send_far.wait()


def backward_call(n_stage, bounds_up, bounds_down, g_up, g_down, w_up, w_down, acts, grad_out, x_next, max_norm):
    d_model, ff_local = g_up.shape
    ff_half, half, n_row = ff_local // 2, d_model // 2, acts.shape[0]
    dma = pltpu.SemaphoreType.DMA
    anywhere = pl.BlockSpec(memory_space=pl.ANY)
    f32, bf16 = jnp.float32, jnp.bfloat16
    shapes = [jax.ShapeDtypeStruct((hi - lo, ff_half), f32) for lo, hi in bounds_up[1:]]
    shapes += [jax.ShapeDtypeStruct((d_model, ff_half), f32), jax.ShapeDtypeStruct((ff_half, d_model), f32)]
    shapes += [jax.ShapeDtypeStruct((bounds_up[0][1], ff_half), f32), jax.ShapeDtypeStruct(x_next.shape, bf16), jax.ShapeDtypeStruct((8, ff_half), f32)]
    n_chunk = max(d_model, ff_half) // BLOCK
    return pl.pallas_call(
        functools.partial(backward_body, n_stage, n_chunk, bounds_up, bounds_down),
        out_shape=shapes,
        in_specs=[anywhere] * 7 + [pl.BlockSpec(memory_space=pltpu.SMEM)],
        out_specs=[anywhere] * (len(shapes) - 1) + [pl.BlockSpec(memory_space=pltpu.VMEM)],
        scratch_shapes=[
            pltpu.VMEM((d_model, ff_local), bf16),
            pltpu.VMEM((ff_local, d_model), bf16),
            pltpu.VMEM((2, 256, ff_local), f32),
            pltpu.VMEM((2, 512, d_model), f32),
            pltpu.VMEM((d_model, ff_half), f32),
            pltpu.VMEM((ff_half, d_model), f32),
            pltpu.VMEM((d_model, ff_half), f32),
            pltpu.VMEM((ff_half, d_model), f32),
            pltpu.VMEM((ff_half, d_model), f32),
            pltpu.VMEM((n_row, ff_local), bf16),
            pltpu.VMEM((n_row, ff_local), f32),
            pltpu.VMEM((n_row, ff_local), bf16),
            pltpu.VMEM((2, n_row, half), bf16),
            pltpu.VMEM((n_row, half), f32),
            pltpu.VMEM((n_row, half), f32),
            pltpu.VMEM((n_row, half), bf16),
            pltpu.VMEM((2 * n_row, d_model), bf16),
            pltpu.VMEM((2 * n_row, ff_half), bf16),
            pltpu.VMEM((2 * n_stage, 8, 128), f32),
            pltpu.VMEM((2, 8, 128), f32),
            dma((2, 2)),
            dma((3,)),
            dma(()),
            dma((2,)),
            dma((2, max(2 * len(bounds_up), len(bounds_down)))),
            dma((2,)),
            dma((2,)),
            dma((2,)),
            dma((2, n_chunk)),
            dma((2, n_chunk)),
            dma((2,)),
            dma((2,)),
            dma((2,)),
            dma((2 * n_stage,)),
            dma((2 * n_stage + 1,)),
            pltpu.VMEM((n_row, half), bf16),
            dma((3,)),
            dma((2,)),
            dma((n_stage, 2)),
        ],
        compiler_params=pltpu.CompilerParams(collective_id=0, has_side_effects=True, vmem_limit_bytes=67043328),
        name="reduce_and_norm",
    )(g_up, g_down, w_up, w_down, acts, grad_out, x_next, max_norm)


def forward_body(n_stage, lead, x_ref, xf_ref, up_ref, down_ref, mean_ref, y_ref, far_ref, inbox, hid, mine, zout, zin, keep, yout, yin, done, x_sem, in_sem, z_ssem, z_rsem, s_ssem, s_rsem, r_ssem, r_rsem, pass_ssem, y_ssem, y_rsem, piece_ssem, piece_rsem):
    model, data, stage = lax.axis_index('model'), lax.axis_index('data'), lax.axis_index('stage')
    mesh_id = pl.DeviceIdType.MESH
    last = n_stage - 1
    n_group, _, rows2, half = inbox.shape
    rows = rows2 // 2
    n_piece = piece_ssem.shape[0]
    piece = mean_ref.shape[0] // n_piece
    peer = {'data': 1 - data}
    near = pl.ds(pl.multiple_of(model * half, half), half)
    far = pl.ds(pl.multiple_of((1 - model) * half, half), half)
    own_rows = pl.ds(pl.multiple_of(data * rows, rows), rows)
    peer_rows = pl.ds(pl.multiple_of((1 - data) * rows, rows), rows)

    def remote(src, dst, ssem, rsem, where):
        return pltpu.make_async_remote_copy(src_ref=src, dst_ref=dst, send_sem=ssem, recv_sem=rsem, device_id=where, device_id_type=mesh_id)

    barrier = pltpu.get_barrier_semaphore()
    group = [(dm, ds) for dm in range(2) for ds in range(n_stage) if dm or ds]
    where = [{'model': lax.rem(model + dm, 2), 'stage': lax.rem(stage + ds, n_stage)} for dm, ds in group]
    for target in where + [peer]:
        pl.semaphore_signal(barrier, inc=1, device_id=target, device_id_type=mesh_id)

    def load_x(b, c, from_ref, to_rows, i):
        return pltpu.make_async_copy(from_ref.at[b, :, pl.ds(c * half, half)], inbox.at[b, c, to_rows], x_sem.at[b, c, i])

    def loads(b):
        return [load_x(b, c, *pair) for c in range(2) for pair in ((x_ref, own_rows, 0), (xf_ref, peer_rows, 1))]

    @pl.when(stage == 0)
    def _():
        for b in range(n_group):
            for copy in loads(b):
                copy.start()

    pl.semaphore_wait(barrier, len(where) + 1)

    def send_piece(p):
        span = pl.ds(pl.multiple_of(p * piece, piece), piece)
        return remote(mean_ref.at[span], far_ref.at[span], piece_ssem.at[p], piece_rsem.at[p], peer)

    def start_pieces(low, high):
        def one(p, carry):
            send_piece(p).start()
            return carry

        lax.fori_loop(low, high, one, 0)

    n_turn = n_group + 3
    base, slope = lead
    begin = base + slope * stage
    start_pieces(0, begin)

    def arrival(b, c):
        return remote(done.at[b], inbox.at[b, c], pass_ssem.at[b, 0], in_sem.at[b, c], {'model': model})

    def trade_z(b):
        return remote(zout.at[b], zin.at[b], z_ssem.at[b], z_rsem.at[b], {'model': 1 - model})

    def trade_s(b):
        return remote(yout.at[b], yin.at[b], s_ssem.at[b], s_rsem.at[b], peer)

    def trade_r(b):
        return remote(done.at[b, own_rows], done.at[b, own_rows], r_ssem.at[b], r_rsem.at[b], peer)

    def hand_on(b, to):
        return remote(done.at[b], inbox.at[b, model], pass_ssem.at[b, to], in_sem.at[b, model], {'model': to, 'stage': stage + 1})

    def landing(b, c):
        return y_ref.at[b, :, pl.ds(pl.multiple_of(c * half, half), half)]

    def publish(b, k):
        return remote(done.at[b, own_rows], landing(b, model), y_ssem.at[b, k], y_rsem.at[b, model], where[k])

    def y_arrival(b, c):
        return remote(done.at[b, own_rows], landing(b, c), y_ssem.at[b, 0], y_rsem.at[b, c], {'model': model})

    def turn(t, carry):
        @pl.when(t < n_group)
        def _():
            @pl.when(stage == 0)
            def _():
                for copy in loads(t):
                    copy.wait()

            @pl.when(stage > 0)
            def _():
                for c in range(2):
                    arrival(t, c).wait_recv()

            pre = jnp.dot(inbox[t, 0], up_ref[:half], preferred_element_type=jnp.float32)
            pre = pre + jnp.dot(inbox[t, 1], up_ref[half:], preferred_element_type=jnp.float32)
            hid[...] = jax.nn.gelu(pre).astype(jnp.bfloat16)
            zout[t] = jnp.dot(hid[...], down_ref[:, far], preferred_element_type=jnp.float32)
            trade_z(t).start()
            mine[t] = jnp.dot(hid[...], down_ref[:, near], preferred_element_type=jnp.float32)

        @pl.when((t >= 1) & (t < n_group + 1))
        def _():
            b = t - 1
            trade_z(b).wait_recv()
            yout[b] = mine[b, peer_rows] + zin[b, peer_rows]
            trade_s(b).start()
            keep[b] = mine[b, own_rows] + zin[b, own_rows]

        @pl.when((t >= 2) & (t < n_group + 2))
        def _():
            b = t - 2
            trade_s(b).wait_recv()
            total = inbox[b, model, own_rows].astype(jnp.float32) + (keep[b] + yin[b])
            result = total.astype(jnp.bfloat16)
            done[b, own_rows] = result

            @pl.when(stage < last)
            def _():
                trade_r(b).start()

            @pl.when(stage == last)
            def _():
                y_ref[b, :, near] = result
                for k in range(len(group)):
                    publish(b, k).start()

        @pl.when((t >= 3) & (stage < last))
        def _():
            b = t - 3
            remote(done.at[b, own_rows], done.at[b, peer_rows], r_ssem.at[b], r_rsem.at[b], peer).wait_recv()
            for to in range(2):
                hand_on(b, to).start()

        @pl.when(begin + t < n_piece)
        def _():
            send_piece(begin + t).start()

        return carry

    lax.fori_loop(0, n_turn, turn, 0)
    start_pieces(jnp.minimum(begin + n_turn, n_piece), n_piece)

    for b in range(n_group):
        trade_z(b).wait_send()
        trade_s(b).wait_send()

    @pl.when(stage < last)
    def _():
        for b in range(n_group):
            trade_r(b).wait_send()
            for to in range(2):
                hand_on(b, to).wait_send()
            for c in range(2):
                y_arrival(b, c).wait_recv()

    @pl.when(stage == last)
    def _():
        for b in range(n_group):
            for k in range(len(group)):
                publish(b, k).wait_send()
            y_arrival(b, 1 - model).wait_recv()

    def finish(p, carry):
        send_piece(p).wait()
        return carry

    lax.fori_loop(0, n_piece, finish, 0)


def forward_call(n_stage, n_group, n_piece, lead, x_next, x_far, up_bf, down_bf, mean):
    d_model = x_next.shape[2]
    x_next, x_far = [value.reshape(n_group, -1, d_model) for value in (x_next, x_far)]
    rows, half, ff_half = x_next.shape[1], d_model // 2, up_bf.shape[1]
    dma = pltpu.SemaphoreType.DMA
    f32, bf16 = jnp.float32, jnp.bfloat16
    in_vmem = pl.BlockSpec(memory_space=pltpu.VMEM)
    anywhere = pl.BlockSpec(memory_space=pl.ANY)
    return pl.pallas_call(
        functools.partial(forward_body, n_stage, lead),
        out_shape=[jax.ShapeDtypeStruct(x_next.shape, bf16), jax.ShapeDtypeStruct(mean.shape, f32)],
        in_specs=[anywhere, anywhere, in_vmem, in_vmem, anywhere],
        out_specs=[in_vmem, anywhere],
        scratch_shapes=[
            pltpu.VMEM((n_group, 2, 2 * rows, half), bf16),
            pltpu.VMEM((2 * rows, ff_half), bf16),
            pltpu.VMEM((n_group, 2 * rows, half), f32),
            pltpu.VMEM((n_group, 2 * rows, half), f32),
            pltpu.VMEM((n_group, 2 * rows, half), f32),
            pltpu.VMEM((n_group, rows, half), f32),
            pltpu.VMEM((n_group, rows, half), f32),
            pltpu.VMEM((n_group, rows, half), f32),
            pltpu.VMEM((n_group, 2 * rows, half), bf16),
            dma((n_group, 2, 2)),
            dma((n_group, 2)),
            dma((n_group,)),
            dma((n_group,)),
            dma((n_group,)),
            dma((n_group,)),
            dma((n_group,)),
            dma((n_group,)),
            dma((n_group, 2)),
            dma((n_group, 2 * n_stage - 1)),
            dma((n_group, 2)),
            dma((n_piece,)),
            dma((n_piece,)),
        ],
        compiler_params=pltpu.CompilerParams(collective_id=1, has_side_effects=True, vmem_limit_bytes=67043328),
        name="forward_pipe",
    )(x_next, x_far, up_bf, down_bf, mean)


def solution(mesh):
    n_stage = mesh.shape['stage']
    swap = [(0, 1), (1, 0)]
    up_spec = P('stage', None, 'model')
    down_spec = P('stage', 'model', None)
    row_spec = P(None, 'data', None)
    in_specs = (up_spec, down_spec, up_spec, down_spec, up_spec, down_spec, P('data', 'stage', None, 'model'), P('data', 'stage', 'model', None), P('stage', 'data', None), P('data', None), row_spec, P(None), P(None))
    out_specs = (up_spec, down_spec, up_spec, down_spec, up_spec, down_spec, row_spec)

    def device_step(w_up, w_down, m_up, m_down, v_up, v_down, g_up, g_down, acts_last, grad_out, x_next, learn_rate, max_norm):
        data_id = lax.axis_index('data')
        half = data_id.astype(jnp.int32).reshape(1)
        other = (1 - half).astype(jnp.int32)
        d_model, ff_local = w_up.shape[1:]
        ff_half = ff_local // 2
        bounds_up = ((0, 256), (256, 640), (640, 896), (896, d_model))
        bounds_down = ((0, ff_half // 2), (ff_half // 2, ff_half))

        def trade(value):
            return lax.ppermute(value, 'data', swap)

        early, *late, whole_up, whole_down, far_first, x_far, clip = backward_call(n_stage, bounds_up, bounds_down, g_up[0, 0], g_down[0, 0], w_up[0], w_down[0], acts_last[0], grad_out, x_next, max_norm)
        ups = (w_up[0], m_up[0], v_up[0])
        downs = (w_down[0], m_down[0], v_down[0])

        def map_up(low):
            return lambda i, h, r: (low // STEP + i, h[0])

        def map_down(low):
            return lambda i, h, r: ((h[0] * ff_half + low) // STEP + i, 0)

        far_early = trade(early)
        *new_up, up_bf = update_call(half, learn_rate, clip, ups, whole_up, map_up(0), None)
        *new_down, down_bf = update_call(half, learn_rate, clip, downs, whole_down, map_down(0), None, (up_bf,))
        y_next, far_down = forward_call(n_stage, N_GROUP, N_PIECE, LEAD, x_next, x_far, up_bf, down_bf, whole_down)
        late, far_down = lax.optimization_barrier((late, far_down))
        fars = [far_first, far_early] + [trade(value) for value in late]
        *new_down, y_next = update_call(other, learn_rate, clip, downs, far_down, map_down(0), new_down, (), (y_next,))
        y_next = y_next.reshape(x_next.shape)
        for (low, _), part in zip(bounds_up, fars):
            new_up = update_call(other, learn_rate, clip, ups, part, map_up(low), new_up)
        return (new_up[0][None], new_down[0][None], new_up[1][None], new_down[1][None], new_up[2][None], new_down[2][None], y_next)

    return jax.shard_map(device_step, mesh=mesh, in_specs=in_specs, out_specs=out_specs, check_vma=False)
```

```python
import functools

import jax
import jax.numpy as jnp
from jax import lax
from jax.experimental import pallas as pl
from jax.experimental.pallas import tpu as pltpu
from jax.sharding import PartitionSpec as P

ADAM_STEP = 10
BETA_ONE = 0.9
BETA_TWO = 0.95
ADAM_EPS = 1e-8
WEIGHT_DECAY = 0.1
NORM_EPS = 1e-6
CONTRACT_LAST = (((1,), (1,)), ((), ()))
BLOCK = 128
N_GROUP = 8
N_PIECE = 32
LEAD = (2, 7)
HELD = 3


def update_body(skip, carry, half_ref, rate_ref, clip_ref, w_ref, m_ref, v_ref, g_ref, *refs):
    outs = refs[skip:]
    if carry:
        outs[-1][...] = refs[skip - 1][...]
        outs = outs[:-1]
    ow_ref, om_ref, ov_ref = outs[:3]
    rate = rate_ref[0]
    grad = clip_ref[0:1] * g_ref[...]
    weight = w_ref[...]
    mom = BETA_ONE * m_ref[...] + (1.0 - BETA_ONE) * grad
    sec = BETA_TWO * v_ref[...] + (1.0 - BETA_TWO) * grad * grad
    one_corr = 1.0 - BETA_ONE**ADAM_STEP
    two_corr = 1.0 - BETA_TWO**ADAM_STEP
    direction = (mom * (1.0 / one_corr)) / (jnp.sqrt(sec * (1.0 / two_corr)) + ADAM_EPS)
    new = weight - rate * (direction + WEIGHT_DECAY * weight)
    ow_ref[...] = new
    om_ref[...] = mom
    ov_ref[...] = sec
    if len(outs) == 4:
        outs[3][...] = new.astype(jnp.bfloat16)


def step_of(rows):
    return BLOCK if rows % BLOCK == 0 else BLOCK // 2


def update_call(half, rate, clip, weights, grad, full_map, previous, after=(), carry=()):
    rows, cols = grad.shape
    block = step_of(rows)
    shape = weights[0].shape
    spec = pl.BlockSpec((block, cols), full_map)
    flat = pl.BlockSpec((block, cols), lambda i, h, r: (i, 0))
    anywhere = pl.BlockSpec(memory_space=pl.ANY)
    first = previous is None
    extra = list(previous or ()) + list(after)
    passed = [pl.BlockSpec((1,) + value.shape[1:], lambda i, h, r: (i, 0, 0)) for value in carry]
    return pl.pallas_call(
        functools.partial(update_body, len(extra) + len(carry), len(carry)),
        grid_spec=pltpu.PrefetchScalarGridSpec(
            num_scalar_prefetch=2,
            grid=(rows // block,),
            in_specs=[pl.BlockSpec(clip.shape, lambda i, h, r: (0, 0)), spec, spec, spec, flat] + [anywhere] * len(extra) + passed,
            out_specs=[spec] * 3 + [flat] * first + passed,
        ),
        out_shape=[jax.ShapeDtypeStruct(shape, jnp.float32)] * 3 + [jax.ShapeDtypeStruct(grad.shape, jnp.bfloat16)] * first + [jax.ShapeDtypeStruct(value.shape, value.dtype) for value in carry],
        input_output_aliases={7 + i: i for i in range(len(previous or ()))},
        cost_estimate=pl.CostEstimate(flops=60 * rows * cols, bytes_accessed=30 * rows * cols, transcendentals=0),
        compiler_params=pltpu.CompilerParams(vmem_limit_bytes=67043328),
        name="adamw_half",
    )(half, rate, clip, *weights, grad, *extra, *carry)


def backward_body(n_stage, n_raw, bounds_up, bounds_down, gu_ref, gd_ref, wu_ref, wd_ref, acts_ref, gout_ref, x_ref, max_ref, *refs):
    n_up = len(bounds_up) - 1
    outs_up = refs[:n_up]
    whole_up, whole_down, far_ref, x_far, clip_ref = refs[n_up:n_up + 5]
    (up_bf, down_bf, st_up, st_down, acc_up, acc_down, got_up, got_down, fold, hid, slope, grad_pre, gbuf, outbox, landed, ready, rows_a, rows_z, norm_box, norm_pair,
     st_sem, loc_sem, fold_sem, own_sem, out_sem, g_rsem, trade_sem, pass_ssem, rs_ssem, rs_rsem, row_ssem, row_rsem, far_sem, norm_ssem, norm_rsem, x_land, x_sem, xf_ssem, xf_rsem, go_sem) = refs[n_up + 5:]
    model, data, stage = lax.axis_index('model'), lax.axis_index('data'), lax.axis_index('stage')
    mesh_id = pl.DeviceIdType.MESH
    last = n_stage - 1
    d_model, ff_half = acc_up.shape
    half = d_model // 2
    n_row = acts_ref.shape[0]
    n_up_chunk, n_down_chunk = d_model // BLOCK, ff_half // BLOCK
    peer = {'data': 1 - data}
    near = pl.ds(pl.multiple_of(model * half, half), half)
    far = pl.ds(pl.multiple_of((1 - model) * half, half), half)
    own_cols = pl.ds(pl.multiple_of(data * ff_half, ff_half), ff_half)
    peer_cols = pl.ds(pl.multiple_of((1 - data) * ff_half, ff_half), ff_half)
    own_rows = pl.ds(pl.multiple_of(data * n_row, n_row), n_row)
    first_dims = (((0,), (0,)), ((), ()))

    def remote(src, dst, ssem, rsem, where):
        return pltpu.make_async_remote_copy(src_ref=src, dst_ref=dst, send_sem=ssem, recv_sem=rsem, device_id=where, device_id_type=mesh_id)

    barrier = pltpu.get_barrier_semaphore()
    group = [(dm, ds) for dm in range(2) for ds in range(n_stage) if dm or ds]
    where = [{'model': lax.rem(model + dm, 2), 'stage': lax.rem(stage + ds, n_stage)} for dm, ds in group]
    for target in where + [peer]:
        pl.semaphore_signal(barrier, inc=1, device_id=target, device_id_type=mesh_id)

    n_st_up, n_st_down = d_model // st_up.shape[1], 2 * ff_half // st_down.shape[1]

    def load_up(r):
        return pltpu.make_async_copy(wu_ref.at[pl.ds(r * st_up.shape[1], st_up.shape[1])], st_up.at[r % 2], st_sem.at[0, r % 2])

    def load_down(r):
        return pltpu.make_async_copy(wd_ref.at[pl.ds(r * st_down.shape[1], st_down.shape[1])], st_down.at[r % 2], st_sem.at[1, r % 2])

    load_acts = pltpu.make_async_copy(acts_ref, rows_a.at[own_rows], loc_sem.at[0])
    load_acts.start()
    load_up(0).start()
    load_up(1).start()
    load_down(0).start()
    load_down(1).start()

    def load_g(c):
        return pltpu.make_async_copy(gout_ref.at[:, pl.ds(c * half, half)], gbuf.at[c], loc_sem.at[1 + c])

    @pl.when(stage == last)
    def _():
        for c in range(2):
            load_g(c).start()

    pl.semaphore_wait(barrier, len(where) + 1)

    def chunk(k):
        return pl.ds(k * BLOCK, BLOCK)

    raw = [remote(gu_ref.at[chunk(k), peer_cols], got_up.at[chunk(k)], rs_ssem.at[0, k], rs_rsem.at[0, k], peer) for k in range(n_up_chunk)]
    carries_x = stage >= n_stage // 2

    def micro(i):
        return 2 * (stage - n_stage // 2) + i

    def send_x(i):
        return remote(x_ref.at[micro(i), :, near], x_land.at[i], x_sem.at[0, i], x_sem.at[1, i], peer)

    @pl.when(carries_x)
    def _():
        for i in range(2):
            send_x(i).start()

    for copy in raw:
        copy.start()
    send_a = remote(acts_ref, rows_a.at[own_rows], row_ssem.at[0], row_rsem.at[0], peer)
    send_a.start()

    for r in range(n_st_up):
        load_up(r).wait()
        up_bf[pl.ds(r * st_up.shape[1], st_up.shape[1])] = st_up[r % 2].astype(jnp.bfloat16)
        if r + 2 < n_st_up:
            load_up(r + 2).start()
    load_acts.wait()

    tile = 256
    n_tile = hid.shape[1] // tile
    scale = 0.7978845608028654
    cubic = 0.044715

    def pre_tile(j, carry):
        cols = pl.ds(pl.multiple_of(j * tile, tile), tile)
        pre = jnp.dot(rows_a[own_rows], up_bf[:, cols], preferred_element_type=jnp.float32)
        square = pre * pre
        bend = jnp.tanh(scale * (pre + cubic * square * pre))
        hid[:, cols] = (pre * (0.5 * (1.0 + bend))).astype(jnp.bfloat16)
        slope[:, cols] = 0.5 * (1.0 + bend) + 0.5 * pre * (1.0 - bend * bend) * (scale * (1.0 + 3.0 * cubic * square))
        return carry

    lax.fori_loop(0, n_tile, pre_tile, 0)

    for r in range(n_st_down):
        load_down(r).wait()
        down_bf[pl.ds(r * st_down.shape[1], st_down.shape[1])] = st_down[r % 2].astype(jnp.bfloat16)
        if r + 2 < n_st_down:
            load_down(r + 2).start()

    own_up = pltpu.make_async_copy(gu_ref.at[:, own_cols], acc_up, own_sem.at[0])
    own_down = pltpu.make_async_copy(gd_ref.at[own_cols], acc_down, own_sem.at[1])
    load_fold = pltpu.make_async_copy(gd_ref.at[peer_cols], fold, fold_sem)
    load_fold.start()
    own_up.start()
    own_down.start()

    @pl.when(stage == last)
    def _():
        for c in range(2):
            load_g(c).wait()

    @pl.when(stage < last)
    def _():
        for c in range(2):
            remote(ready, gbuf.at[c], pass_ssem.at[0], g_rsem.at[c], {'model': model}).wait_recv()

    def slope_tile(j, carry):
        cols = pl.ds(pl.multiple_of(j * tile, tile), tile)
        grad = lax.dot_general(gbuf[0], down_bf[cols, :half], CONTRACT_LAST, preferred_element_type=jnp.float32)
        grad = grad + lax.dot_general(gbuf[1], down_bf[cols, half:], CONTRACT_LAST, preferred_element_type=jnp.float32)
        grad_pre[:, cols] = (slope[:, cols] * grad).astype(jnp.bfloat16)
        return carry

    lax.fori_loop(0, n_tile, slope_tile, 0)

    trade = remote(outbox, landed, trade_sem.at[0], trade_sem.at[1], {'model': 1 - model})

    def hand_on(to):
        return remote(ready, gbuf.at[model], pass_ssem.at[to], g_rsem.at[model], {'model': to, 'stage': stage - 1})

    @pl.when(stage > 0)
    def _():
        outbox[...] = lax.dot_general(grad_pre[...], up_bf[far], CONTRACT_LAST, preferred_element_type=jnp.float32)
        trade.start()
        mine = lax.dot_general(grad_pre[...], up_bf[near], CONTRACT_LAST, preferred_element_type=jnp.float32)
        trade.wait_recv()
        ready[...] = (gbuf[model].astype(jnp.float32) + (mine + landed[...])).astype(jnp.bfloat16)
        for to in range(2):
            hand_on(to).start()

    rows_z[own_rows] = grad_pre[:, own_cols]
    send_z = remote(grad_pre.at[:, peer_cols], rows_z.at[own_rows], row_ssem.at[1], row_rsem.at[1], peer)
    send_z.start()

    def forward_x(i, to):
        return remote(x_land.at[i], x_far.at[micro(i), :, near], xf_ssem.at[i, to], xf_rsem.at[micro(i), model], {'model': to, 'stage': 0})

    @pl.when(carries_x)
    def _():
        for i in range(2):
            send_x(i).wait_recv()
            for to in range(2):
                forward_x(i, to).start()

    def down_product(k, side):
        cols = pl.ds(pl.multiple_of(side * ff_half + k * BLOCK, BLOCK), BLOCK)
        left = hid[:, cols]
        return [lax.dot_general(left, gbuf[c], first_dims, preferred_element_type=jnp.float32) for c in range(2)]

    load_fold.wait()

    def send_fold(k):
        rows = pl.ds(pl.multiple_of(k * BLOCK, BLOCK), BLOCK)
        return remote(fold.at[rows], got_down.at[rows], rs_ssem.at[1, k], rs_rsem.at[1, k], peer)

    def fold_step(k, carry):
        rows = pl.ds(pl.multiple_of(k * BLOCK, BLOCK), BLOCK)
        low, high = down_product(k, 1 - data)
        fold[rows, :half] += low
        fold[rows, half:] += high
        send_fold(k).start()
        return carry

    lax.fori_loop(0, n_down_chunk, fold_step, 0)
    own_down.wait()

    def own_step(k, carry):
        rows = pl.ds(pl.multiple_of(k * BLOCK, BLOCK), BLOCK)
        low, high = down_product(k, data)
        acc_down[rows, :half] += low
        acc_down[rows, half:] += high
        return carry

    lax.fori_loop(0, n_down_chunk, own_step, 0)

    @pl.when(stage > 0)
    def _():
        trade.wait_send()
        for to in range(2):
            hand_on(to).wait_send()

    own_up.wait()
    send_a.wait_recv()
    squares = jnp.zeros((8, ff_half), jnp.float32)

    def fold_squares(mean):
        return jnp.sum((mean * mean).reshape(-1, 8, mean.shape[1]), axis=0)

    def put(acc, bounds, outs, whole, sem_row):
        copies = []
        for i, (lo, hi) in enumerate(bounds):
            rows = pl.ds(lo, hi - lo)
            copies.append(pltpu.make_async_copy(acc.at[rows], whole.at[rows], out_sem.at[sem_row, i]))
            if outs[i] is not None:
                copies.append(pltpu.make_async_copy(acc.at[rows], outs[i], out_sem.at[sem_row, len(bounds) + i]))
        return copies

    def put_start(k, bounds, copies, outs):
        at = 0
        for i, (lo, hi) in enumerate(bounds):
            count = 1 if outs[i] is None else 2
            if k * BLOCK < hi <= (k + 1) * BLOCK:
                for copy in copies[at:at + count]:
                    copy.start()
            at += count

    outs_up = (None,) + tuple(outs_up)
    outs_down = (None,) * len(bounds_down)
    put_up = put(acc_up, bounds_up, outs_up, whole_up, 0)
    put_down = put(acc_down, bounds_down, outs_down, whole_down, 1)
    for k in range(n_up_chunk):
        raw[k].wait_recv()
        if k == 0:
            send_z.wait_recv()
        product = lax.dot_general(rows_a[:, k * BLOCK:(k + 1) * BLOCK], rows_z[...], first_dims, preferred_element_type=jnp.float32)
        mean = (acc_up[chunk(k)] + got_up[chunk(k)] + product) * 0.5
        acc_up[chunk(k)] = mean
        squares = squares + fold_squares(mean)
        put_start(k, bounds_up, put_up, outs_up)
    n_far = far_sem.shape[1]
    slab = bounds_up[0][1] // n_far
    is_even = lax.rem(stage, 2) == 0

    def send_far(i):
        span = pl.ds(pl.multiple_of(i * slab, slab), slab)
        return remote(acc_up.at[span], far_ref.at[span], far_sem.at[0, i], far_sem.at[1, i], peer)

    for i in range(n_far - HELD):
        send_far(i).start()

    @pl.when(is_even)
    def _():
        for i in range(n_far - HELD, n_far):
            send_far(i).start()

    for k in range(n_down_chunk):
        send_fold(k).wait_recv()
        mean = (acc_down[chunk(k)] + got_down[chunk(k)]) * 0.5
        acc_down[chunk(k)] = mean
        squares = squares + fold_squares(mean)
        put_start(k, bounds_down, put_down, outs_down)

    lanes = norm_box.shape[2]
    part = squares[:, :lanes]
    for j in range(1, ff_half // lanes):
        part = part + squares[:, j * lanes:(j + 1) * lanes]
    me = model * n_stage + stage
    norm_box[me] = part

    def spread(i):
        return remote(norm_box.at[me], norm_box.at[me], norm_ssem.at[i], norm_rsem.at[me], where[i])

    for i in range(len(group)):
        spread(i).start()
    for i, (dm, ds) in enumerate(group):
        them = lax.rem(model + dm, 2) * n_stage + lax.rem(stage + ds, n_stage)
        remote(norm_box.at[me], norm_box.at[them], norm_ssem.at[i], norm_rsem.at[them], where[i]).wait_recv()
    total = norm_box[0]
    for i in range(1, 2 * n_stage):
        total = total + norm_box[i]
    norm_pair[0] = total
    swap = remote(norm_pair.at[0], norm_pair.at[1], norm_ssem.at[len(group)], norm_rsem.at[2 * n_stage], peer)
    swap.start()
    swap.wait_recv()
    norm_sq = jnp.sum(norm_pair[0] + norm_pair[1], axis=(0, 1), keepdims=True)
    norm = jnp.sqrt(jnp.broadcast_to(norm_sq, clip_ref.shape)) + NORM_EPS
    clip_ref[...] = jnp.minimum(1.0, max_ref[0] / norm)

    @pl.when(carries_x)
    def _():
        for i in range(2):
            send_x(i).wait_send()
            for to in range(2):
                forward_x(i, to).wait_send()

    @pl.when(stage == 0)
    def _():
        for s in range(n_stage):
            for m in range(2):
                remote(x_land.at[0], x_far.at[s, :, pl.ds(m * half, half)], xf_ssem.at[0, m], xf_rsem.at[s, m], {'model': model}).wait_recv()

    swap.wait_send()
    for i in range(len(group)):
        spread(i).wait_send()
    for copy in raw + [send_a, send_z]:
        copy.wait_send()
    for k in range(n_down_chunk):
        send_fold(k).wait_send()
    for copy in put_up + put_down:
        copy.wait()

    @pl.when(is_even)
    def _():
        for i in range(n_far):
            send_far(i).wait_send()
        pl.semaphore_signal(go_sem, inc=1, device_id={'stage': stage + 1}, device_id_type=mesh_id)

    @pl.when(jnp.logical_not(is_even))
    def _():
        pl.semaphore_wait(go_sem, 1)
        for i in range(n_far - HELD, n_far):
            send_far(i).start()
        for i in range(n_far):
            send_far(i).wait_send()

    for i in range(n_far):
        send_far(i).wait_recv()


def backward_call(n_stage, bounds_up, bounds_down, g_up, g_down, w_up, w_down, acts, grad_out, x_next, max_norm):
    d_model, ff_local = g_up.shape
    ff_half, half, n_row = ff_local // 2, d_model // 2, acts.shape[0]
    dma = pltpu.SemaphoreType.DMA
    anywhere = pl.BlockSpec(memory_space=pl.ANY)
    f32, bf16 = jnp.float32, jnp.bfloat16
    shapes = [jax.ShapeDtypeStruct((hi - lo, ff_half), f32) for lo, hi in bounds_up[1:]]
    shapes += [jax.ShapeDtypeStruct((d_model, ff_half), f32), jax.ShapeDtypeStruct((ff_half, d_model), f32)]
    shapes += [jax.ShapeDtypeStruct((bounds_up[0][1], ff_half), f32), jax.ShapeDtypeStruct(x_next.shape, bf16), jax.ShapeDtypeStruct((8, ff_half), f32)]
    n_chunk = max(d_model, ff_half) // BLOCK
    return pl.pallas_call(
        functools.partial(backward_body, n_stage, n_chunk, bounds_up, bounds_down),
        out_shape=shapes,
        in_specs=[anywhere] * 7 + [pl.BlockSpec(memory_space=pltpu.SMEM)],
        out_specs=[anywhere] * (len(shapes) - 1) + [pl.BlockSpec(memory_space=pltpu.VMEM)],
        scratch_shapes=[
            pltpu.VMEM((d_model, ff_local), bf16),
            pltpu.VMEM((ff_local, d_model), bf16),
            pltpu.VMEM((2, 256, ff_local), f32),
            pltpu.VMEM((2, 512, d_model), f32),
            pltpu.VMEM((d_model, ff_half), f32),
            pltpu.VMEM((ff_half, d_model), f32),
            pltpu.VMEM((d_model, ff_half), f32),
            pltpu.VMEM((ff_half, d_model), f32),
            pltpu.VMEM((ff_half, d_model), f32),
            pltpu.VMEM((n_row, ff_local), bf16),
            pltpu.VMEM((n_row, ff_local), f32),
            pltpu.VMEM((n_row, ff_local), bf16),
            pltpu.VMEM((2, n_row, half), bf16),
            pltpu.VMEM((n_row, half), f32),
            pltpu.VMEM((n_row, half), f32),
            pltpu.VMEM((n_row, half), bf16),
            pltpu.VMEM((2 * n_row, d_model), bf16),
            pltpu.VMEM((2 * n_row, ff_half), bf16),
            pltpu.VMEM((2 * n_stage, 8, 128), f32),
            pltpu.VMEM((2, 8, 128), f32),
            dma((2, 2)),
            dma((3,)),
            dma(()),
            dma((2,)),
            dma((2, max(2 * len(bounds_up), len(bounds_down)))),
            dma((2,)),
            dma((2,)),
            dma((2,)),
            dma((2, n_chunk)),
            dma((2, n_chunk)),
            dma((2,)),
            dma((2,)),
            dma((2, 8)),
            dma((2 * n_stage,)),
            dma((2 * n_stage + 1,)),
            pltpu.VMEM((2, n_row, half), bf16),
            dma((2, 2)),
            dma((2, 2)),
            dma((n_stage, 2)),
            pltpu.SemaphoreType.REGULAR,
        ],
        compiler_params=pltpu.CompilerParams(collective_id=0, has_side_effects=True, vmem_limit_bytes=67043328),
        name="reduce_and_norm",
    )(g_up, g_down, w_up, w_down, acts, grad_out, x_next, max_norm)


def forward_body(n_stage, lead, x_ref, xf_ref, up_ref, down_ref, mean_ref, y_ref, far_ref, inbox, hid, mine, zout, zin, keep, yout, yin, done, x_sem, in_sem, z_ssem, z_rsem, s_ssem, s_rsem, r_ssem, r_rsem, pass_ssem, y_ssem, y_rsem, piece_ssem, piece_rsem, go_sem):
    model, data, stage = lax.axis_index('model'), lax.axis_index('data'), lax.axis_index('stage')
    mesh_id = pl.DeviceIdType.MESH
    last = n_stage - 1
    n_group, _, rows2, half = inbox.shape
    rows = rows2 // 2
    n_piece = piece_ssem.shape[0]
    piece = mean_ref.shape[0] // n_piece
    peer = {'data': 1 - data}
    near = pl.ds(pl.multiple_of(model * half, half), half)
    far = pl.ds(pl.multiple_of((1 - model) * half, half), half)
    own_rows = pl.ds(pl.multiple_of(data * rows, rows), rows)
    peer_rows = pl.ds(pl.multiple_of((1 - data) * rows, rows), rows)

    def remote(src, dst, ssem, rsem, where):
        return pltpu.make_async_remote_copy(src_ref=src, dst_ref=dst, send_sem=ssem, recv_sem=rsem, device_id=where, device_id_type=mesh_id)

    barrier = pltpu.get_barrier_semaphore()
    group = [(dm, ds) for dm in range(2) for ds in range(n_stage) if dm or ds]
    where = [{'model': lax.rem(model + dm, 2), 'stage': lax.rem(stage + ds, n_stage)} for dm, ds in group]
    for target in where + [peer]:
        pl.semaphore_signal(barrier, inc=1, device_id=target, device_id_type=mesh_id)

    def load_x(b, c, from_ref, to_rows, i):
        return pltpu.make_async_copy(from_ref.at[b, :, pl.ds(c * half, half)], inbox.at[b, c, to_rows], x_sem.at[b, c, i])

    def loads(b):
        return [load_x(b, c, *pair) for c in range(2) for pair in ((x_ref, own_rows, 0), (xf_ref, peer_rows, 1))]

    @pl.when(stage == 0)
    def _():
        for b in range(n_group):
            for copy in loads(b):
                copy.start()

    pl.semaphore_wait(barrier, len(where) + 1)

    def send_piece(p):
        span = pl.ds(pl.multiple_of(p * piece, piece), piece)
        return remote(mean_ref.at[span], far_ref.at[span], piece_ssem.at[p], piece_rsem.at[p], peer)

    def start_pieces(low, high):
        def one(p, carry):
            send_piece(p).start()
            return carry

        lax.fori_loop(low, high, one, 0)

    n_turn = n_group + 3
    base, slope = lead
    begin = base + slope * stage
    is_even = lax.rem(stage, 2) == 0
    limit = n_piece - HELD * lax.rem(stage, 2)
    start_pieces(0, begin)

    def arrival(b, c):
        return remote(done.at[b], inbox.at[b, c], pass_ssem.at[b, 0], in_sem.at[b, c], {'model': model})

    def trade_z(b):
        return remote(zout.at[b], zin.at[b], z_ssem.at[b], z_rsem.at[b], {'model': 1 - model})

    def trade_s(b):
        return remote(yout.at[b], yin.at[b], s_ssem.at[b], s_rsem.at[b], peer)

    def trade_r(b):
        return remote(done.at[b, own_rows], done.at[b, own_rows], r_ssem.at[b], r_rsem.at[b], peer)

    def hand_on(b, to):
        return remote(done.at[b], inbox.at[b, model], pass_ssem.at[b, to], in_sem.at[b, model], {'model': to, 'stage': stage + 1})

    def landing(b, c):
        return y_ref.at[b, :, pl.ds(pl.multiple_of(c * half, half), half)]

    def publish(b, k):
        return remote(done.at[b, own_rows], landing(b, model), y_ssem.at[b, k], y_rsem.at[b, model], where[k])

    def y_arrival(b, c):
        return remote(done.at[b, own_rows], landing(b, c), y_ssem.at[b, 0], y_rsem.at[b, c], {'model': model})

    def turn(t, carry):
        @pl.when(t < n_group)
        def _():
            @pl.when(stage == 0)
            def _():
                for copy in loads(t):
                    copy.wait()

            @pl.when(stage > 0)
            def _():
                for c in range(2):
                    arrival(t, c).wait_recv()

            pre = jnp.dot(inbox[t, 0], up_ref[:half], preferred_element_type=jnp.float32)
            pre = pre + jnp.dot(inbox[t, 1], up_ref[half:], preferred_element_type=jnp.float32)
            hid[...] = jax.nn.gelu(pre).astype(jnp.bfloat16)
            zout[t] = jnp.dot(hid[...], down_ref[:, far], preferred_element_type=jnp.float32)
            trade_z(t).start()
            mine[t] = jnp.dot(hid[...], down_ref[:, near], preferred_element_type=jnp.float32)

        @pl.when((t >= 1) & (t < n_group + 1))
        def _():
            b = t - 1
            trade_z(b).wait_recv()
            yout[b] = mine[b, peer_rows] + zin[b, peer_rows]
            trade_s(b).start()
            keep[b] = mine[b, own_rows] + zin[b, own_rows]

        @pl.when((t >= 2) & (t < n_group + 2))
        def _():
            b = t - 2
            trade_s(b).wait_recv()
            total = inbox[b, model, own_rows].astype(jnp.float32) + (keep[b] + yin[b])
            result = total.astype(jnp.bfloat16)
            done[b, own_rows] = result

            @pl.when(stage < last)
            def _():
                trade_r(b).start()

            @pl.when(stage == last)
            def _():
                y_ref[b, :, near] = result
                for k in range(len(group)):
                    publish(b, k).start()

        @pl.when((t >= 3) & (stage < last))
        def _():
            b = t - 3
            remote(done.at[b, own_rows], done.at[b, peer_rows], r_ssem.at[b], r_rsem.at[b], peer).wait_recv()
            for to in range(2):
                hand_on(b, to).start()

        @pl.when(begin + t < limit)
        def _():
            send_piece(begin + t).start()

        return carry

    lax.fori_loop(0, n_turn, turn, 0)
    start_pieces(jnp.minimum(begin + n_turn, limit), limit)

    for b in range(n_group):
        trade_z(b).wait_send()
        trade_s(b).wait_send()

    @pl.when(stage < last)
    def _():
        for b in range(n_group):
            trade_r(b).wait_send()
            for to in range(2):
                hand_on(b, to).wait_send()
            for c in range(2):
                y_arrival(b, c).wait_recv()

    @pl.when(stage == last)
    def _():
        for b in range(n_group):
            for k in range(len(group)):
                publish(b, k).wait_send()
            y_arrival(b, 1 - model).wait_recv()

    def sent(p, carry):
        send_piece(p).wait_send()
        return carry

    def landed(p, carry):
        send_piece(p).wait_recv()
        return carry

    lax.fori_loop(0, limit, sent, 0)

    @pl.when(is_even)
    def _():
        pl.semaphore_signal(go_sem, inc=1, device_id={'stage': stage + 1}, device_id_type=mesh_id)

    @pl.when(jnp.logical_not(is_even))
    def _():
        pl.semaphore_wait(go_sem, 1)
        start_pieces(limit, n_piece)
        lax.fori_loop(limit, n_piece, sent, 0)

    lax.fori_loop(0, n_piece, landed, 0)


def forward_call(n_stage, n_group, n_piece, lead, x_next, x_far, up_bf, down_bf, mean):
    d_model = x_next.shape[2]
    x_next, x_far = [value.reshape(n_group, -1, d_model) for value in (x_next, x_far)]
    rows, half, ff_half = x_next.shape[1], d_model // 2, up_bf.shape[1]
    dma = pltpu.SemaphoreType.DMA
    f32, bf16 = jnp.float32, jnp.bfloat16
    in_vmem = pl.BlockSpec(memory_space=pltpu.VMEM)
    anywhere = pl.BlockSpec(memory_space=pl.ANY)
    return pl.pallas_call(
        functools.partial(forward_body, n_stage, lead),
        out_shape=[jax.ShapeDtypeStruct(x_next.shape, bf16), jax.ShapeDtypeStruct(mean.shape, f32)],
        in_specs=[anywhere, anywhere, in_vmem, in_vmem, anywhere],
        out_specs=[in_vmem, anywhere],
        scratch_shapes=[
            pltpu.VMEM((n_group, 2, 2 * rows, half), bf16),
            pltpu.VMEM((2 * rows, ff_half), bf16),
            pltpu.VMEM((n_group, 2 * rows, half), f32),
            pltpu.VMEM((n_group, 2 * rows, half), f32),
            pltpu.VMEM((n_group, 2 * rows, half), f32),
            pltpu.VMEM((n_group, rows, half), f32),
            pltpu.VMEM((n_group, rows, half), f32),
            pltpu.VMEM((n_group, rows, half), f32),
            pltpu.VMEM((n_group, 2 * rows, half), bf16),
            dma((n_group, 2, 2)),
            dma((n_group, 2)),
            dma((n_group,)),
            dma((n_group,)),
            dma((n_group,)),
            dma((n_group,)),
            dma((n_group,)),
            dma((n_group,)),
            dma((n_group, 2)),
            dma((n_group, 2 * n_stage - 1)),
            dma((n_group, 2)),
            dma((n_piece,)),
            dma((n_piece,)),
            pltpu.SemaphoreType.REGULAR,
        ],
        compiler_params=pltpu.CompilerParams(collective_id=1, has_side_effects=True, vmem_limit_bytes=67043328),
        name="forward_pipe",
    )(x_next, x_far, up_bf, down_bf, mean)


def solution(mesh):
    n_stage = mesh.shape['stage']
    swap = [(0, 1), (1, 0)]
    up_spec = P('stage', None, 'model')
    down_spec = P('stage', 'model', None)
    row_spec = P(None, 'data', None)
    in_specs = (up_spec, down_spec, up_spec, down_spec, up_spec, down_spec, P('data', 'stage', None, 'model'), P('data', 'stage', 'model', None), P('stage', 'data', None), P('data', None), row_spec, P(None), P(None))
    out_specs = (up_spec, down_spec, up_spec, down_spec, up_spec, down_spec, row_spec)

    def device_step(w_up, w_down, m_up, m_down, v_up, v_down, g_up, g_down, acts_last, grad_out, x_next, learn_rate, max_norm):
        data_id = lax.axis_index('data')
        half = data_id.astype(jnp.int32).reshape(1)
        other = (1 - half).astype(jnp.int32)
        d_model, ff_local = w_up.shape[1:]
        ff_half = ff_local // 2
        bounds_up = ((0, 256), (256, 640), (640, 960), (960, d_model))
        bounds_down = ((0, ff_half // 2), (ff_half // 2, ff_half))

        def trade(value):
            return lax.ppermute(value, 'data', swap)

        early, *late, whole_up, whole_down, far_first, x_far, clip = backward_call(n_stage, bounds_up, bounds_down, g_up[0, 0], g_down[0, 0], w_up[0], w_down[0], acts_last[0], grad_out, x_next, max_norm)
        ups = (w_up[0], m_up[0], v_up[0])
        downs = (w_down[0], m_down[0], v_down[0])

        def map_up(low, high):
            return lambda i, h, r: (low // step_of(high - low) + i, h[0])

        def map_down(i, h, r):
            return h[0] * (ff_half // step_of(ff_half)) + i, 0

        far_early = trade(early)
        *new_up, up_bf = update_call(half, learn_rate, clip, ups, whole_up, map_up(0, d_model), None)
        *new_down, down_bf = update_call(half, learn_rate, clip, downs, whole_down, map_down, None, (up_bf,))
        y_next, far_down = forward_call(n_stage, N_GROUP, N_PIECE, LEAD, x_next, x_far, up_bf, down_bf, whole_down)
        late, far_down = lax.optimization_barrier((late, far_down))
        fars = [far_first, far_early] + [trade(value) for value in late]
        *new_down, y_next = update_call(other, learn_rate, clip, downs, far_down, map_down, new_down, (), (y_next,))
        y_next = y_next.reshape(x_next.shape)
        for bounds, part in zip(bounds_up, fars):
            new_up = update_call(other, learn_rate, clip, ups, part, map_up(*bounds), new_up)
        return (new_up[0][None], new_down[0][None], new_up[1][None], new_down[1][None], new_up[2][None], new_down[2][None], y_next)

    return jax.shard_map(device_step, mesh=mesh, in_specs=in_specs, out_specs=out_specs, check_vma=False)
```

```python
import functools

import jax
import jax.numpy as jnp
from jax import lax
from jax.experimental import pallas as pl
from jax.experimental.pallas import tpu as pltpu
from jax.sharding import PartitionSpec as P

ADAM_STEP = 10
BETA_ONE = 0.9
BETA_TWO = 0.95
ADAM_EPS = 1e-8
WEIGHT_DECAY = 0.1
NORM_EPS = 1e-6
CONTRACT_LAST = (((1,), (1,)), ((), ()))
BLOCK = 128
N_GROUP = 8
N_PIECE = 32
LEAD = (2, 7)
HELD = 3
N_RAW = 4


def update_body(skip, carry, half_ref, rate_ref, clip_ref, w_ref, m_ref, v_ref, g_ref, *refs):
    outs = refs[skip:]
    if carry:
        outs[-1][...] = refs[skip - 1][...]
        outs = outs[:-1]
    ow_ref, om_ref, ov_ref = outs[:3]
    rate = rate_ref[0]
    grad = clip_ref[0:1] * g_ref[...]
    weight = w_ref[...]
    mom = BETA_ONE * m_ref[...] + (1.0 - BETA_ONE) * grad
    sec = BETA_TWO * v_ref[...] + (1.0 - BETA_TWO) * grad * grad
    one_corr = 1.0 - BETA_ONE**ADAM_STEP
    two_corr = 1.0 - BETA_TWO**ADAM_STEP
    direction = (mom * (1.0 / one_corr)) / (jnp.sqrt(sec * (1.0 / two_corr)) + ADAM_EPS)
    new = weight - rate * (direction + WEIGHT_DECAY * weight)
    ow_ref[...] = new
    om_ref[...] = mom
    ov_ref[...] = sec
    if len(outs) == 4:
        outs[3][...] = new.astype(jnp.bfloat16)


def step_of(low, high):
    return BLOCK if low % BLOCK == 0 and high % BLOCK == 0 else BLOCK // 2


def update_call(half, rate, clip, weights, grad, full_map, previous, after=(), carry=(), block=BLOCK):
    rows, cols = grad.shape
    shape = weights[0].shape
    spec = pl.BlockSpec((block, cols), full_map)
    flat = pl.BlockSpec((block, cols), lambda i, h, r: (i, 0))
    anywhere = pl.BlockSpec(memory_space=pl.ANY)
    first = previous is None
    extra = list(previous or ()) + list(after)
    passed = [pl.BlockSpec((1,) + value.shape[1:], lambda i, h, r: (i, 0, 0)) for value in carry]
    return pl.pallas_call(
        functools.partial(update_body, len(extra) + len(carry), len(carry)),
        grid_spec=pltpu.PrefetchScalarGridSpec(
            num_scalar_prefetch=2,
            grid=(rows // block,),
            in_specs=[pl.BlockSpec(clip.shape, lambda i, h, r: (0, 0)), spec, spec, spec, flat] + [anywhere] * len(extra) + passed,
            out_specs=[spec] * 3 + [flat] * first + passed,
        ),
        out_shape=[jax.ShapeDtypeStruct(shape, jnp.float32)] * 3 + [jax.ShapeDtypeStruct(grad.shape, jnp.bfloat16)] * first + [jax.ShapeDtypeStruct(value.shape, value.dtype) for value in carry],
        input_output_aliases={7 + i: i for i in range(len(previous or ()))},
        cost_estimate=pl.CostEstimate(flops=60 * rows * cols, bytes_accessed=30 * rows * cols, transcendentals=0),
        compiler_params=pltpu.CompilerParams(vmem_limit_bytes=67043328),
        name="adamw_half",
    )(half, rate, clip, *weights, grad, *extra, *carry)


def backward_body(n_stage, n_raw, bounds_up, bounds_down, gu_ref, gd_ref, wu_ref, wd_ref, acts_ref, gout_ref, x_ref, max_ref, *refs):
    n_up = len(bounds_up) - 1
    outs_up = refs[:n_up]
    whole_up, whole_down, far_ref, x_far, clip_ref = refs[n_up:n_up + 5]
    (up_bf, down_bf, st_up, st_down, acc_up, acc_down, got_up, got_down, fold, hid, slope, grad_pre, gbuf, outbox, landed, ready, rows_a, rows_z, norm_box, norm_pair,
     st_sem, loc_sem, fold_sem, own_sem, out_sem, g_rsem, trade_sem, pass_ssem, rs_ssem, rs_rsem, row_ssem, row_rsem, far_sem, norm_ssem, norm_rsem, x_land, x_sem, xf_ssem, xf_rsem, go_sem, fold_up, fold_up_sem) = refs[n_up + 5:]
    model, data, stage = lax.axis_index('model'), lax.axis_index('data'), lax.axis_index('stage')
    mesh_id = pl.DeviceIdType.MESH
    last = n_stage - 1
    d_model, ff_half = acc_up.shape
    half = d_model // 2
    n_row = acts_ref.shape[0]
    n_up_chunk, n_down_chunk = d_model // BLOCK, ff_half // BLOCK
    peer = {'data': 1 - data}
    near = pl.ds(pl.multiple_of(model * half, half), half)
    far = pl.ds(pl.multiple_of((1 - model) * half, half), half)
    own_cols = pl.ds(pl.multiple_of(data * ff_half, ff_half), ff_half)
    peer_cols = pl.ds(pl.multiple_of((1 - data) * ff_half, ff_half), ff_half)
    own_rows = pl.ds(pl.multiple_of(data * n_row, n_row), n_row)
    first_dims = (((0,), (0,)), ((), ()))

    def remote(src, dst, ssem, rsem, where):
        return pltpu.make_async_remote_copy(src_ref=src, dst_ref=dst, send_sem=ssem, recv_sem=rsem, device_id=where, device_id_type=mesh_id)

    barrier = pltpu.get_barrier_semaphore()
    group = [(dm, ds) for dm in range(2) for ds in range(n_stage) if dm or ds]
    where = [{'model': lax.rem(model + dm, 2), 'stage': lax.rem(stage + ds, n_stage)} for dm, ds in group]
    for target in where + [peer]:
        pl.semaphore_signal(barrier, inc=1, device_id=target, device_id_type=mesh_id)

    n_st_up, n_st_down = d_model // st_up.shape[1], 2 * ff_half // st_down.shape[1]

    def load_up(r):
        return pltpu.make_async_copy(wu_ref.at[pl.ds(r * st_up.shape[1], st_up.shape[1])], st_up.at[r % 2], st_sem.at[0, r % 2])

    def load_down(r):
        return pltpu.make_async_copy(wd_ref.at[pl.ds(r * st_down.shape[1], st_down.shape[1])], st_down.at[r % 2], st_sem.at[1, r % 2])

    load_acts = pltpu.make_async_copy(acts_ref, rows_a.at[own_rows], loc_sem.at[0])
    load_acts.start()
    load_up(0).start()
    load_up(1).start()
    load_down(0).start()
    load_down(1).start()

    def load_g(c):
        return pltpu.make_async_copy(gout_ref.at[:, pl.ds(c * half, half)], gbuf.at[c], loc_sem.at[1 + c])

    @pl.when(stage == last)
    def _():
        for c in range(2):
            load_g(c).start()

    pl.semaphore_wait(barrier, len(where) + 1)

    def chunk(k):
        return pl.ds(k * BLOCK, BLOCK)

    raw_rows = n_raw * BLOCK
    raw = [remote(gu_ref.at[chunk(k), peer_cols], got_up.at[chunk(k)], rs_ssem.at[0, k], rs_rsem.at[0, k], peer) for k in range(n_raw)]
    carries_x = stage >= n_stage // 2

    def micro(i):
        return 2 * (stage - n_stage // 2) + i

    def send_x(i):
        return remote(x_ref.at[micro(i), :, near], x_land.at[i], x_sem.at[0, i], x_sem.at[1, i], peer)

    @pl.when(carries_x)
    def _():
        for i in range(2):
            send_x(i).start()

    for copy in raw:
        copy.start()
    send_a = remote(acts_ref.at[:, :raw_rows], rows_a.at[own_rows, :raw_rows], row_ssem.at[0], row_rsem.at[0], peer)
    send_a.start()

    for r in range(n_st_up):
        load_up(r).wait()
        up_bf[pl.ds(r * st_up.shape[1], st_up.shape[1])] = st_up[r % 2].astype(jnp.bfloat16)
        if r + 2 < n_st_up:
            load_up(r + 2).start()
    load_acts.wait()

    tile = 256
    n_tile = hid.shape[1] // tile
    scale = 0.7978845608028654
    cubic = 0.044715

    def pre_tile(j, carry):
        cols = pl.ds(pl.multiple_of(j * tile, tile), tile)
        pre = jnp.dot(rows_a[own_rows], up_bf[:, cols], preferred_element_type=jnp.float32)
        square = pre * pre
        bend = jnp.tanh(scale * (pre + cubic * square * pre))
        hid[:, cols] = (pre * (0.5 * (1.0 + bend))).astype(jnp.bfloat16)
        slope[:, cols] = 0.5 * (1.0 + bend) + 0.5 * pre * (1.0 - bend * bend) * (scale * (1.0 + 3.0 * cubic * square))
        return carry

    lax.fori_loop(0, n_tile, pre_tile, 0)

    for r in range(n_st_down):
        load_down(r).wait()
        down_bf[pl.ds(r * st_down.shape[1], st_down.shape[1])] = st_down[r % 2].astype(jnp.bfloat16)
        if r + 2 < n_st_down:
            load_down(r + 2).start()

    own_up = pltpu.make_async_copy(gu_ref.at[:, own_cols], acc_up, own_sem.at[0])
    own_down = pltpu.make_async_copy(gd_ref.at[own_cols], acc_down, own_sem.at[1])
    load_fold = pltpu.make_async_copy(gd_ref.at[peer_cols], fold, fold_sem)
    load_fold_up = pltpu.make_async_copy(gu_ref.at[raw_rows:, peer_cols], fold_up, fold_up_sem)
    load_fold_up.start()
    load_fold.start()
    own_up.start()
    own_down.start()

    @pl.when(stage == last)
    def _():
        for c in range(2):
            load_g(c).wait()

    @pl.when(stage < last)
    def _():
        for c in range(2):
            remote(ready, gbuf.at[c], pass_ssem.at[0], g_rsem.at[c], {'model': model}).wait_recv()

    def slope_tile(j, carry):
        cols = pl.ds(pl.multiple_of(j * tile, tile), tile)
        grad = lax.dot_general(gbuf[0], down_bf[cols, :half], CONTRACT_LAST, preferred_element_type=jnp.float32)
        grad = grad + lax.dot_general(gbuf[1], down_bf[cols, half:], CONTRACT_LAST, preferred_element_type=jnp.float32)
        grad_pre[:, cols] = (slope[:, cols] * grad).astype(jnp.bfloat16)
        return carry

    lax.fori_loop(0, n_tile, slope_tile, 0)

    trade = remote(outbox, landed, trade_sem.at[0], trade_sem.at[1], {'model': 1 - model})

    def hand_on(to):
        return remote(ready, gbuf.at[model], pass_ssem.at[to], g_rsem.at[model], {'model': to, 'stage': stage - 1})

    @pl.when(stage > 0)
    def _():
        outbox[...] = lax.dot_general(grad_pre[...], up_bf[far], CONTRACT_LAST, preferred_element_type=jnp.float32)
        trade.start()
        mine = lax.dot_general(grad_pre[...], up_bf[near], CONTRACT_LAST, preferred_element_type=jnp.float32)
        trade.wait_recv()
        ready[...] = (gbuf[model].astype(jnp.float32) + (mine + landed[...])).astype(jnp.bfloat16)
        for to in range(2):
            hand_on(to).start()

    rows_z[own_rows] = grad_pre[:, own_cols]
    send_z = remote(grad_pre.at[:, peer_cols], rows_z.at[own_rows], row_ssem.at[1], row_rsem.at[1], peer)
    send_z.start()

    load_fold_up.wait()

    def send_fold_up(k):
        rows = pl.ds(pl.multiple_of(k * BLOCK, BLOCK), BLOCK)
        at = pl.ds(pl.multiple_of((n_raw + k) * BLOCK, BLOCK), BLOCK)
        return remote(fold_up.at[rows], got_up.at[at], rs_ssem.at[0, n_raw + k], rs_rsem.at[0, n_raw + k], peer)

    def fold_up_step(k, carry):
        rows = pl.ds(pl.multiple_of(k * BLOCK, BLOCK), BLOCK)
        at = pl.ds(pl.multiple_of((n_raw + k) * BLOCK, BLOCK), BLOCK)
        fold_up[rows] += lax.dot_general(rows_a[own_rows, at], grad_pre[:, peer_cols], first_dims, preferred_element_type=jnp.float32)
        send_fold_up(k).start()
        return carry

    lax.fori_loop(0, n_up_chunk - n_raw, fold_up_step, 0)

    def forward_x(i, to):
        return remote(x_land.at[i], x_far.at[micro(i), :, near], xf_ssem.at[i, to], xf_rsem.at[micro(i), model], {'model': to, 'stage': 0})

    @pl.when(carries_x)
    def _():
        for i in range(2):
            send_x(i).wait_recv()
            for to in range(2):
                forward_x(i, to).start()

    def down_product(k, side):
        cols = pl.ds(pl.multiple_of(side * ff_half + k * BLOCK, BLOCK), BLOCK)
        left = hid[:, cols]
        return [lax.dot_general(left, gbuf[c], first_dims, preferred_element_type=jnp.float32) for c in range(2)]

    load_fold.wait()

    def send_fold(k):
        rows = pl.ds(pl.multiple_of(k * BLOCK, BLOCK), BLOCK)
        return remote(fold.at[rows], got_down.at[rows], rs_ssem.at[1, k], rs_rsem.at[1, k], peer)

    def fold_step(k, carry):
        rows = pl.ds(pl.multiple_of(k * BLOCK, BLOCK), BLOCK)
        low, high = down_product(k, 1 - data)
        fold[rows, :half] += low
        fold[rows, half:] += high
        send_fold(k).start()
        return carry

    lax.fori_loop(0, n_down_chunk, fold_step, 0)
    own_down.wait()

    def own_step(k, carry):
        rows = pl.ds(pl.multiple_of(k * BLOCK, BLOCK), BLOCK)
        low, high = down_product(k, data)
        acc_down[rows, :half] += low
        acc_down[rows, half:] += high
        return carry

    lax.fori_loop(0, n_down_chunk, own_step, 0)

    @pl.when(stage > 0)
    def _():
        trade.wait_send()
        for to in range(2):
            hand_on(to).wait_send()

    own_up.wait()
    send_a.wait_recv()
    squares = jnp.zeros((8, ff_half), jnp.float32)

    def fold_squares(mean):
        return jnp.sum((mean * mean).reshape(-1, 8, mean.shape[1]), axis=0)

    def put(acc, bounds, outs, whole, sem_row):
        copies = []
        for i, (lo, hi) in enumerate(bounds):
            rows = pl.ds(lo, hi - lo)
            copies.append(pltpu.make_async_copy(acc.at[rows], whole.at[rows], out_sem.at[sem_row, i]))
            if outs[i] is not None:
                copies.append(pltpu.make_async_copy(acc.at[rows], outs[i], out_sem.at[sem_row, len(bounds) + i]))
        return copies

    def put_start(k, bounds, copies, outs):
        at = 0
        for i, (lo, hi) in enumerate(bounds):
            count = 1 if outs[i] is None else 2
            if k * BLOCK < hi <= (k + 1) * BLOCK:
                for copy in copies[at:at + count]:
                    copy.start()
            at += count

    outs_up = (None,) + tuple(outs_up)
    outs_down = (None,) * len(bounds_down)
    put_up = put(acc_up, bounds_up, outs_up, whole_up, 0)
    put_down = put(acc_down, bounds_down, outs_down, whole_down, 1)
    for k in range(n_up_chunk):
        if k == 0:
            send_z.wait_recv()
        if k < n_raw:
            raw[k].wait_recv()
            product = lax.dot_general(rows_a[:, chunk(k)], rows_z[...], first_dims, preferred_element_type=jnp.float32)
        else:
            send_fold_up(k - n_raw).wait_recv()
            product = lax.dot_general(rows_a[own_rows, chunk(k)], rows_z[own_rows], first_dims, preferred_element_type=jnp.float32)
        mean = (acc_up[chunk(k)] + got_up[chunk(k)] + product) * 0.5
        acc_up[chunk(k)] = mean
        squares = squares + fold_squares(mean)
        put_start(k, bounds_up, put_up, outs_up)
    n_far = far_sem.shape[1]
    slab = bounds_up[0][1] // n_far
    is_even = lax.rem(stage, 2) == 0

    def send_far(i):
        span = pl.ds(pl.multiple_of(i * slab, slab), slab)
        return remote(acc_up.at[span], far_ref.at[span], far_sem.at[0, i], far_sem.at[1, i], peer)

    for i in range(n_far - HELD):
        send_far(i).start()

    @pl.when(is_even)
    def _():
        for i in range(n_far - HELD, n_far):
            send_far(i).start()

    for k in range(n_down_chunk):
        send_fold(k).wait_recv()
        mean = (acc_down[chunk(k)] + got_down[chunk(k)]) * 0.5
        acc_down[chunk(k)] = mean
        squares = squares + fold_squares(mean)
        put_start(k, bounds_down, put_down, outs_down)

    lanes = norm_box.shape[2]
    part = squares[:, :lanes]
    for j in range(1, ff_half // lanes):
        part = part + squares[:, j * lanes:(j + 1) * lanes]
    me = model * n_stage + stage
    norm_box[me] = part

    def spread(i):
        return remote(norm_box.at[me], norm_box.at[me], norm_ssem.at[i], norm_rsem.at[me], where[i])

    for i in range(len(group)):
        spread(i).start()
    for i, (dm, ds) in enumerate(group):
        them = lax.rem(model + dm, 2) * n_stage + lax.rem(stage + ds, n_stage)
        remote(norm_box.at[me], norm_box.at[them], norm_ssem.at[i], norm_rsem.at[them], where[i]).wait_recv()
    total = norm_box[0]
    for i in range(1, 2 * n_stage):
        total = total + norm_box[i]
    norm_pair[0] = total
    swap = remote(norm_pair.at[0], norm_pair.at[1], norm_ssem.at[len(group)], norm_rsem.at[2 * n_stage], peer)
    swap.start()
    swap.wait_recv()
    norm_sq = jnp.sum(norm_pair[0] + norm_pair[1], axis=(0, 1), keepdims=True)
    norm = jnp.sqrt(jnp.broadcast_to(norm_sq, clip_ref.shape)) + NORM_EPS
    clip_ref[...] = jnp.minimum(1.0, max_ref[0] / norm)

    @pl.when(carries_x)
    def _():
        for i in range(2):
            send_x(i).wait_send()
            for to in range(2):
                forward_x(i, to).wait_send()

    @pl.when(stage == 0)
    def _():
        for s in range(n_stage):
            for m in range(2):
                remote(x_land.at[0], x_far.at[s, :, pl.ds(m * half, half)], xf_ssem.at[0, m], xf_rsem.at[s, m], {'model': model}).wait_recv()

    swap.wait_send()
    for i in range(len(group)):
        spread(i).wait_send()
    for copy in raw + [send_a, send_z]:
        copy.wait_send()
    for k in range(n_down_chunk):
        send_fold(k).wait_send()
    for k in range(n_up_chunk - n_raw):
        send_fold_up(k).wait_send()
    for copy in put_up + put_down:
        copy.wait()

    @pl.when(is_even)
    def _():
        for i in range(n_far):
            send_far(i).wait_send()
        pl.semaphore_signal(go_sem, inc=1, device_id={'stage': stage + 1}, device_id_type=mesh_id)

    @pl.when(jnp.logical_not(is_even))
    def _():
        pl.semaphore_wait(go_sem, 1)
        for i in range(n_far - HELD, n_far):
            send_far(i).start()
        for i in range(n_far):
            send_far(i).wait_send()

    for i in range(n_far):
        send_far(i).wait_recv()


def backward_call(n_stage, bounds_up, bounds_down, g_up, g_down, w_up, w_down, acts, grad_out, x_next, max_norm):
    d_model, ff_local = g_up.shape
    ff_half, half, n_row = ff_local // 2, d_model // 2, acts.shape[0]
    dma = pltpu.SemaphoreType.DMA
    anywhere = pl.BlockSpec(memory_space=pl.ANY)
    f32, bf16 = jnp.float32, jnp.bfloat16
    shapes = [jax.ShapeDtypeStruct((hi - lo, ff_half), f32) for lo, hi in bounds_up[1:]]
    shapes += [jax.ShapeDtypeStruct((d_model, ff_half), f32), jax.ShapeDtypeStruct((ff_half, d_model), f32)]
    shapes += [jax.ShapeDtypeStruct((bounds_up[0][1], ff_half), f32), jax.ShapeDtypeStruct(x_next.shape, bf16), jax.ShapeDtypeStruct((8, ff_half), f32)]
    n_chunk = max(d_model, ff_half) // BLOCK
    return pl.pallas_call(
        functools.partial(backward_body, n_stage, N_RAW, bounds_up, bounds_down),
        out_shape=shapes,
        in_specs=[anywhere] * 7 + [pl.BlockSpec(memory_space=pltpu.SMEM)],
        out_specs=[anywhere] * (len(shapes) - 1) + [pl.BlockSpec(memory_space=pltpu.VMEM)],
        scratch_shapes=[
            pltpu.VMEM((d_model, ff_local), bf16),
            pltpu.VMEM((ff_local, d_model), bf16),
            pltpu.VMEM((2, 256, ff_local), f32),
            pltpu.VMEM((2, 512, d_model), f32),
            pltpu.VMEM((d_model, ff_half), f32),
            pltpu.VMEM((ff_half, d_model), f32),
            pltpu.VMEM((d_model, ff_half), f32),
            pltpu.VMEM((ff_half, d_model), f32),
            pltpu.VMEM((ff_half, d_model), f32),
            pltpu.VMEM((n_row, ff_local), bf16),
            pltpu.VMEM((n_row, ff_local), f32),
            pltpu.VMEM((n_row, ff_local), bf16),
            pltpu.VMEM((2, n_row, half), bf16),
            pltpu.VMEM((n_row, half), f32),
            pltpu.VMEM((n_row, half), f32),
            pltpu.VMEM((n_row, half), bf16),
            pltpu.VMEM((2 * n_row, d_model), bf16),
            pltpu.VMEM((2 * n_row, ff_half), bf16),
            pltpu.VMEM((2 * n_stage, 8, 128), f32),
            pltpu.VMEM((2, 8, 128), f32),
            dma((2, 2)),
            dma((3,)),
            dma(()),
            dma((2,)),
            dma((2, max(2 * len(bounds_up), len(bounds_down)))),
            dma((2,)),
            dma((2,)),
            dma((2,)),
            dma((2, n_chunk)),
            dma((2, n_chunk)),
            dma((2,)),
            dma((2,)),
            dma((2, 8)),
            dma((2 * n_stage,)),
            dma((2 * n_stage + 1,)),
            pltpu.VMEM((2, n_row, half), bf16),
            dma((2, 2)),
            dma((2, 2)),
            dma((n_stage, 2)),
            pltpu.SemaphoreType.REGULAR,
            pltpu.VMEM((d_model - N_RAW * BLOCK, ff_half), f32),
            dma(()),
        ],
        compiler_params=pltpu.CompilerParams(collective_id=0, has_side_effects=True, vmem_limit_bytes=67043328),
        name="reduce_and_norm",
    )(g_up, g_down, w_up, w_down, acts, grad_out, x_next, max_norm)


def forward_body(n_stage, lead, x_ref, xf_ref, up_ref, down_ref, mean_ref, y_ref, far_ref, inbox, hid, mine, zout, zin, keep, yout, yin, done, x_sem, in_sem, z_ssem, z_rsem, s_ssem, s_rsem, r_ssem, r_rsem, pass_ssem, y_ssem, y_rsem, piece_ssem, piece_rsem, go_sem):
    model, data, stage = lax.axis_index('model'), lax.axis_index('data'), lax.axis_index('stage')
    mesh_id = pl.DeviceIdType.MESH
    last = n_stage - 1
    n_group, _, rows2, half = inbox.shape
    rows = rows2 // 2
    n_piece = piece_ssem.shape[0]
    piece = mean_ref.shape[0] // n_piece
    peer = {'data': 1 - data}
    near = pl.ds(pl.multiple_of(model * half, half), half)
    far = pl.ds(pl.multiple_of((1 - model) * half, half), half)
    own_rows = pl.ds(pl.multiple_of(data * rows, rows), rows)
    peer_rows = pl.ds(pl.multiple_of((1 - data) * rows, rows), rows)

    def remote(src, dst, ssem, rsem, where):
        return pltpu.make_async_remote_copy(src_ref=src, dst_ref=dst, send_sem=ssem, recv_sem=rsem, device_id=where, device_id_type=mesh_id)

    barrier = pltpu.get_barrier_semaphore()
    group = [(dm, ds) for dm in range(2) for ds in range(n_stage) if dm or ds]
    where = [{'model': lax.rem(model + dm, 2), 'stage': lax.rem(stage + ds, n_stage)} for dm, ds in group]
    for target in where + [peer]:
        pl.semaphore_signal(barrier, inc=1, device_id=target, device_id_type=mesh_id)

    def load_x(b, c, from_ref, to_rows, i):
        return pltpu.make_async_copy(from_ref.at[b, :, pl.ds(c * half, half)], inbox.at[b, c, to_rows], x_sem.at[b, c, i])

    def loads(b):
        return [load_x(b, c, *pair) for c in range(2) for pair in ((x_ref, own_rows, 0), (xf_ref, peer_rows, 1))]

    @pl.when(stage == 0)
    def _():
        for b in range(n_group):
            for copy in loads(b):
                copy.start()

    pl.semaphore_wait(barrier, len(where) + 1)

    def send_piece(p):
        span = pl.ds(pl.multiple_of(p * piece, piece), piece)
        return remote(mean_ref.at[span], far_ref.at[span], piece_ssem.at[p], piece_rsem.at[p], peer)

    def start_pieces(low, high):
        def one(p, carry):
            send_piece(p).start()
            return carry

        lax.fori_loop(low, high, one, 0)

    n_turn = n_group + 3
    base, slope = lead
    begin = base + slope * stage
    is_even = lax.rem(stage, 2) == 0
    limit = n_piece - HELD * lax.rem(stage, 2)
    start_pieces(0, begin)

    def arrival(b, c):
        return remote(done.at[b], inbox.at[b, c], pass_ssem.at[b, 0], in_sem.at[b, c], {'model': model})

    def trade_z(b):
        return remote(zout.at[b], zin.at[b], z_ssem.at[b], z_rsem.at[b], {'model': 1 - model})

    def trade_s(b):
        return remote(yout.at[b], yin.at[b], s_ssem.at[b], s_rsem.at[b], peer)

    def trade_r(b):
        return remote(done.at[b, own_rows], done.at[b, own_rows], r_ssem.at[b], r_rsem.at[b], peer)

    def hand_on(b, to):
        return remote(done.at[b], inbox.at[b, model], pass_ssem.at[b, to], in_sem.at[b, model], {'model': to, 'stage': stage + 1})

    def landing(b, c):
        return y_ref.at[b, :, pl.ds(pl.multiple_of(c * half, half), half)]

    def publish(b, k):
        return remote(done.at[b, own_rows], landing(b, model), y_ssem.at[b, k], y_rsem.at[b, model], where[k])

    def y_arrival(b, c):
        return remote(done.at[b, own_rows], landing(b, c), y_ssem.at[b, 0], y_rsem.at[b, c], {'model': model})

    def turn(t, carry):
        @pl.when(t < n_group)
        def _():
            @pl.when(stage == 0)
            def _():
                for copy in loads(t):
                    copy.wait()

            @pl.when(stage > 0)
            def _():
                for c in range(2):
                    arrival(t, c).wait_recv()

            pre = jnp.dot(inbox[t, 0], up_ref[:half], preferred_element_type=jnp.float32)
            pre = pre + jnp.dot(inbox[t, 1], up_ref[half:], preferred_element_type=jnp.float32)
            hid[...] = jax.nn.gelu(pre).astype(jnp.bfloat16)
            zout[t] = jnp.dot(hid[...], down_ref[:, far], preferred_element_type=jnp.float32)
            trade_z(t).start()
            mine[t] = jnp.dot(hid[...], down_ref[:, near], preferred_element_type=jnp.float32)

        @pl.when((t >= 1) & (t < n_group + 1))
        def _():
            b = t - 1
            trade_z(b).wait_recv()
            yout[b] = mine[b, peer_rows] + zin[b, peer_rows]
            trade_s(b).start()
            keep[b] = mine[b, own_rows] + zin[b, own_rows]

        @pl.when((t >= 2) & (t < n_group + 2))
        def _():
            b = t - 2
            trade_s(b).wait_recv()
            total = inbox[b, model, own_rows].astype(jnp.float32) + (keep[b] + yin[b])
            result = total.astype(jnp.bfloat16)
            done[b, own_rows] = result

            @pl.when(stage < last)
            def _():
                trade_r(b).start()

            @pl.when(stage == last)
            def _():
                y_ref[b, :, near] = result
                for k in range(len(group)):
                    publish(b, k).start()

        @pl.when((t >= 3) & (stage < last))
        def _():
            b = t - 3
            remote(done.at[b, own_rows], done.at[b, peer_rows], r_ssem.at[b], r_rsem.at[b], peer).wait_recv()
            for to in range(2):
                hand_on(b, to).start()

        @pl.when(begin + t < limit)
        def _():
            send_piece(begin + t).start()

        return carry

    lax.fori_loop(0, n_turn, turn, 0)
    start_pieces(jnp.minimum(begin + n_turn, limit), limit)

    for b in range(n_group):
        trade_z(b).wait_send()
        trade_s(b).wait_send()

    @pl.when(stage < last)
    def _():
        for b in range(n_group):
            trade_r(b).wait_send()
            for to in range(2):
                hand_on(b, to).wait_send()
            for c in range(2):
                y_arrival(b, c).wait_recv()

    @pl.when(stage == last)
    def _():
        for b in range(n_group):
            for k in range(len(group)):
                publish(b, k).wait_send()
            y_arrival(b, 1 - model).wait_recv()

    def sent(p, carry):
        send_piece(p).wait_send()
        return carry

    def landed(p, carry):
        send_piece(p).wait_recv()
        return carry

    lax.fori_loop(0, limit, sent, 0)

    @pl.when(is_even)
    def _():
        pl.semaphore_signal(go_sem, inc=1, device_id={'stage': stage + 1}, device_id_type=mesh_id)

    @pl.when(jnp.logical_not(is_even))
    def _():
        pl.semaphore_wait(go_sem, 1)
        start_pieces(limit, n_piece)
        lax.fori_loop(limit, n_piece, sent, 0)

    lax.fori_loop(0, n_piece, landed, 0)


def forward_call(n_stage, n_group, n_piece, lead, x_next, x_far, up_bf, down_bf, mean):
    d_model = x_next.shape[2]
    x_next, x_far = [value.reshape(n_group, -1, d_model) for value in (x_next, x_far)]
    rows, half, ff_half = x_next.shape[1], d_model // 2, up_bf.shape[1]
    dma = pltpu.SemaphoreType.DMA
    f32, bf16 = jnp.float32, jnp.bfloat16
    in_vmem = pl.BlockSpec(memory_space=pltpu.VMEM)
    anywhere = pl.BlockSpec(memory_space=pl.ANY)
    return pl.pallas_call(
        functools.partial(forward_body, n_stage, lead),
        out_shape=[jax.ShapeDtypeStruct(x_next.shape, bf16), jax.ShapeDtypeStruct(mean.shape, f32)],
        in_specs=[anywhere, anywhere, in_vmem, in_vmem, anywhere],
        out_specs=[in_vmem, anywhere],
        scratch_shapes=[
            pltpu.VMEM((n_group, 2, 2 * rows, half), bf16),
            pltpu.VMEM((2 * rows, ff_half), bf16),
            pltpu.VMEM((n_group, 2 * rows, half), f32),
            pltpu.VMEM((n_group, 2 * rows, half), f32),
            pltpu.VMEM((n_group, 2 * rows, half), f32),
            pltpu.VMEM((n_group, rows, half), f32),
            pltpu.VMEM((n_group, rows, half), f32),
            pltpu.VMEM((n_group, rows, half), f32),
            pltpu.VMEM((n_group, 2 * rows, half), bf16),
            dma((n_group, 2, 2)),
            dma((n_group, 2)),
            dma((n_group,)),
            dma((n_group,)),
            dma((n_group,)),
            dma((n_group,)),
            dma((n_group,)),
            dma((n_group,)),
            dma((n_group, 2)),
            dma((n_group, 2 * n_stage - 1)),
            dma((n_group, 2)),
            dma((n_piece,)),
            dma((n_piece,)),
            pltpu.SemaphoreType.REGULAR,
        ],
        compiler_params=pltpu.CompilerParams(collective_id=1, has_side_effects=True, vmem_limit_bytes=67043328),
        name="forward_pipe",
    )(x_next, x_far, up_bf, down_bf, mean)


def solution(mesh):
    n_stage = mesh.shape['stage']
    swap = [(0, 1), (1, 0)]
    up_spec = P('stage', None, 'model')
    down_spec = P('stage', 'model', None)
    row_spec = P(None, 'data', None)
    in_specs = (up_spec, down_spec, up_spec, down_spec, up_spec, down_spec, P('data', 'stage', None, 'model'), P('data', 'stage', 'model', None), P('stage', 'data', None), P('data', None), row_spec, P(None), P(None))
    out_specs = (up_spec, down_spec, up_spec, down_spec, up_spec, down_spec, row_spec)

    def device_step(w_up, w_down, m_up, m_down, v_up, v_down, g_up, g_down, acts_last, grad_out, x_next, learn_rate, max_norm):
        data_id = lax.axis_index('data')
        half = data_id.astype(jnp.int32).reshape(1)
        other = (1 - half).astype(jnp.int32)
        d_model, ff_local = w_up.shape[1:]
        ff_half = ff_local // 2
        bounds_up = ((0, 256), (256, 640), (640, 832), (832, 960), (960, d_model))
        bounds_down = ((0, ff_half // 2), (ff_half // 2, ff_half))

        def trade(value):
            return lax.ppermute(value, 'data', swap)

        early, *late, whole_up, whole_down, far_first, x_far, clip = backward_call(n_stage, bounds_up, bounds_down, g_up[0, 0], g_down[0, 0], w_up[0], w_down[0], acts_last[0], grad_out, x_next, max_norm)
        ups = (w_up[0], m_up[0], v_up[0])
        downs = (w_down[0], m_down[0], v_down[0])

        def map_up(low, high):
            return lambda i, h, r: (low // step_of(low, high) + i, h[0])

        def map_down(i, h, r):
            return h[0] * (ff_half // BLOCK) + i, 0

        far_early = trade(early)
        *new_up, up_bf = update_call(half, learn_rate, clip, ups, whole_up, map_up(0, d_model), None)
        *new_down, down_bf = update_call(half, learn_rate, clip, downs, whole_down, map_down, None, (up_bf,))
        new_up = update_call(other, learn_rate, clip, ups, far_first, map_up(*bounds_up[0]), new_up, (down_bf,))
        down_bf, new_up = lax.optimization_barrier((down_bf, new_up))
        y_next, far_down = forward_call(n_stage, N_GROUP, N_PIECE, LEAD, x_next, x_far, up_bf, down_bf, whole_down)
        late, far_down = lax.optimization_barrier((late, far_down))
        fars = [far_early] + [trade(value) for value in late]
        *new_down, y_next = update_call(other, learn_rate, clip, downs, far_down, map_down, new_down, (), (y_next,))
        y_next = y_next.reshape(x_next.shape)
        for bounds, part in zip(bounds_up[1:], fars):
            new_up = update_call(other, learn_rate, clip, ups, part, map_up(*bounds), new_up, block=step_of(*bounds))
        return (new_up[0][None], new_down[0][None], new_up[1][None], new_down[1][None], new_up[2][None], new_down[2][None], y_next)

    return jax.shard_map(device_step, mesh=mesh, in_specs=in_specs, out_specs=out_specs, check_vma=False)
```

```python
import functools

import jax
import jax.numpy as jnp
from jax import lax
from jax.experimental import pallas as pl
from jax.experimental.pallas import tpu as pltpu
from jax.sharding import PartitionSpec as P

ADAM_STEP = 10
BETA_ONE = 0.9
BETA_TWO = 0.95
ADAM_EPS = 1e-8
WEIGHT_DECAY = 0.1
NORM_EPS = 1e-6
CONTRACT_LAST = (((1,), (1,)), ((), ()))
BLOCK = 128
N_GROUP = 8
N_PIECE = 32
LEAD = (2, 7)
HELD = 2
HELD_FWD = 3
LAG = 2
N_RAW = 4


def update_body(skip, carry, half_ref, rate_ref, clip_ref, w_ref, m_ref, v_ref, g_ref, *refs):
    outs = refs[skip:]
    if carry:
        outs[-1][...] = refs[skip - 1][...]
        outs = outs[:-1]
    ow_ref, om_ref, ov_ref = outs[:3]
    rate = rate_ref[0]
    grad = clip_ref[0:1] * g_ref[...]
    weight = w_ref[...]
    mom = BETA_ONE * m_ref[...] + (1.0 - BETA_ONE) * grad
    sec = BETA_TWO * v_ref[...] + (1.0 - BETA_TWO) * grad * grad
    one_corr = 1.0 - BETA_ONE**ADAM_STEP
    two_corr = 1.0 - BETA_TWO**ADAM_STEP
    direction = (mom * (1.0 / one_corr)) / (jnp.sqrt(sec * (1.0 / two_corr)) + ADAM_EPS)
    new = weight - rate * (direction + WEIGHT_DECAY * weight)
    ow_ref[...] = new
    om_ref[...] = mom
    ov_ref[...] = sec
    if len(outs) == 4:
        outs[3][...] = new.astype(jnp.bfloat16)


def step_of(low, high):
    return BLOCK if low % BLOCK == 0 and high % BLOCK == 0 else BLOCK // 2


def update_call(half, rate, clip, weights, grad, full_map, previous, after=(), carry=(), block=BLOCK):
    rows, cols = grad.shape
    shape = weights[0].shape
    spec = pl.BlockSpec((block, cols), full_map)
    flat = pl.BlockSpec((block, cols), lambda i, h, r: (i, 0))
    anywhere = pl.BlockSpec(memory_space=pl.ANY)
    first = previous is None
    extra = list(previous or ()) + list(after)
    passed = [pl.BlockSpec((1,) + value.shape[1:], lambda i, h, r: (i, 0, 0)) for value in carry]
    return pl.pallas_call(
        functools.partial(update_body, len(extra) + len(carry), len(carry)),
        grid_spec=pltpu.PrefetchScalarGridSpec(
            num_scalar_prefetch=2,
            grid=(rows // block,),
            in_specs=[pl.BlockSpec(clip.shape, lambda i, h, r: (0, 0)), spec, spec, spec, flat] + [anywhere] * len(extra) + passed,
            out_specs=[spec] * 3 + [flat] * first + passed,
        ),
        out_shape=[jax.ShapeDtypeStruct(shape, jnp.float32)] * 3 + [jax.ShapeDtypeStruct(grad.shape, jnp.bfloat16)] * first + [jax.ShapeDtypeStruct(value.shape, value.dtype) for value in carry],
        input_output_aliases={7 + i: i for i in range(len(previous or ()))},
        cost_estimate=pl.CostEstimate(flops=60 * rows * cols, bytes_accessed=30 * rows * cols, transcendentals=0),
        compiler_params=pltpu.CompilerParams(vmem_limit_bytes=67043328),
        name="adamw_half",
    )(half, rate, clip, *weights, grad, *extra, *carry)


def backward_body(n_stage, n_raw, bounds_up, bounds_down, gu_ref, gd_ref, wu_ref, wd_ref, acts_ref, gout_ref, x_ref, max_ref, *refs):
    n_up = len(bounds_up) - 1
    outs_up = refs[:n_up]
    whole_up, whole_down, far_ref, x_far, clip_ref = refs[n_up:n_up + 5]
    (up_bf, down_bf, st_up, st_down, acc_up, acc_down, got_up, got_down, fold, hid, slope, grad_pre, gbuf, outbox, landed, ready, rows_a, rows_z, norm_box, norm_pair,
     st_sem, loc_sem, fold_sem, own_sem, out_sem, g_rsem, trade_sem, pass_ssem, rs_ssem, rs_rsem, row_ssem, row_rsem, far_sem, norm_ssem, norm_rsem, x_land, x_sem, xf_ssem, xf_rsem, go_sem, fold_up, fold_up_sem) = refs[n_up + 5:]
    model, data, stage = lax.axis_index('model'), lax.axis_index('data'), lax.axis_index('stage')
    mesh_id = pl.DeviceIdType.MESH
    last = n_stage - 1
    d_model, ff_half = acc_up.shape
    half = d_model // 2
    n_row = acts_ref.shape[0]
    n_up_chunk, n_down_chunk = d_model // BLOCK, ff_half // BLOCK
    peer = {'data': 1 - data}
    near = pl.ds(pl.multiple_of(model * half, half), half)
    far = pl.ds(pl.multiple_of((1 - model) * half, half), half)
    own_cols = pl.ds(pl.multiple_of(data * ff_half, ff_half), ff_half)
    peer_cols = pl.ds(pl.multiple_of((1 - data) * ff_half, ff_half), ff_half)
    own_rows = pl.ds(pl.multiple_of(data * n_row, n_row), n_row)
    first_dims = (((0,), (0,)), ((), ()))

    def remote(src, dst, ssem, rsem, where):
        return pltpu.make_async_remote_copy(src_ref=src, dst_ref=dst, send_sem=ssem, recv_sem=rsem, device_id=where, device_id_type=mesh_id)

    barrier = pltpu.get_barrier_semaphore()
    group = [(dm, ds) for dm in range(2) for ds in range(n_stage) if dm or ds]
    where = [{'model': lax.rem(model + dm, 2), 'stage': lax.rem(stage + ds, n_stage)} for dm, ds in group]
    for target in where + [peer]:
        pl.semaphore_signal(barrier, inc=1, device_id=target, device_id_type=mesh_id)

    n_st_up, n_st_down = d_model // st_up.shape[1], 2 * ff_half // st_down.shape[1]

    def load_up(r):
        return pltpu.make_async_copy(wu_ref.at[pl.ds(r * st_up.shape[1], st_up.shape[1])], st_up.at[r % 2], st_sem.at[0, r % 2])

    def load_down(r):
        return pltpu.make_async_copy(wd_ref.at[pl.ds(r * st_down.shape[1], st_down.shape[1])], st_down.at[r % 2], st_sem.at[1, r % 2])

    load_acts = pltpu.make_async_copy(acts_ref, rows_a.at[own_rows], loc_sem.at[0])
    load_acts.start()
    load_up(0).start()
    load_up(1).start()
    load_down(0).start()
    load_down(1).start()

    def load_g(c):
        return pltpu.make_async_copy(gout_ref.at[:, pl.ds(c * half, half)], gbuf.at[c], loc_sem.at[1 + c])

    @pl.when(stage == last)
    def _():
        for c in range(2):
            load_g(c).start()

    pl.semaphore_wait(barrier, len(where) + 1)

    def chunk(k):
        return pl.ds(k * BLOCK, BLOCK)

    raw_rows = n_raw * BLOCK
    raw = [remote(gu_ref.at[chunk(k), peer_cols], got_up.at[chunk(k)], rs_ssem.at[0, k], rs_rsem.at[0, k], peer) for k in range(n_raw)]
    carries_x = stage >= n_stage // 2

    def micro(i):
        return 2 * (stage - n_stage // 2) + i

    def send_x(i):
        return remote(x_ref.at[micro(i), :, near], x_land.at[i], x_sem.at[0, i], x_sem.at[1, i], peer)

    @pl.when(carries_x)
    def _():
        for i in range(2):
            send_x(i).start()

    for copy in raw:
        copy.start()
    send_a = remote(acts_ref.at[:, :raw_rows], rows_a.at[own_rows, :raw_rows], row_ssem.at[0], row_rsem.at[0], peer)
    send_a.start()

    for r in range(n_st_up):
        load_up(r).wait()
        up_bf[pl.ds(r * st_up.shape[1], st_up.shape[1])] = st_up[r % 2].astype(jnp.bfloat16)
        if r + 2 < n_st_up:
            load_up(r + 2).start()
    load_acts.wait()

    tile = 256
    n_tile = hid.shape[1] // tile
    scale = 0.7978845608028654
    cubic = 0.044715

    def pre_tile(j, carry):
        cols = pl.ds(pl.multiple_of(j * tile, tile), tile)
        pre = jnp.dot(rows_a[own_rows], up_bf[:, cols], preferred_element_type=jnp.float32)
        square = pre * pre
        bend = jnp.tanh(scale * (pre + cubic * square * pre))
        hid[:, cols] = (pre * (0.5 * (1.0 + bend))).astype(jnp.bfloat16)
        slope[:, cols] = 0.5 * (1.0 + bend) + 0.5 * pre * (1.0 - bend * bend) * (scale * (1.0 + 3.0 * cubic * square))
        return carry

    lax.fori_loop(0, n_tile, pre_tile, 0)

    for r in range(n_st_down):
        load_down(r).wait()
        down_bf[pl.ds(r * st_down.shape[1], st_down.shape[1])] = st_down[r % 2].astype(jnp.bfloat16)
        if r + 2 < n_st_down:
            load_down(r + 2).start()

    own_up = pltpu.make_async_copy(gu_ref.at[:, own_cols], acc_up, own_sem.at[0])
    own_down = pltpu.make_async_copy(gd_ref.at[own_cols], acc_down, own_sem.at[1])
    load_fold = pltpu.make_async_copy(gd_ref.at[peer_cols], fold, fold_sem)
    load_fold_up = pltpu.make_async_copy(gu_ref.at[raw_rows:, peer_cols], fold_up, fold_up_sem)
    load_fold_up.start()
    load_fold.start()
    own_up.start()
    own_down.start()

    @pl.when(stage == last)
    def _():
        for c in range(2):
            load_g(c).wait()

    @pl.when(stage < last)
    def _():
        for c in range(2):
            remote(ready, gbuf.at[c], pass_ssem.at[0], g_rsem.at[c], {'model': model}).wait_recv()

    def slope_tile(j, carry):
        cols = pl.ds(pl.multiple_of(j * tile, tile), tile)
        grad = lax.dot_general(gbuf[0], down_bf[cols, :half], CONTRACT_LAST, preferred_element_type=jnp.float32)
        grad = grad + lax.dot_general(gbuf[1], down_bf[cols, half:], CONTRACT_LAST, preferred_element_type=jnp.float32)
        grad_pre[:, cols] = (slope[:, cols] * grad).astype(jnp.bfloat16)
        return carry

    lax.fori_loop(0, n_tile, slope_tile, 0)

    trade = remote(outbox, landed, trade_sem.at[0], trade_sem.at[1], {'model': 1 - model})

    def hand_on(to):
        return remote(ready, gbuf.at[model], pass_ssem.at[to], g_rsem.at[model], {'model': to, 'stage': stage - 1})

    @pl.when(stage > 0)
    def _():
        outbox[...] = lax.dot_general(grad_pre[...], up_bf[far], CONTRACT_LAST, preferred_element_type=jnp.float32)
        trade.start()
        mine = lax.dot_general(grad_pre[...], up_bf[near], CONTRACT_LAST, preferred_element_type=jnp.float32)
        trade.wait_recv()
        ready[...] = (gbuf[model].astype(jnp.float32) + (mine + landed[...])).astype(jnp.bfloat16)
        for to in range(2):
            hand_on(to).start()

    rows_z[own_rows] = grad_pre[:, own_cols]
    send_z = remote(grad_pre.at[:, peer_cols], rows_z.at[own_rows], row_ssem.at[1], row_rsem.at[1], peer)
    send_z.start()

    load_fold_up.wait()

    def send_fold_up(k):
        rows = pl.ds(pl.multiple_of(k * BLOCK, BLOCK), BLOCK)
        at = pl.ds(pl.multiple_of((n_raw + k) * BLOCK, BLOCK), BLOCK)
        return remote(fold_up.at[rows], got_up.at[at], rs_ssem.at[0, n_raw + k], rs_rsem.at[0, n_raw + k], peer)

    def fold_up_step(k, carry):
        rows = pl.ds(pl.multiple_of(k * BLOCK, BLOCK), BLOCK)
        at = pl.ds(pl.multiple_of((n_raw + k) * BLOCK, BLOCK), BLOCK)
        fold_up[rows] += lax.dot_general(rows_a[own_rows, at], grad_pre[:, peer_cols], first_dims, preferred_element_type=jnp.float32)
        send_fold_up(k).start()
        return carry

    lax.fori_loop(0, n_up_chunk - n_raw, fold_up_step, 0)

    def forward_x(i, to):
        return remote(x_land.at[i], x_far.at[micro(i), :, near], xf_ssem.at[i, to], xf_rsem.at[micro(i), model], {'model': to, 'stage': 0})

    @pl.when(carries_x)
    def _():
        for i in range(2):
            send_x(i).wait_recv()
            for to in range(2):
                forward_x(i, to).start()

    def down_product(k, side):
        cols = pl.ds(pl.multiple_of(side * ff_half + k * BLOCK, BLOCK), BLOCK)
        left = hid[:, cols]
        return [lax.dot_general(left, gbuf[c], first_dims, preferred_element_type=jnp.float32) for c in range(2)]

    load_fold.wait()

    def send_fold(k):
        rows = pl.ds(pl.multiple_of(k * BLOCK, BLOCK), BLOCK)
        return remote(fold.at[rows], got_down.at[rows], rs_ssem.at[1, k], rs_rsem.at[1, k], peer)

    def fold_step(k, carry):
        rows = pl.ds(pl.multiple_of(k * BLOCK, BLOCK), BLOCK)
        low, high = down_product(k, 1 - data)
        fold[rows, :half] += low
        fold[rows, half:] += high
        send_fold(k).start()
        return carry

    lax.fori_loop(0, n_down_chunk, fold_step, 0)
    own_down.wait()

    def own_step(k, carry):
        rows = pl.ds(pl.multiple_of(k * BLOCK, BLOCK), BLOCK)
        low, high = down_product(k, data)
        acc_down[rows, :half] += low
        acc_down[rows, half:] += high
        return carry

    lax.fori_loop(0, n_down_chunk, own_step, 0)

    @pl.when(stage > 0)
    def _():
        trade.wait_send()
        for to in range(2):
            hand_on(to).wait_send()

    own_up.wait()
    send_a.wait_recv()
    squares = jnp.zeros((8, ff_half), jnp.float32)

    def fold_squares(mean):
        return jnp.sum((mean * mean).reshape(-1, 8, mean.shape[1]), axis=0)

    def put(acc, bounds, outs, whole, sem_row):
        copies = []
        for i, (lo, hi) in enumerate(bounds):
            rows = pl.ds(lo, hi - lo)
            copies.append(pltpu.make_async_copy(acc.at[rows], whole.at[rows], out_sem.at[sem_row, i]))
            if outs[i] is not None:
                copies.append(pltpu.make_async_copy(acc.at[rows], outs[i], out_sem.at[sem_row, len(bounds) + i]))
        return copies

    def put_start(k, bounds, copies, outs):
        at = 0
        for i, (lo, hi) in enumerate(bounds):
            count = 1 if outs[i] is None else 2
            if k * BLOCK < hi <= (k + 1) * BLOCK:
                for copy in copies[at:at + count]:
                    copy.start()
            at += count

    outs_up = (None,) + tuple(outs_up)
    outs_down = (None,) * len(bounds_down)
    put_up = put(acc_up, bounds_up, outs_up, whole_up, 0)
    put_down = put(acc_down, bounds_down, outs_down, whole_down, 1)
    for k in range(n_up_chunk):
        if k == 0:
            send_z.wait_recv()
        if k < n_raw:
            raw[k].wait_recv()
            product = lax.dot_general(rows_a[:, chunk(k)], rows_z[...], first_dims, preferred_element_type=jnp.float32)
        else:
            send_fold_up(k - n_raw).wait_recv()
            product = lax.dot_general(rows_a[own_rows, chunk(k)], rows_z[own_rows], first_dims, preferred_element_type=jnp.float32)
        mean = (acc_up[chunk(k)] + got_up[chunk(k)] + product) * 0.5
        acc_up[chunk(k)] = mean
        squares = squares + fold_squares(mean)
        put_start(k, bounds_up, put_up, outs_up)
    n_far = far_sem.shape[1]
    slab = bounds_up[0][1] // n_far
    is_even = lax.rem(stage, 2) == 0

    def send_far(i):
        span = pl.ds(pl.multiple_of(i * slab, slab), slab)
        return remote(acc_up.at[span], far_ref.at[span], far_sem.at[0, i], far_sem.at[1, i], peer)

    for i in range(n_far - HELD):
        send_far(i).start()

    @pl.when(is_even)
    def _():
        for i in range(n_far - HELD, n_far):
            send_far(i).start()

    for k in range(n_down_chunk):
        send_fold(k).wait_recv()
        mean = (acc_down[chunk(k)] + got_down[chunk(k)]) * 0.5
        acc_down[chunk(k)] = mean
        squares = squares + fold_squares(mean)
        put_start(k, bounds_down, put_down, outs_down)

    lanes = norm_box.shape[2]
    part = squares[:, :lanes]
    for j in range(1, ff_half // lanes):
        part = part + squares[:, j * lanes:(j + 1) * lanes]
    me = model * n_stage + stage
    norm_box[me] = part

    def spread(i):
        return remote(norm_box.at[me], norm_box.at[me], norm_ssem.at[i], norm_rsem.at[me], where[i])

    for i in range(len(group)):
        spread(i).start()
    for i, (dm, ds) in enumerate(group):
        them = lax.rem(model + dm, 2) * n_stage + lax.rem(stage + ds, n_stage)
        remote(norm_box.at[me], norm_box.at[them], norm_ssem.at[i], norm_rsem.at[them], where[i]).wait_recv()
    total = norm_box[0]
    for i in range(1, 2 * n_stage):
        total = total + norm_box[i]
    norm_pair[0] = total
    swap = remote(norm_pair.at[0], norm_pair.at[1], norm_ssem.at[len(group)], norm_rsem.at[2 * n_stage], peer)
    swap.start()
    swap.wait_recv()
    norm_sq = jnp.sum(norm_pair[0] + norm_pair[1], axis=(0, 1), keepdims=True)
    norm = jnp.sqrt(jnp.broadcast_to(norm_sq, clip_ref.shape)) + NORM_EPS
    clip_ref[...] = jnp.minimum(1.0, max_ref[0] / norm)

    @pl.when(carries_x)
    def _():
        for i in range(2):
            send_x(i).wait_send()
            for to in range(2):
                forward_x(i, to).wait_send()

    @pl.when(stage == 0)
    def _():
        for s in range(n_stage):
            for m in range(2):
                remote(x_land.at[0], x_far.at[s, :, pl.ds(m * half, half)], xf_ssem.at[0, m], xf_rsem.at[s, m], {'model': model}).wait_recv()

    swap.wait_send()
    for i in range(len(group)):
        spread(i).wait_send()
    for copy in raw + [send_a, send_z]:
        copy.wait_send()
    for k in range(n_down_chunk):
        send_fold(k).wait_send()
    for k in range(n_up_chunk - n_raw):
        send_fold_up(k).wait_send()
    for copy in put_up + put_down:
        copy.wait()

    @pl.when(is_even)
    def _():
        for i in range(n_far):
            send_far(i).wait_send()
        pl.semaphore_signal(go_sem, inc=1, device_id={'stage': stage + 1}, device_id_type=mesh_id)

    @pl.when(jnp.logical_not(is_even))
    def _():
        pl.semaphore_wait(go_sem, 1)
        for i in range(n_far - HELD, n_far):
            send_far(i).start()
        for i in range(n_far):
            send_far(i).wait_send()

    for i in range(n_far):
        send_far(i).wait_recv()


def backward_call(n_stage, bounds_up, bounds_down, g_up, g_down, w_up, w_down, acts, grad_out, x_next, max_norm):
    d_model, ff_local = g_up.shape
    ff_half, half, n_row = ff_local // 2, d_model // 2, acts.shape[0]
    dma = pltpu.SemaphoreType.DMA
    anywhere = pl.BlockSpec(memory_space=pl.ANY)
    f32, bf16 = jnp.float32, jnp.bfloat16
    shapes = [jax.ShapeDtypeStruct((hi - lo, ff_half), f32) for lo, hi in bounds_up[1:]]
    shapes += [jax.ShapeDtypeStruct((d_model, ff_half), f32), jax.ShapeDtypeStruct((ff_half, d_model), f32)]
    shapes += [jax.ShapeDtypeStruct((bounds_up[0][1], ff_half), f32), jax.ShapeDtypeStruct(x_next.shape, bf16), jax.ShapeDtypeStruct((8, ff_half), f32)]
    n_chunk = max(d_model, ff_half) // BLOCK
    return pl.pallas_call(
        functools.partial(backward_body, n_stage, N_RAW, bounds_up, bounds_down),
        out_shape=shapes,
        in_specs=[anywhere] * 7 + [pl.BlockSpec(memory_space=pltpu.SMEM)],
        out_specs=[anywhere] * (len(shapes) - 1) + [pl.BlockSpec(memory_space=pltpu.VMEM)],
        scratch_shapes=[
            pltpu.VMEM((d_model, ff_local), bf16),
            pltpu.VMEM((ff_local, d_model), bf16),
            pltpu.VMEM((2, 256, ff_local), f32),
            pltpu.VMEM((2, 512, d_model), f32),
            pltpu.VMEM((d_model, ff_half), f32),
            pltpu.VMEM((ff_half, d_model), f32),
            pltpu.VMEM((d_model, ff_half), f32),
            pltpu.VMEM((ff_half, d_model), f32),
            pltpu.VMEM((ff_half, d_model), f32),
            pltpu.VMEM((n_row, ff_local), bf16),
            pltpu.VMEM((n_row, ff_local), f32),
            pltpu.VMEM((n_row, ff_local), bf16),
            pltpu.VMEM((2, n_row, half), bf16),
            pltpu.VMEM((n_row, half), f32),
            pltpu.VMEM((n_row, half), f32),
            pltpu.VMEM((n_row, half), bf16),
            pltpu.VMEM((2 * n_row, d_model), bf16),
            pltpu.VMEM((2 * n_row, ff_half), bf16),
            pltpu.VMEM((2 * n_stage, 8, 128), f32),
            pltpu.VMEM((2, 8, 128), f32),
            dma((2, 2)),
            dma((3,)),
            dma(()),
            dma((2,)),
            dma((2, max(2 * len(bounds_up), len(bounds_down)))),
            dma((2,)),
            dma((2,)),
            dma((2,)),
            dma((2, n_chunk)),
            dma((2, n_chunk)),
            dma((2,)),
            dma((2,)),
            dma((2, 8)),
            dma((2 * n_stage,)),
            dma((2 * n_stage + 1,)),
            pltpu.VMEM((2, n_row, half), bf16),
            dma((2, 2)),
            dma((2, 2)),
            dma((n_stage, 2)),
            pltpu.SemaphoreType.REGULAR,
            pltpu.VMEM((d_model - N_RAW * BLOCK, ff_half), f32),
            dma(()),
        ],
        compiler_params=pltpu.CompilerParams(collective_id=0, has_side_effects=True, vmem_limit_bytes=67043328),
        name="reduce_and_norm",
    )(g_up, g_down, w_up, w_down, acts, grad_out, x_next, max_norm)


def forward_body(n_stage, lead, x_ref, xf_ref, up_ref, down_ref, mean_ref, y_ref, far_ref, inbox, hid, mine, zout, zin, keep, yout, yin, done, x_sem, in_sem, z_ssem, z_rsem, s_ssem, s_rsem, r_ssem, r_rsem, pass_ssem, y_ssem, y_rsem, piece_ssem, piece_rsem, go_sem):
    model, data, stage = lax.axis_index('model'), lax.axis_index('data'), lax.axis_index('stage')
    mesh_id = pl.DeviceIdType.MESH
    last = n_stage - 1
    n_group, _, rows2, half = inbox.shape
    rows = rows2 // 2
    n_piece = piece_ssem.shape[0]
    piece = mean_ref.shape[0] // n_piece
    peer = {'data': 1 - data}
    near = pl.ds(pl.multiple_of(model * half, half), half)
    far = pl.ds(pl.multiple_of((1 - model) * half, half), half)
    own_rows = pl.ds(pl.multiple_of(data * rows, rows), rows)
    peer_rows = pl.ds(pl.multiple_of((1 - data) * rows, rows), rows)

    def remote(src, dst, ssem, rsem, where):
        return pltpu.make_async_remote_copy(src_ref=src, dst_ref=dst, send_sem=ssem, recv_sem=rsem, device_id=where, device_id_type=mesh_id)

    barrier = pltpu.get_barrier_semaphore()
    group = [(dm, ds) for dm in range(2) for ds in range(n_stage) if dm or ds]
    where = [{'model': lax.rem(model + dm, 2), 'stage': lax.rem(stage + ds, n_stage)} for dm, ds in group]
    for target in where + [peer]:
        pl.semaphore_signal(barrier, inc=1, device_id=target, device_id_type=mesh_id)

    def load_x(b, c, from_ref, to_rows, i):
        return pltpu.make_async_copy(from_ref.at[b, :, pl.ds(c * half, half)], inbox.at[b, c, to_rows], x_sem.at[b, c, i])

    def loads(b):
        return [load_x(b, c, *pair) for c in range(2) for pair in ((x_ref, own_rows, 0), (xf_ref, peer_rows, 1))]

    @pl.when(stage == 0)
    def _():
        for b in range(n_group):
            for copy in loads(b):
                copy.start()

    pl.semaphore_wait(barrier, len(where) + 1)

    def send_piece(p):
        span = pl.ds(pl.multiple_of(p * piece, piece), piece)
        return remote(mean_ref.at[span], far_ref.at[span], piece_ssem.at[p], piece_rsem.at[p], peer)

    def start_pieces(low, high):
        def one(p, carry):
            send_piece(p).start()
            return carry

        lax.fori_loop(low, high, one, 0)

    n_turn = n_group + 3 * LAG
    base, slope = lead
    begin = base + slope * stage
    is_even = lax.rem(stage, 2) == 0
    limit = n_piece - HELD_FWD * lax.rem(stage, 2)
    start_pieces(0, begin)

    def arrival(b, c):
        return remote(done.at[b], inbox.at[b, c], pass_ssem.at[b, 0], in_sem.at[b, c], {'model': model})

    def trade_z(b):
        return remote(zout.at[b], zin.at[b], z_ssem.at[b], z_rsem.at[b], {'model': 1 - model})

    def trade_s(b):
        return remote(yout.at[b], yin.at[b], s_ssem.at[b], s_rsem.at[b], peer)

    def trade_r(b):
        return remote(done.at[b, own_rows], done.at[b, own_rows], r_ssem.at[b], r_rsem.at[b], peer)

    def hand_on(b, to):
        return remote(done.at[b], inbox.at[b, model], pass_ssem.at[b, to], in_sem.at[b, model], {'model': to, 'stage': stage + 1})

    def landing(b, c):
        return y_ref.at[b, :, pl.ds(pl.multiple_of(c * half, half), half)]

    def publish(b, k):
        return remote(done.at[b, own_rows], landing(b, model), y_ssem.at[b, k], y_rsem.at[b, model], where[k])

    def y_arrival(b, c):
        return remote(done.at[b, own_rows], landing(b, c), y_ssem.at[b, 0], y_rsem.at[b, c], {'model': model})

    def turn(t, carry):
        @pl.when(t < n_group)
        def _():
            @pl.when(stage == 0)
            def _():
                for copy in loads(t):
                    copy.wait()

            @pl.when(stage > 0)
            def _():
                for c in range(2):
                    arrival(t, c).wait_recv()

            pre = jnp.dot(inbox[t, 0], up_ref[:half], preferred_element_type=jnp.float32)
            pre = pre + jnp.dot(inbox[t, 1], up_ref[half:], preferred_element_type=jnp.float32)
            hid[...] = jax.nn.gelu(pre).astype(jnp.bfloat16)
            zout[t] = jnp.dot(hid[...], down_ref[:, far], preferred_element_type=jnp.float32)
            trade_z(t).start()
            mine[t] = jnp.dot(hid[...], down_ref[:, near], preferred_element_type=jnp.float32)

        @pl.when((t >= LAG) & (t < n_group + LAG))
        def _():
            b = t - LAG
            trade_z(b).wait_recv()
            yout[b] = mine[b, peer_rows] + zin[b, peer_rows]
            trade_s(b).start()
            keep[b] = mine[b, own_rows] + zin[b, own_rows]

        @pl.when((t >= 2 * LAG) & (t < n_group + 2 * LAG))
        def _():
            b = t - 2 * LAG
            trade_s(b).wait_recv()
            total = inbox[b, model, own_rows].astype(jnp.float32) + (keep[b] + yin[b])
            result = total.astype(jnp.bfloat16)
            done[b, own_rows] = result

            @pl.when(stage < last)
            def _():
                trade_r(b).start()

            @pl.when(stage == last)
            def _():
                y_ref[b, :, near] = result
                for k in range(len(group)):
                    publish(b, k).start()

        @pl.when((t >= 3 * LAG) & (stage < last))
        def _():
            b = t - 3 * LAG
            remote(done.at[b, own_rows], done.at[b, peer_rows], r_ssem.at[b], r_rsem.at[b], peer).wait_recv()
            for to in range(2):
                hand_on(b, to).start()

        at = begin + t // 2

        @pl.when((lax.rem(t, 2) == 0) & (at < limit))
        def _():
            send_piece(at).start()

        return carry

    lax.fori_loop(0, n_turn, turn, 0)
    start_pieces(jnp.minimum(begin + (n_turn + 1) // 2, limit), limit)

    for b in range(n_group):
        trade_z(b).wait_send()
        trade_s(b).wait_send()

    @pl.when(stage < last)
    def _():
        for b in range(n_group):
            trade_r(b).wait_send()
            for to in range(2):
                hand_on(b, to).wait_send()
            for c in range(2):
                y_arrival(b, c).wait_recv()

    @pl.when(stage == last)
    def _():
        for b in range(n_group):
            for k in range(len(group)):
                publish(b, k).wait_send()
            y_arrival(b, 1 - model).wait_recv()

    def sent(p, carry):
        send_piece(p).wait_send()
        return carry

    def landed(p, carry):
        send_piece(p).wait_recv()
        return carry

    lax.fori_loop(0, limit, sent, 0)

    @pl.when(is_even)
    def _():
        pl.semaphore_signal(go_sem, inc=1, device_id={'stage': stage + 1}, device_id_type=mesh_id)

    @pl.when(jnp.logical_not(is_even))
    def _():
        pl.semaphore_wait(go_sem, 1)
        start_pieces(limit, n_piece)
        lax.fori_loop(limit, n_piece, sent, 0)

    lax.fori_loop(0, n_piece, landed, 0)


def forward_call(n_stage, n_group, n_piece, lead, x_next, x_far, up_bf, down_bf, mean):
    d_model = x_next.shape[2]
    x_next, x_far = [value.reshape(n_group, -1, d_model) for value in (x_next, x_far)]
    rows, half, ff_half = x_next.shape[1], d_model // 2, up_bf.shape[1]
    dma = pltpu.SemaphoreType.DMA
    f32, bf16 = jnp.float32, jnp.bfloat16
    in_vmem = pl.BlockSpec(memory_space=pltpu.VMEM)
    anywhere = pl.BlockSpec(memory_space=pl.ANY)
    return pl.pallas_call(
        functools.partial(forward_body, n_stage, lead),
        out_shape=[jax.ShapeDtypeStruct(x_next.shape, bf16), jax.ShapeDtypeStruct(mean.shape, f32)],
        in_specs=[anywhere, anywhere, in_vmem, in_vmem, anywhere],
        out_specs=[in_vmem, anywhere],
        scratch_shapes=[
            pltpu.VMEM((n_group, 2, 2 * rows, half), bf16),
            pltpu.VMEM((2 * rows, ff_half), bf16),
            pltpu.VMEM((n_group, 2 * rows, half), f32),
            pltpu.VMEM((n_group, 2 * rows, half), f32),
            pltpu.VMEM((n_group, 2 * rows, half), f32),
            pltpu.VMEM((n_group, rows, half), f32),
            pltpu.VMEM((n_group, rows, half), f32),
            pltpu.VMEM((n_group, rows, half), f32),
            pltpu.VMEM((n_group, 2 * rows, half), bf16),
            dma((n_group, 2, 2)),
            dma((n_group, 2)),
            dma((n_group,)),
            dma((n_group,)),
            dma((n_group,)),
            dma((n_group,)),
            dma((n_group,)),
            dma((n_group,)),
            dma((n_group, 2)),
            dma((n_group, 2 * n_stage - 1)),
            dma((n_group, 2)),
            dma((n_piece,)),
            dma((n_piece,)),
            pltpu.SemaphoreType.REGULAR,
        ],
        compiler_params=pltpu.CompilerParams(collective_id=1, has_side_effects=True, vmem_limit_bytes=67043328),
        name="forward_pipe",
    )(x_next, x_far, up_bf, down_bf, mean)


def solution(mesh):
    n_stage = mesh.shape['stage']
    swap = [(0, 1), (1, 0)]
    up_spec = P('stage', None, 'model')
    down_spec = P('stage', 'model', None)
    row_spec = P(None, 'data', None)
    in_specs = (up_spec, down_spec, up_spec, down_spec, up_spec, down_spec, P('data', 'stage', None, 'model'), P('data', 'stage', 'model', None), P('stage', 'data', None), P('data', None), row_spec, P(None), P(None))
    out_specs = (up_spec, down_spec, up_spec, down_spec, up_spec, down_spec, row_spec)

    def device_step(w_up, w_down, m_up, m_down, v_up, v_down, g_up, g_down, acts_last, grad_out, x_next, learn_rate, max_norm):
        data_id = lax.axis_index('data')
        half = data_id.astype(jnp.int32).reshape(1)
        other = (1 - half).astype(jnp.int32)
        d_model, ff_local = w_up.shape[1:]
        ff_half = ff_local // 2
        bounds_up = ((0, 256), (256, 704), (704, 896), (896, 960), (960, d_model))
        bounds_down = ((0, ff_half // 2), (ff_half // 2, ff_half))

        def trade(value):
            return lax.ppermute(value, 'data', swap)

        early, *late, whole_up, whole_down, far_first, x_far, clip = backward_call(n_stage, bounds_up, bounds_down, g_up[0, 0], g_down[0, 0], w_up[0], w_down[0], acts_last[0], grad_out, x_next, max_norm)
        ups = (w_up[0], m_up[0], v_up[0])
        downs = (w_down[0], m_down[0], v_down[0])

        def map_up(low, high):
            return lambda i, h, r: (low // step_of(low, high) + i, h[0])

        def map_down(i, h, r):
            return h[0] * (ff_half // BLOCK) + i, 0

        far_early = trade(early)
        *new_up, up_bf = update_call(half, learn_rate, clip, ups, whole_up, map_up(0, d_model), None)
        *new_down, down_bf = update_call(half, learn_rate, clip, downs, whole_down, map_down, None, (up_bf,))
        new_up = update_call(other, learn_rate, clip, ups, far_first, map_up(*bounds_up[0]), new_up, (down_bf,))
        down_bf, new_up = lax.optimization_barrier((down_bf, new_up))
        y_next, far_down = forward_call(n_stage, N_GROUP, N_PIECE, LEAD, x_next, x_far, up_bf, down_bf, whole_down)
        late, far_down = lax.optimization_barrier((late, far_down))
        fars = [far_early] + [trade(value) for value in late]
        *new_down, y_next = update_call(other, learn_rate, clip, downs, far_down, map_down, new_down, (), (y_next,))
        y_next = y_next.reshape(x_next.shape)
        for bounds, part in zip(bounds_up[1:], fars):
            new_up = update_call(other, learn_rate, clip, ups, part, map_up(*bounds), new_up, block=step_of(*bounds))
        return (new_up[0][None], new_down[0][None], new_up[1][None], new_down[1][None], new_up[2][None], new_down[2][None], y_next)

    return jax.shard_map(device_step, mesh=mesh, in_specs=in_specs, out_specs=out_specs, check_vma=False)
```

```python
import functools

import jax
import jax.numpy as jnp
from jax import lax
from jax.experimental import pallas as pl
from jax.experimental.pallas import tpu as pltpu
from jax.sharding import PartitionSpec as P

ADAM_STEP = 10
BETA_ONE = 0.9
BETA_TWO = 0.95
ADAM_EPS = 1e-8
WEIGHT_DECAY = 0.1
NORM_EPS = 1e-6
CONTRACT_LAST = (((1,), (1,)), ((), ()))
BLOCK = 128
N_GROUP = 8
N_PIECE = 24
LEAD = (2, 6)
HELD = 2
HELD_FWD = 3
LAG = 2
N_RAW = 4


def update_body(skip, carry, half_ref, rate_ref, clip_ref, w_ref, m_ref, v_ref, g_ref, *refs):
    outs = refs[skip:]
    if carry:
        outs[-1][...] = refs[skip - 1][...]
        outs = outs[:-1]
    ow_ref, om_ref, ov_ref = outs[:3]
    rate = rate_ref[0]
    grad = clip_ref[0:1] * g_ref[...]
    weight = w_ref[...]
    mom = BETA_ONE * m_ref[...] + (1.0 - BETA_ONE) * grad
    sec = BETA_TWO * v_ref[...] + (1.0 - BETA_TWO) * grad * grad
    one_corr = 1.0 - BETA_ONE**ADAM_STEP
    two_corr = 1.0 - BETA_TWO**ADAM_STEP
    direction = (mom * (1.0 / one_corr)) / (jnp.sqrt(sec * (1.0 / two_corr)) + ADAM_EPS)
    new = weight - rate * (direction + WEIGHT_DECAY * weight)
    ow_ref[...] = new
    om_ref[...] = mom
    ov_ref[...] = sec
    if len(outs) == 4:
        outs[3][...] = new.astype(jnp.bfloat16)


def step_of(low, high):
    return BLOCK if low % BLOCK == 0 and high % BLOCK == 0 else BLOCK // 2


def update_call(half, rate, clip, weights, grad, full_map, previous, after=(), carry=(), block=BLOCK):
    rows, cols = grad.shape
    shape = weights[0].shape
    spec = pl.BlockSpec((block, cols), full_map)
    flat = pl.BlockSpec((block, cols), lambda i, h, r: (i, 0))
    anywhere = pl.BlockSpec(memory_space=pl.ANY)
    first = previous is None
    extra = list(previous or ()) + list(after)
    passed = [pl.BlockSpec((1,) + value.shape[1:], lambda i, h, r: (jnp.minimum(i, value.shape[0] - 1), 0, 0)) for value in carry]
    return pl.pallas_call(
        functools.partial(update_body, len(extra) + len(carry), len(carry)),
        grid_spec=pltpu.PrefetchScalarGridSpec(
            num_scalar_prefetch=2,
            grid=(rows // block,),
            in_specs=[pl.BlockSpec(clip.shape, lambda i, h, r: (0, 0)), spec, spec, spec, flat] + [anywhere] * len(extra) + passed,
            out_specs=[spec] * 3 + [flat] * first + passed,
        ),
        out_shape=[jax.ShapeDtypeStruct(shape, jnp.float32)] * 3 + [jax.ShapeDtypeStruct(grad.shape, jnp.bfloat16)] * first + [jax.ShapeDtypeStruct(value.shape, value.dtype) for value in carry],
        input_output_aliases={7 + i: i for i in range(len(previous or ()))},
        cost_estimate=pl.CostEstimate(flops=60 * rows * cols, bytes_accessed=30 * rows * cols, transcendentals=0),
        compiler_params=pltpu.CompilerParams(vmem_limit_bytes=67043328),
        name="adamw_half",
    )(half, rate, clip, *weights, grad, *extra, *carry)


def backward_body(n_stage, n_raw, bounds_up, bounds_down, gu_ref, gd_ref, wu_ref, wd_ref, acts_ref, gout_ref, x_ref, max_ref, *refs):
    n_up, n_down = len(bounds_up) - 1, len(bounds_down) - 1
    outs_up, outs_down = refs[:n_up], refs[n_up:n_up + n_down]
    whole_up, whole_down, far_ref, x_far, clip_ref = refs[n_up + n_down:n_up + n_down + 5]
    (up_bf, down_bf, st_up, st_down, acc_up, acc_down, got_up, got_down, fold, hid, slope, grad_pre, gbuf, outbox, landed, ready, rows_a, rows_z, norm_box, norm_pair,
     st_sem, loc_sem, fold_sem, own_sem, out_sem, g_rsem, trade_sem, pass_ssem, rs_ssem, rs_rsem, row_ssem, row_rsem, far_sem, norm_ssem, norm_rsem, x_land, x_sem, xf_ssem, xf_rsem, go_sem, fold_up, fold_up_sem) = refs[n_up + n_down + 5:]
    model, data, stage = lax.axis_index('model'), lax.axis_index('data'), lax.axis_index('stage')
    mesh_id = pl.DeviceIdType.MESH
    last = n_stage - 1
    d_model, ff_half = acc_up.shape
    half = d_model // 2
    n_row = acts_ref.shape[0]
    n_up_chunk, n_down_chunk = d_model // BLOCK, ff_half // BLOCK
    peer = {'data': 1 - data}
    near = pl.ds(pl.multiple_of(model * half, half), half)
    far = pl.ds(pl.multiple_of((1 - model) * half, half), half)
    own_cols = pl.ds(pl.multiple_of(data * ff_half, ff_half), ff_half)
    peer_cols = pl.ds(pl.multiple_of((1 - data) * ff_half, ff_half), ff_half)
    own_rows = pl.ds(pl.multiple_of(data * n_row, n_row), n_row)
    first_dims = (((0,), (0,)), ((), ()))

    def remote(src, dst, ssem, rsem, where):
        return pltpu.make_async_remote_copy(src_ref=src, dst_ref=dst, send_sem=ssem, recv_sem=rsem, device_id=where, device_id_type=mesh_id)

    barrier = pltpu.get_barrier_semaphore()
    group = [(dm, ds) for dm in range(2) for ds in range(n_stage) if dm or ds]
    where = [{'model': lax.rem(model + dm, 2), 'stage': lax.rem(stage + ds, n_stage)} for dm, ds in group]
    for target in where + [peer]:
        pl.semaphore_signal(barrier, inc=1, device_id=target, device_id_type=mesh_id)

    n_st_up, n_st_down = d_model // st_up.shape[1], 2 * ff_half // st_down.shape[1]

    def load_up(r):
        return pltpu.make_async_copy(wu_ref.at[pl.ds(r * st_up.shape[1], st_up.shape[1])], st_up.at[r % 2], st_sem.at[0, r % 2])

    def load_down(r):
        return pltpu.make_async_copy(wd_ref.at[pl.ds(r * st_down.shape[1], st_down.shape[1])], st_down.at[r % 2], st_sem.at[1, r % 2])

    load_acts = pltpu.make_async_copy(acts_ref, rows_a.at[own_rows], loc_sem.at[0])
    load_acts.start()
    load_up(0).start()
    load_up(1).start()
    load_down(0).start()
    load_down(1).start()

    def load_g(c):
        return pltpu.make_async_copy(gout_ref.at[:, pl.ds(c * half, half)], gbuf.at[c], loc_sem.at[1 + c])

    @pl.when(stage == last)
    def _():
        for c in range(2):
            load_g(c).start()

    pl.semaphore_wait(barrier, len(where) + 1)

    def chunk(k):
        return pl.ds(k * BLOCK, BLOCK)

    raw_rows = n_raw * BLOCK
    raw = [remote(gu_ref.at[chunk(k), peer_cols], got_up.at[chunk(k)], rs_ssem.at[0, k], rs_rsem.at[0, k], peer) for k in range(n_raw)]
    carries_x = stage >= n_stage // 2

    def micro(i):
        return 2 * (stage - n_stage // 2) + i

    def send_x(i):
        return remote(x_ref.at[micro(i), :, near], x_land.at[i], x_sem.at[0, i], x_sem.at[1, i], peer)

    @pl.when(carries_x)
    def _():
        for i in range(2):
            send_x(i).start()

    for copy in raw:
        copy.start()
    send_a = remote(acts_ref.at[:, :raw_rows], rows_a.at[own_rows, :raw_rows], row_ssem.at[0], row_rsem.at[0], peer)
    send_a.start()

    for r in range(n_st_up):
        load_up(r).wait()
        up_bf[pl.ds(r * st_up.shape[1], st_up.shape[1])] = st_up[r % 2].astype(jnp.bfloat16)
        if r + 2 < n_st_up:
            load_up(r + 2).start()
    load_acts.wait()

    tile = 256
    n_tile = hid.shape[1] // tile
    scale = 0.7978845608028654
    cubic = 0.044715

    def pre_tile(j, carry):
        cols = pl.ds(pl.multiple_of(j * tile, tile), tile)
        pre = jnp.dot(rows_a[own_rows], up_bf[:, cols], preferred_element_type=jnp.float32)
        square = pre * pre
        bend = jnp.tanh(scale * (pre + cubic * square * pre))
        hid[:, cols] = (pre * (0.5 * (1.0 + bend))).astype(jnp.bfloat16)
        slope[:, cols] = 0.5 * (1.0 + bend) + 0.5 * pre * (1.0 - bend * bend) * (scale * (1.0 + 3.0 * cubic * square))
        return carry

    lax.fori_loop(0, n_tile, pre_tile, 0)

    for r in range(n_st_down):
        load_down(r).wait()
        down_bf[pl.ds(r * st_down.shape[1], st_down.shape[1])] = st_down[r % 2].astype(jnp.bfloat16)
        if r + 2 < n_st_down:
            load_down(r + 2).start()

    own_up = pltpu.make_async_copy(gu_ref.at[:, own_cols], acc_up, own_sem.at[0])
    own_down = pltpu.make_async_copy(gd_ref.at[own_cols], acc_down, own_sem.at[1])
    load_fold = pltpu.make_async_copy(gd_ref.at[peer_cols], fold, fold_sem)
    load_fold_up = pltpu.make_async_copy(gu_ref.at[raw_rows:, peer_cols], fold_up, fold_up_sem)
    load_fold_up.start()
    load_fold.start()
    own_up.start()
    own_down.start()

    @pl.when(stage == last)
    def _():
        for c in range(2):
            load_g(c).wait()

    @pl.when(stage < last)
    def _():
        for c in range(2):
            remote(ready, gbuf.at[c], pass_ssem.at[0], g_rsem.at[c], {'model': model}).wait_recv()

    def slope_tile(j, carry):
        cols = pl.ds(pl.multiple_of(j * tile, tile), tile)
        grad = lax.dot_general(gbuf[0], down_bf[cols, :half], CONTRACT_LAST, preferred_element_type=jnp.float32)
        grad = grad + lax.dot_general(gbuf[1], down_bf[cols, half:], CONTRACT_LAST, preferred_element_type=jnp.float32)
        grad_pre[:, cols] = (slope[:, cols] * grad).astype(jnp.bfloat16)
        return carry

    lax.fori_loop(0, n_tile, slope_tile, 0)

    trade = remote(outbox, landed, trade_sem.at[0], trade_sem.at[1], {'model': 1 - model})

    def hand_on(to):
        return remote(ready, gbuf.at[model], pass_ssem.at[to], g_rsem.at[model], {'model': to, 'stage': stage - 1})

    @pl.when(stage > 0)
    def _():
        outbox[...] = lax.dot_general(grad_pre[...], up_bf[far], CONTRACT_LAST, preferred_element_type=jnp.float32)
        trade.start()
        mine = lax.dot_general(grad_pre[...], up_bf[near], CONTRACT_LAST, preferred_element_type=jnp.float32)
        trade.wait_recv()
        ready[...] = (gbuf[model].astype(jnp.float32) + (mine + landed[...])).astype(jnp.bfloat16)
        for to in range(2):
            hand_on(to).start()

    rows_z[own_rows] = grad_pre[:, own_cols]
    send_z = remote(grad_pre.at[:, peer_cols], rows_z.at[own_rows], row_ssem.at[1], row_rsem.at[1], peer)
    send_z.start()

    load_fold_up.wait()

    def send_fold_up(k):
        rows = pl.ds(pl.multiple_of(k * BLOCK, BLOCK), BLOCK)
        at = pl.ds(pl.multiple_of((n_raw + k) * BLOCK, BLOCK), BLOCK)
        return remote(fold_up.at[rows], got_up.at[at], rs_ssem.at[0, n_raw + k], rs_rsem.at[0, n_raw + k], peer)

    def fold_up_step(k, carry):
        rows = pl.ds(pl.multiple_of(k * BLOCK, BLOCK), BLOCK)
        at = pl.ds(pl.multiple_of((n_raw + k) * BLOCK, BLOCK), BLOCK)
        fold_up[rows] += lax.dot_general(rows_a[own_rows, at], grad_pre[:, peer_cols], first_dims, preferred_element_type=jnp.float32)
        send_fold_up(k).start()
        return carry

    lax.fori_loop(0, n_up_chunk - n_raw, fold_up_step, 0)

    def forward_x(i, to):
        return remote(x_land.at[i], x_far.at[micro(i), :, near], xf_ssem.at[i, to], xf_rsem.at[micro(i), model], {'model': to, 'stage': 0})

    @pl.when(carries_x)
    def _():
        for i in range(2):
            send_x(i).wait_recv()
            for to in range(2):
                forward_x(i, to).start()

    def down_product(k, side):
        cols = pl.ds(pl.multiple_of(side * ff_half + k * BLOCK, BLOCK), BLOCK)
        left = hid[:, cols]
        return [lax.dot_general(left, gbuf[c], first_dims, preferred_element_type=jnp.float32) for c in range(2)]

    load_fold.wait()

    def send_fold(k):
        rows = pl.ds(pl.multiple_of(k * BLOCK, BLOCK), BLOCK)
        return remote(fold.at[rows], got_down.at[rows], rs_ssem.at[1, k], rs_rsem.at[1, k], peer)

    def fold_step(k, carry):
        rows = pl.ds(pl.multiple_of(k * BLOCK, BLOCK), BLOCK)
        low, high = down_product(k, 1 - data)
        fold[rows, :half] += low
        fold[rows, half:] += high
        send_fold(k).start()
        return carry

    lax.fori_loop(0, n_down_chunk, fold_step, 0)
    own_down.wait()

    def own_step(k, carry):
        rows = pl.ds(pl.multiple_of(k * BLOCK, BLOCK), BLOCK)
        low, high = down_product(k, data)
        acc_down[rows, :half] += low
        acc_down[rows, half:] += high
        return carry

    lax.fori_loop(0, n_down_chunk, own_step, 0)

    @pl.when(stage > 0)
    def _():
        trade.wait_send()
        for to in range(2):
            hand_on(to).wait_send()

    own_up.wait()
    send_a.wait_recv()
    squares = jnp.zeros((8, ff_half), jnp.float32)

    def fold_squares(mean):
        return jnp.sum((mean * mean).reshape(-1, 8, mean.shape[1]), axis=0)

    def put(acc, bounds, outs, whole, sem_row):
        copies = []
        for i, (lo, hi) in enumerate(bounds):
            rows = pl.ds(lo, hi - lo)
            copies.append(pltpu.make_async_copy(acc.at[rows], whole.at[rows], out_sem.at[sem_row, i]))
            if outs[i] is not None:
                copies.append(pltpu.make_async_copy(acc.at[rows], outs[i], out_sem.at[sem_row, len(bounds) + i]))
        return copies

    def put_start(k, bounds, copies, outs):
        at = 0
        for i, (lo, hi) in enumerate(bounds):
            count = 1 if outs[i] is None else 2
            if k * BLOCK < hi <= (k + 1) * BLOCK:
                for copy in copies[at:at + count]:
                    copy.start()
            at += count

    outs_up = (None,) + tuple(outs_up)
    outs_down = (None,) + tuple(outs_down)
    put_up = put(acc_up, bounds_up, outs_up, whole_up, 0)
    put_down = put(acc_down, bounds_down, outs_down, whole_down, 1)
    for k in range(n_up_chunk):
        if k == 0:
            send_z.wait_recv()
        if k < n_raw:
            raw[k].wait_recv()
            product = lax.dot_general(rows_a[:, chunk(k)], rows_z[...], first_dims, preferred_element_type=jnp.float32)
        else:
            send_fold_up(k - n_raw).wait_recv()
            product = lax.dot_general(rows_a[own_rows, chunk(k)], rows_z[own_rows], first_dims, preferred_element_type=jnp.float32)
        mean = (acc_up[chunk(k)] + got_up[chunk(k)] + product) * 0.5
        acc_up[chunk(k)] = mean
        squares = squares + fold_squares(mean)
        put_start(k, bounds_up, put_up, outs_up)
    n_far = far_sem.shape[1]
    slab = bounds_up[0][1] // n_far
    is_even = lax.rem(stage, 2) == 0

    def send_far(i):
        span = pl.ds(pl.multiple_of(i * slab, slab), slab)
        return remote(acc_up.at[span], far_ref.at[span], far_sem.at[0, i], far_sem.at[1, i], peer)

    for i in range(n_far - HELD):
        send_far(i).start()

    @pl.when(is_even)
    def _():
        for i in range(n_far - HELD, n_far):
            send_far(i).start()

    for k in range(n_down_chunk):
        send_fold(k).wait_recv()
        mean = (acc_down[chunk(k)] + got_down[chunk(k)]) * 0.5
        acc_down[chunk(k)] = mean
        squares = squares + fold_squares(mean)
        put_start(k, bounds_down, put_down, outs_down)

    lanes = norm_box.shape[2]
    part = squares[:, :lanes]
    for j in range(1, ff_half // lanes):
        part = part + squares[:, j * lanes:(j + 1) * lanes]
    me = model * n_stage + stage
    norm_box[me] = part

    def spread(i):
        return remote(norm_box.at[me], norm_box.at[me], norm_ssem.at[i], norm_rsem.at[me], where[i])

    for i in range(len(group)):
        spread(i).start()
    for i, (dm, ds) in enumerate(group):
        them = lax.rem(model + dm, 2) * n_stage + lax.rem(stage + ds, n_stage)
        remote(norm_box.at[me], norm_box.at[them], norm_ssem.at[i], norm_rsem.at[them], where[i]).wait_recv()
    total = norm_box[0]
    for i in range(1, 2 * n_stage):
        total = total + norm_box[i]
    norm_pair[0] = total
    swap = remote(norm_pair.at[0], norm_pair.at[1], norm_ssem.at[len(group)], norm_rsem.at[2 * n_stage], peer)
    swap.start()
    swap.wait_recv()
    norm_sq = jnp.sum(norm_pair[0] + norm_pair[1], axis=(0, 1), keepdims=True)
    norm = jnp.sqrt(jnp.broadcast_to(norm_sq, clip_ref.shape)) + NORM_EPS
    clip_ref[...] = jnp.minimum(1.0, max_ref[0] / norm)

    @pl.when(carries_x)
    def _():
        for i in range(2):
            send_x(i).wait_send()
            for to in range(2):
                forward_x(i, to).wait_send()

    @pl.when(stage == 0)
    def _():
        for s in range(n_stage):
            for m in range(2):
                remote(x_land.at[0], x_far.at[s, :, pl.ds(m * half, half)], xf_ssem.at[0, m], xf_rsem.at[s, m], {'model': model}).wait_recv()

    swap.wait_send()
    for i in range(len(group)):
        spread(i).wait_send()
    for copy in raw + [send_a, send_z]:
        copy.wait_send()
    for k in range(n_down_chunk):
        send_fold(k).wait_send()
    for k in range(n_up_chunk - n_raw):
        send_fold_up(k).wait_send()
    for copy in put_up + put_down:
        copy.wait()

    @pl.when(is_even)
    def _():
        for i in range(n_far):
            send_far(i).wait_send()
        pl.semaphore_signal(go_sem, inc=1, device_id={'stage': stage + 1}, device_id_type=mesh_id)

    @pl.when(jnp.logical_not(is_even))
    def _():
        pl.semaphore_wait(go_sem, 1)
        for i in range(n_far - HELD, n_far):
            send_far(i).start()
        for i in range(n_far):
            send_far(i).wait_send()

    for i in range(n_far):
        send_far(i).wait_recv()


def backward_call(n_stage, bounds_up, bounds_down, g_up, g_down, w_up, w_down, acts, grad_out, x_next, max_norm):
    d_model, ff_local = g_up.shape
    ff_half, half, n_row = ff_local // 2, d_model // 2, acts.shape[0]
    dma = pltpu.SemaphoreType.DMA
    anywhere = pl.BlockSpec(memory_space=pl.ANY)
    f32, bf16 = jnp.float32, jnp.bfloat16
    shapes = [jax.ShapeDtypeStruct((hi - lo, ff_half), f32) for lo, hi in bounds_up[1:]]
    shapes += [jax.ShapeDtypeStruct((hi - lo, d_model), f32) for lo, hi in bounds_down[1:]]
    shapes += [jax.ShapeDtypeStruct((d_model, ff_half), f32), jax.ShapeDtypeStruct((ff_half, d_model), f32)]
    shapes += [jax.ShapeDtypeStruct((bounds_up[0][1], ff_half), f32), jax.ShapeDtypeStruct(x_next.shape, bf16), jax.ShapeDtypeStruct((8, ff_half), f32)]
    n_chunk = max(d_model, ff_half) // BLOCK
    return pl.pallas_call(
        functools.partial(backward_body, n_stage, N_RAW, bounds_up, bounds_down),
        out_shape=shapes,
        in_specs=[anywhere] * 7 + [pl.BlockSpec(memory_space=pltpu.SMEM)],
        out_specs=[anywhere] * (len(shapes) - 1) + [pl.BlockSpec(memory_space=pltpu.VMEM)],
        scratch_shapes=[
            pltpu.VMEM((d_model, ff_local), bf16),
            pltpu.VMEM((ff_local, d_model), bf16),
            pltpu.VMEM((2, 256, ff_local), f32),
            pltpu.VMEM((2, 512, d_model), f32),
            pltpu.VMEM((d_model, ff_half), f32),
            pltpu.VMEM((ff_half, d_model), f32),
            pltpu.VMEM((d_model, ff_half), f32),
            pltpu.VMEM((ff_half, d_model), f32),
            pltpu.VMEM((ff_half, d_model), f32),
            pltpu.VMEM((n_row, ff_local), bf16),
            pltpu.VMEM((n_row, ff_local), f32),
            pltpu.VMEM((n_row, ff_local), bf16),
            pltpu.VMEM((2, n_row, half), bf16),
            pltpu.VMEM((n_row, half), f32),
            pltpu.VMEM((n_row, half), f32),
            pltpu.VMEM((n_row, half), bf16),
            pltpu.VMEM((2 * n_row, d_model), bf16),
            pltpu.VMEM((2 * n_row, ff_half), bf16),
            pltpu.VMEM((2 * n_stage, 8, 128), f32),
            pltpu.VMEM((2, 8, 128), f32),
            dma((2, 2)),
            dma((3,)),
            dma(()),
            dma((2,)),
            dma((2, 2 * max(len(bounds_up), len(bounds_down)))),
            dma((2,)),
            dma((2,)),
            dma((2,)),
            dma((2, n_chunk)),
            dma((2, n_chunk)),
            dma((2,)),
            dma((2,)),
            dma((2, 8)),
            dma((2 * n_stage,)),
            dma((2 * n_stage + 1,)),
            pltpu.VMEM((2, n_row, half), bf16),
            dma((2, 2)),
            dma((2, 2)),
            dma((n_stage, 2)),
            pltpu.SemaphoreType.REGULAR,
            pltpu.VMEM((d_model - N_RAW * BLOCK, ff_half), f32),
            dma(()),
        ],
        compiler_params=pltpu.CompilerParams(collective_id=0, has_side_effects=True, vmem_limit_bytes=67043328),
        name="reduce_and_norm",
    )(g_up, g_down, w_up, w_down, acts, grad_out, x_next, max_norm)


def forward_body(n_stage, lead, x_ref, xf_ref, up_ref, down_ref, mean_ref, y_ref, far_ref, inbox, hid, mine, zout, zin, keep, yout, yin, done, x_sem, in_sem, z_ssem, z_rsem, s_ssem, s_rsem, r_ssem, r_rsem, pass_ssem, y_ssem, y_rsem, piece_ssem, piece_rsem, go_sem):
    model, data, stage = lax.axis_index('model'), lax.axis_index('data'), lax.axis_index('stage')
    mesh_id = pl.DeviceIdType.MESH
    last = n_stage - 1
    n_group, _, rows2, half = inbox.shape
    rows = rows2 // 2
    n_piece = piece_ssem.shape[0]
    piece = far_ref.shape[0] // n_piece
    peer = {'data': 1 - data}
    near = pl.ds(pl.multiple_of(model * half, half), half)
    far = pl.ds(pl.multiple_of((1 - model) * half, half), half)
    own_rows = pl.ds(pl.multiple_of(data * rows, rows), rows)
    peer_rows = pl.ds(pl.multiple_of((1 - data) * rows, rows), rows)

    def remote(src, dst, ssem, rsem, where):
        return pltpu.make_async_remote_copy(src_ref=src, dst_ref=dst, send_sem=ssem, recv_sem=rsem, device_id=where, device_id_type=mesh_id)

    barrier = pltpu.get_barrier_semaphore()
    group = [(dm, ds) for dm in range(2) for ds in range(n_stage) if dm or ds]
    where = [{'model': lax.rem(model + dm, 2), 'stage': lax.rem(stage + ds, n_stage)} for dm, ds in group]
    for target in where + [peer]:
        pl.semaphore_signal(barrier, inc=1, device_id=target, device_id_type=mesh_id)

    def load_x(b, c, from_ref, to_rows, i):
        return pltpu.make_async_copy(from_ref.at[b, :, pl.ds(c * half, half)], inbox.at[b, c, to_rows], x_sem.at[b, c, i])

    def loads(b):
        return [load_x(b, c, *pair) for c in range(2) for pair in ((x_ref, own_rows, 0), (xf_ref, peer_rows, 1))]

    @pl.when(stage == 0)
    def _():
        for b in range(n_group):
            for copy in loads(b):
                copy.start()

    pl.semaphore_wait(barrier, len(where) + 1)

    def send_piece(p):
        span = pl.ds(pl.multiple_of(p * piece, piece), piece)
        return remote(mean_ref.at[span], far_ref.at[span], piece_ssem.at[p], piece_rsem.at[p], peer)

    def start_pieces(low, high):
        def one(p, carry):
            send_piece(p).start()
            return carry

        lax.fori_loop(low, high, one, 0)

    n_turn = n_group + 3 * LAG
    base, slope = lead
    is_even = lax.rem(stage, 2) == 0
    limit = n_piece - HELD_FWD * lax.rem(stage, 2)
    begin = jnp.minimum(base + slope * stage, limit)
    start_pieces(0, begin)

    def arrival(b, c):
        return remote(done.at[b], inbox.at[b, c], pass_ssem.at[b, 0], in_sem.at[b, c], {'model': model})

    def trade_z(b):
        return remote(zout.at[b], zin.at[b], z_ssem.at[b], z_rsem.at[b], {'model': 1 - model})

    def trade_s(b):
        return remote(yout.at[b], yin.at[b], s_ssem.at[b], s_rsem.at[b], peer)

    def trade_r(b):
        return remote(done.at[b, own_rows], done.at[b, own_rows], r_ssem.at[b], r_rsem.at[b], peer)

    def hand_on(b, to):
        return remote(done.at[b], inbox.at[b, model], pass_ssem.at[b, to], in_sem.at[b, model], {'model': to, 'stage': stage + 1})

    def landing(b, c):
        return y_ref.at[b, :, pl.ds(pl.multiple_of(c * half, half), half)]

    def publish(b, k):
        return remote(done.at[b, own_rows], landing(b, model), y_ssem.at[b, k], y_rsem.at[b, model], where[k])

    def y_arrival(b, c):
        return remote(done.at[b, own_rows], landing(b, c), y_ssem.at[b, 0], y_rsem.at[b, c], {'model': model})

    def turn(t, carry):
        @pl.when(t < n_group)
        def _():
            @pl.when(stage == 0)
            def _():
                for copy in loads(t):
                    copy.wait()

            @pl.when(stage > 0)
            def _():
                for c in range(2):
                    arrival(t, c).wait_recv()

            pre = jnp.dot(inbox[t, 0], up_ref[:half], preferred_element_type=jnp.float32)
            pre = pre + jnp.dot(inbox[t, 1], up_ref[half:], preferred_element_type=jnp.float32)
            hid[...] = jax.nn.gelu(pre).astype(jnp.bfloat16)
            zout[t] = jnp.dot(hid[...], down_ref[:, far], preferred_element_type=jnp.float32)
            trade_z(t).start()
            mine[t] = jnp.dot(hid[...], down_ref[:, near], preferred_element_type=jnp.float32)

        @pl.when((t >= LAG) & (t < n_group + LAG))
        def _():
            b = t - LAG
            trade_z(b).wait_recv()
            yout[b] = mine[b, peer_rows] + zin[b, peer_rows]
            trade_s(b).start()
            keep[b] = mine[b, own_rows] + zin[b, own_rows]

        @pl.when((t >= 2 * LAG) & (t < n_group + 2 * LAG))
        def _():
            b = t - 2 * LAG
            trade_s(b).wait_recv()
            total = inbox[b, model, own_rows].astype(jnp.float32) + (keep[b] + yin[b])
            result = total.astype(jnp.bfloat16)
            done[b, own_rows] = result

            @pl.when(stage < last)
            def _():
                trade_r(b).start()

            @pl.when(stage == last)
            def _():
                y_ref[b, :, near] = result
                for k in range(len(group)):
                    publish(b, k).start()

        @pl.when((t >= 3 * LAG) & (stage < last))
        def _():
            b = t - 3 * LAG
            remote(done.at[b, own_rows], done.at[b, peer_rows], r_ssem.at[b], r_rsem.at[b], peer).wait_recv()
            for to in range(2):
                hand_on(b, to).start()

        at = begin + t // 2

        @pl.when((lax.rem(t, 2) == 0) & (at < limit))
        def _():
            send_piece(at).start()

        return carry

    lax.fori_loop(0, n_turn, turn, 0)
    start_pieces(jnp.minimum(begin + (n_turn + 1) // 2, limit), limit)

    for b in range(n_group):
        trade_z(b).wait_send()
        trade_s(b).wait_send()

    @pl.when(stage < last)
    def _():
        for b in range(n_group):
            trade_r(b).wait_send()
            for to in range(2):
                hand_on(b, to).wait_send()
            for c in range(2):
                y_arrival(b, c).wait_recv()

    @pl.when(stage == last)
    def _():
        for b in range(n_group):
            for k in range(len(group)):
                publish(b, k).wait_send()
            y_arrival(b, 1 - model).wait_recv()

    def sent(p, carry):
        send_piece(p).wait_send()
        return carry

    def landed(p, carry):
        send_piece(p).wait_recv()
        return carry

    lax.fori_loop(0, limit, sent, 0)

    @pl.when(is_even)
    def _():
        pl.semaphore_signal(go_sem, inc=1, device_id={'stage': stage + 1}, device_id_type=mesh_id)

    @pl.when(jnp.logical_not(is_even))
    def _():
        pl.semaphore_wait(go_sem, 1)
        start_pieces(limit, n_piece)
        lax.fori_loop(limit, n_piece, sent, 0)

    lax.fori_loop(0, n_piece, landed, 0)


def forward_call(n_stage, n_group, n_piece, lead, n_far, x_next, x_far, up_bf, down_bf, mean):
    d_model = x_next.shape[2]
    x_next, x_far = [value.reshape(n_group, -1, d_model) for value in (x_next, x_far)]
    rows, half, ff_half = x_next.shape[1], d_model // 2, up_bf.shape[1]
    dma = pltpu.SemaphoreType.DMA
    f32, bf16 = jnp.float32, jnp.bfloat16
    in_vmem = pl.BlockSpec(memory_space=pltpu.VMEM)
    anywhere = pl.BlockSpec(memory_space=pl.ANY)
    return pl.pallas_call(
        functools.partial(forward_body, n_stage, lead),
        out_shape=[jax.ShapeDtypeStruct(x_next.shape, bf16), jax.ShapeDtypeStruct((n_far, d_model), f32)],
        in_specs=[anywhere, anywhere, in_vmem, in_vmem, anywhere],
        out_specs=[in_vmem, anywhere],
        scratch_shapes=[
            pltpu.VMEM((n_group, 2, 2 * rows, half), bf16),
            pltpu.VMEM((2 * rows, ff_half), bf16),
            pltpu.VMEM((n_group, 2 * rows, half), f32),
            pltpu.VMEM((n_group, 2 * rows, half), f32),
            pltpu.VMEM((n_group, 2 * rows, half), f32),
            pltpu.VMEM((n_group, rows, half), f32),
            pltpu.VMEM((n_group, rows, half), f32),
            pltpu.VMEM((n_group, rows, half), f32),
            pltpu.VMEM((n_group, 2 * rows, half), bf16),
            dma((n_group, 2, 2)),
            dma((n_group, 2)),
            dma((n_group,)),
            dma((n_group,)),
            dma((n_group,)),
            dma((n_group,)),
            dma((n_group,)),
            dma((n_group,)),
            dma((n_group, 2)),
            dma((n_group, 2 * n_stage - 1)),
            dma((n_group, 2)),
            dma((n_piece,)),
            dma((n_piece,)),
            pltpu.SemaphoreType.REGULAR,
        ],
        compiler_params=pltpu.CompilerParams(collective_id=1, has_side_effects=True, vmem_limit_bytes=67043328),
        name="forward_pipe",
    )(x_next, x_far, up_bf, down_bf, mean)


def solution(mesh):
    n_stage = mesh.shape['stage']
    swap = [(0, 1), (1, 0)]
    up_spec = P('stage', None, 'model')
    down_spec = P('stage', 'model', None)
    row_spec = P(None, 'data', None)
    in_specs = (up_spec, down_spec, up_spec, down_spec, up_spec, down_spec, P('data', 'stage', None, 'model'), P('data', 'stage', 'model', None), P('stage', 'data', None), P('data', None), row_spec, P(None), P(None))
    out_specs = (up_spec, down_spec, up_spec, down_spec, up_spec, down_spec, row_spec)

    def device_step(w_up, w_down, m_up, m_down, v_up, v_down, g_up, g_down, acts_last, grad_out, x_next, learn_rate, max_norm):
        data_id = lax.axis_index('data')
        half = data_id.astype(jnp.int32).reshape(1)
        other = (1 - half).astype(jnp.int32)
        d_model, ff_local = w_up.shape[1:]
        ff_half = ff_local // 2
        bounds_up = ((0, 256), (256, 704), (704, 896), (896, 960), (960, d_model))
        bounds_down = ((0, N_PIECE * 32), (N_PIECE * 32, ff_half))

        def trade(value):
            return lax.ppermute(value, 'data', swap)

        early, *late, late_down, whole_up, whole_down, far_first, x_far, clip = backward_call(n_stage, bounds_up, bounds_down, g_up[0, 0], g_down[0, 0], w_up[0], w_down[0], acts_last[0], grad_out, x_next, max_norm)
        ups = (w_up[0], m_up[0], v_up[0])
        downs = (w_down[0], m_down[0], v_down[0])

        def map_up(low, high):
            return lambda i, h, r: (low // step_of(low, high) + i, h[0])

        def map_down(low):
            return lambda i, h, r: ((h[0] * ff_half + low) // BLOCK + i, 0)

        far_early = trade(early)
        *new_up, up_bf = update_call(half, learn_rate, clip, ups, whole_up, map_up(0, d_model), None)
        *new_down, down_bf = update_call(half, learn_rate, clip, downs, whole_down, map_down(0), None, (up_bf,))
        new_up = update_call(other, learn_rate, clip, ups, far_first, map_up(*bounds_up[0]), new_up, (down_bf,))
        down_bf, new_up = lax.optimization_barrier((down_bf, new_up))
        y_next, far_down = forward_call(n_stage, N_GROUP, N_PIECE, LEAD, bounds_down[0][1], x_next, x_far, up_bf, down_bf, whole_down)
        y_next = y_next.reshape(x_next.shape)
        late, late_down, far_down = lax.optimization_barrier((late, late_down, far_down))
        far_last = trade(late_down)
        fars = [trade(value) for value in late]
        *new_down, y_next = update_call(other, learn_rate, clip, downs, far_down, map_down(0), new_down, (), (y_next,))
        new_up = update_call(other, learn_rate, clip, ups, far_early, map_up(*bounds_up[1]), new_up, (new_down[0],), block=step_of(*bounds_up[1]))
        new_down = update_call(other, learn_rate, clip, downs, far_last, map_down(bounds_down[1][0]), new_down, (new_up[0],))
        after = (new_down[0],)
        for bounds, part in zip(bounds_up[2:], fars):
            new_up = update_call(other, learn_rate, clip, ups, part, map_up(*bounds), new_up, after, block=step_of(*bounds))
            after = ()
        return (new_up[0][None], new_down[0][None], new_up[1][None], new_down[1][None], new_up[2][None], new_down[2][None], y_next)

    return jax.shard_map(device_step, mesh=mesh, in_specs=in_specs, out_specs=out_specs, check_vma=False)
```

```python
import functools

import jax
import jax.numpy as jnp
from jax import lax
from jax.experimental import pallas as pl
from jax.experimental.pallas import tpu as pltpu
from jax.sharding import PartitionSpec as P

ADAM_STEP = 10
BETA_ONE = 0.9
BETA_TWO = 0.95
ADAM_EPS = 1e-8
WEIGHT_DECAY = 0.1
NORM_EPS = 1e-6
CONTRACT_LAST = (((1,), (1,)), ((), ()))
BLOCK = 128
N_GROUP = 8
N_PIECE = 28
LEAD = (3, 7)
HELD = 2
HELD_FWD = 3
LAG = 2
N_RAW = 4


def update_body(skip, carry, half_ref, rate_ref, clip_ref, w_ref, m_ref, v_ref, g_ref, *refs):
    outs = refs[skip:]
    if carry:
        outs[-1][...] = refs[skip - 1][...]
        outs = outs[:-1]
    ow_ref, om_ref, ov_ref = outs[:3]
    rate = rate_ref[0]
    grad = clip_ref[0:1] * g_ref[...]
    weight = w_ref[...]
    mom = BETA_ONE * m_ref[...] + (1.0 - BETA_ONE) * grad
    sec = BETA_TWO * v_ref[...] + (1.0 - BETA_TWO) * grad * grad
    one_corr = 1.0 - BETA_ONE**ADAM_STEP
    two_corr = 1.0 - BETA_TWO**ADAM_STEP
    direction = (mom * (1.0 / one_corr)) / (jnp.sqrt(sec * (1.0 / two_corr)) + ADAM_EPS)
    new = weight - rate * (direction + WEIGHT_DECAY * weight)
    ow_ref[...] = new
    om_ref[...] = mom
    ov_ref[...] = sec
    if len(outs) == 4:
        outs[3][...] = new.astype(jnp.bfloat16)


def step_of(low, high):
    return BLOCK if low % BLOCK == 0 and high % BLOCK == 0 else BLOCK // 2


def update_call(half, rate, clip, weights, grad, full_map, previous, after=(), carry=(), block=BLOCK):
    rows, cols = grad.shape
    shape = weights[0].shape
    spec = pl.BlockSpec((block, cols), full_map)
    flat = pl.BlockSpec((block, cols), lambda i, h, r: (i, 0))
    anywhere = pl.BlockSpec(memory_space=pl.ANY)
    first = previous is None
    extra = list(previous or ()) + list(after)
    passed = [pl.BlockSpec((1,) + value.shape[1:], lambda i, h, r: (jnp.minimum(i, value.shape[0] - 1), 0, 0)) for value in carry]
    return pl.pallas_call(
        functools.partial(update_body, len(extra) + len(carry), len(carry)),
        grid_spec=pltpu.PrefetchScalarGridSpec(
            num_scalar_prefetch=2,
            grid=(rows // block,),
            in_specs=[pl.BlockSpec(clip.shape, lambda i, h, r: (0, 0)), spec, spec, spec, flat] + [anywhere] * len(extra) + passed,
            out_specs=[spec] * 3 + [flat] * first + passed,
        ),
        out_shape=[jax.ShapeDtypeStruct(shape, jnp.float32)] * 3 + [jax.ShapeDtypeStruct(grad.shape, jnp.bfloat16)] * first + [jax.ShapeDtypeStruct(value.shape, value.dtype) for value in carry],
        input_output_aliases={7 + i: i for i in range(len(previous or ()))},
        cost_estimate=pl.CostEstimate(flops=60 * rows * cols, bytes_accessed=30 * rows * cols, transcendentals=0),
        compiler_params=pltpu.CompilerParams(vmem_limit_bytes=67043328),
        name="adamw_half",
    )(half, rate, clip, *weights, grad, *extra, *carry)


def backward_body(n_stage, n_raw, bounds_up, bounds_down, gu_ref, gd_ref, wu_ref, wd_ref, acts_ref, gout_ref, x_ref, max_ref, *refs):
    n_up, n_down = len(bounds_up) - 1, len(bounds_down) - 1
    outs_up, outs_down = refs[:n_up], refs[n_up:n_up + n_down]
    whole_up, whole_down, far_ref, x_far, clip_ref = refs[n_up + n_down:n_up + n_down + 5]
    (up_bf, down_bf, st_up, st_down, acc_up, acc_down, got_up, got_down, fold, hid, slope, grad_pre, gbuf, outbox, landed, ready, rows_a, rows_z, norm_box, norm_pair,
     st_sem, loc_sem, fold_sem, own_sem, out_sem, g_rsem, trade_sem, pass_ssem, rs_ssem, rs_rsem, row_ssem, row_rsem, far_sem, norm_ssem, norm_rsem, x_land, x_sem, xf_ssem, xf_rsem, go_sem, fold_up, fold_up_sem) = refs[n_up + n_down + 5:]
    model, data, stage = lax.axis_index('model'), lax.axis_index('data'), lax.axis_index('stage')
    mesh_id = pl.DeviceIdType.MESH
    last = n_stage - 1
    d_model, ff_half = acc_up.shape
    half = d_model // 2
    n_row = acts_ref.shape[0]
    n_up_chunk, n_down_chunk = d_model // BLOCK, ff_half // BLOCK
    peer = {'data': 1 - data}
    near = pl.ds(pl.multiple_of(model * half, half), half)
    far = pl.ds(pl.multiple_of((1 - model) * half, half), half)
    own_cols = pl.ds(pl.multiple_of(data * ff_half, ff_half), ff_half)
    peer_cols = pl.ds(pl.multiple_of((1 - data) * ff_half, ff_half), ff_half)
    own_rows = pl.ds(pl.multiple_of(data * n_row, n_row), n_row)
    first_dims = (((0,), (0,)), ((), ()))

    def remote(src, dst, ssem, rsem, where):
        return pltpu.make_async_remote_copy(src_ref=src, dst_ref=dst, send_sem=ssem, recv_sem=rsem, device_id=where, device_id_type=mesh_id)

    barrier = pltpu.get_barrier_semaphore()
    group = [(dm, ds) for dm in range(2) for ds in range(n_stage) if dm or ds]
    where = [{'model': lax.rem(model + dm, 2), 'stage': lax.rem(stage + ds, n_stage)} for dm, ds in group]
    for target in where + [peer]:
        pl.semaphore_signal(barrier, inc=1, device_id=target, device_id_type=mesh_id)

    n_st_up, n_st_down = d_model // st_up.shape[1], 2 * ff_half // st_down.shape[1]

    def load_up(r):
        return pltpu.make_async_copy(wu_ref.at[pl.ds(r * st_up.shape[1], st_up.shape[1])], st_up.at[r % 2], st_sem.at[0, r % 2])

    def load_down(r):
        return pltpu.make_async_copy(wd_ref.at[pl.ds(r * st_down.shape[1], st_down.shape[1])], st_down.at[r % 2], st_sem.at[1, r % 2])

    load_acts = pltpu.make_async_copy(acts_ref, rows_a.at[own_rows], loc_sem.at[0])
    load_acts.start()
    load_up(0).start()
    load_up(1).start()
    load_down(0).start()
    load_down(1).start()

    def load_g(c):
        return pltpu.make_async_copy(gout_ref.at[:, pl.ds(c * half, half)], gbuf.at[c], loc_sem.at[1 + c])

    @pl.when(stage == last)
    def _():
        for c in range(2):
            load_g(c).start()

    pl.semaphore_wait(barrier, len(where) + 1)

    def chunk(k):
        return pl.ds(k * BLOCK, BLOCK)

    raw_rows = n_raw * BLOCK
    raw = [remote(gu_ref.at[chunk(k), peer_cols], got_up.at[chunk(k)], rs_ssem.at[0, k], rs_rsem.at[0, k], peer) for k in range(n_raw)]
    carries_x = stage >= n_stage // 2

    def micro(i):
        return 2 * (stage - n_stage // 2) + i

    def send_x(i):
        return remote(x_ref.at[micro(i), :, near], x_land.at[i], x_sem.at[0, i], x_sem.at[1, i], peer)

    @pl.when(carries_x)
    def _():
        for i in range(2):
            send_x(i).start()

    for copy in raw:
        copy.start()
    send_a = remote(acts_ref.at[:, :raw_rows], rows_a.at[own_rows, :raw_rows], row_ssem.at[0], row_rsem.at[0], peer)
    send_a.start()

    for r in range(n_st_up):
        load_up(r).wait()
        up_bf[pl.ds(r * st_up.shape[1], st_up.shape[1])] = st_up[r % 2].astype(jnp.bfloat16)
        if r + 2 < n_st_up:
            load_up(r + 2).start()
    load_acts.wait()

    tile = 256
    n_tile = hid.shape[1] // tile
    scale = 0.7978845608028654
    cubic = 0.044715

    def pre_tile(j, carry):
        cols = pl.ds(pl.multiple_of(j * tile, tile), tile)
        pre = jnp.dot(rows_a[own_rows], up_bf[:, cols], preferred_element_type=jnp.float32)
        square = pre * pre
        bend = jnp.tanh(scale * (pre + cubic * square * pre))
        hid[:, cols] = (pre * (0.5 * (1.0 + bend))).astype(jnp.bfloat16)
        slope[:, cols] = 0.5 * (1.0 + bend) + 0.5 * pre * (1.0 - bend * bend) * (scale * (1.0 + 3.0 * cubic * square))
        return carry

    lax.fori_loop(0, n_tile, pre_tile, 0)

    for r in range(n_st_down):
        load_down(r).wait()
        down_bf[pl.ds(r * st_down.shape[1], st_down.shape[1])] = st_down[r % 2].astype(jnp.bfloat16)
        if r + 2 < n_st_down:
            load_down(r + 2).start()

    own_up = pltpu.make_async_copy(gu_ref.at[:, own_cols], acc_up, own_sem.at[0])
    own_down = pltpu.make_async_copy(gd_ref.at[own_cols], acc_down, own_sem.at[1])
    load_fold = pltpu.make_async_copy(gd_ref.at[peer_cols], fold, fold_sem)
    load_fold_up = pltpu.make_async_copy(gu_ref.at[raw_rows:, peer_cols], fold_up, fold_up_sem)
    load_fold_up.start()
    load_fold.start()
    own_up.start()
    own_down.start()

    @pl.when(stage == last)
    def _():
        for c in range(2):
            load_g(c).wait()

    @pl.when(stage < last)
    def _():
        for c in range(2):
            remote(ready, gbuf.at[c], pass_ssem.at[0], g_rsem.at[c], {'model': model}).wait_recv()

    def slope_tile(j, carry):
        cols = pl.ds(pl.multiple_of(j * tile, tile), tile)
        grad = lax.dot_general(gbuf[0], down_bf[cols, :half], CONTRACT_LAST, preferred_element_type=jnp.float32)
        grad = grad + lax.dot_general(gbuf[1], down_bf[cols, half:], CONTRACT_LAST, preferred_element_type=jnp.float32)
        grad_pre[:, cols] = (slope[:, cols] * grad).astype(jnp.bfloat16)
        return carry

    lax.fori_loop(0, n_tile, slope_tile, 0)

    trade = remote(outbox, landed, trade_sem.at[0], trade_sem.at[1], {'model': 1 - model})

    def hand_on(to):
        return remote(ready, gbuf.at[model], pass_ssem.at[to], g_rsem.at[model], {'model': to, 'stage': stage - 1})

    @pl.when(stage > 0)
    def _():
        outbox[...] = lax.dot_general(grad_pre[...], up_bf[far], CONTRACT_LAST, preferred_element_type=jnp.float32)
        trade.start()
        mine = lax.dot_general(grad_pre[...], up_bf[near], CONTRACT_LAST, preferred_element_type=jnp.float32)
        trade.wait_recv()
        ready[...] = (gbuf[model].astype(jnp.float32) + (mine + landed[...])).astype(jnp.bfloat16)
        for to in range(2):
            hand_on(to).start()

    rows_z[own_rows] = grad_pre[:, own_cols]
    send_z = remote(grad_pre.at[:, peer_cols], rows_z.at[own_rows], row_ssem.at[1], row_rsem.at[1], peer)
    send_z.start()

    load_fold_up.wait()

    def send_fold_up(k):
        rows = pl.ds(pl.multiple_of(k * BLOCK, BLOCK), BLOCK)
        at = pl.ds(pl.multiple_of((n_raw + k) * BLOCK, BLOCK), BLOCK)
        return remote(fold_up.at[rows], got_up.at[at], rs_ssem.at[0, n_raw + k], rs_rsem.at[0, n_raw + k], peer)

    def fold_up_step(k, carry):
        rows = pl.ds(pl.multiple_of(k * BLOCK, BLOCK), BLOCK)
        at = pl.ds(pl.multiple_of((n_raw + k) * BLOCK, BLOCK), BLOCK)
        fold_up[rows] += lax.dot_general(rows_a[own_rows, at], grad_pre[:, peer_cols], first_dims, preferred_element_type=jnp.float32)
        send_fold_up(k).start()
        return carry

    lax.fori_loop(0, n_up_chunk - n_raw, fold_up_step, 0)

    def forward_x(i, to):
        return remote(x_land.at[i], x_far.at[micro(i), :, near], xf_ssem.at[i, to], xf_rsem.at[micro(i), model], {'model': to, 'stage': 0})

    @pl.when(carries_x)
    def _():
        for i in range(2):
            send_x(i).wait_recv()
            for to in range(2):
                forward_x(i, to).start()

    def down_product(k, side):
        cols = pl.ds(pl.multiple_of(side * ff_half + k * BLOCK, BLOCK), BLOCK)
        left = hid[:, cols]
        return [lax.dot_general(left, gbuf[c], first_dims, preferred_element_type=jnp.float32) for c in range(2)]

    load_fold.wait()

    def send_fold(k):
        rows = pl.ds(pl.multiple_of(k * BLOCK, BLOCK), BLOCK)
        return remote(fold.at[rows], got_down.at[rows], rs_ssem.at[1, k], rs_rsem.at[1, k], peer)

    def fold_step(k, carry):
        rows = pl.ds(pl.multiple_of(k * BLOCK, BLOCK), BLOCK)
        low, high = down_product(k, 1 - data)
        fold[rows, :half] += low
        fold[rows, half:] += high
        send_fold(k).start()
        return carry

    lax.fori_loop(0, n_down_chunk, fold_step, 0)
    own_down.wait()

    def own_step(k, carry):
        rows = pl.ds(pl.multiple_of(k * BLOCK, BLOCK), BLOCK)
        low, high = down_product(k, data)
        acc_down[rows, :half] += low
        acc_down[rows, half:] += high
        return carry

    lax.fori_loop(0, n_down_chunk, own_step, 0)

    @pl.when(stage > 0)
    def _():
        trade.wait_send()
        for to in range(2):
            hand_on(to).wait_send()

    own_up.wait()
    send_a.wait_recv()
    squares = jnp.zeros((8, ff_half), jnp.float32)

    def fold_squares(mean):
        return jnp.sum((mean * mean).reshape(-1, 8, mean.shape[1]), axis=0)

    def put(acc, bounds, outs, whole, sem_row):
        copies = []
        for i, (lo, hi) in enumerate(bounds):
            rows = pl.ds(lo, hi - lo)
            copies.append(pltpu.make_async_copy(acc.at[rows], whole.at[rows], out_sem.at[sem_row, i]))
            if outs[i] is not None:
                copies.append(pltpu.make_async_copy(acc.at[rows], outs[i], out_sem.at[sem_row, len(bounds) + i]))
        return copies

    def put_start(k, bounds, copies, outs):
        at = 0
        for i, (lo, hi) in enumerate(bounds):
            count = 1 if outs[i] is None else 2
            if k * BLOCK < hi <= (k + 1) * BLOCK:
                for copy in copies[at:at + count]:
                    copy.start()
            at += count

    outs_up = (None,) + tuple(outs_up)
    outs_down = (None,) + tuple(outs_down)
    put_up = put(acc_up, bounds_up, outs_up, whole_up, 0)
    put_down = put(acc_down, bounds_down, outs_down, whole_down, 1)
    for k in range(n_up_chunk):
        if k == 0:
            send_z.wait_recv()
        if k < n_raw:
            raw[k].wait_recv()
            product = lax.dot_general(rows_a[:, chunk(k)], rows_z[...], first_dims, preferred_element_type=jnp.float32)
        else:
            send_fold_up(k - n_raw).wait_recv()
            product = lax.dot_general(rows_a[own_rows, chunk(k)], rows_z[own_rows], first_dims, preferred_element_type=jnp.float32)
        mean = (acc_up[chunk(k)] + got_up[chunk(k)] + product) * 0.5
        acc_up[chunk(k)] = mean
        squares = squares + fold_squares(mean)
        put_start(k, bounds_up, put_up, outs_up)
    n_far = far_sem.shape[1]
    slab = bounds_up[0][1] // n_far
    is_even = lax.rem(stage, 2) == 0

    def send_far(i):
        span = pl.ds(pl.multiple_of(i * slab, slab), slab)
        return remote(acc_up.at[span], far_ref.at[span], far_sem.at[0, i], far_sem.at[1, i], peer)

    for i in range(n_far - HELD):
        send_far(i).start()

    @pl.when(is_even)
    def _():
        for i in range(n_far - HELD, n_far):
            send_far(i).start()

    for k in range(n_down_chunk):
        send_fold(k).wait_recv()
        mean = (acc_down[chunk(k)] + got_down[chunk(k)]) * 0.5
        acc_down[chunk(k)] = mean
        squares = squares + fold_squares(mean)
        put_start(k, bounds_down, put_down, outs_down)

    lanes = norm_box.shape[2]
    part = squares[:, :lanes]
    for j in range(1, ff_half // lanes):
        part = part + squares[:, j * lanes:(j + 1) * lanes]
    me = model * n_stage + stage
    norm_box[me] = part

    def spread(i):
        return remote(norm_box.at[me], norm_box.at[me], norm_ssem.at[i], norm_rsem.at[me], where[i])

    for i in range(len(group)):
        spread(i).start()
    for i, (dm, ds) in enumerate(group):
        them = lax.rem(model + dm, 2) * n_stage + lax.rem(stage + ds, n_stage)
        remote(norm_box.at[me], norm_box.at[them], norm_ssem.at[i], norm_rsem.at[them], where[i]).wait_recv()
    total = norm_box[0]
    for i in range(1, 2 * n_stage):
        total = total + norm_box[i]
    norm_pair[0] = total
    swap = remote(norm_pair.at[0], norm_pair.at[1], norm_ssem.at[len(group)], norm_rsem.at[2 * n_stage], peer)
    swap.start()
    swap.wait_recv()
    norm_sq = jnp.sum(norm_pair[0] + norm_pair[1], axis=(0, 1), keepdims=True)
    norm = jnp.sqrt(jnp.broadcast_to(norm_sq, clip_ref.shape)) + NORM_EPS
    clip_ref[...] = jnp.minimum(1.0, max_ref[0] / norm)

    @pl.when(carries_x)
    def _():
        for i in range(2):
            send_x(i).wait_send()
            for to in range(2):
                forward_x(i, to).wait_send()

    @pl.when(stage == 0)
    def _():
        for s in range(n_stage):
            for m in range(2):
                remote(x_land.at[0], x_far.at[s, :, pl.ds(m * half, half)], xf_ssem.at[0, m], xf_rsem.at[s, m], {'model': model}).wait_recv()

    swap.wait_send()
    for i in range(len(group)):
        spread(i).wait_send()
    for copy in raw + [send_a, send_z]:
        copy.wait_send()
    for k in range(n_down_chunk):
        send_fold(k).wait_send()
    for k in range(n_up_chunk - n_raw):
        send_fold_up(k).wait_send()
    for copy in put_up + put_down:
        copy.wait()

    @pl.when(is_even)
    def _():
        for i in range(n_far):
            send_far(i).wait_send()
        pl.semaphore_signal(go_sem, inc=1, device_id={'stage': stage + 1}, device_id_type=mesh_id)

    @pl.when(jnp.logical_not(is_even))
    def _():
        pl.semaphore_wait(go_sem, 1)
        for i in range(n_far - HELD, n_far):
            send_far(i).start()
        for i in range(n_far):
            send_far(i).wait_send()

    for i in range(n_far):
        send_far(i).wait_recv()


def backward_call(n_stage, bounds_up, bounds_down, g_up, g_down, w_up, w_down, acts, grad_out, x_next, max_norm):
    d_model, ff_local = g_up.shape
    ff_half, half, n_row = ff_local // 2, d_model // 2, acts.shape[0]
    dma = pltpu.SemaphoreType.DMA
    anywhere = pl.BlockSpec(memory_space=pl.ANY)
    f32, bf16 = jnp.float32, jnp.bfloat16
    shapes = [jax.ShapeDtypeStruct((hi - lo, ff_half), f32) for lo, hi in bounds_up[1:]]
    shapes += [jax.ShapeDtypeStruct((hi - lo, d_model), f32) for lo, hi in bounds_down[1:]]
    shapes += [jax.ShapeDtypeStruct((d_model, ff_half), f32), jax.ShapeDtypeStruct((ff_half, d_model), f32)]
    shapes += [jax.ShapeDtypeStruct((bounds_up[0][1], ff_half), f32), jax.ShapeDtypeStruct(x_next.shape, bf16), jax.ShapeDtypeStruct((8, ff_half), f32)]
    n_chunk = max(d_model, ff_half) // BLOCK
    return pl.pallas_call(
        functools.partial(backward_body, n_stage, N_RAW, bounds_up, bounds_down),
        out_shape=shapes,
        in_specs=[anywhere] * 7 + [pl.BlockSpec(memory_space=pltpu.SMEM)],
        out_specs=[anywhere] * (len(shapes) - 1) + [pl.BlockSpec(memory_space=pltpu.VMEM)],
        scratch_shapes=[
            pltpu.VMEM((d_model, ff_local), bf16),
            pltpu.VMEM((ff_local, d_model), bf16),
            pltpu.VMEM((2, 256, ff_local), f32),
            pltpu.VMEM((2, 512, d_model), f32),
            pltpu.VMEM((d_model, ff_half), f32),
            pltpu.VMEM((ff_half, d_model), f32),
            pltpu.VMEM((d_model, ff_half), f32),
            pltpu.VMEM((ff_half, d_model), f32),
            pltpu.VMEM((ff_half, d_model), f32),
            pltpu.VMEM((n_row, ff_local), bf16),
            pltpu.VMEM((n_row, ff_local), f32),
            pltpu.VMEM((n_row, ff_local), bf16),
            pltpu.VMEM((2, n_row, half), bf16),
            pltpu.VMEM((n_row, half), f32),
            pltpu.VMEM((n_row, half), f32),
            pltpu.VMEM((n_row, half), bf16),
            pltpu.VMEM((2 * n_row, d_model), bf16),
            pltpu.VMEM((2 * n_row, ff_half), bf16),
            pltpu.VMEM((2 * n_stage, 8, 128), f32),
            pltpu.VMEM((2, 8, 128), f32),
            dma((2, 2)),
            dma((3,)),
            dma(()),
            dma((2,)),
            dma((2, 2 * max(len(bounds_up), len(bounds_down)))),
            dma((2,)),
            dma((2,)),
            dma((2,)),
            dma((2, n_chunk)),
            dma((2, n_chunk)),
            dma((2,)),
            dma((2,)),
            dma((2, 8)),
            dma((2 * n_stage,)),
            dma((2 * n_stage + 1,)),
            pltpu.VMEM((2, n_row, half), bf16),
            dma((2, 2)),
            dma((2, 2)),
            dma((n_stage, 2)),
            pltpu.SemaphoreType.REGULAR,
            pltpu.VMEM((d_model - N_RAW * BLOCK, ff_half), f32),
            dma(()),
        ],
        compiler_params=pltpu.CompilerParams(collective_id=0, has_side_effects=True, vmem_limit_bytes=67043328),
        name="reduce_and_norm",
    )(g_up, g_down, w_up, w_down, acts, grad_out, x_next, max_norm)


def forward_body(n_stage, lead, x_ref, xf_ref, up_ref, down_ref, mean_ref, y_ref, far_ref, inbox, hid, mine, zout, zin, keep, yout, yin, done, x_sem, in_sem, z_ssem, z_rsem, s_ssem, s_rsem, r_ssem, r_rsem, pass_ssem, y_ssem, y_rsem, piece_ssem, piece_rsem, go_sem):
    model, data, stage = lax.axis_index('model'), lax.axis_index('data'), lax.axis_index('stage')
    mesh_id = pl.DeviceIdType.MESH
    last = n_stage - 1
    n_group, _, rows2, half = inbox.shape
    rows = rows2 // 2
    n_piece = piece_ssem.shape[0]
    piece = far_ref.shape[0] // n_piece
    peer = {'data': 1 - data}
    near = pl.ds(pl.multiple_of(model * half, half), half)
    far = pl.ds(pl.multiple_of((1 - model) * half, half), half)
    own_rows = pl.ds(pl.multiple_of(data * rows, rows), rows)
    peer_rows = pl.ds(pl.multiple_of((1 - data) * rows, rows), rows)

    def remote(src, dst, ssem, rsem, where):
        return pltpu.make_async_remote_copy(src_ref=src, dst_ref=dst, send_sem=ssem, recv_sem=rsem, device_id=where, device_id_type=mesh_id)

    barrier = pltpu.get_barrier_semaphore()
    group = [(dm, ds) for dm in range(2) for ds in range(n_stage) if dm or ds]
    where = [{'model': lax.rem(model + dm, 2), 'stage': lax.rem(stage + ds, n_stage)} for dm, ds in group]
    for target in where + [peer]:
        pl.semaphore_signal(barrier, inc=1, device_id=target, device_id_type=mesh_id)

    def load_x(b, c, from_ref, to_rows, i):
        return pltpu.make_async_copy(from_ref.at[b, :, pl.ds(c * half, half)], inbox.at[b, c, to_rows], x_sem.at[b, c, i])

    def loads(b):
        return [load_x(b, c, *pair) for c in range(2) for pair in ((x_ref, own_rows, 0), (xf_ref, peer_rows, 1))]

    @pl.when(stage == 0)
    def _():
        for b in range(n_group):
            for copy in loads(b):
                copy.start()

    pl.semaphore_wait(barrier, len(where) + 1)

    def send_piece(p):
        span = pl.ds(pl.multiple_of(p * piece, piece), piece)
        return remote(mean_ref.at[span], far_ref.at[span], piece_ssem.at[p], piece_rsem.at[p], peer)

    def start_pieces(low, high):
        def one(p, carry):
            send_piece(p).start()
            return carry

        lax.fori_loop(low, high, one, 0)

    n_turn = n_group + 3 * LAG
    base, slope = lead
    is_even = lax.rem(stage, 2) == 0
    limit = n_piece - HELD_FWD * lax.rem(stage, 2)
    begin = jnp.minimum(base + slope * stage, limit)
    start_pieces(0, begin)

    def arrival(b, c):
        return remote(done.at[b], inbox.at[b, c], pass_ssem.at[b, 0], in_sem.at[b, c], {'model': model})

    def trade_z(b):
        return remote(zout.at[b], zin.at[b], z_ssem.at[b], z_rsem.at[b], {'model': 1 - model})

    def trade_s(b):
        return remote(yout.at[b], yin.at[b], s_ssem.at[b], s_rsem.at[b], peer)

    def trade_r(b):
        return remote(done.at[b, own_rows], done.at[b, own_rows], r_ssem.at[b], r_rsem.at[b], peer)

    def hand_on(b, to):
        return remote(done.at[b], inbox.at[b, model], pass_ssem.at[b, to], in_sem.at[b, model], {'model': to, 'stage': stage + 1})

    def landing(b, c):
        return y_ref.at[b, :, pl.ds(pl.multiple_of(c * half, half), half)]

    def publish(b, k):
        return remote(done.at[b, own_rows], landing(b, model), y_ssem.at[b, k], y_rsem.at[b, model], where[k])

    def y_arrival(b, c):
        return remote(done.at[b, own_rows], landing(b, c), y_ssem.at[b, 0], y_rsem.at[b, c], {'model': model})

    def project(t):
        @pl.when(t < n_group)
        def _():
            @pl.when(stage == 0)
            def _():
                for copy in loads(t):
                    copy.wait()

            @pl.when(stage > 0)
            def _():
                for c in range(2):
                    arrival(t, c).wait_recv()

            pre = jnp.dot(inbox[t, 0], up_ref[:half], preferred_element_type=jnp.float32)
            pre = pre + jnp.dot(inbox[t, 1], up_ref[half:], preferred_element_type=jnp.float32)
            hid[...] = jax.nn.gelu(pre).astype(jnp.bfloat16)
            zout[t] = jnp.dot(hid[...], down_ref[:, far], preferred_element_type=jnp.float32)
            trade_z(t).start()
            mine[t] = jnp.dot(hid[...], down_ref[:, near], preferred_element_type=jnp.float32)

    def reduce_z(t):
        @pl.when((t >= LAG) & (t < n_group + LAG))
        def _():
            b = t - LAG
            trade_z(b).wait_recv()
            yout[b] = mine[b, peer_rows] + zin[b, peer_rows]
            trade_s(b).start()
            keep[b] = mine[b, own_rows] + zin[b, own_rows]

    def reduce_y(t):
        @pl.when((t >= 2 * LAG) & (t < n_group + 2 * LAG))
        def _():
            b = t - 2 * LAG
            trade_s(b).wait_recv()
            total = inbox[b, model, own_rows].astype(jnp.float32) + (keep[b] + yin[b])
            result = total.astype(jnp.bfloat16)
            done[b, own_rows] = result

            @pl.when(stage < last)
            def _():
                trade_r(b).start()

            @pl.when(stage == last)
            def _():
                y_ref[b, :, near] = result
                for k in range(len(group)):
                    publish(b, k).start()

    def pass_on(t):
        @pl.when((t >= 3 * LAG) & (stage < last))
        def _():
            b = t - 3 * LAG
            remote(done.at[b, own_rows], done.at[b, peer_rows], r_ssem.at[b], r_rsem.at[b], peer).wait_recv()
            for to in range(2):
                hand_on(b, to).start()

    def turn(t, carry):
        for phase in (project, reduce_z, reduce_y, pass_on):
            phase(t)
        return carry

    lax.fori_loop(0, n_turn, turn, 0)
    start_pieces(begin, limit)

    for b in range(n_group):
        trade_z(b).wait_send()
        trade_s(b).wait_send()

    @pl.when(stage < last)
    def _():
        for b in range(n_group):
            trade_r(b).wait_send()
            for to in range(2):
                hand_on(b, to).wait_send()
            for c in range(2):
                y_arrival(b, c).wait_recv()

    @pl.when(stage == last)
    def _():
        for b in range(n_group):
            for k in range(len(group)):
                publish(b, k).wait_send()
            y_arrival(b, 1 - model).wait_recv()

    def sent(p, carry):
        send_piece(p).wait_send()
        return carry

    def landed(p, carry):
        send_piece(p).wait_recv()
        return carry

    lax.fori_loop(0, limit, sent, 0)

    @pl.when(is_even)
    def _():
        pl.semaphore_signal(go_sem, inc=1, device_id={'stage': stage + 1}, device_id_type=mesh_id)

    @pl.when(jnp.logical_not(is_even))
    def _():
        pl.semaphore_wait(go_sem, 1)
        start_pieces(limit, n_piece)
        lax.fori_loop(limit, n_piece, sent, 0)

    lax.fori_loop(0, n_piece, landed, 0)


def forward_call(n_stage, n_group, n_piece, lead, n_far, x_next, x_far, up_bf, down_bf, mean):
    d_model = x_next.shape[2]
    x_next, x_far = [value.reshape(n_group, -1, d_model) for value in (x_next, x_far)]
    rows, half, ff_half = x_next.shape[1], d_model // 2, up_bf.shape[1]
    dma = pltpu.SemaphoreType.DMA
    f32, bf16 = jnp.float32, jnp.bfloat16
    in_vmem = pl.BlockSpec(memory_space=pltpu.VMEM)
    anywhere = pl.BlockSpec(memory_space=pl.ANY)
    return pl.pallas_call(
        functools.partial(forward_body, n_stage, lead),
        out_shape=[jax.ShapeDtypeStruct(x_next.shape, bf16), jax.ShapeDtypeStruct((n_far, d_model), f32)],
        in_specs=[anywhere, anywhere, in_vmem, in_vmem, anywhere],
        out_specs=[in_vmem, anywhere],
        scratch_shapes=[
            pltpu.VMEM((n_group, 2, 2 * rows, half), bf16),
            pltpu.VMEM((2 * rows, ff_half), bf16),
            pltpu.VMEM((n_group, 2 * rows, half), f32),
            pltpu.VMEM((n_group, 2 * rows, half), f32),
            pltpu.VMEM((n_group, 2 * rows, half), f32),
            pltpu.VMEM((n_group, rows, half), f32),
            pltpu.VMEM((n_group, rows, half), f32),
            pltpu.VMEM((n_group, rows, half), f32),
            pltpu.VMEM((n_group, 2 * rows, half), bf16),
            dma((n_group, 2, 2)),
            dma((n_group, 2)),
            dma((n_group,)),
            dma((n_group,)),
            dma((n_group,)),
            dma((n_group,)),
            dma((n_group,)),
            dma((n_group,)),
            dma((n_group, 2)),
            dma((n_group, 2 * n_stage - 1)),
            dma((n_group, 2)),
            dma((n_piece,)),
            dma((n_piece,)),
            pltpu.SemaphoreType.REGULAR,
        ],
        compiler_params=pltpu.CompilerParams(collective_id=1, has_side_effects=True, vmem_limit_bytes=67043328),
        name="forward_pipe",
    )(x_next, x_far, up_bf, down_bf, mean)


def solution(mesh):
    n_stage = mesh.shape['stage']
    swap = [(0, 1), (1, 0)]
    up_spec = P('stage', None, 'model')
    down_spec = P('stage', 'model', None)
    row_spec = P(None, 'data', None)
    in_specs = (up_spec, down_spec, up_spec, down_spec, up_spec, down_spec, P('data', 'stage', None, 'model'), P('data', 'stage', 'model', None), P('stage', 'data', None), P('data', None), row_spec, P(None), P(None))
    out_specs = (up_spec, down_spec, up_spec, down_spec, up_spec, down_spec, row_spec)

    def device_step(w_up, w_down, m_up, m_down, v_up, v_down, g_up, g_down, acts_last, grad_out, x_next, learn_rate, max_norm):
        data_id = lax.axis_index('data')
        half = data_id.astype(jnp.int32).reshape(1)
        other = (1 - half).astype(jnp.int32)
        d_model, ff_local = w_up.shape[1:]
        ff_half = ff_local // 2
        bounds_up = ((0, 256), (256, 704), (704, 896), (896, 960), (960, d_model))
        bounds_down = ((0, N_PIECE * 32), (N_PIECE * 32, ff_half))

        def trade(value):
            return lax.ppermute(value, 'data', swap)

        early, *late, late_down, whole_up, whole_down, far_first, x_far, clip = backward_call(n_stage, bounds_up, bounds_down, g_up[0, 0], g_down[0, 0], w_up[0], w_down[0], acts_last[0], grad_out, x_next, max_norm)
        ups = (w_up[0], m_up[0], v_up[0])
        downs = (w_down[0], m_down[0], v_down[0])

        def map_up(low, high):
            return lambda i, h, r: (low // step_of(low, high) + i, h[0])

        def map_down(low):
            return lambda i, h, r: ((h[0] * ff_half + low) // BLOCK + i, 0)

        far_early = trade(early)
        *new_up, up_bf = update_call(half, learn_rate, clip, ups, whole_up, map_up(0, d_model), None)
        *new_down, down_bf = update_call(half, learn_rate, clip, downs, whole_down, map_down(0), None, (up_bf,))
        new_up = update_call(other, learn_rate, clip, ups, far_first, map_up(*bounds_up[0]), new_up, (down_bf,))
        down_bf, new_up = lax.optimization_barrier((down_bf, new_up))
        y_next, far_down = forward_call(n_stage, N_GROUP, N_PIECE, LEAD, bounds_down[0][1], x_next, x_far, up_bf, down_bf, whole_down)
        y_next = y_next.reshape(x_next.shape)
        late, late_down, far_down = lax.optimization_barrier((late, late_down, far_down))
        far_last = trade(late_down)
        fars = [trade(value) for value in late]
        *new_down, y_next = update_call(other, learn_rate, clip, downs, far_down, map_down(0), new_down, (), (y_next,))
        new_up = update_call(other, learn_rate, clip, ups, far_early, map_up(*bounds_up[1]), new_up, (new_down[0],), block=step_of(*bounds_up[1]))
        new_down = update_call(other, learn_rate, clip, downs, far_last, map_down(bounds_down[1][0]), new_down, (new_up[0],))
        after = (new_down[0],)
        for bounds, part in zip(bounds_up[2:], fars):
            new_up = update_call(other, learn_rate, clip, ups, part, map_up(*bounds), new_up, after, block=step_of(*bounds))
            after = ()
        return (new_up[0][None], new_down[0][None], new_up[1][None], new_down[1][None], new_up[2][None], new_down[2][None], y_next)

    return jax.shard_map(device_step, mesh=mesh, in_specs=in_specs, out_specs=out_specs, check_vma=False)
```

```python
import functools

import jax
import jax.numpy as jnp
from jax import lax
from jax.experimental import pallas as pl
from jax.experimental.pallas import tpu as pltpu
from jax.sharding import PartitionSpec as P

ADAM_STEP = 10
BETA_ONE = 0.9
BETA_TWO = 0.95
ADAM_EPS = 1e-8
WEIGHT_DECAY = 0.1
NORM_EPS = 1e-6
CONTRACT_LAST = (((1,), (1,)), ((), ()))
BLOCK = 128
N_GROUP = 8
N_PIECE = 28
LEAD = (3, 7)
HELD = 2
HELD_FWD = 3
LAG = 2
N_RAW = 4


def update_body(skip, carry, half_ref, rate_ref, clip_ref, w_ref, m_ref, v_ref, g_ref, *refs):
    outs = refs[skip:]
    if carry:
        outs[-1][...] = refs[skip - 1][...]
        outs = outs[:-1]
    ow_ref, om_ref, ov_ref = outs[:3]
    rate = rate_ref[0]
    grad = clip_ref[0:1] * g_ref[...]
    weight = w_ref[...]
    mom = BETA_ONE * m_ref[...] + (1.0 - BETA_ONE) * grad
    sec = BETA_TWO * v_ref[...] + (1.0 - BETA_TWO) * grad * grad
    one_corr = 1.0 - BETA_ONE**ADAM_STEP
    two_corr = 1.0 - BETA_TWO**ADAM_STEP
    direction = (mom * (1.0 / one_corr)) / (jnp.sqrt(sec * (1.0 / two_corr)) + ADAM_EPS)
    new = weight - rate * (direction + WEIGHT_DECAY * weight)
    ow_ref[...] = new
    om_ref[...] = mom
    ov_ref[...] = sec
    if len(outs) == 4:
        outs[3][...] = new.astype(jnp.bfloat16)


def step_of(low, high):
    return BLOCK if low % BLOCK == 0 and high % BLOCK == 0 else BLOCK // 2


def update_call(half, rate, clip, weights, grad, full_map, previous, after=(), carry=(), block=BLOCK):
    rows, cols = grad.shape
    shape = weights[0].shape
    spec = pl.BlockSpec((block, cols), full_map)
    flat = pl.BlockSpec((block, cols), lambda i, h, r: (i, 0))
    anywhere = pl.BlockSpec(memory_space=pl.ANY)
    first = previous is None
    extra = list(previous or ()) + list(after)
    passed = [pl.BlockSpec((1,) + value.shape[1:], lambda i, h, r: (jnp.minimum(i, value.shape[0] - 1), 0, 0)) for value in carry]
    return pl.pallas_call(
        functools.partial(update_body, len(extra) + len(carry), len(carry)),
        grid_spec=pltpu.PrefetchScalarGridSpec(
            num_scalar_prefetch=2,
            grid=(rows // block,),
            in_specs=[pl.BlockSpec(clip.shape, lambda i, h, r: (0, 0)), spec, spec, spec, flat] + [anywhere] * len(extra) + passed,
            out_specs=[spec] * 3 + [flat] * first + passed,
        ),
        out_shape=[jax.ShapeDtypeStruct(shape, jnp.float32)] * 3 + [jax.ShapeDtypeStruct(grad.shape, jnp.bfloat16)] * first + [jax.ShapeDtypeStruct(value.shape, value.dtype) for value in carry],
        input_output_aliases={7 + i: i for i in range(len(previous or ()))},
        cost_estimate=pl.CostEstimate(flops=60 * rows * cols, bytes_accessed=30 * rows * cols, transcendentals=0),
        compiler_params=pltpu.CompilerParams(vmem_limit_bytes=67043328),
        name="adamw_half",
    )(half, rate, clip, *weights, grad, *extra, *carry)


def backward_body(n_stage, n_raw, bounds_up, bounds_down, gu_ref, gd_ref, wu_ref, wd_ref, acts_ref, gout_ref, x_ref, max_ref, *refs):
    n_up, n_down = len(bounds_up) - 1, len(bounds_down) - 1
    outs_up, outs_down = refs[:n_up], refs[n_up:n_up + n_down]
    whole_up, whole_down, far_ref, x_far, clip_ref = refs[n_up + n_down:n_up + n_down + 5]
    (up_bf, down_bf, st_up, st_down, acc_up, acc_down, got_up, got_down, fold, hid, slope, grad_pre, gbuf, outbox, landed, ready, rows_a, rows_z, norm_box, norm_pair,
     st_sem, loc_sem, fold_sem, own_sem, out_sem, g_rsem, trade_sem, pass_ssem, rs_ssem, rs_rsem, row_ssem, row_rsem, far_sem, norm_ssem, norm_rsem, x_land, x_sem, xf_ssem, xf_rsem, go_sem, fold_up, fold_up_sem) = refs[n_up + n_down + 5:]
    model, data, stage = lax.axis_index('model'), lax.axis_index('data'), lax.axis_index('stage')
    mesh_id = pl.DeviceIdType.MESH
    last = n_stage - 1
    d_model, ff_half = acc_up.shape
    half = d_model // 2
    n_row = acts_ref.shape[0]
    n_up_chunk, n_down_chunk = d_model // BLOCK, ff_half // BLOCK
    peer = {'data': 1 - data}
    near = pl.ds(pl.multiple_of(model * half, half), half)
    far = pl.ds(pl.multiple_of((1 - model) * half, half), half)
    own_cols = pl.ds(pl.multiple_of(data * ff_half, ff_half), ff_half)
    peer_cols = pl.ds(pl.multiple_of((1 - data) * ff_half, ff_half), ff_half)
    own_rows = pl.ds(pl.multiple_of(data * n_row, n_row), n_row)
    first_dims = (((0,), (0,)), ((), ()))

    def remote(src, dst, ssem, rsem, where):
        return pltpu.make_async_remote_copy(src_ref=src, dst_ref=dst, send_sem=ssem, recv_sem=rsem, device_id=where, device_id_type=mesh_id)

    barrier = pltpu.get_barrier_semaphore()
    group = [(dm, ds) for dm in range(2) for ds in range(n_stage) if dm or ds]
    where = [{'model': lax.rem(model + dm, 2), 'stage': lax.rem(stage + ds, n_stage)} for dm, ds in group]
    for target in where + [peer]:
        pl.semaphore_signal(barrier, inc=1, device_id=target, device_id_type=mesh_id)

    n_st_up, n_st_down = d_model // st_up.shape[1], 2 * ff_half // st_down.shape[1]

    def load_up(r):
        return pltpu.make_async_copy(wu_ref.at[pl.ds(r * st_up.shape[1], st_up.shape[1])], st_up.at[r % 2], st_sem.at[0, r % 2])

    def load_down(r):
        return pltpu.make_async_copy(wd_ref.at[pl.ds(r * st_down.shape[1], st_down.shape[1])], st_down.at[r % 2], st_sem.at[1, r % 2])

    load_acts = pltpu.make_async_copy(acts_ref, rows_a.at[own_rows], loc_sem.at[0])
    load_acts.start()
    load_up(0).start()
    load_up(1).start()
    load_down(0).start()
    load_down(1).start()

    def load_g(c):
        return pltpu.make_async_copy(gout_ref.at[:, pl.ds(c * half, half)], gbuf.at[c], loc_sem.at[1 + c])

    @pl.when(stage == last)
    def _():
        for c in range(2):
            load_g(c).start()

    pl.semaphore_wait(barrier, len(where) + 1)

    def chunk(k):
        return pl.ds(k * BLOCK, BLOCK)

    raw_rows = n_raw * BLOCK
    raw = [remote(gu_ref.at[chunk(k), peer_cols], got_up.at[chunk(k)], rs_ssem.at[0, k], rs_rsem.at[0, k], peer) for k in range(n_raw)]
    carries_x = stage >= n_stage // 2

    def micro(i):
        return 2 * (stage - n_stage // 2) + i

    def send_x(i):
        return remote(x_ref.at[micro(i), :, near], x_land.at[i], x_sem.at[0, i], x_sem.at[1, i], peer)

    @pl.when(carries_x)
    def _():
        for i in range(2):
            send_x(i).start()

    for copy in raw:
        copy.start()
    send_a = remote(acts_ref.at[:, :raw_rows], rows_a.at[own_rows, :raw_rows], row_ssem.at[0], row_rsem.at[0], peer)
    send_a.start()

    for r in range(n_st_up):
        load_up(r).wait()
        up_bf[pl.ds(r * st_up.shape[1], st_up.shape[1])] = st_up[r % 2].astype(jnp.bfloat16)
        if r + 2 < n_st_up:
            load_up(r + 2).start()
    load_acts.wait()

    tile = 256
    n_tile = hid.shape[1] // tile
    scale = 0.7978845608028654
    cubic = 0.044715

    def pre_tile(j, carry):
        cols = pl.ds(pl.multiple_of(j * tile, tile), tile)
        pre = jnp.dot(rows_a[own_rows], up_bf[:, cols], preferred_element_type=jnp.float32)
        square = pre * pre
        bend = jnp.tanh(scale * (pre + cubic * square * pre))
        hid[:, cols] = (pre * (0.5 * (1.0 + bend))).astype(jnp.bfloat16)
        slope[:, cols] = 0.5 * (1.0 + bend) + 0.5 * pre * (1.0 - bend * bend) * (scale * (1.0 + 3.0 * cubic * square))
        return carry

    lax.fori_loop(0, n_tile, pre_tile, 0)

    for r in range(n_st_down):
        load_down(r).wait()
        down_bf[pl.ds(r * st_down.shape[1], st_down.shape[1])] = st_down[r % 2].astype(jnp.bfloat16)
        if r + 2 < n_st_down:
            load_down(r + 2).start()

    own_up = pltpu.make_async_copy(gu_ref.at[:, own_cols], acc_up, own_sem.at[0])
    own_down = pltpu.make_async_copy(gd_ref.at[own_cols], acc_down, own_sem.at[1])
    load_fold = pltpu.make_async_copy(gd_ref.at[peer_cols], fold, fold_sem)
    load_fold_up = pltpu.make_async_copy(gu_ref.at[raw_rows:, peer_cols], fold_up, fold_up_sem)
    load_fold_up.start()
    load_fold.start()
    own_up.start()
    own_down.start()

    @pl.when(stage == last)
    def _():
        for c in range(2):
            load_g(c).wait()

    @pl.when(stage < last)
    def _():
        for c in range(2):
            remote(ready, gbuf.at[c], pass_ssem.at[0], g_rsem.at[c], {'model': model}).wait_recv()

    def slope_tile(j, carry):
        cols = pl.ds(pl.multiple_of(j * tile, tile), tile)
        grad = lax.dot_general(gbuf[0], down_bf[cols, :half], CONTRACT_LAST, preferred_element_type=jnp.float32)
        grad = grad + lax.dot_general(gbuf[1], down_bf[cols, half:], CONTRACT_LAST, preferred_element_type=jnp.float32)
        grad_pre[:, cols] = (slope[:, cols] * grad).astype(jnp.bfloat16)
        return carry

    lax.fori_loop(0, n_tile, slope_tile, 0)

    trade = remote(outbox, landed, trade_sem.at[0], trade_sem.at[1], {'model': 1 - model})

    def hand_on(to):
        return remote(ready, gbuf.at[model], pass_ssem.at[to], g_rsem.at[model], {'model': to, 'stage': stage - 1})

    @pl.when(stage > 0)
    def _():
        outbox[...] = lax.dot_general(grad_pre[...], up_bf[far], CONTRACT_LAST, preferred_element_type=jnp.float32)
        trade.start()
        mine = lax.dot_general(grad_pre[...], up_bf[near], CONTRACT_LAST, preferred_element_type=jnp.float32)
        trade.wait_recv()
        ready[...] = (gbuf[model].astype(jnp.float32) + (mine + landed[...])).astype(jnp.bfloat16)
        for to in range(2):
            hand_on(to).start()

    rows_z[own_rows] = grad_pre[:, own_cols]
    send_z = remote(grad_pre.at[:, peer_cols], rows_z.at[own_rows], row_ssem.at[1], row_rsem.at[1], peer)
    send_z.start()

    load_fold_up.wait()

    def send_fold_up(k):
        rows = pl.ds(pl.multiple_of(k * BLOCK, BLOCK), BLOCK)
        at = pl.ds(pl.multiple_of((n_raw + k) * BLOCK, BLOCK), BLOCK)
        return remote(fold_up.at[rows], got_up.at[at], rs_ssem.at[0, n_raw + k], rs_rsem.at[0, n_raw + k], peer)

    def fold_up_step(k, carry):
        rows = pl.ds(pl.multiple_of(k * BLOCK, BLOCK), BLOCK)
        at = pl.ds(pl.multiple_of((n_raw + k) * BLOCK, BLOCK), BLOCK)
        fold_up[rows] += lax.dot_general(rows_a[own_rows, at], grad_pre[:, peer_cols], first_dims, preferred_element_type=jnp.float32)
        send_fold_up(k).start()
        return carry

    lax.fori_loop(0, n_up_chunk - n_raw, fold_up_step, 0)

    def forward_x(i, to):
        return remote(x_land.at[i], x_far.at[micro(i), :, near], xf_ssem.at[i, to], xf_rsem.at[micro(i), model], {'model': to, 'stage': 0})

    @pl.when(carries_x)
    def _():
        for i in range(2):
            send_x(i).wait_recv()
            for to in range(2):
                forward_x(i, to).start()

    def down_product(k, side):
        cols = pl.ds(pl.multiple_of(side * ff_half + k * BLOCK, BLOCK), BLOCK)
        left = hid[:, cols]
        return [lax.dot_general(left, gbuf[c], first_dims, preferred_element_type=jnp.float32) for c in range(2)]

    load_fold.wait()

    def send_fold(k):
        rows = pl.ds(pl.multiple_of(k * BLOCK, BLOCK), BLOCK)
        return remote(fold.at[rows], got_down.at[rows], rs_ssem.at[1, k], rs_rsem.at[1, k], peer)

    def fold_step(k, carry):
        rows = pl.ds(pl.multiple_of(k * BLOCK, BLOCK), BLOCK)
        low, high = down_product(k, 1 - data)
        fold[rows, :half] += low
        fold[rows, half:] += high
        send_fold(k).start()
        return carry

    lax.fori_loop(0, n_down_chunk, fold_step, 0)
    own_down.wait()

    def own_step(k, carry):
        rows = pl.ds(pl.multiple_of(k * BLOCK, BLOCK), BLOCK)
        low, high = down_product(k, data)
        acc_down[rows, :half] += low
        acc_down[rows, half:] += high
        return carry

    lax.fori_loop(0, n_down_chunk, own_step, 0)

    @pl.when(stage > 0)
    def _():
        trade.wait_send()
        for to in range(2):
            hand_on(to).wait_send()

    own_up.wait()
    send_a.wait_recv()
    squares = jnp.zeros((8, ff_half), jnp.float32)

    def fold_squares(mean):
        return jnp.sum((mean * mean).reshape(-1, 8, mean.shape[1]), axis=0)

    def put(acc, bounds, outs, whole, sem_row):
        copies = []
        for i, (lo, hi) in enumerate(bounds):
            rows = pl.ds(lo, hi - lo)
            copies.append(pltpu.make_async_copy(acc.at[rows], whole.at[rows], out_sem.at[sem_row, i]))
            if outs[i] is not None:
                copies.append(pltpu.make_async_copy(acc.at[rows], outs[i], out_sem.at[sem_row, len(bounds) + i]))
        return copies

    def put_start(k, bounds, copies, outs):
        at = 0
        for i, (lo, hi) in enumerate(bounds):
            count = 1 if outs[i] is None else 2
            if k * BLOCK < hi <= (k + 1) * BLOCK:
                for copy in copies[at:at + count]:
                    copy.start()
            at += count

    outs_up = (None,) + tuple(outs_up)
    outs_down = (None,) + tuple(outs_down)
    put_up = put(acc_up, bounds_up, outs_up, whole_up, 0)
    put_down = put(acc_down, bounds_down, outs_down, whole_down, 1)
    for k in range(n_up_chunk):
        if k == 0:
            send_z.wait_recv()
        if k < n_raw:
            raw[k].wait_recv()
            product = lax.dot_general(rows_a[:, chunk(k)], rows_z[...], first_dims, preferred_element_type=jnp.float32)
        else:
            send_fold_up(k - n_raw).wait_recv()
            product = lax.dot_general(rows_a[own_rows, chunk(k)], rows_z[own_rows], first_dims, preferred_element_type=jnp.float32)
        mean = (acc_up[chunk(k)] + got_up[chunk(k)] + product) * 0.5
        acc_up[chunk(k)] = mean
        squares = squares + fold_squares(mean)
        put_start(k, bounds_up, put_up, outs_up)
    n_far = far_sem.shape[1]
    slab = bounds_up[0][1] // n_far
    is_even = lax.rem(stage, 2) == 0

    def send_far(i):
        span = pl.ds(pl.multiple_of(i * slab, slab), slab)
        return remote(acc_up.at[span], far_ref.at[span], far_sem.at[0, i], far_sem.at[1, i], peer)

    for i in range(n_far - HELD):
        send_far(i).start()

    @pl.when(is_even)
    def _():
        for i in range(n_far - HELD, n_far):
            send_far(i).start()

    for k in range(n_down_chunk):
        send_fold(k).wait_recv()
        mean = (acc_down[chunk(k)] + got_down[chunk(k)]) * 0.5
        acc_down[chunk(k)] = mean
        squares = squares + fold_squares(mean)
        put_start(k, bounds_down, put_down, outs_down)

    lanes = norm_box.shape[2]
    part = squares[:, :lanes]
    for j in range(1, ff_half // lanes):
        part = part + squares[:, j * lanes:(j + 1) * lanes]
    me = model * n_stage + stage
    norm_box[me] = part

    def spread(i):
        return remote(norm_box.at[me], norm_box.at[me], norm_ssem.at[i], norm_rsem.at[me], where[i])

    for i in range(len(group)):
        spread(i).start()
    for i, (dm, ds) in enumerate(group):
        them = lax.rem(model + dm, 2) * n_stage + lax.rem(stage + ds, n_stage)
        remote(norm_box.at[me], norm_box.at[them], norm_ssem.at[i], norm_rsem.at[them], where[i]).wait_recv()
    total = norm_box[0]
    for i in range(1, 2 * n_stage):
        total = total + norm_box[i]
    norm_pair[0] = total
    swap = remote(norm_pair.at[0], norm_pair.at[1], norm_ssem.at[len(group)], norm_rsem.at[2 * n_stage], peer)
    swap.start()
    swap.wait_recv()
    norm_sq = jnp.sum(norm_pair[0] + norm_pair[1], axis=(0, 1), keepdims=True)
    norm = jnp.sqrt(jnp.broadcast_to(norm_sq, clip_ref.shape)) + NORM_EPS
    clip_ref[...] = jnp.minimum(1.0, max_ref[0] / norm)

    @pl.when(carries_x)
    def _():
        for i in range(2):
            send_x(i).wait_send()
            for to in range(2):
                forward_x(i, to).wait_send()

    @pl.when(stage == 0)
    def _():
        for s in range(n_stage):
            for m in range(2):
                remote(x_land.at[0], x_far.at[s, :, pl.ds(m * half, half)], xf_ssem.at[0, m], xf_rsem.at[s, m], {'model': model}).wait_recv()

    swap.wait_send()
    for i in range(len(group)):
        spread(i).wait_send()
    for copy in raw + [send_a, send_z]:
        copy.wait_send()
    for k in range(n_down_chunk):
        send_fold(k).wait_send()
    for k in range(n_up_chunk - n_raw):
        send_fold_up(k).wait_send()
    for copy in put_up + put_down:
        copy.wait()

    @pl.when(is_even)
    def _():
        for i in range(n_far):
            send_far(i).wait_send()
        pl.semaphore_signal(go_sem, inc=1, device_id={'stage': stage + 1}, device_id_type=mesh_id)

    @pl.when(jnp.logical_not(is_even))
    def _():
        pl.semaphore_wait(go_sem, 1)
        for i in range(n_far - HELD, n_far):
            send_far(i).start()
        for i in range(n_far):
            send_far(i).wait_send()

    for i in range(n_far):
        send_far(i).wait_recv()


def backward_call(n_stage, bounds_up, bounds_down, g_up, g_down, w_up, w_down, acts, grad_out, x_next, max_norm):
    d_model, ff_local = g_up.shape
    ff_half, half, n_row = ff_local // 2, d_model // 2, acts.shape[0]
    dma = pltpu.SemaphoreType.DMA
    anywhere = pl.BlockSpec(memory_space=pl.ANY)
    f32, bf16 = jnp.float32, jnp.bfloat16
    shapes = [jax.ShapeDtypeStruct((hi - lo, ff_half), f32) for lo, hi in bounds_up[1:]]
    shapes += [jax.ShapeDtypeStruct((hi - lo, d_model), f32) for lo, hi in bounds_down[1:]]
    shapes += [jax.ShapeDtypeStruct((d_model, ff_half), f32), jax.ShapeDtypeStruct((ff_half, d_model), f32)]
    shapes += [jax.ShapeDtypeStruct((bounds_up[0][1], ff_half), f32), jax.ShapeDtypeStruct(x_next.shape, bf16), jax.ShapeDtypeStruct((8, ff_half), f32)]
    n_chunk = max(d_model, ff_half) // BLOCK
    return pl.pallas_call(
        functools.partial(backward_body, n_stage, N_RAW, bounds_up, bounds_down),
        out_shape=shapes,
        in_specs=[anywhere] * 7 + [pl.BlockSpec(memory_space=pltpu.SMEM)],
        out_specs=[anywhere] * (len(shapes) - 1) + [pl.BlockSpec(memory_space=pltpu.VMEM)],
        scratch_shapes=[
            pltpu.VMEM((d_model, ff_local), bf16),
            pltpu.VMEM((ff_local, d_model), bf16),
            pltpu.VMEM((2, 256, ff_local), f32),
            pltpu.VMEM((2, 512, d_model), f32),
            pltpu.VMEM((d_model, ff_half), f32),
            pltpu.VMEM((ff_half, d_model), f32),
            pltpu.VMEM((d_model, ff_half), f32),
            pltpu.VMEM((ff_half, d_model), f32),
            pltpu.VMEM((ff_half, d_model), f32),
            pltpu.VMEM((n_row, ff_local), bf16),
            pltpu.VMEM((n_row, ff_local), f32),
            pltpu.VMEM((n_row, ff_local), bf16),
            pltpu.VMEM((2, n_row, half), bf16),
            pltpu.VMEM((n_row, half), f32),
            pltpu.VMEM((n_row, half), f32),
            pltpu.VMEM((n_row, half), bf16),
            pltpu.VMEM((2 * n_row, d_model), bf16),
            pltpu.VMEM((2 * n_row, ff_half), bf16),
            pltpu.VMEM((2 * n_stage, 8, 128), f32),
            pltpu.VMEM((2, 8, 128), f32),
            dma((2, 2)),
            dma((3,)),
            dma(()),
            dma((2,)),
            dma((2, 2 * max(len(bounds_up), len(bounds_down)))),
            dma((2,)),
            dma((2,)),
            dma((2,)),
            dma((2, n_chunk)),
            dma((2, n_chunk)),
            dma((2,)),
            dma((2,)),
            dma((2, 8)),
            dma((2 * n_stage,)),
            dma((2 * n_stage + 1,)),
            pltpu.VMEM((2, n_row, half), bf16),
            dma((2, 2)),
            dma((2, 2)),
            dma((n_stage, 2)),
            pltpu.SemaphoreType.REGULAR,
            pltpu.VMEM((d_model - N_RAW * BLOCK, ff_half), f32),
            dma(()),
        ],
        compiler_params=pltpu.CompilerParams(collective_id=0, has_side_effects=True, vmem_limit_bytes=67043328),
        name="reduce_and_norm",
    )(g_up, g_down, w_up, w_down, acts, grad_out, x_next, max_norm)


def forward_body(n_stage, lead, x_ref, xf_ref, up_ref, down_ref, mean_ref, y_ref, far_ref, inbox, hid, mine, zout, zin, keep, yout, yin, done, x_sem, in_sem, z_ssem, z_rsem, s_ssem, s_rsem, r_ssem, r_rsem, pass_ssem, y_ssem, y_rsem, piece_ssem, piece_rsem, go_sem):
    model, data, stage = lax.axis_index('model'), lax.axis_index('data'), lax.axis_index('stage')
    mesh_id = pl.DeviceIdType.MESH
    last = n_stage - 1
    n_group, _, rows2, half = inbox.shape
    rows = rows2 // 2
    n_piece = piece_ssem.shape[0]
    piece = far_ref.shape[0] // n_piece
    peer = {'data': 1 - data}
    near = pl.ds(pl.multiple_of(model * half, half), half)
    far = pl.ds(pl.multiple_of((1 - model) * half, half), half)
    own_rows = pl.ds(pl.multiple_of(data * rows, rows), rows)
    peer_rows = pl.ds(pl.multiple_of((1 - data) * rows, rows), rows)

    def remote(src, dst, ssem, rsem, where):
        return pltpu.make_async_remote_copy(src_ref=src, dst_ref=dst, send_sem=ssem, recv_sem=rsem, device_id=where, device_id_type=mesh_id)

    barrier = pltpu.get_barrier_semaphore()
    group = [(dm, ds) for dm in range(2) for ds in range(n_stage) if dm or ds]
    where = [{'model': lax.rem(model + dm, 2), 'stage': lax.rem(stage + ds, n_stage)} for dm, ds in group]
    for target in where + [peer]:
        pl.semaphore_signal(barrier, inc=1, device_id=target, device_id_type=mesh_id)

    def load_x(b, c, from_ref, to_rows, i):
        return pltpu.make_async_copy(from_ref.at[b, :, pl.ds(c * half, half)], inbox.at[b, c, to_rows], x_sem.at[b, c, i])

    def loads(b):
        return [load_x(b, c, *pair) for c in range(2) for pair in ((x_ref, own_rows, 0), (xf_ref, peer_rows, 1))]

    @pl.when(stage == 0)
    def _():
        for b in range(n_group):
            for copy in loads(b):
                copy.start()

    pl.semaphore_wait(barrier, len(where) + 1)

    def send_piece(p):
        span = pl.ds(pl.multiple_of(p * piece, piece), piece)
        return remote(mean_ref.at[span], far_ref.at[span], piece_ssem.at[p], piece_rsem.at[p], peer)

    def start_pieces(low, high):
        def one(p, carry):
            send_piece(p).start()
            return carry

        lax.fori_loop(low, high, one, 0)

    n_turn = n_group + 3 * LAG
    base, slope = lead
    is_even = lax.rem(stage, 2) == 0
    limit = n_piece - HELD_FWD * lax.rem(stage, 2)
    begin = jnp.minimum(base + slope * stage, limit)
    start_pieces(0, begin)

    def arrival(b, c):
        return remote(done.at[b], inbox.at[b, c], pass_ssem.at[b, 0], in_sem.at[b, c], {'model': model})

    def trade_z(b):
        return remote(zout.at[b], zin.at[b], z_ssem.at[b], z_rsem.at[b], {'model': 1 - model})

    def trade_s(b):
        return remote(yout.at[b], yin.at[b], s_ssem.at[b], s_rsem.at[b], peer)

    def trade_r(b):
        return remote(done.at[b, own_rows], done.at[b, own_rows], r_ssem.at[b], r_rsem.at[b], peer)

    def hand_on(b, to):
        return remote(done.at[b], inbox.at[b, model], pass_ssem.at[b, to], in_sem.at[b, model], {'model': to, 'stage': stage + 1})

    def landing(b, c):
        return y_ref.at[b, :, pl.ds(pl.multiple_of(c * half, half), half)]

    def publish(b, k):
        return remote(done.at[b, own_rows], landing(b, model), y_ssem.at[b, k], y_rsem.at[b, model], where[k])

    def y_arrival(b, c):
        return remote(done.at[b, own_rows], landing(b, c), y_ssem.at[b, 0], y_rsem.at[b, c], {'model': model})

    def project(t):
        @pl.when(t < n_group)
        def _():
            @pl.when(stage == 0)
            def _():
                for copy in loads(t):
                    copy.wait()

            @pl.when(stage > 0)
            def _():
                for c in range(2):
                    arrival(t, c).wait_recv()

            pre = jnp.dot(inbox[t, 0], up_ref[:half], preferred_element_type=jnp.float32)
            pre = pre + jnp.dot(inbox[t, 1], up_ref[half:], preferred_element_type=jnp.float32)
            hid[...] = jax.nn.gelu(pre).astype(jnp.bfloat16)
            zout[t] = jnp.dot(hid[...], down_ref[:, far], preferred_element_type=jnp.float32)
            trade_z(t).start()
            mine[t] = jnp.dot(hid[...], down_ref[:, near], preferred_element_type=jnp.float32)

    def reduce_z(t):
        @pl.when((t >= LAG) & (t < n_group + LAG))
        def _():
            b = t - LAG
            trade_z(b).wait_recv()
            yout[b] = mine[b, peer_rows] + zin[b, peer_rows]
            trade_s(b).start()
            keep[b] = mine[b, own_rows] + zin[b, own_rows]

    def reduce_y(t):
        @pl.when((t >= 2 * LAG) & (t < n_group + 2 * LAG))
        def _():
            b = t - 2 * LAG
            trade_s(b).wait_recv()
            total = inbox[b, model, own_rows].astype(jnp.float32) + (keep[b] + yin[b])
            result = total.astype(jnp.bfloat16)
            done[b, own_rows] = result

            @pl.when(stage < last)
            def _():
                trade_r(b).start()

            @pl.when(stage == last)
            def _():
                y_ref[b, :, near] = result
                for k in range(len(group)):
                    publish(b, k).start()

    def pass_on(t):
        @pl.when((t >= 3 * LAG) & (stage < last))
        def _():
            b = t - 3 * LAG
            remote(done.at[b, own_rows], done.at[b, peer_rows], r_ssem.at[b], r_rsem.at[b], peer).wait_recv()
            for to in range(2):
                hand_on(b, to).start()

    def turn(t, carry):
        for phase in (project, reduce_z, reduce_y, pass_on):
            phase(t)
        return carry

    lax.fori_loop(0, n_turn, turn, 0)
    start_pieces(begin, limit)

    for b in range(n_group):
        trade_z(b).wait_send()
        trade_s(b).wait_send()

    @pl.when(stage < last)
    def _():
        for b in range(n_group):
            trade_r(b).wait_send()
            for to in range(2):
                hand_on(b, to).wait_send()
            for c in range(2):
                y_arrival(b, c).wait_recv()

    @pl.when(stage == last)
    def _():
        for b in range(n_group):
            for k in range(len(group)):
                publish(b, k).wait_send()
            y_arrival(b, 1 - model).wait_recv()

    def sent(p, carry):
        send_piece(p).wait_send()
        return carry

    def landed(p, carry):
        send_piece(p).wait_recv()
        return carry

    lax.fori_loop(0, limit, sent, 0)

    @pl.when(is_even)
    def _():
        pl.semaphore_signal(go_sem, inc=1, device_id={'stage': stage + 1}, device_id_type=mesh_id)

    @pl.when(jnp.logical_not(is_even))
    def _():
        pl.semaphore_wait(go_sem, 1)
        start_pieces(limit, n_piece)
        lax.fori_loop(limit, n_piece, sent, 0)

    lax.fori_loop(0, n_piece, landed, 0)


def forward_call(n_stage, n_group, n_piece, lead, n_far, x_next, x_far, up_bf, down_bf, mean):
    d_model = x_next.shape[2]
    x_next, x_far = [value.reshape(n_group, -1, d_model) for value in (x_next, x_far)]
    rows, half, ff_half = x_next.shape[1], d_model // 2, up_bf.shape[1]
    dma = pltpu.SemaphoreType.DMA
    f32, bf16 = jnp.float32, jnp.bfloat16
    in_vmem = pl.BlockSpec(memory_space=pltpu.VMEM)
    anywhere = pl.BlockSpec(memory_space=pl.ANY)
    return pl.pallas_call(
        functools.partial(forward_body, n_stage, lead),
        out_shape=[jax.ShapeDtypeStruct(x_next.shape, bf16), jax.ShapeDtypeStruct((n_far, d_model), f32)],
        in_specs=[anywhere, anywhere, in_vmem, in_vmem, anywhere],
        out_specs=[in_vmem, anywhere],
        scratch_shapes=[
            pltpu.VMEM((n_group, 2, 2 * rows, half), bf16),
            pltpu.VMEM((2 * rows, ff_half), bf16),
            pltpu.VMEM((n_group, 2 * rows, half), f32),
            pltpu.VMEM((n_group, 2 * rows, half), f32),
            pltpu.VMEM((n_group, 2 * rows, half), f32),
            pltpu.VMEM((n_group, rows, half), f32),
            pltpu.VMEM((n_group, rows, half), f32),
            pltpu.VMEM((n_group, rows, half), f32),
            pltpu.VMEM((n_group, 2 * rows, half), bf16),
            dma((n_group, 2, 2)),
            dma((n_group, 2)),
            dma((n_group,)),
            dma((n_group,)),
            dma((n_group,)),
            dma((n_group,)),
            dma((n_group,)),
            dma((n_group,)),
            dma((n_group, 2)),
            dma((n_group, 2 * n_stage - 1)),
            dma((n_group, 2)),
            dma((n_piece,)),
            dma((n_piece,)),
            pltpu.SemaphoreType.REGULAR,
        ],
        compiler_params=pltpu.CompilerParams(collective_id=1, has_side_effects=True, vmem_limit_bytes=67043328),
        name="forward_pipe",
    )(x_next, x_far, up_bf, down_bf, mean)


def solution(mesh):
    n_stage = mesh.shape['stage']
    swap = [(0, 1), (1, 0)]
    up_spec = P('stage', None, 'model')
    down_spec = P('stage', 'model', None)
    row_spec = P(None, 'data', None)
    in_specs = (up_spec, down_spec, up_spec, down_spec, up_spec, down_spec, P('data', 'stage', None, 'model'), P('data', 'stage', 'model', None), P('stage', 'data', None), P('data', None), row_spec, P(None), P(None))
    out_specs = (up_spec, down_spec, up_spec, down_spec, up_spec, down_spec, row_spec)

    def device_step(w_up, w_down, m_up, m_down, v_up, v_down, g_up, g_down, acts_last, grad_out, x_next, learn_rate, max_norm):
        data_id = lax.axis_index('data')
        half = data_id.astype(jnp.int32).reshape(1)
        other = (1 - half).astype(jnp.int32)
        d_model, ff_local = w_up.shape[1:]
        ff_half = ff_local // 2
        bounds_up = ((0, 256), (256, 640), (640, 896), (896, 960), (960, d_model))
        bounds_down = ((0, N_PIECE * 32), (N_PIECE * 32, ff_half))

        def trade(value):
            return lax.ppermute(value, 'data', swap)

        early, *late, late_down, whole_up, whole_down, far_first, x_far, clip = backward_call(n_stage, bounds_up, bounds_down, g_up[0, 0], g_down[0, 0], w_up[0], w_down[0], acts_last[0], grad_out, x_next, max_norm)
        ups = (w_up[0], m_up[0], v_up[0])
        downs = (w_down[0], m_down[0], v_down[0])

        def map_up(low, block):
            return lambda i, h, r: (low // block + i, h[0])

        def map_down(low, block):
            return lambda i, h, r: ((h[0] * ff_half + low) // block + i, 0)

        far_early = trade(early)
        *new_up, up_bf = update_call(half, learn_rate, clip, ups, whole_up, map_up(0, 2 * BLOCK), None, block=2 * BLOCK)
        *new_down, down_bf = update_call(half, learn_rate, clip, downs, whole_down, map_down(0, 2 * BLOCK), None, (up_bf,), block=2 * BLOCK)
        new_up = update_call(other, learn_rate, clip, ups, far_first, map_up(0, BLOCK), new_up, (down_bf,))
        down_bf, new_up = lax.optimization_barrier((down_bf, new_up))
        y_next, far_down = forward_call(n_stage, N_GROUP, N_PIECE, LEAD, bounds_down[0][1], x_next, x_far, up_bf, down_bf, whole_down)
        y_next = y_next.reshape(x_next.shape)
        late, late_down, far_down = lax.optimization_barrier((late, late_down, far_down))
        fars = [trade(late[0])]
        far_last = trade(late_down)
        fars += [trade(value) for value in late[1:]]
        *new_down, y_next = update_call(other, learn_rate, clip, downs, far_down, map_down(0, BLOCK), new_down, (), (y_next,))
        after = (new_down[0],)
        for bounds, part in zip(bounds_up[1:3], (far_early, fars[0])):
            new_up = update_call(other, learn_rate, clip, ups, part, map_up(bounds[0], step_of(*bounds)), new_up, after, block=step_of(*bounds))
            after = ()
        new_down = update_call(other, learn_rate, clip, downs, far_last, map_down(bounds_down[1][0], BLOCK // 2), new_down, (new_up[0],), block=BLOCK // 2)
        after = (new_down[0],)
        for bounds, part in zip(bounds_up[3:], fars[1:]):
            new_up = update_call(other, learn_rate, clip, ups, part, map_up(bounds[0], step_of(*bounds)), new_up, after, block=step_of(*bounds))
            after = ()
        return (new_up[0][None], new_down[0][None], new_up[1][None], new_down[1][None], new_up[2][None], new_down[2][None], y_next)

    return jax.shard_map(device_step, mesh=mesh, in_specs=in_specs, out_specs=out_specs, check_vma=False)
```

```python
import functools

import jax
import jax.numpy as jnp
from jax import lax
from jax.experimental import pallas as pl
from jax.experimental.pallas import tpu as pltpu
from jax.sharding import PartitionSpec as P

ADAM_STEP = 10
BETA_ONE = 0.9
BETA_TWO = 0.95
ADAM_EPS = 1e-8
WEIGHT_DECAY = 0.1
NORM_EPS = 1e-6
CONTRACT_LAST = (((1,), (1,)), ((), ()))
BLOCK = 128
N_GROUP = 8
N_PIECE = 28
LEAD = (3, 7)
HELD = 2
HELD_FWD = 3
LAG = 2
N_RAW = 4


def update_body(skip, carry, half_ref, rate_ref, clip_ref, w_ref, m_ref, v_ref, g_ref, *refs):
    outs = refs[skip:]
    if carry:
        outs[-1][...] = refs[skip - 1][...]
        outs = outs[:-1]
    ow_ref, om_ref, ov_ref = outs[:3]
    rate = rate_ref[0]
    grad = clip_ref[0:1] * g_ref[...]
    weight = w_ref[...]
    mom = BETA_ONE * m_ref[...] + (1.0 - BETA_ONE) * grad
    sec = BETA_TWO * v_ref[...] + (1.0 - BETA_TWO) * grad * grad
    one_corr = 1.0 - BETA_ONE**ADAM_STEP
    two_corr = 1.0 - BETA_TWO**ADAM_STEP
    direction = (mom * (1.0 / one_corr)) / (jnp.sqrt(sec * (1.0 / two_corr)) + ADAM_EPS)
    new = weight - rate * (direction + WEIGHT_DECAY * weight)
    ow_ref[...] = new
    om_ref[...] = mom
    ov_ref[...] = sec
    if len(outs) == 4:
        outs[3][...] = new.astype(jnp.bfloat16)


def step_of(low, high):
    return BLOCK if low % BLOCK == 0 and high % BLOCK == 0 else BLOCK // 2


def update_call(half, rate, clip, weights, grad, full_map, previous, after=(), carry=(), block=BLOCK):
    rows, cols = grad.shape
    shape = weights[0].shape
    spec = pl.BlockSpec((block, cols), full_map)
    flat = pl.BlockSpec((block, cols), lambda i, h, r: (i, 0))
    anywhere = pl.BlockSpec(memory_space=pl.ANY)
    first = previous is None
    extra = list(previous or ()) + list(after)
    passed = [pl.BlockSpec((1,) + value.shape[1:], lambda i, h, r: (jnp.minimum(i, value.shape[0] - 1), 0, 0)) for value in carry]
    return pl.pallas_call(
        functools.partial(update_body, len(extra) + len(carry), len(carry)),
        grid_spec=pltpu.PrefetchScalarGridSpec(
            num_scalar_prefetch=2,
            grid=(rows // block,),
            in_specs=[pl.BlockSpec(clip.shape, lambda i, h, r: (0, 0)), spec, spec, spec, flat] + [anywhere] * len(extra) + passed,
            out_specs=[spec] * 3 + [flat] * first + passed,
        ),
        out_shape=[jax.ShapeDtypeStruct(shape, jnp.float32)] * 3 + [jax.ShapeDtypeStruct(grad.shape, jnp.bfloat16)] * first + [jax.ShapeDtypeStruct(value.shape, value.dtype) for value in carry],
        input_output_aliases={7 + i: i for i in range(len(previous or ()))},
        cost_estimate=pl.CostEstimate(flops=60 * rows * cols, bytes_accessed=30 * rows * cols, transcendentals=0),
        compiler_params=pltpu.CompilerParams(vmem_limit_bytes=67043328),
        name="adamw_half",
    )(half, rate, clip, *weights, grad, *extra, *carry)


def backward_body(n_stage, n_raw, bounds_up, bounds_down, gu_ref, gd_ref, wu_ref, wd_ref, acts_ref, gout_ref, x_ref, max_ref, *refs):
    n_up, n_down = len(bounds_up) - 1, len(bounds_down) - 1
    outs_up, outs_down = refs[:n_up], refs[n_up:n_up + n_down]
    whole_up, whole_down, far_ref, x_far, clip_ref = refs[n_up + n_down:n_up + n_down + 5]
    (up_bf, down_bf, st_up, st_down, acc_up, acc_down, got_up, got_down, fold, hid, slope, grad_pre, gbuf, outbox, landed, ready, rows_a, rows_z, norm_box, norm_pair,
     st_sem, loc_sem, fold_sem, own_sem, out_sem, g_rsem, trade_sem, pass_ssem, rs_ssem, rs_rsem, row_ssem, row_rsem, far_sem, norm_ssem, norm_rsem, x_land, x_sem, xf_ssem, xf_rsem, go_sem, fold_up, fold_up_sem) = refs[n_up + n_down + 5:]
    model, data, stage = lax.axis_index('model'), lax.axis_index('data'), lax.axis_index('stage')
    mesh_id = pl.DeviceIdType.MESH
    last = n_stage - 1
    d_model, ff_half = acc_up.shape
    half = d_model // 2
    n_row = acts_ref.shape[0]
    n_up_chunk, n_down_chunk = d_model // BLOCK, ff_half // BLOCK
    peer = {'data': 1 - data}
    near = pl.ds(pl.multiple_of(model * half, half), half)
    far = pl.ds(pl.multiple_of((1 - model) * half, half), half)
    own_cols = pl.ds(pl.multiple_of(data * ff_half, ff_half), ff_half)
    peer_cols = pl.ds(pl.multiple_of((1 - data) * ff_half, ff_half), ff_half)
    own_rows = pl.ds(pl.multiple_of(data * n_row, n_row), n_row)
    first_dims = (((0,), (0,)), ((), ()))

    def remote(src, dst, ssem, rsem, where):
        return pltpu.make_async_remote_copy(src_ref=src, dst_ref=dst, send_sem=ssem, recv_sem=rsem, device_id=where, device_id_type=mesh_id)

    barrier = pltpu.get_barrier_semaphore()
    group = [(dm, ds) for dm in range(2) for ds in range(n_stage) if dm or ds]
    where = [{'model': lax.rem(model + dm, 2), 'stage': lax.rem(stage + ds, n_stage)} for dm, ds in group]
    for target in where + [peer]:
        pl.semaphore_signal(barrier, inc=1, device_id=target, device_id_type=mesh_id)

    n_st_up, n_st_down = d_model // st_up.shape[1], 2 * ff_half // st_down.shape[1]

    def load_up(r):
        return pltpu.make_async_copy(wu_ref.at[pl.ds(r * st_up.shape[1], st_up.shape[1])], st_up.at[r % 2], st_sem.at[0, r % 2])

    def load_down(r):
        return pltpu.make_async_copy(wd_ref.at[pl.ds(r * st_down.shape[1], st_down.shape[1])], st_down.at[r % 2], st_sem.at[1, r % 2])

    load_acts = pltpu.make_async_copy(acts_ref, rows_a.at[own_rows], loc_sem.at[0])
    load_acts.start()
    load_up(0).start()
    load_up(1).start()
    load_down(0).start()
    load_down(1).start()

    def load_g(c):
        return pltpu.make_async_copy(gout_ref.at[:, pl.ds(c * half, half)], gbuf.at[c], loc_sem.at[1 + c])

    @pl.when(stage == last)
    def _():
        for c in range(2):
            load_g(c).start()

    pl.semaphore_wait(barrier, len(where) + 1)

    def chunk(k):
        return pl.ds(k * BLOCK, BLOCK)

    raw_rows = n_raw * BLOCK
    raw = [remote(gu_ref.at[chunk(k), peer_cols], got_up.at[chunk(k)], rs_ssem.at[0, k], rs_rsem.at[0, k], peer) for k in range(n_raw)]
    carries_x = stage >= n_stage // 2

    def micro(i):
        return 2 * (stage - n_stage // 2) + i

    def send_x(i):
        return remote(x_ref.at[micro(i), :, near], x_land.at[i], x_sem.at[0, i], x_sem.at[1, i], peer)

    @pl.when(carries_x)
    def _():
        for i in range(2):
            send_x(i).start()

    for copy in raw:
        copy.start()
    send_a = remote(acts_ref.at[:, :raw_rows], rows_a.at[own_rows, :raw_rows], row_ssem.at[0], row_rsem.at[0], peer)
    send_a.start()

    for r in range(n_st_up):
        load_up(r).wait()
        up_bf[pl.ds(r * st_up.shape[1], st_up.shape[1])] = st_up[r % 2].astype(jnp.bfloat16)
        if r + 2 < n_st_up:
            load_up(r + 2).start()
    load_acts.wait()

    tile = 256
    n_tile = hid.shape[1] // tile
    scale = 0.7978845608028654
    cubic = 0.044715

    def pre_tile(j, carry):
        cols = pl.ds(pl.multiple_of(j * tile, tile), tile)
        pre = jnp.dot(rows_a[own_rows], up_bf[:, cols], preferred_element_type=jnp.float32)
        square = pre * pre
        bend = jnp.tanh(scale * (pre + cubic * square * pre))
        hid[:, cols] = (pre * (0.5 * (1.0 + bend))).astype(jnp.bfloat16)
        slope[:, cols] = 0.5 * (1.0 + bend) + 0.5 * pre * (1.0 - bend * bend) * (scale * (1.0 + 3.0 * cubic * square))
        return carry

    lax.fori_loop(0, n_tile, pre_tile, 0)

    for r in range(n_st_down):
        load_down(r).wait()
        down_bf[pl.ds(r * st_down.shape[1], st_down.shape[1])] = st_down[r % 2].astype(jnp.bfloat16)
        if r + 2 < n_st_down:
            load_down(r + 2).start()

    own_up = pltpu.make_async_copy(gu_ref.at[:, own_cols], acc_up, own_sem.at[0])
    own_down = pltpu.make_async_copy(gd_ref.at[own_cols], acc_down, own_sem.at[1])
    load_fold = pltpu.make_async_copy(gd_ref.at[peer_cols], fold, fold_sem)
    load_fold_up = pltpu.make_async_copy(gu_ref.at[raw_rows:, peer_cols], fold_up, fold_up_sem)
    load_fold_up.start()
    load_fold.start()
    own_up.start()
    own_down.start()

    @pl.when(stage == last)
    def _():
        for c in range(2):
            load_g(c).wait()

    @pl.when(stage < last)
    def _():
        for c in range(2):
            remote(ready, gbuf.at[c], pass_ssem.at[0], g_rsem.at[c], {'model': model}).wait_recv()

    def slope_tile(j, carry):
        cols = pl.ds(pl.multiple_of(j * tile, tile), tile)
        grad = lax.dot_general(gbuf[0], down_bf[cols, :half], CONTRACT_LAST, preferred_element_type=jnp.float32)
        grad = grad + lax.dot_general(gbuf[1], down_bf[cols, half:], CONTRACT_LAST, preferred_element_type=jnp.float32)
        grad_pre[:, cols] = (slope[:, cols] * grad).astype(jnp.bfloat16)
        return carry

    lax.fori_loop(0, n_tile, slope_tile, 0)

    trade = remote(outbox, landed, trade_sem.at[0], trade_sem.at[1], {'model': 1 - model})

    def hand_on(to):
        return remote(ready, gbuf.at[model], pass_ssem.at[to], g_rsem.at[model], {'model': to, 'stage': stage - 1})

    @pl.when(stage > 0)
    def _():
        outbox[...] = lax.dot_general(grad_pre[...], up_bf[far], CONTRACT_LAST, preferred_element_type=jnp.float32)
        trade.start()
        mine = lax.dot_general(grad_pre[...], up_bf[near], CONTRACT_LAST, preferred_element_type=jnp.float32)
        trade.wait_recv()
        ready[...] = (gbuf[model].astype(jnp.float32) + (mine + landed[...])).astype(jnp.bfloat16)
        for to in range(2):
            hand_on(to).start()

    rows_z[own_rows] = grad_pre[:, own_cols]
    send_z = remote(grad_pre.at[:, peer_cols], rows_z.at[own_rows], row_ssem.at[1], row_rsem.at[1], peer)
    send_z.start()

    load_fold_up.wait()

    def send_fold_up(k):
        rows = pl.ds(pl.multiple_of(k * BLOCK, BLOCK), BLOCK)
        at = pl.ds(pl.multiple_of((n_raw + k) * BLOCK, BLOCK), BLOCK)
        return remote(fold_up.at[rows], got_up.at[at], rs_ssem.at[0, n_raw + k], rs_rsem.at[0, n_raw + k], peer)

    def fold_up_step(k, carry):
        rows = pl.ds(pl.multiple_of(k * BLOCK, BLOCK), BLOCK)
        at = pl.ds(pl.multiple_of((n_raw + k) * BLOCK, BLOCK), BLOCK)
        fold_up[rows] += lax.dot_general(rows_a[own_rows, at], grad_pre[:, peer_cols], first_dims, preferred_element_type=jnp.float32)
        send_fold_up(k).start()
        return carry

    lax.fori_loop(0, n_up_chunk - n_raw, fold_up_step, 0)

    def forward_x(i, to):
        return remote(x_land.at[i], x_far.at[micro(i), :, near], xf_ssem.at[i, to], xf_rsem.at[micro(i), model], {'model': to, 'stage': 0})

    @pl.when(carries_x)
    def _():
        for i in range(2):
            send_x(i).wait_recv()
            for to in range(2):
                forward_x(i, to).start()

    def down_product(k, side):
        cols = pl.ds(pl.multiple_of(side * ff_half + k * BLOCK, BLOCK), BLOCK)
        left = hid[:, cols]
        return [lax.dot_general(left, gbuf[c], first_dims, preferred_element_type=jnp.float32) for c in range(2)]

    load_fold.wait()

    def send_fold(k):
        rows = pl.ds(pl.multiple_of(k * BLOCK, BLOCK), BLOCK)
        return remote(fold.at[rows], got_down.at[rows], rs_ssem.at[1, k], rs_rsem.at[1, k], peer)

    def fold_step(k, carry):
        rows = pl.ds(pl.multiple_of(k * BLOCK, BLOCK), BLOCK)
        low, high = down_product(k, 1 - data)
        fold[rows, :half] += low
        fold[rows, half:] += high
        send_fold(k).start()
        return carry

    lax.fori_loop(0, n_down_chunk, fold_step, 0)
    own_down.wait()

    def own_step(k, carry):
        rows = pl.ds(pl.multiple_of(k * BLOCK, BLOCK), BLOCK)
        low, high = down_product(k, data)
        acc_down[rows, :half] += low
        acc_down[rows, half:] += high
        return carry

    lax.fori_loop(0, n_down_chunk, own_step, 0)

    @pl.when(stage > 0)
    def _():
        trade.wait_send()
        for to in range(2):
            hand_on(to).wait_send()

    own_up.wait()
    send_a.wait_recv()
    squares = jnp.zeros((8, ff_half), jnp.float32)

    def fold_squares(mean):
        return jnp.sum((mean * mean).reshape(-1, 8, mean.shape[1]), axis=0)

    def put(acc, bounds, outs, whole, sem_row):
        copies = []
        for i, (lo, hi) in enumerate(bounds):
            rows = pl.ds(lo, hi - lo)
            copies.append(pltpu.make_async_copy(acc.at[rows], whole.at[rows], out_sem.at[sem_row, i]))
            if outs[i] is not None:
                copies.append(pltpu.make_async_copy(acc.at[rows], outs[i], out_sem.at[sem_row, len(bounds) + i]))
        return copies

    def put_start(k, bounds, copies, outs):
        at = 0
        for i, (lo, hi) in enumerate(bounds):
            count = 1 if outs[i] is None else 2
            if k * BLOCK < hi <= (k + 1) * BLOCK:
                for copy in copies[at:at + count]:
                    copy.start()
            at += count

    outs_up = (None,) + tuple(outs_up)
    outs_down = (None,) + tuple(outs_down)
    put_up = put(acc_up, bounds_up, outs_up, whole_up, 0)
    put_down = put(acc_down, bounds_down, outs_down, whole_down, 1)
    for k in range(n_up_chunk):
        if k == 0:
            send_z.wait_recv()
        if k < n_raw:
            raw[k].wait_recv()
            product = lax.dot_general(rows_a[:, chunk(k)], rows_z[...], first_dims, preferred_element_type=jnp.float32)
        else:
            send_fold_up(k - n_raw).wait_recv()
            product = lax.dot_general(rows_a[own_rows, chunk(k)], rows_z[own_rows], first_dims, preferred_element_type=jnp.float32)
        mean = (acc_up[chunk(k)] + got_up[chunk(k)] + product) * 0.5
        acc_up[chunk(k)] = mean
        squares = squares + fold_squares(mean)
        put_start(k, bounds_up, put_up, outs_up)
    n_far = far_sem.shape[1]
    slab = bounds_up[0][1] // n_far
    is_even = lax.rem(stage, 2) == 0

    def send_far(i):
        span = pl.ds(pl.multiple_of(i * slab, slab), slab)
        return remote(acc_up.at[span], far_ref.at[span], far_sem.at[0, i], far_sem.at[1, i], peer)

    for i in range(n_far - HELD):
        send_far(i).start()

    @pl.when(is_even)
    def _():
        for i in range(n_far - HELD, n_far):
            send_far(i).start()

    for k in range(n_down_chunk):
        send_fold(k).wait_recv()
        mean = (acc_down[chunk(k)] + got_down[chunk(k)]) * 0.5
        acc_down[chunk(k)] = mean
        squares = squares + fold_squares(mean)
        put_start(k, bounds_down, put_down, outs_down)

    lanes = norm_box.shape[2]
    part = squares[:, :lanes]
    for j in range(1, ff_half // lanes):
        part = part + squares[:, j * lanes:(j + 1) * lanes]
    me = model * n_stage + stage
    norm_box[me] = part

    def spread(i):
        return remote(norm_box.at[me], norm_box.at[me], norm_ssem.at[i], norm_rsem.at[me], where[i])

    for i in range(len(group)):
        spread(i).start()
    for i, (dm, ds) in enumerate(group):
        them = lax.rem(model + dm, 2) * n_stage + lax.rem(stage + ds, n_stage)
        remote(norm_box.at[me], norm_box.at[them], norm_ssem.at[i], norm_rsem.at[them], where[i]).wait_recv()
    total = norm_box[0]
    for i in range(1, 2 * n_stage):
        total = total + norm_box[i]
    norm_pair[0] = total
    swap = remote(norm_pair.at[0], norm_pair.at[1], norm_ssem.at[len(group)], norm_rsem.at[2 * n_stage], peer)
    swap.start()
    swap.wait_recv()
    norm_sq = jnp.sum(norm_pair[0] + norm_pair[1], axis=(0, 1), keepdims=True)
    norm = jnp.sqrt(jnp.broadcast_to(norm_sq, clip_ref.shape)) + NORM_EPS
    clip_ref[...] = jnp.minimum(1.0, max_ref[0] / norm)

    @pl.when(carries_x)
    def _():
        for i in range(2):
            send_x(i).wait_send()
            for to in range(2):
                forward_x(i, to).wait_send()

    @pl.when(stage == 0)
    def _():
        for s in range(n_stage):
            for m in range(2):
                remote(x_land.at[0], x_far.at[s, :, pl.ds(m * half, half)], xf_ssem.at[0, m], xf_rsem.at[s, m], {'model': model}).wait_recv()

    swap.wait_send()
    for i in range(len(group)):
        spread(i).wait_send()
    for copy in raw + [send_a, send_z]:
        copy.wait_send()
    for k in range(n_down_chunk):
        send_fold(k).wait_send()
    for k in range(n_up_chunk - n_raw):
        send_fold_up(k).wait_send()
    for copy in put_up + put_down:
        copy.wait()

    @pl.when(is_even)
    def _():
        for i in range(n_far):
            send_far(i).wait_send()
        pl.semaphore_signal(go_sem, inc=1, device_id={'stage': stage + 1}, device_id_type=mesh_id)

    @pl.when(jnp.logical_not(is_even))
    def _():
        pl.semaphore_wait(go_sem, 1)
        for i in range(n_far - HELD, n_far):
            send_far(i).start()
        for i in range(n_far):
            send_far(i).wait_send()

    for i in range(n_far):
        send_far(i).wait_recv()


def backward_call(n_stage, bounds_up, bounds_down, g_up, g_down, w_up, w_down, acts, grad_out, x_next, max_norm):
    d_model, ff_local = g_up.shape
    ff_half, half, n_row = ff_local // 2, d_model // 2, acts.shape[0]
    dma = pltpu.SemaphoreType.DMA
    anywhere = pl.BlockSpec(memory_space=pl.ANY)
    f32, bf16 = jnp.float32, jnp.bfloat16
    shapes = [jax.ShapeDtypeStruct((hi - lo, ff_half), f32) for lo, hi in bounds_up[1:]]
    shapes += [jax.ShapeDtypeStruct((hi - lo, d_model), f32) for lo, hi in bounds_down[1:]]
    shapes += [jax.ShapeDtypeStruct((d_model, ff_half), f32), jax.ShapeDtypeStruct((ff_half, d_model), f32)]
    shapes += [jax.ShapeDtypeStruct((bounds_up[0][1], ff_half), f32), jax.ShapeDtypeStruct(x_next.shape, bf16), jax.ShapeDtypeStruct((8, ff_half), f32)]
    n_chunk = max(d_model, ff_half) // BLOCK
    return pl.pallas_call(
        functools.partial(backward_body, n_stage, N_RAW, bounds_up, bounds_down),
        out_shape=shapes,
        in_specs=[anywhere] * 7 + [pl.BlockSpec(memory_space=pltpu.SMEM)],
        out_specs=[anywhere] * (len(shapes) - 1) + [pl.BlockSpec(memory_space=pltpu.VMEM)],
        scratch_shapes=[
            pltpu.VMEM((d_model, ff_local), bf16),
            pltpu.VMEM((ff_local, d_model), bf16),
            pltpu.VMEM((2, 256, ff_local), f32),
            pltpu.VMEM((2, 512, d_model), f32),
            pltpu.VMEM((d_model, ff_half), f32),
            pltpu.VMEM((ff_half, d_model), f32),
            pltpu.VMEM((d_model, ff_half), f32),
            pltpu.VMEM((ff_half, d_model), f32),
            pltpu.VMEM((ff_half, d_model), f32),
            pltpu.VMEM((n_row, ff_local), bf16),
            pltpu.VMEM((n_row, ff_local), f32),
            pltpu.VMEM((n_row, ff_local), bf16),
            pltpu.VMEM((2, n_row, half), bf16),
            pltpu.VMEM((n_row, half), f32),
            pltpu.VMEM((n_row, half), f32),
            pltpu.VMEM((n_row, half), bf16),
            pltpu.VMEM((2 * n_row, d_model), bf16),
            pltpu.VMEM((2 * n_row, ff_half), bf16),
            pltpu.VMEM((2 * n_stage, 8, 128), f32),
            pltpu.VMEM((2, 8, 128), f32),
            dma((2, 2)),
            dma((3,)),
            dma(()),
            dma((2,)),
            dma((2, 2 * max(len(bounds_up), len(bounds_down)))),
            dma((2,)),
            dma((2,)),
            dma((2,)),
            dma((2, n_chunk)),
            dma((2, n_chunk)),
            dma((2,)),
            dma((2,)),
            dma((2, 8)),
            dma((2 * n_stage,)),
            dma((2 * n_stage + 1,)),
            pltpu.VMEM((2, n_row, half), bf16),
            dma((2, 2)),
            dma((2, 2)),
            dma((n_stage, 2)),
            pltpu.SemaphoreType.REGULAR,
            pltpu.VMEM((d_model - N_RAW * BLOCK, ff_half), f32),
            dma(()),
        ],
        compiler_params=pltpu.CompilerParams(collective_id=0, has_side_effects=True, vmem_limit_bytes=67043328),
        name="reduce_and_norm",
    )(g_up, g_down, w_up, w_down, acts, grad_out, x_next, max_norm)


def forward_body(n_stage, lead, x_ref, xf_ref, up_ref, down_ref, mean_ref, y_ref, far_ref, inbox, hid, mine, zout, zin, keep, yout, yin, done, x_sem, in_sem, z_ssem, z_rsem, s_ssem, s_rsem, r_ssem, r_rsem, pass_ssem, y_ssem, y_rsem, piece_ssem, piece_rsem, go_sem):
    model, data, stage = lax.axis_index('model'), lax.axis_index('data'), lax.axis_index('stage')
    mesh_id = pl.DeviceIdType.MESH
    last = n_stage - 1
    n_group, _, rows2, half = inbox.shape
    rows = rows2 // 2
    n_piece = piece_ssem.shape[0]
    piece = far_ref.shape[0] // n_piece
    peer = {'data': 1 - data}
    near = pl.ds(pl.multiple_of(model * half, half), half)
    far = pl.ds(pl.multiple_of((1 - model) * half, half), half)
    own_rows = pl.ds(pl.multiple_of(data * rows, rows), rows)
    peer_rows = pl.ds(pl.multiple_of((1 - data) * rows, rows), rows)

    def remote(src, dst, ssem, rsem, where):
        return pltpu.make_async_remote_copy(src_ref=src, dst_ref=dst, send_sem=ssem, recv_sem=rsem, device_id=where, device_id_type=mesh_id)

    barrier = pltpu.get_barrier_semaphore()
    group = [(dm, ds) for dm in range(2) for ds in range(n_stage) if dm or ds]
    where = [{'model': lax.rem(model + dm, 2), 'stage': lax.rem(stage + ds, n_stage)} for dm, ds in group]
    for target in where + [peer]:
        pl.semaphore_signal(barrier, inc=1, device_id=target, device_id_type=mesh_id)

    def load_x(b, c, from_ref, to_rows, i):
        return pltpu.make_async_copy(from_ref.at[b, :, pl.ds(c * half, half)], inbox.at[b, c, to_rows], x_sem.at[b, c, i])

    def loads(b):
        return [load_x(b, c, *pair) for c in range(2) for pair in ((x_ref, own_rows, 0), (xf_ref, peer_rows, 1))]

    @pl.when(stage == 0)
    def _():
        for b in range(n_group):
            for copy in loads(b):
                copy.start()

    pl.semaphore_wait(barrier, len(where) + 1)

    def send_piece(p):
        span = pl.ds(pl.multiple_of(p * piece, piece), piece)
        return remote(mean_ref.at[span], far_ref.at[span], piece_ssem.at[p], piece_rsem.at[p], peer)

    def start_pieces(low, high):
        def one(p, carry):
            send_piece(p).start()
            return carry

        lax.fori_loop(low, high, one, 0)

    n_turn = n_group + 3 * LAG
    base, slope = lead
    is_even = lax.rem(stage, 2) == 0
    limit = n_piece - HELD_FWD * lax.rem(stage, 2)
    begin = jnp.minimum(base + slope * stage, limit)
    start_pieces(0, begin)

    def arrival(b, c):
        return remote(done.at[b], inbox.at[b, c], pass_ssem.at[b, 0], in_sem.at[b, c], {'model': model})

    def trade_z(b):
        return remote(zout.at[b], zin.at[b], z_ssem.at[b], z_rsem.at[b], {'model': 1 - model})

    def trade_s(b):
        return remote(yout.at[b], yin.at[b], s_ssem.at[b], s_rsem.at[b], peer)

    def trade_r(b):
        return remote(done.at[b, own_rows], done.at[b, own_rows], r_ssem.at[b], r_rsem.at[b], peer)

    def hand_on(b, to):
        return remote(done.at[b], inbox.at[b, model], pass_ssem.at[b, to], in_sem.at[b, model], {'model': to, 'stage': stage + 1})

    def landing(b, c):
        return y_ref.at[b, :, pl.ds(pl.multiple_of(c * half, half), half)]

    def publish(b, k):
        return remote(done.at[b, own_rows], landing(b, model), y_ssem.at[b, k], y_rsem.at[b, model], where[k])

    def y_arrival(b, c):
        return remote(done.at[b, own_rows], landing(b, c), y_ssem.at[b, 0], y_rsem.at[b, c], {'model': model})

    def project(t):
        @pl.when(t < n_group)
        def _():
            @pl.when(stage == 0)
            def _():
                for copy in loads(t):
                    copy.wait()

            @pl.when(stage > 0)
            def _():
                for c in range(2):
                    arrival(t, c).wait_recv()

            pre = jnp.dot(inbox[t, 0], up_ref[:half], preferred_element_type=jnp.float32)
            pre = pre + jnp.dot(inbox[t, 1], up_ref[half:], preferred_element_type=jnp.float32)
            hid[...] = jax.nn.gelu(pre).astype(jnp.bfloat16)
            zout[t] = jnp.dot(hid[...], down_ref[:, far], preferred_element_type=jnp.float32)
            trade_z(t).start()
            mine[t] = jnp.dot(hid[...], down_ref[:, near], preferred_element_type=jnp.float32)

    def reduce_z(t):
        @pl.when((t >= LAG) & (t < n_group + LAG))
        def _():
            b = t - LAG
            trade_z(b).wait_recv()
            yout[b] = mine[b, peer_rows] + zin[b, peer_rows]
            trade_s(b).start()
            keep[b] = mine[b, own_rows] + zin[b, own_rows]

    def reduce_y(t):
        @pl.when((t >= 2 * LAG) & (t < n_group + 2 * LAG))
        def _():
            b = t - 2 * LAG
            trade_s(b).wait_recv()
            total = inbox[b, model, own_rows].astype(jnp.float32) + (keep[b] + yin[b])
            result = total.astype(jnp.bfloat16)
            done[b, own_rows] = result

            @pl.when(stage < last)
            def _():
                trade_r(b).start()

            @pl.when(stage == last)
            def _():
                y_ref[b, :, near] = result
                for k in range(len(group)):
                    publish(b, k).start()

    def pass_on(t):
        @pl.when((t >= 3 * LAG) & (stage < last))
        def _():
            b = t - 3 * LAG
            remote(done.at[b, own_rows], done.at[b, peer_rows], r_ssem.at[b], r_rsem.at[b], peer).wait_recv()
            for to in range(2):
                hand_on(b, to).start()

    def turn(t, carry):
        for phase in (project, reduce_z, reduce_y, pass_on):
            phase(t)
        return carry

    lax.fori_loop(0, n_turn, turn, 0)
    start_pieces(begin, limit)

    for b in range(n_group):
        trade_z(b).wait_send()
        trade_s(b).wait_send()

    @pl.when(stage < last)
    def _():
        for b in range(n_group):
            trade_r(b).wait_send()
            for to in range(2):
                hand_on(b, to).wait_send()
            for c in range(2):
                y_arrival(b, c).wait_recv()

    @pl.when(stage == last)
    def _():
        for b in range(n_group):
            for k in range(len(group)):
                publish(b, k).wait_send()
            y_arrival(b, 1 - model).wait_recv()

    def sent(p, carry):
        send_piece(p).wait_send()
        return carry

    def landed(p, carry):
        send_piece(p).wait_recv()
        return carry

    lax.fori_loop(0, limit, sent, 0)

    @pl.when(is_even)
    def _():
        pl.semaphore_signal(go_sem, inc=1, device_id={'stage': stage + 1}, device_id_type=mesh_id)

    @pl.when(jnp.logical_not(is_even))
    def _():
        pl.semaphore_wait(go_sem, 1)
        start_pieces(limit, n_piece)
        lax.fori_loop(limit, n_piece, sent, 0)

    lax.fori_loop(0, n_piece, landed, 0)


def forward_call(n_stage, n_group, n_piece, lead, n_far, x_next, x_far, up_bf, down_bf, mean):
    d_model = x_next.shape[2]
    x_next, x_far = [value.reshape(n_group, -1, d_model) for value in (x_next, x_far)]
    rows, half, ff_half = x_next.shape[1], d_model // 2, up_bf.shape[1]
    dma = pltpu.SemaphoreType.DMA
    f32, bf16 = jnp.float32, jnp.bfloat16
    in_vmem = pl.BlockSpec(memory_space=pltpu.VMEM)
    anywhere = pl.BlockSpec(memory_space=pl.ANY)
    return pl.pallas_call(
        functools.partial(forward_body, n_stage, lead),
        out_shape=[jax.ShapeDtypeStruct(x_next.shape, bf16), jax.ShapeDtypeStruct((n_far, d_model), f32)],
        in_specs=[anywhere, anywhere, in_vmem, in_vmem, anywhere],
        out_specs=[in_vmem, anywhere],
        scratch_shapes=[
            pltpu.VMEM((n_group, 2, 2 * rows, half), bf16),
            pltpu.VMEM((2 * rows, ff_half), bf16),
            pltpu.VMEM((n_group, 2 * rows, half), f32),
            pltpu.VMEM((n_group, 2 * rows, half), f32),
            pltpu.VMEM((n_group, 2 * rows, half), f32),
            pltpu.VMEM((n_group, rows, half), f32),
            pltpu.VMEM((n_group, rows, half), f32),
            pltpu.VMEM((n_group, rows, half), f32),
            pltpu.VMEM((n_group, 2 * rows, half), bf16),
            dma((n_group, 2, 2)),
            dma((n_group, 2)),
            dma((n_group,)),
            dma((n_group,)),
            dma((n_group,)),
            dma((n_group,)),
            dma((n_group,)),
            dma((n_group,)),
            dma((n_group, 2)),
            dma((n_group, 2 * n_stage - 1)),
            dma((n_group, 2)),
            dma((n_piece,)),
            dma((n_piece,)),
            pltpu.SemaphoreType.REGULAR,
        ],
        compiler_params=pltpu.CompilerParams(collective_id=1, has_side_effects=True, vmem_limit_bytes=67043328),
        name="forward_pipe",
    )(x_next, x_far, up_bf, down_bf, mean)


def solution(mesh):
    n_stage = mesh.shape['stage']
    swap = [(0, 1), (1, 0)]
    up_spec = P('stage', None, 'model')
    down_spec = P('stage', 'model', None)
    row_spec = P(None, 'data', None)
    in_specs = (up_spec, down_spec, up_spec, down_spec, up_spec, down_spec, P('data', 'stage', None, 'model'), P('data', 'stage', 'model', None), P('stage', 'data', None), P('data', None), row_spec, P(None), P(None))
    out_specs = (up_spec, down_spec, up_spec, down_spec, up_spec, down_spec, row_spec)

    def device_step(w_up, w_down, m_up, m_down, v_up, v_down, g_up, g_down, acts_last, grad_out, x_next, learn_rate, max_norm):
        data_id = lax.axis_index('data')
        half = data_id.astype(jnp.int32).reshape(1)
        other = (1 - half).astype(jnp.int32)
        d_model, ff_local = w_up.shape[1:]
        ff_half = ff_local // 2
        bounds_up = ((0, 256), (256, 640), (640, 896), (896, 960), (960, d_model))
        bounds_down = ((0, N_PIECE * 32), (N_PIECE * 32, ff_half))

        def trade(value):
            return lax.ppermute(value, 'data', swap)

        early, *late, late_down, whole_up, whole_down, far_first, x_far, clip = backward_call(n_stage, bounds_up, bounds_down, g_up[0, 0], g_down[0, 0], w_up[0], w_down[0], acts_last[0], grad_out, x_next, max_norm)
        ups = (w_up[0], m_up[0], v_up[0])
        downs = (w_down[0], m_down[0], v_down[0])

        def map_up(low, block):
            return lambda i, h, r: (low // block + i, h[0])

        def map_down(low, block):
            return lambda i, h, r: ((h[0] * ff_half + low) // block + i, 0)

        far_early = trade(early)
        *new_up, up_bf = update_call(half, learn_rate, clip, ups, whole_up, map_up(0, 2 * BLOCK), None, block=2 * BLOCK)
        *new_down, down_bf = update_call(half, learn_rate, clip, downs, whole_down, map_down(0, 2 * BLOCK), None, (up_bf,), block=2 * BLOCK)
        y_next, far_down = forward_call(n_stage, N_GROUP, N_PIECE, LEAD, bounds_down[0][1], x_next, x_far, up_bf, down_bf, whole_down)
        y_next = y_next.reshape(x_next.shape)
        late, late_down, far_down = lax.optimization_barrier((late, late_down, far_down))
        fars = [trade(late[0])]
        far_last = trade(late_down)
        fars += [trade(value) for value in late[1:]]
        *new_down, y_next = update_call(other, learn_rate, clip, downs, far_down, map_down(0, BLOCK), new_down, (), (y_next,))
        after = (new_down[0],)
        for bounds, part in zip(bounds_up[:3], (far_first, far_early, fars[0])):
            new_up = update_call(other, learn_rate, clip, ups, part, map_up(bounds[0], step_of(*bounds)), new_up, after, block=step_of(*bounds))
            after = ()
        new_down = update_call(other, learn_rate, clip, downs, far_last, map_down(bounds_down[1][0], BLOCK // 2), new_down, (new_up[0],), block=BLOCK // 2)
        after = (new_down[0],)
        for bounds, part in zip(bounds_up[3:], fars[1:]):
            new_up = update_call(other, learn_rate, clip, ups, part, map_up(bounds[0], step_of(*bounds)), new_up, after, block=step_of(*bounds))
            after = ()
        return (new_up[0][None], new_down[0][None], new_up[1][None], new_down[1][None], new_up[2][None], new_down[2][None], y_next)

    return jax.shard_map(device_step, mesh=mesh, in_specs=in_specs, out_specs=out_specs, check_vma=False)
```

```python
import functools

import jax
import jax.numpy as jnp
from jax import lax
from jax.experimental import pallas as pl
from jax.experimental.pallas import tpu as pltpu
from jax.sharding import PartitionSpec as P

ADAM_STEP = 10
BETA_ONE = 0.9
BETA_TWO = 0.95
ADAM_EPS = 1e-8
WEIGHT_DECAY = 0.1
NORM_EPS = 1e-6
CONTRACT_LAST = (((1,), (1,)), ((), ()))
BLOCK = 128
N_GROUP = 8
N_PIECE = 28
LEAD = (5, 12, 17, 24)
HELD = 2
HELD_FWD = 3
LAG = 2
N_RAW = 4


def update_body(skip, carry, half_ref, rate_ref, clip_ref, w_ref, m_ref, v_ref, g_ref, *refs):
    outs = refs[skip:]
    if carry:
        outs[-1][...] = refs[skip - 1][...]
        outs = outs[:-1]
    ow_ref, om_ref, ov_ref = outs[:3]
    rate = rate_ref[0]
    grad = clip_ref[0:1] * g_ref[...]
    weight = w_ref[...]
    mom = BETA_ONE * m_ref[...] + (1.0 - BETA_ONE) * grad
    sec = BETA_TWO * v_ref[...] + (1.0 - BETA_TWO) * grad * grad
    one_corr = 1.0 - BETA_ONE**ADAM_STEP
    two_corr = 1.0 - BETA_TWO**ADAM_STEP
    direction = (mom * (1.0 / one_corr)) / (jnp.sqrt(sec * (1.0 / two_corr)) + ADAM_EPS)
    new = weight - rate * (direction + WEIGHT_DECAY * weight)
    ow_ref[...] = new
    om_ref[...] = mom
    ov_ref[...] = sec
    if len(outs) == 4:
        outs[3][...] = new.astype(jnp.bfloat16)


def step_of(low, high):
    return BLOCK if low % BLOCK == 0 and high % BLOCK == 0 else BLOCK // 2


def update_call(half, rate, clip, weights, grad, full_map, previous, after=(), carry=(), block=BLOCK):
    rows, cols = grad.shape
    shape = weights[0].shape
    spec = pl.BlockSpec((block, cols), full_map)
    flat = pl.BlockSpec((block, cols), lambda i, h, r: (i, 0))
    anywhere = pl.BlockSpec(memory_space=pl.ANY)
    first = previous is None
    extra = list(previous or ()) + list(after)
    passed = [pl.BlockSpec((1,) + value.shape[1:], lambda i, h, r: (jnp.minimum(i, value.shape[0] - 1), 0, 0)) for value in carry]
    return pl.pallas_call(
        functools.partial(update_body, len(extra) + len(carry), len(carry)),
        grid_spec=pltpu.PrefetchScalarGridSpec(
            num_scalar_prefetch=2,
            grid=(rows // block,),
            in_specs=[pl.BlockSpec(clip.shape, lambda i, h, r: (0, 0)), spec, spec, spec, flat] + [anywhere] * len(extra) + passed,
            out_specs=[spec] * 3 + [flat] * first + passed,
        ),
        out_shape=[jax.ShapeDtypeStruct(shape, jnp.float32)] * 3 + [jax.ShapeDtypeStruct(grad.shape, jnp.bfloat16)] * first + [jax.ShapeDtypeStruct(value.shape, value.dtype) for value in carry],
        input_output_aliases={7 + i: i for i in range(len(previous or ()))},
        cost_estimate=pl.CostEstimate(flops=60 * rows * cols, bytes_accessed=30 * rows * cols, transcendentals=0),
        compiler_params=pltpu.CompilerParams(vmem_limit_bytes=67043328),
        name="adamw_half",
    )(half, rate, clip, *weights, grad, *extra, *carry)


def backward_body(n_stage, n_raw, bounds_up, bounds_down, gu_ref, gd_ref, wu_ref, wd_ref, acts_ref, gout_ref, x_ref, max_ref, *refs):
    n_up, n_down = len(bounds_up) - 1, len(bounds_down) - 1
    outs_up, outs_down = refs[:n_up], refs[n_up:n_up + n_down]
    whole_up, whole_down, far_ref, x_far, clip_ref = refs[n_up + n_down:n_up + n_down + 5]
    (up_bf, down_bf, st_up, st_down, acc_up, acc_down, got_up, got_down, fold, hid, slope, grad_pre, gbuf, outbox, landed, ready, rows_a, rows_z, norm_box, norm_pair,
     st_sem, loc_sem, fold_sem, own_sem, out_sem, g_rsem, trade_sem, pass_ssem, rs_ssem, rs_rsem, row_ssem, row_rsem, far_sem, norm_ssem, norm_rsem, x_land, x_sem, xf_ssem, xf_rsem, go_sem, fold_up, fold_up_sem) = refs[n_up + n_down + 5:]
    model, data, stage = lax.axis_index('model'), lax.axis_index('data'), lax.axis_index('stage')
    mesh_id = pl.DeviceIdType.MESH
    last = n_stage - 1
    d_model, ff_half = acc_up.shape
    half = d_model // 2
    n_row = acts_ref.shape[0]
    n_up_chunk, n_down_chunk = d_model // BLOCK, ff_half // BLOCK
    peer = {'data': 1 - data}
    near = pl.ds(pl.multiple_of(model * half, half), half)
    far = pl.ds(pl.multiple_of((1 - model) * half, half), half)
    own_cols = pl.ds(pl.multiple_of(data * ff_half, ff_half), ff_half)
    peer_cols = pl.ds(pl.multiple_of((1 - data) * ff_half, ff_half), ff_half)
    own_rows = pl.ds(pl.multiple_of(data * n_row, n_row), n_row)
    first_dims = (((0,), (0,)), ((), ()))

    def remote(src, dst, ssem, rsem, where):
        return pltpu.make_async_remote_copy(src_ref=src, dst_ref=dst, send_sem=ssem, recv_sem=rsem, device_id=where, device_id_type=mesh_id)

    barrier = pltpu.get_barrier_semaphore()
    group = [(dm, ds) for dm in range(2) for ds in range(n_stage) if dm or ds]
    where = [{'model': lax.rem(model + dm, 2), 'stage': lax.rem(stage + ds, n_stage)} for dm, ds in group]
    for target in where + [peer]:
        pl.semaphore_signal(barrier, inc=1, device_id=target, device_id_type=mesh_id)

    n_st_up, n_st_down = d_model // st_up.shape[1], 2 * ff_half // st_down.shape[1]

    def load_up(r):
        return pltpu.make_async_copy(wu_ref.at[pl.ds(r * st_up.shape[1], st_up.shape[1])], st_up.at[r % 2], st_sem.at[0, r % 2])

    def load_down(r):
        return pltpu.make_async_copy(wd_ref.at[pl.ds(r * st_down.shape[1], st_down.shape[1])], st_down.at[r % 2], st_sem.at[1, r % 2])

    load_acts = pltpu.make_async_copy(acts_ref, rows_a.at[own_rows], loc_sem.at[0])
    load_acts.start()
    load_up(0).start()
    load_up(1).start()
    load_down(0).start()
    load_down(1).start()

    def load_g(c):
        return pltpu.make_async_copy(gout_ref.at[:, pl.ds(c * half, half)], gbuf.at[c], loc_sem.at[1 + c])

    @pl.when(stage == last)
    def _():
        for c in range(2):
            load_g(c).start()

    pl.semaphore_wait(barrier, len(where) + 1)

    def chunk(k):
        return pl.ds(k * BLOCK, BLOCK)

    raw_rows = n_raw * BLOCK
    raw = [remote(gu_ref.at[chunk(k), peer_cols], got_up.at[chunk(k)], rs_ssem.at[0, k], rs_rsem.at[0, k], peer) for k in range(n_raw)]
    carries_x = stage >= n_stage // 2

    def micro(i):
        return 2 * (stage - n_stage // 2) + i

    def send_x(i):
        return remote(x_ref.at[micro(i), :, near], x_land.at[i], x_sem.at[0, i], x_sem.at[1, i], peer)

    @pl.when(carries_x)
    def _():
        for i in range(2):
            send_x(i).start()

    for copy in raw:
        copy.start()
    send_a = remote(acts_ref.at[:, :raw_rows], rows_a.at[own_rows, :raw_rows], row_ssem.at[0], row_rsem.at[0], peer)
    send_a.start()

    for r in range(n_st_up):
        load_up(r).wait()
        up_bf[pl.ds(r * st_up.shape[1], st_up.shape[1])] = st_up[r % 2].astype(jnp.bfloat16)
        if r + 2 < n_st_up:
            load_up(r + 2).start()
    load_acts.wait()

    tile = 256
    n_tile = hid.shape[1] // tile
    scale = 0.7978845608028654
    cubic = 0.044715

    def pre_tile(j, carry):
        cols = pl.ds(pl.multiple_of(j * tile, tile), tile)
        pre = jnp.dot(rows_a[own_rows], up_bf[:, cols], preferred_element_type=jnp.float32)
        square = pre * pre
        bend = jnp.tanh(scale * (pre + cubic * square * pre))
        hid[:, cols] = (pre * (0.5 * (1.0 + bend))).astype(jnp.bfloat16)
        slope[:, cols] = 0.5 * (1.0 + bend) + 0.5 * pre * (1.0 - bend * bend) * (scale * (1.0 + 3.0 * cubic * square))
        return carry

    lax.fori_loop(0, n_tile, pre_tile, 0)

    for r in range(n_st_down):
        load_down(r).wait()
        down_bf[pl.ds(r * st_down.shape[1], st_down.shape[1])] = st_down[r % 2].astype(jnp.bfloat16)
        if r + 2 < n_st_down:
            load_down(r + 2).start()

    own_up = pltpu.make_async_copy(gu_ref.at[:, own_cols], acc_up, own_sem.at[0])
    own_down = pltpu.make_async_copy(gd_ref.at[own_cols], acc_down, own_sem.at[1])
    load_fold = pltpu.make_async_copy(gd_ref.at[peer_cols], fold, fold_sem)
    load_fold_up = pltpu.make_async_copy(gu_ref.at[raw_rows:, peer_cols], fold_up, fold_up_sem)
    load_fold_up.start()
    load_fold.start()
    own_up.start()
    own_down.start()

    @pl.when(stage == last)
    def _():
        for c in range(2):
            load_g(c).wait()

    @pl.when(stage < last)
    def _():
        for c in range(2):
            remote(ready, gbuf.at[c], pass_ssem.at[0], g_rsem.at[c], {'model': model}).wait_recv()

    def slope_tile(j, carry):
        cols = pl.ds(pl.multiple_of(j * tile, tile), tile)
        grad = lax.dot_general(gbuf[0], down_bf[cols, :half], CONTRACT_LAST, preferred_element_type=jnp.float32)
        grad = grad + lax.dot_general(gbuf[1], down_bf[cols, half:], CONTRACT_LAST, preferred_element_type=jnp.float32)
        grad_pre[:, cols] = (slope[:, cols] * grad).astype(jnp.bfloat16)
        return carry

    lax.fori_loop(0, n_tile, slope_tile, 0)

    trade = remote(outbox, landed, trade_sem.at[0], trade_sem.at[1], {'model': 1 - model})

    def hand_on(to):
        return remote(ready, gbuf.at[model], pass_ssem.at[to], g_rsem.at[model], {'model': to, 'stage': stage - 1})

    @pl.when(stage > 0)
    def _():
        outbox[...] = lax.dot_general(grad_pre[...], up_bf[far], CONTRACT_LAST, preferred_element_type=jnp.float32)
        trade.start()
        mine = lax.dot_general(grad_pre[...], up_bf[near], CONTRACT_LAST, preferred_element_type=jnp.float32)
        trade.wait_recv()
        ready[...] = (gbuf[model].astype(jnp.float32) + (mine + landed[...])).astype(jnp.bfloat16)
        for to in range(2):
            hand_on(to).start()

    rows_z[own_rows] = grad_pre[:, own_cols]
    send_z = remote(grad_pre.at[:, peer_cols], rows_z.at[own_rows], row_ssem.at[1], row_rsem.at[1], peer)
    send_z.start()

    load_fold_up.wait()

    def send_fold_up(k):
        rows = pl.ds(pl.multiple_of(k * BLOCK, BLOCK), BLOCK)
        at = pl.ds(pl.multiple_of((n_raw + k) * BLOCK, BLOCK), BLOCK)
        return remote(fold_up.at[rows], got_up.at[at], rs_ssem.at[0, n_raw + k], rs_rsem.at[0, n_raw + k], peer)

    def fold_up_step(k, carry):
        rows = pl.ds(pl.multiple_of(k * BLOCK, BLOCK), BLOCK)
        at = pl.ds(pl.multiple_of((n_raw + k) * BLOCK, BLOCK), BLOCK)
        fold_up[rows] += lax.dot_general(rows_a[own_rows, at], grad_pre[:, peer_cols], first_dims, preferred_element_type=jnp.float32)
        send_fold_up(k).start()
        return carry

    lax.fori_loop(0, n_up_chunk - n_raw, fold_up_step, 0)

    def forward_x(i, to):
        return remote(x_land.at[i], x_far.at[micro(i), :, near], xf_ssem.at[i, to], xf_rsem.at[micro(i), model], {'model': to, 'stage': 0})

    @pl.when(carries_x)
    def _():
        for i in range(2):
            send_x(i).wait_recv()
            for to in range(2):
                forward_x(i, to).start()

    def down_product(k, side):
        cols = pl.ds(pl.multiple_of(side * ff_half + k * BLOCK, BLOCK), BLOCK)
        left = hid[:, cols]
        return [lax.dot_general(left, gbuf[c], first_dims, preferred_element_type=jnp.float32) for c in range(2)]

    load_fold.wait()

    def send_fold(k):
        rows = pl.ds(pl.multiple_of(k * BLOCK, BLOCK), BLOCK)
        return remote(fold.at[rows], got_down.at[rows], rs_ssem.at[1, k], rs_rsem.at[1, k], peer)

    def fold_step(k, carry):
        rows = pl.ds(pl.multiple_of(k * BLOCK, BLOCK), BLOCK)
        low, high = down_product(k, 1 - data)
        fold[rows, :half] += low
        fold[rows, half:] += high
        send_fold(k).start()
        return carry

    lax.fori_loop(0, n_down_chunk, fold_step, 0)
    own_down.wait()

    def own_step(k, carry):
        rows = pl.ds(pl.multiple_of(k * BLOCK, BLOCK), BLOCK)
        low, high = down_product(k, data)
        acc_down[rows, :half] += low
        acc_down[rows, half:] += high
        return carry

    lax.fori_loop(0, n_down_chunk, own_step, 0)

    @pl.when(stage > 0)
    def _():
        trade.wait_send()
        for to in range(2):
            hand_on(to).wait_send()

    own_up.wait()
    send_a.wait_recv()
    squares = jnp.zeros((8, ff_half), jnp.float32)

    def fold_squares(mean):
        return jnp.sum((mean * mean).reshape(-1, 8, mean.shape[1]), axis=0)

    def put(acc, bounds, outs, whole, sem_row):
        copies = []
        for i, (lo, hi) in enumerate(bounds):
            rows = pl.ds(lo, hi - lo)
            copies.append(pltpu.make_async_copy(acc.at[rows], whole.at[rows], out_sem.at[sem_row, i]))
            if outs[i] is not None:
                copies.append(pltpu.make_async_copy(acc.at[rows], outs[i], out_sem.at[sem_row, len(bounds) + i]))
        return copies

    def put_start(k, bounds, copies, outs):
        at = 0
        for i, (lo, hi) in enumerate(bounds):
            count = 1 if outs[i] is None else 2
            if k * BLOCK < hi <= (k + 1) * BLOCK:
                for copy in copies[at:at + count]:
                    copy.start()
            at += count

    outs_up = (None,) + tuple(outs_up)
    outs_down = (None,) + tuple(outs_down)
    put_up = put(acc_up, bounds_up, outs_up, whole_up, 0)
    put_down = put(acc_down, bounds_down, outs_down, whole_down, 1)
    for k in range(n_up_chunk):
        if k == 0:
            send_z.wait_recv()
        if k < n_raw:
            raw[k].wait_recv()
            product = lax.dot_general(rows_a[:, chunk(k)], rows_z[...], first_dims, preferred_element_type=jnp.float32)
        else:
            send_fold_up(k - n_raw).wait_recv()
            product = lax.dot_general(rows_a[own_rows, chunk(k)], rows_z[own_rows], first_dims, preferred_element_type=jnp.float32)
        mean = (acc_up[chunk(k)] + got_up[chunk(k)] + product) * 0.5
        acc_up[chunk(k)] = mean
        squares = squares + fold_squares(mean)
        put_start(k, bounds_up, put_up, outs_up)
    n_far = far_sem.shape[1]
    slab = bounds_up[0][1] // n_far
    is_even = lax.rem(stage, 2) == 0

    def send_far(i):
        span = pl.ds(pl.multiple_of(i * slab, slab), slab)
        return remote(acc_up.at[span], far_ref.at[span], far_sem.at[0, i], far_sem.at[1, i], peer)

    for i in range(n_far - HELD):
        send_far(i).start()

    @pl.when(is_even)
    def _():
        for i in range(n_far - HELD, n_far):
            send_far(i).start()

    for k in range(n_down_chunk):
        send_fold(k).wait_recv()
        mean = (acc_down[chunk(k)] + got_down[chunk(k)]) * 0.5
        acc_down[chunk(k)] = mean
        squares = squares + fold_squares(mean)
        put_start(k, bounds_down, put_down, outs_down)

    lanes = norm_box.shape[2]
    part = squares[:, :lanes]
    for j in range(1, ff_half // lanes):
        part = part + squares[:, j * lanes:(j + 1) * lanes]
    me = model * n_stage + stage
    norm_box[me] = part

    def spread(i):
        return remote(norm_box.at[me], norm_box.at[me], norm_ssem.at[i], norm_rsem.at[me], where[i])

    for i in range(len(group)):
        spread(i).start()
    for i, (dm, ds) in enumerate(group):
        them = lax.rem(model + dm, 2) * n_stage + lax.rem(stage + ds, n_stage)
        remote(norm_box.at[me], norm_box.at[them], norm_ssem.at[i], norm_rsem.at[them], where[i]).wait_recv()
    total = norm_box[0]
    for i in range(1, 2 * n_stage):
        total = total + norm_box[i]
    norm_pair[0] = total
    swap = remote(norm_pair.at[0], norm_pair.at[1], norm_ssem.at[len(group)], norm_rsem.at[2 * n_stage], peer)
    swap.start()
    swap.wait_recv()
    norm_sq = jnp.sum(norm_pair[0] + norm_pair[1], axis=(0, 1), keepdims=True)
    norm = jnp.sqrt(jnp.broadcast_to(norm_sq, clip_ref.shape)) + NORM_EPS
    clip_ref[...] = jnp.minimum(1.0, max_ref[0] / norm)

    @pl.when(carries_x)
    def _():
        for i in range(2):
            send_x(i).wait_send()
            for to in range(2):
                forward_x(i, to).wait_send()

    @pl.when(stage == 0)
    def _():
        for s in range(n_stage):
            for m in range(2):
                remote(x_land.at[0], x_far.at[s, :, pl.ds(m * half, half)], xf_ssem.at[0, m], xf_rsem.at[s, m], {'model': model}).wait_recv()

    swap.wait_send()
    for i in range(len(group)):
        spread(i).wait_send()
    for copy in raw + [send_a, send_z]:
        copy.wait_send()
    for k in range(n_down_chunk):
        send_fold(k).wait_send()
    for k in range(n_up_chunk - n_raw):
        send_fold_up(k).wait_send()
    for copy in put_up + put_down:
        copy.wait()

    @pl.when(is_even)
    def _():
        for i in range(n_far):
            send_far(i).wait_send()
        pl.semaphore_signal(go_sem, inc=1, device_id={'stage': stage + 1}, device_id_type=mesh_id)

    @pl.when(jnp.logical_not(is_even))
    def _():
        pl.semaphore_wait(go_sem, 1)
        for i in range(n_far - HELD, n_far):
            send_far(i).start()
        for i in range(n_far):
            send_far(i).wait_send()

    for i in range(n_far):
        send_far(i).wait_recv()


def backward_call(n_stage, bounds_up, bounds_down, g_up, g_down, w_up, w_down, acts, grad_out, x_next, max_norm):
    d_model, ff_local = g_up.shape
    ff_half, half, n_row = ff_local // 2, d_model // 2, acts.shape[0]
    dma = pltpu.SemaphoreType.DMA
    anywhere = pl.BlockSpec(memory_space=pl.ANY)
    f32, bf16 = jnp.float32, jnp.bfloat16
    shapes = [jax.ShapeDtypeStruct((hi - lo, ff_half), f32) for lo, hi in bounds_up[1:]]
    shapes += [jax.ShapeDtypeStruct((hi - lo, d_model), f32) for lo, hi in bounds_down[1:]]
    shapes += [jax.ShapeDtypeStruct((d_model, ff_half), f32), jax.ShapeDtypeStruct((ff_half, d_model), f32)]
    shapes += [jax.ShapeDtypeStruct((bounds_up[0][1], ff_half), f32), jax.ShapeDtypeStruct(x_next.shape, bf16), jax.ShapeDtypeStruct((8, ff_half), f32)]
    n_chunk = max(d_model, ff_half) // BLOCK
    return pl.pallas_call(
        functools.partial(backward_body, n_stage, N_RAW, bounds_up, bounds_down),
        out_shape=shapes,
        in_specs=[anywhere] * 7 + [pl.BlockSpec(memory_space=pltpu.SMEM)],
        out_specs=[anywhere] * (len(shapes) - 1) + [pl.BlockSpec(memory_space=pltpu.VMEM)],
        scratch_shapes=[
            pltpu.VMEM((d_model, ff_local), bf16),
            pltpu.VMEM((ff_local, d_model), bf16),
            pltpu.VMEM((2, 256, ff_local), f32),
            pltpu.VMEM((2, 512, d_model), f32),
            pltpu.VMEM((d_model, ff_half), f32),
            pltpu.VMEM((ff_half, d_model), f32),
            pltpu.VMEM((d_model, ff_half), f32),
            pltpu.VMEM((ff_half, d_model), f32),
            pltpu.VMEM((ff_half, d_model), f32),
            pltpu.VMEM((n_row, ff_local), bf16),
            pltpu.VMEM((n_row, ff_local), f32),
            pltpu.VMEM((n_row, ff_local), bf16),
            pltpu.VMEM((2, n_row, half), bf16),
            pltpu.VMEM((n_row, half), f32),
            pltpu.VMEM((n_row, half), f32),
            pltpu.VMEM((n_row, half), bf16),
            pltpu.VMEM((2 * n_row, d_model), bf16),
            pltpu.VMEM((2 * n_row, ff_half), bf16),
            pltpu.VMEM((2 * n_stage, 8, 128), f32),
            pltpu.VMEM((2, 8, 128), f32),
            dma((2, 2)),
            dma((3,)),
            dma(()),
            dma((2,)),
            dma((2, 2 * max(len(bounds_up), len(bounds_down)))),
            dma((2,)),
            dma((2,)),
            dma((2,)),
            dma((2, n_chunk)),
            dma((2, n_chunk)),
            dma((2,)),
            dma((2,)),
            dma((2, 8)),
            dma((2 * n_stage,)),
            dma((2 * n_stage + 1,)),
            pltpu.VMEM((2, n_row, half), bf16),
            dma((2, 2)),
            dma((2, 2)),
            dma((n_stage, 2)),
            pltpu.SemaphoreType.REGULAR,
            pltpu.VMEM((d_model - N_RAW * BLOCK, ff_half), f32),
            dma(()),
        ],
        compiler_params=pltpu.CompilerParams(collective_id=0, has_side_effects=True, vmem_limit_bytes=67043328),
        name="reduce_and_norm",
    )(g_up, g_down, w_up, w_down, acts, grad_out, x_next, max_norm)


def forward_body(n_stage, lead, x_ref, xf_ref, up_ref, down_ref, mean_ref, y_ref, far_ref, inbox, hid, mine, zout, zin, keep, yout, yin, done, x_sem, in_sem, z_ssem, z_rsem, s_ssem, s_rsem, r_ssem, r_rsem, pass_ssem, y_ssem, y_rsem, piece_ssem, piece_rsem, go_sem):
    model, data, stage = lax.axis_index('model'), lax.axis_index('data'), lax.axis_index('stage')
    mesh_id = pl.DeviceIdType.MESH
    last = n_stage - 1
    n_group, _, rows2, half = inbox.shape
    rows = rows2 // 2
    n_piece = piece_ssem.shape[0]
    piece = far_ref.shape[0] // n_piece
    peer = {'data': 1 - data}
    near = pl.ds(pl.multiple_of(model * half, half), half)
    far = pl.ds(pl.multiple_of((1 - model) * half, half), half)
    own_rows = pl.ds(pl.multiple_of(data * rows, rows), rows)
    peer_rows = pl.ds(pl.multiple_of((1 - data) * rows, rows), rows)

    def remote(src, dst, ssem, rsem, where):
        return pltpu.make_async_remote_copy(src_ref=src, dst_ref=dst, send_sem=ssem, recv_sem=rsem, device_id=where, device_id_type=mesh_id)

    barrier = pltpu.get_barrier_semaphore()
    group = [(dm, ds) for dm in range(2) for ds in range(n_stage) if dm or ds]
    where = [{'model': lax.rem(model + dm, 2), 'stage': lax.rem(stage + ds, n_stage)} for dm, ds in group]
    for target in where + [peer]:
        pl.semaphore_signal(barrier, inc=1, device_id=target, device_id_type=mesh_id)

    def load_x(b, c, from_ref, to_rows, i):
        return pltpu.make_async_copy(from_ref.at[b, :, pl.ds(c * half, half)], inbox.at[b, c, to_rows], x_sem.at[b, c, i])

    def loads(b):
        return [load_x(b, c, *pair) for c in range(2) for pair in ((x_ref, own_rows, 0), (xf_ref, peer_rows, 1))]

    @pl.when(stage == 0)
    def _():
        for b in range(n_group):
            for copy in loads(b):
                copy.start()

    pl.semaphore_wait(barrier, len(where) + 1)

    def send_piece(p):
        span = pl.ds(pl.multiple_of(p * piece, piece), piece)
        return remote(mean_ref.at[span], far_ref.at[span], piece_ssem.at[p], piece_rsem.at[p], peer)

    def start_pieces(low, high):
        def one(p, carry):
            send_piece(p).start()
            return carry

        lax.fori_loop(low, high, one, 0)

    n_turn = n_group + 3 * LAG
    is_even = lax.rem(stage, 2) == 0
    limit = n_piece - HELD_FWD * lax.rem(stage, 2)
    begin = sum(jnp.where(stage == i, count, 0) for i, count in enumerate(lead))
    start_pieces(0, begin)

    def arrival(b, c):
        return remote(done.at[b], inbox.at[b, c], pass_ssem.at[b, 0], in_sem.at[b, c], {'model': model})

    def trade_z(b):
        return remote(zout.at[b], zin.at[b], z_ssem.at[b], z_rsem.at[b], {'model': 1 - model})

    def trade_s(b):
        return remote(yout.at[b], yin.at[b], s_ssem.at[b], s_rsem.at[b], peer)

    def trade_r(b):
        return remote(done.at[b, own_rows], done.at[b, own_rows], r_ssem.at[b], r_rsem.at[b], peer)

    def hand_on(b, to):
        return remote(done.at[b], inbox.at[b, model], pass_ssem.at[b, to], in_sem.at[b, model], {'model': to, 'stage': stage + 1})

    def landing(b, c):
        return y_ref.at[b, :, pl.ds(pl.multiple_of(c * half, half), half)]

    def publish(b, k):
        return remote(done.at[b, own_rows], landing(b, model), y_ssem.at[b, k], y_rsem.at[b, model], where[k])

    def y_arrival(b, c):
        return remote(done.at[b, own_rows], landing(b, c), y_ssem.at[b, 0], y_rsem.at[b, c], {'model': model})

    def project(t):
        @pl.when(t < n_group)
        def _():
            @pl.when(stage == 0)
            def _():
                for copy in loads(t):
                    copy.wait()

            @pl.when(stage > 0)
            def _():
                for c in range(2):
                    arrival(t, c).wait_recv()

            pre = jnp.dot(inbox[t, 0], up_ref[:half], preferred_element_type=jnp.float32)
            pre = pre + jnp.dot(inbox[t, 1], up_ref[half:], preferred_element_type=jnp.float32)
            hid[...] = jax.nn.gelu(pre).astype(jnp.bfloat16)
            zout[t] = jnp.dot(hid[...], down_ref[:, far], preferred_element_type=jnp.float32)
            trade_z(t).start()
            mine[t] = jnp.dot(hid[...], down_ref[:, near], preferred_element_type=jnp.float32)

    def reduce_z(t):
        @pl.when((t >= LAG) & (t < n_group + LAG))
        def _():
            b = t - LAG
            trade_z(b).wait_recv()
            yout[b] = mine[b, peer_rows] + zin[b, peer_rows]
            trade_s(b).start()
            keep[b] = mine[b, own_rows] + zin[b, own_rows]

    def reduce_y(t):
        @pl.when((t >= 2 * LAG) & (t < n_group + 2 * LAG))
        def _():
            b = t - 2 * LAG
            trade_s(b).wait_recv()
            total = inbox[b, model, own_rows].astype(jnp.float32) + (keep[b] + yin[b])
            result = total.astype(jnp.bfloat16)
            done[b, own_rows] = result

            @pl.when(stage < last)
            def _():
                trade_r(b).start()

            @pl.when(stage == last)
            def _():
                y_ref[b, :, near] = result
                for k in range(len(group)):
                    publish(b, k).start()

    def pass_on(t):
        @pl.when((t >= 3 * LAG) & (stage < last))
        def _():
            b = t - 3 * LAG
            remote(done.at[b, own_rows], done.at[b, peer_rows], r_ssem.at[b], r_rsem.at[b], peer).wait_recv()
            for to in range(2):
                hand_on(b, to).start()

    def turn(t, carry):
        for phase in (project, reduce_z, reduce_y, pass_on):
            phase(t)
        return carry

    lax.fori_loop(0, n_turn, turn, 0)
    start_pieces(begin, limit)

    for b in range(n_group):
        trade_z(b).wait_send()
        trade_s(b).wait_send()

    @pl.when(stage < last)
    def _():
        for b in range(n_group):
            trade_r(b).wait_send()
            for to in range(2):
                hand_on(b, to).wait_send()
            for c in range(2):
                y_arrival(b, c).wait_recv()

    @pl.when(stage == last)
    def _():
        for b in range(n_group):
            for k in range(len(group)):
                publish(b, k).wait_send()
            y_arrival(b, 1 - model).wait_recv()

    def sent(p, carry):
        send_piece(p).wait_send()
        return carry

    def landed(p, carry):
        send_piece(p).wait_recv()
        return carry

    lax.fori_loop(0, limit, sent, 0)

    @pl.when(is_even)
    def _():
        pl.semaphore_signal(go_sem, inc=1, device_id={'stage': stage + 1}, device_id_type=mesh_id)

    @pl.when(jnp.logical_not(is_even))
    def _():
        pl.semaphore_wait(go_sem, 1)
        start_pieces(limit, n_piece)
        lax.fori_loop(limit, n_piece, sent, 0)

    lax.fori_loop(0, n_piece, landed, 0)


def forward_call(n_stage, n_group, n_piece, lead, n_far, x_next, x_far, up_bf, down_bf, mean):
    d_model = x_next.shape[2]
    x_next, x_far = [value.reshape(n_group, -1, d_model) for value in (x_next, x_far)]
    rows, half, ff_half = x_next.shape[1], d_model // 2, up_bf.shape[1]
    dma = pltpu.SemaphoreType.DMA
    f32, bf16 = jnp.float32, jnp.bfloat16
    in_vmem = pl.BlockSpec(memory_space=pltpu.VMEM)
    anywhere = pl.BlockSpec(memory_space=pl.ANY)
    return pl.pallas_call(
        functools.partial(forward_body, n_stage, lead),
        out_shape=[jax.ShapeDtypeStruct(x_next.shape, bf16), jax.ShapeDtypeStruct((n_far, d_model), f32)],
        in_specs=[anywhere, anywhere, in_vmem, in_vmem, anywhere],
        out_specs=[in_vmem, anywhere],
        scratch_shapes=[
            pltpu.VMEM((n_group, 2, 2 * rows, half), bf16),
            pltpu.VMEM((2 * rows, ff_half), bf16),
            pltpu.VMEM((n_group, 2 * rows, half), f32),
            pltpu.VMEM((n_group, 2 * rows, half), f32),
            pltpu.VMEM((n_group, 2 * rows, half), f32),
            pltpu.VMEM((n_group, rows, half), f32),
            pltpu.VMEM((n_group, rows, half), f32),
            pltpu.VMEM((n_group, rows, half), f32),
            pltpu.VMEM((n_group, 2 * rows, half), bf16),
            dma((n_group, 2, 2)),
            dma((n_group, 2)),
            dma((n_group,)),
            dma((n_group,)),
            dma((n_group,)),
            dma((n_group,)),
            dma((n_group,)),
            dma((n_group,)),
            dma((n_group, 2)),
            dma((n_group, 2 * n_stage - 1)),
            dma((n_group, 2)),
            dma((n_piece,)),
            dma((n_piece,)),
            pltpu.SemaphoreType.REGULAR,
        ],
        compiler_params=pltpu.CompilerParams(collective_id=1, has_side_effects=True, vmem_limit_bytes=67043328),
        name="forward_pipe",
    )(x_next, x_far, up_bf, down_bf, mean)


def solution(mesh):
    n_stage = mesh.shape['stage']
    swap = [(0, 1), (1, 0)]
    up_spec = P('stage', None, 'model')
    down_spec = P('stage', 'model', None)
    row_spec = P(None, 'data', None)
    in_specs = (up_spec, down_spec, up_spec, down_spec, up_spec, down_spec, P('data', 'stage', None, 'model'), P('data', 'stage', 'model', None), P('stage', 'data', None), P('data', None), row_spec, P(None), P(None))
    out_specs = (up_spec, down_spec, up_spec, down_spec, up_spec, down_spec, row_spec)

    def device_step(w_up, w_down, m_up, m_down, v_up, v_down, g_up, g_down, acts_last, grad_out, x_next, learn_rate, max_norm):
        data_id = lax.axis_index('data')
        half = data_id.astype(jnp.int32).reshape(1)
        other = (1 - half).astype(jnp.int32)
        d_model, ff_local = w_up.shape[1:]
        ff_half = ff_local // 2
        bounds_up = ((0, 256), (256, 640), (640, 896), (896, 960), (960, d_model))
        bounds_down = ((0, N_PIECE * 32), (N_PIECE * 32, ff_half))

        def trade(value):
            return lax.ppermute(value, 'data', swap)

        early, *late, late_down, whole_up, whole_down, far_first, x_far, clip = backward_call(n_stage, bounds_up, bounds_down, g_up[0, 0], g_down[0, 0], w_up[0], w_down[0], acts_last[0], grad_out, x_next, max_norm)
        ups = (w_up[0], m_up[0], v_up[0])
        downs = (w_down[0], m_down[0], v_down[0])

        def map_up(low, block):
            return lambda i, h, r: (low // block + i, h[0])

        def map_down(low, block):
            return lambda i, h, r: ((h[0] * ff_half + low) // block + i, 0)

        far_early = trade(early)
        *new_up, up_bf = update_call(half, learn_rate, clip, ups, whole_up, map_up(0, 2 * BLOCK), None, block=2 * BLOCK)
        *new_down, down_bf = update_call(half, learn_rate, clip, downs, whole_down, map_down(0, 2 * BLOCK), None, (up_bf,), block=2 * BLOCK)
        y_next, far_down = forward_call(n_stage, N_GROUP, N_PIECE, LEAD, bounds_down[0][1], x_next, x_far, up_bf, down_bf, whole_down)
        y_next = y_next.reshape(x_next.shape)
        late, late_down, far_down = lax.optimization_barrier((late, late_down, far_down))
        fars = [trade(late[0])]
        far_last = trade(late_down)
        fars += [trade(value) for value in late[1:]]
        *new_down, y_next = update_call(other, learn_rate, clip, downs, far_down, map_down(0, BLOCK), new_down, (), (y_next,))
        after = (new_down[0],)
        for bounds, part in zip(bounds_up[:3], (far_first, far_early, fars[0])):
            new_up = update_call(other, learn_rate, clip, ups, part, map_up(bounds[0], step_of(*bounds)), new_up, after, block=step_of(*bounds))
            after = ()
        new_down = update_call(other, learn_rate, clip, downs, far_last, map_down(bounds_down[1][0], BLOCK // 2), new_down, (new_up[0],), block=BLOCK // 2)
        after = (new_down[0],)
        for bounds, part in zip(bounds_up[3:], fars[1:]):
            new_up = update_call(other, learn_rate, clip, ups, part, map_up(bounds[0], step_of(*bounds)), new_up, after, block=step_of(*bounds))
            after = ()
        return (new_up[0][None], new_down[0][None], new_up[1][None], new_down[1][None], new_up[2][None], new_down[2][None], y_next)

    return jax.shard_map(device_step, mesh=mesh, in_specs=in_specs, out_specs=out_specs, check_vma=False)
```
